32 devices in a mesh: dp: 8 (over z, x), tensor: 4 (over y, core).
Axes of the slice: x: 2, y: 2, z: 4, core: 2. Of those that a mesh axis runs over, the one named last changes fastest.
Arguments:
- block_input: bfloat16 [24576, 1024], P('dp'), may hold values from -6 to 6
- pre_gain: float32 [1024], replicated, may hold values from 0.25 to 1.75
- w_zx: bfloat16 [1024, 2, 2048], P(None, None, 'tensor'), may hold values from -0.1875 to 0.1875
- w_bc: bfloat16 [1024, 256], replicated, may hold values from -0.1875 to 0.1875
- w_dt: bfloat16 [1024, 32], P(None, 'tensor'), may hold values from -0.1875 to 0.1875
- conv_x_w: float32 [4, 2048], P(None, 'tensor'), may hold values from -3 to 3
- conv_x_b: float32 [2048], P('tensor'), may hold values from -3 to 3
- conv_bc_w: float32 [4, 256], replicated, may hold values from -3 to 3
- conv_bc_b: float32 [256], replicated, may hold values from -3 to 3
- dt_bias: float32 [32], P('tensor'), may hold values from -5 to -1
- a_log: float32 [32], P('tensor'), may hold values from -1.5 to 2.5
- d_skip: float32 [32], P('tensor'), may hold values from 0.5 to 2
- gate_gain: float32 [2048], P('tensor'), may hold values from 0.25 to 1.75
- w_out: bfloat16 [2048, 1024], P('tensor'), may hold values from -0.125 to 0.125
- out_grad: bfloat16 [24576, 1024], P('dp'), may hold values from -6 to 6
Outputs:
- block_output: bfloat16 [24576, 1024], P('dp')
- grad_input: float32 [24576, 1024], P('dp')
- grad_pre_gain: float32 [1024], replicated
- grad_w_zx: float32 [1024, 2, 2048], P(None, None, 'tensor')
- grad_w_bc: float32 [1024, 256], replicated
- grad_w_dt: float32 [1024, 32], P(None, 'tensor')
- grad_conv_x_w: float32 [4, 2048], P(None, 'tensor')
- grad_conv_x_b: float32 [2048], P('tensor')
- grad_conv_bc_w: float32 [4, 256], replicated
- grad_conv_bc_b: float32 [256], replicated
- grad_dt_bias: float32 [32], P('tensor')
- grad_a_log: float32 [32], P('tensor')
- grad_d_skip: float32 [32], P('tensor')
- grad_gate_gain: float32 [2048], P('tensor')
- grad_w_out: float32 [2048, 1024], P('tensor')
The draws below stay inside these ranges and needn't reach their ends.
All inputs are finite; a program needn't handle non-finite values.
Results may differ from the reference program's by a relative error of at most 0.023.
Values may be sent and summed in bfloat16 or wider, within the bound.
A program may use at most 320 MiB of HBM per device.

```python
from functools import partial
import jax
import jax.numpy as jnp
from jax import lax

D = 1024
HEADS = 32
STATE = 128
INNER = 2048
CONV = 4
SPAN = 256
SEQ_LEN = 512
TOK_DEV = 3072
TOKENS = 24576
N_DP = 8
N_TENSOR = 4


def level_of(stream_key, extent, pieces, least, high):
    gain, own = 1.0, jax.random.fold_in(stream_key, 6)
    for axis_at, parts in pieces:
        heights = jnp.exp(jax.random.uniform(jax.random.fold_in(own, axis_at), (parts,), jnp.float32, least / len(pieces), high / len(pieces)))
        gain = gain * jnp.repeat(heights, extent[axis_at] // parts).reshape([-1 if axis == axis_at else 1 for axis in range(len(extent))])
    return gain


def bell_draw(key, extent, width, most, cuts=(), kind=jnp.bfloat16):
    drawn = jax.random.normal(key, extent, jnp.float32) * width
    if len(cuts) > 0:
        drawn = level_of(key, extent, cuts, -0.22, 0.18) * drawn
    return jnp.clip(drawn, min=-most, max=most).astype(kind)


def setup_inputs(seed: int = 0) -> dict:
    streams_of = jax.random.split(jax.random.key(seed), 16)
    return {
        "block_input": bell_draw(streams_of[0], (TOKENS, D), 1.0, 6.0, ((0, 8),)),
        "pre_gain": jnp.clip(1.0 + 0.15 * jax.random.normal(streams_of[1], (D,), jnp.float32), 0.25, 1.75),
        "w_zx": bell_draw(streams_of[2], (D, 2, INNER), D ** -0.5, 0.1875, ((2, 4),)),
        "w_bc": bell_draw(streams_of[3], (D, 2 * STATE), D ** -0.5, 0.1875),
        "w_dt": bell_draw(streams_of[4], (D, HEADS), D ** -0.5, 0.1875, ((1, 4),)),
        "conv_x_w": bell_draw(streams_of[5], (CONV, INNER), CONV ** -0.5, 3.0, ((1, 4),), jnp.float32),
        "conv_x_b": bell_draw(streams_of[6], (INNER,), 0.5, 3.0, ((0, 4),), jnp.float32),
        "conv_bc_w": bell_draw(streams_of[7], (CONV, 2 * STATE), CONV ** -0.5, 3.0, (), jnp.float32),
        "conv_bc_b": bell_draw(streams_of[8], (2 * STATE,), 0.5, 3.0, (), jnp.float32),
        "dt_bias": jnp.clip(-5.0 + 4.0 * jax.random.uniform(streams_of[9], (HEADS,), jnp.float32) ** level_of(streams_of[9], (HEADS,), ((0, 4),), -0.2, 0.2), -5.0, -1.0),
        "a_log": jnp.clip(-1.5 + 4.0 * jax.random.uniform(streams_of[10], (HEADS,), jnp.float32) ** level_of(streams_of[10], (HEADS,), ((0, 4),), -0.2, 0.2), -1.5, 2.5),
        "d_skip": jnp.clip(0.5 + 1.5 * jax.random.uniform(streams_of[11], (HEADS,), jnp.float32) ** level_of(streams_of[11], (HEADS,), ((0, 4),), -0.2, 0.2), 0.5, 2.0),
        "gate_gain": jnp.clip(1.0 + 0.15 * jax.random.normal(streams_of[12], (INNER,), jnp.float32), 0.25, 1.75),
        "w_out": bell_draw(streams_of[13], (INNER, D), INNER ** -0.5, 0.125, ((0, 4),)),
        "out_grad": bell_draw(streams_of[14], (TOKENS, D), 1.0, 6.0, ((0, 8),)),
    }


epsilon = 1e-05
precise = lax.Precision.HIGHEST

def causal_conv(sequence, kernel_w, kernel_b):
    tap_count = kernel_w.shape[0]
    length = sequence.shape[1]
    padded = jnp.pad(sequence, ((0, 0), (tap_count - 1, 0), (0, 0)))
    summed = jnp.zeros(sequence.shape, jnp.float32) + kernel_b
    for offset in range(tap_count):
        summed = summed + padded[:, offset:offset + length, :] * kernel_w[offset]
    return summed

def bc_convolve(bc_linear, kernel_w, kernel_b):
    return jax.nn.silu(causal_conv(bc_linear, kernel_w, kernel_b))

def ssd_scan(values, dt_values, a_rates, b_proj, c_proj, block_len):
    seq_count, length, head_count, head_width = values.shape
    span_count = length // block_len
    state_width = b_proj.shape[-1]
    weighted = (values * dt_values[..., None]).reshape(seq_count, span_count, block_len, head_count, head_width)
    cumulative = jnp.cumsum(jnp.transpose((dt_values * a_rates).reshape(seq_count, span_count, block_len, head_count), (0, 1, 3, 2)), axis=-1)
    b_blocks = b_proj.reshape(seq_count, span_count, block_len, state_width)
    c_blocks = c_proj.reshape(seq_count, span_count, block_len, state_width)
    intersection = jnp.einsum('scin,scjn->scij', c_blocks, b_blocks, precision=precise)
    differences = cumulative[..., :, None] - cumulative[..., None, :]
    lower_mask = jnp.tril(jnp.ones((block_len, block_len), bool))
    decays = jnp.exp(jnp.where(lower_mask, differences, -jnp.inf))
    kernel_mat = decays * intersection[:, :, None]
    y_within = jnp.einsum('schij,scjhp->scihp', kernel_mat, weighted, precision=precise)
    final_cum = cumulative[..., -1:]
    state_decay = jnp.exp(final_cum - cumulative)
    block_states = jnp.einsum('scjn,schj,scjhp->schpn', b_blocks, state_decay, weighted, precision=precise)
    block_decay = jnp.exp(cumulative[..., -1])
    running = jnp.zeros((seq_count, head_count, head_width, state_width), jnp.float32)
    entering = []
    for number in range(span_count):
        entering.append(running)
        running = running * block_decay[:, number, :, None, None] + block_states[:, number]
    prior_states = jnp.stack(entering, axis=1)
    y_across = jnp.einsum('scin,schpn,schi->scihp', c_blocks, prior_states, jnp.exp(cumulative), precision=precise)
    merged = (y_within + y_across).reshape(seq_count, length, head_count, head_width)
    return merged + values * d_skip_view(a_rates, values)

def d_skip_view(a_rates, values):
    return jnp.zeros((values.shape[2], 1), jnp.float32)

def mixer(block_len, z_linear, x_linear, dt_linear, bc_active, conv_weight, conv_bias, dt_bias, a_log, d_skip):
    seq_count, length, channels = x_linear.shape
    x_active = jax.nn.silu(causal_conv(x_linear, conv_weight, conv_bias))
    dt_values = jax.nn.softplus(dt_linear + dt_bias)
    a_rates = -jnp.exp(a_log)
    head_count = dt_values.shape[-1]
    state_width = bc_active.shape[-1] // 2
    values = x_active.reshape(seq_count, length, head_count, channels // head_count)
    scanned = ssd_scan(values, dt_values, a_rates, bc_active[..., :state_width], bc_active[..., state_width:], block_len)
    scanned = scanned + values * d_skip[:, None]
    return scanned.reshape(seq_count, length, channels) * jax.nn.silu(z_linear)

def one_block(params, block_u, block_dy):
    pre_gain, w_zx, w_bc, w_dt, conv_x_w, conv_x_b, conv_bc_w, conv_bc_b, dt_bias, a_log, d_skip, gate_gain, w_out = params
    tok_rows = block_u.shape[0]
    model_width = block_u.shape[1]
    inner_width = w_zx.shape[2]
    seq_count = tok_rows // SEQ_LEN
    input_f32 = block_u.astype(jnp.float32)
    rms_input = lax.rsqrt(lax.optimization_barrier(jnp.mean(input_f32 * input_f32, axis=1, keepdims=True)) + epsilon)
    normed = input_f32 * rms_input
    hidden = (normed * pre_gain).astype(jnp.bfloat16)
    w_zx_flat = w_zx.reshape(model_width, 2 * inner_width)
    zx_linear = jnp.dot(hidden, w_zx_flat, preferred_element_type=jnp.float32)
    bc_linear = jnp.dot(hidden, w_bc, preferred_element_type=jnp.float32)
    dt_linear = jnp.dot(hidden, w_dt, preferred_element_type=jnp.float32)

    def to_seqs(matrix):
        return matrix.reshape(seq_count, SEQ_LEN, matrix.shape[-1])
    bc_active, bc_back = jax.vjp(bc_convolve, to_seqs(bc_linear), conv_bc_w, conv_bc_b)
    gated_seq, mixer_back = jax.vjp(partial(mixer, SPAN), to_seqs(zx_linear[:, :inner_width]), to_seqs(zx_linear[:, inner_width:]), to_seqs(dt_linear), bc_active, conv_x_w, conv_x_b, dt_bias, a_log, d_skip)
    gated = gated_seq.reshape(tok_rows, inner_width)
    rms_gate = lax.rsqrt(lax.optimization_barrier(jnp.mean(gated * gated, axis=1, keepdims=True)) + epsilon)
    quantized = (gated * gate_gain).astype(jnp.bfloat16)
    block_width = inner_width // N_TENSOR
    q_blocks = quantized.reshape(tok_rows, N_TENSOR, block_width).astype(jnp.float32)
    w_blocks = w_out.reshape(N_TENSOR, block_width, model_width).astype(jnp.float32)
    partials = jnp.einsum('rkc,kcd->krd', q_blocks, w_blocks)
    partials = lax.optimization_barrier(partials.astype(jnp.bfloat16)).astype(jnp.float32)
    projected = lax.optimization_barrier(jnp.sum(partials, axis=0))
    block_output = (input_f32 + rms_gate * projected).astype(jnp.bfloat16)
    grad_f32 = block_dy.astype(jnp.float32)
    scaled = (rms_gate * grad_f32).astype(jnp.bfloat16)
    grad_w_out = jnp.dot(quantized.T, scaled, preferred_element_type=jnp.float32)
    d_quant = jnp.dot(scaled, w_out.T, preferred_element_type=jnp.float32)
    grad_gate_gain = lax.optimization_barrier(jnp.sum(d_quant * gated, axis=0))
    row_dots = lax.optimization_barrier(jnp.sum(d_quant * gated * gate_gain, axis=1, keepdims=True))
    d_gated = d_quant * gate_gain - rms_gate * rms_gate * gated * (row_dots / INNER)
    d_z, d_x, d_dt, d_bc_active, grad_conv_x_w, grad_conv_x_b, grad_dt_bias, grad_a_log, grad_d_skip = mixer_back(d_gated.reshape(gated_seq.shape))
    d_bc_linear, grad_conv_bc_w, grad_conv_bc_b = bc_back(d_bc_active)
    d_zx = jnp.concatenate([d_z.reshape(tok_rows, inner_width), d_x.reshape(tok_rows, inner_width)], axis=1).astype(jnp.bfloat16)
    d_dt_low = d_dt.reshape(tok_rows, -1).astype(jnp.bfloat16)
    d_bc_low = d_bc_linear.reshape(tok_rows, -1).astype(jnp.bfloat16)
    grad_w_zx = jnp.dot(hidden.T, d_zx, preferred_element_type=jnp.float32).reshape(w_zx.shape)
    grad_w_dt = jnp.dot(hidden.T, d_dt_low, preferred_element_type=jnp.float32)
    grad_w_bc = jnp.dot(hidden.T, d_bc_low, preferred_element_type=jnp.float32)
    d_hidden = jnp.dot(d_zx, w_zx_flat.T, preferred_element_type=jnp.float32)
    d_hidden = d_hidden + jnp.dot(d_dt_low, w_dt.T, preferred_element_type=jnp.float32)
    d_hidden = d_hidden + jnp.dot(d_bc_low, w_bc.T, preferred_element_type=jnp.float32)
    grad_pre_gain = lax.optimization_barrier(jnp.sum(d_hidden * normed, axis=0))
    d_normed = d_hidden * pre_gain
    grad_input = grad_f32 + rms_input * (d_normed - normed * lax.optimization_barrier(jnp.mean(d_normed * normed, axis=1, keepdims=True)))
    grads = (grad_pre_gain, grad_w_zx, grad_w_bc, grad_w_dt, grad_conv_x_w, grad_conv_x_b, grad_conv_bc_w, grad_conv_bc_b, grad_dt_bias, grad_a_log, grad_d_skip, grad_gate_gain, grad_w_out)
    return (block_output, grad_input, grads)

def reference(block_input, pre_gain, w_zx, w_bc, w_dt, conv_x_w, conv_x_b, conv_bc_w, conv_bc_b, dt_bias, a_log, d_skip, gate_gain, w_out, out_grad):
    params = (pre_gain, w_zx, w_bc, w_dt, conv_x_w, conv_x_b, conv_bc_w, conv_bc_b, dt_bias, a_log, d_skip, gate_gain, w_out)
    inputs = block_input.reshape(N_DP, TOK_DEV, D)
    cotangents = out_grad.reshape(N_DP, TOK_DEV, D)

    def accumulate(running, block_pair):
        block_output, grad_input, grads = one_block(params, block_pair[0], block_pair[1])
        updated = tuple((before + added for before, added in zip(running, grads)))
        return (updated, (block_output, grad_input))
    initial = tuple((jnp.zeros(param.shape, jnp.float32) for param in params))
    totals, stacked = lax.scan(accumulate, initial, (inputs, cotangents))
    block_output = stacked[0].reshape(TOKENS, D)
    grad_input = stacked[1].reshape(TOKENS, D)
    return (block_output, grad_input, totals[0], totals[1], totals[2], totals[3], totals[4], totals[5], totals[6], totals[7], totals[8], totals[9], totals[10], totals[11], totals[12])
```

```python
from functools import partial

import jax
import jax.numpy as jnp
from jax import lax
from jax.experimental import pallas as pl
from jax.experimental.pallas import tpu as pltpu
from jax.sharding import PartitionSpec as P

SEQ_LEN = 512
L = 128
HEAD = 64
PAD = 8
epsilon = 1e-05
f32 = jnp.float32
bf16 = jnp.bfloat16
HI = lax.Precision.HIGHEST
MESH = pl.DeviceIdType.MESH


def nn(a, b):
    return lax.dot_general(a, b, (((1,), (0,)), ((), ())), preferred_element_type=f32)


def nt(a, b):
    return lax.dot_general(a, b, (((1,), (1,)), ((), ())), preferred_element_type=f32)


def tn(a, b):
    return lax.dot_general(a, b, (((0,), (0,)), ((), ())), preferred_element_type=f32)


def exact(a, b):
    return lax.dot_general(
        a, b, (((1,), (0,)), ((), ())), precision=HI, preferred_element_type=f32
    )


def sigmoid(v):
    return 0.5 + 0.5 * jnp.tanh(0.5 * v)


def softplus(v):
    u = jnp.exp(-jnp.abs(v))
    return jnp.maximum(v, 0.0) + jnp.where(u < 1e-3, u - 0.5 * u * u, jnp.log(1.0 + u))


def fold_rows(v):
    return jnp.sum(v.reshape(v.shape[0] // 8, 8, v.shape[1]), axis=0)


def lane_iota(shape):
    return lax.broadcasted_iota(jnp.int32, shape, 1)


def row_iota(shape):
    return lax.broadcasted_iota(jnp.int32, shape, 0)


def conv(window, taps, bias):
    total = bias
    for k in range(4):
        total = total + window[PAD - 3 + k : PAD - 3 + k + L] * taps[k : k + 1]
    return total


def spread(cols, head):
    return jnp.broadcast_to(cols[:, head : head + 1], (L, L))


def span_decay(dtl, hp):
    pre = dtl + hp[0:1]
    dt = softplus(pre)
    ltri = (row_iota((L, L)) >= lane_iota((L, L))).astype(f32)
    cum = exact(ltri, dt * hp[1:2])
    return pre, dt, cum, cum.T


def remote(src, dst, send, recv, where):
    return pltpu.make_async_remote_copy(
        src_ref=src,
        dst_ref=dst,
        send_sem=send,
        recv_sem=recv,
        device_id=where,
        device_id_type=MESH,
    )


def greet(peers):
    barrier = pltpu.get_barrier_semaphore()
    for peer in peers:
        pl.semaphore_signal(barrier, inc=1, device_id=peer, device_id_type=MESH)
    pl.semaphore_wait(barrier, len(peers))


def bit_peers(axis, base, first, count):
    me = lax.axis_index(axis)
    peers, bits = [], []
    for k in range(count):
        step = base * 2**k
        bit = lax.rem(me // step, 2)
        peers.append({axis: me + step * (1 - 2 * bit)})
        bits.append(bit)
    return peers, bits


class Halving:
    def __init__(self, links, rows, src, work, recvs, full, sems):
        self.links, self.rows = links, rows
        self.src, self.work, self.recvs, self.full, self.sems = src, work, recvs, full, sems
        self.n = len(links)
        offs, size = [0], rows
        for _, bit in links:
            size //= 2
            offs.append(offs[-1] + bit * size)
        self.offs = offs

    def size(self, k):
        return self.rows >> k

    def at(self, off, size):
        return pl.ds(pl.multiple_of(off, size), size)

    def scatter(self, k):
        peer, bit = self.links[k]
        half = self.size(k + 1)
        off = self.offs[k] + (1 - bit) * half
        if k == 0:
            src = self.src.at[self.at(off, half)]
        else:
            src = self.work.at[self.at(off - self.offs[1], half)]
        return remote(src, self.recvs[k], self.sems.at[0, k], self.sems.at[1, k], peer)

    def fold(self, k):
        self.scatter(k).wait()
        half = self.size(k + 1)
        step = min(half, 64)
        keep = self.offs[k + 1]

        @pl.loop(0, half // step)
        def _(i):
            off = i * step
            rows = pl.ds(pl.multiple_of(off, step), step)
            near = pl.ds(pl.multiple_of(keep - self.offs[1] + off, step), step)
            if k == 0:
                mine = self.src[pl.ds(pl.multiple_of(keep + off, step), step), :]
            else:
                mine = self.work[near, :]
            total = mine.astype(f32) + self.recvs[k][rows, :].astype(f32)
            self.work[near, :] = total.astype(self.work.dtype)

    def own_copy(self):
        last = self.size(self.n)
        return pltpu.make_async_copy(
            self.work.at[self.at(self.offs[self.n] - self.offs[1], last)],
            self.full.at[self.at(self.offs[self.n], last)],
            self.sems.at[0, 2 * self.n],
        )

    def gather(self, k):
        peer, _ = self.links[k]
        rows = self.at(self.offs[k + 1], self.size(k + 1))
        sems = self.sems
        return remote(
            self.full.at[rows],
            self.full.at[rows],
            sems.at[0, self.n + k],
            sems.at[1, self.n + k],
            peer,
        )

    def close(self, j):
        n = self.n
        if 1 <= j <= n:
            self.fold(j - 1)
        elif j > n:
            self.gather(2 * n - j).wait()

    def begin(self, j):
        n = self.n
        if j < n:
            self.scatter(j).start()
            return
        if j == n:
            self.own_copy().start()
            self.own_copy().wait()
        if j < 2 * n:
            self.gather(2 * n - 1 - j).start()

    @staticmethod
    def scratch(rows, cols, n, dtype):
        recvs = [pltpu.VMEM((rows >> (k + 1), cols), dtype) for k in range(n)]
        return [pltpu.VMEM((rows // 2, cols), dtype)] + recvs + [
            pltpu.SemaphoreType.DMA((2, 2 * n + 1))
        ]


class Doubling:
    def __init__(self, peers, acc, recv, sems):
        self.peers, self.acc, self.recv, self.sems = peers, acc, recv, sems

    def copy(self, k):
        return remote(
            self.acc.at[k],
            self.recv.at[k],
            self.sems.at[0, k],
            self.sems.at[1, k],
            self.peers[k],
        )

    def close(self, j):
        if j > 0:
            self.copy(j - 1).wait()
            self.acc[j] = self.acc[j - 1] + self.recv[j - 1]

    def begin(self, j):
        if j < len(self.peers):
            self.copy(j).start()

    @staticmethod
    def scratch(n, rows, cols):
        return [
            pltpu.VMEM((n + 1, rows, cols), f32),
            pltpu.VMEM((n, rows, cols), f32),
            pltpu.SemaphoreType.DMA((2, n)),
        ]


def correction(x, dh, gain):
    v = x.astype(f32)
    r = lax.rsqrt(jnp.mean(v * v, axis=1, keepdims=True) + epsilon)
    normed = v * r
    dn = dh * gain
    return r * (dn - normed * jnp.mean(dn * normed, axis=1, keepdims=True))


def log2(n):
    return n.bit_length() - 1


def forward_kernel(
    width,
    _seq,
    x_ref,
    g_ref,
    gain_ref,
    w_ref,
    wo_ref,
    prm_ref,
    bcp_ref,
    hp_ref,
    hid_ref,
    z_ref,
    xl_ref,
    bcl_ref,
    dtl_ref,
    u_ref,
    y_ref,
    sin_ref,
    st_ref,
    po_ref,
    q_scr,
    bca_scr,
    s_scr,
    cs_scr,
    xs_scr,
):
    rows_all = x_ref.shape[0]
    model = x_ref.shape[1]
    pairs = width // L

    @pl.loop(0, rows_all // 32)
    def _(i):
        rows = pl.ds(pl.multiple_of(i * 32, 32), 32)
        v = x_ref[rows, :].astype(f32)
        r = lax.rsqrt(jnp.mean(v * v, axis=1, keepdims=True) + epsilon)
        hid_ref[rows, :] = (v * r * gain_ref[...]).astype(bf16)

    xl_ref[0:PAD, :] = jnp.zeros((PAD, width), f32)
    bcl_ref[0:PAD, :] = jnp.zeros((PAD, 256), f32)

    @pl.loop(0, width // 256)
    def _(j):
        cols = pl.ds(pl.multiple_of(j * 256, 256), 256)
        z_ref[:, cols] = nn(hid_ref[...], w_ref[:, cols])

    @pl.loop(0, width // 256)
    def _(j):
        cols = pl.ds(pl.multiple_of(j * 256, 256), 256)
        wcols = pl.ds(pl.multiple_of(width + j * 256, 256), 256)
        xl_ref[PAD : PAD + rows_all, cols] = nn(hid_ref[...], w_ref[:, wcols])

    bcl_ref[PAD : PAD + rows_all, :] = nn(hid_ref[...], w_ref[:, 2 * width : 2 * width + 256])
    dtl_ref[...] = nn(hid_ref[...], w_ref[:, 2 * width + 256 : 2 * width + 384])

    @pl.loop(0, width // 256)
    def _(j):
        cols = pl.ds(pl.multiple_of(j * 256, 256), 256)
        u_ref[:, cols] = nt(g_ref[...], wo_ref[cols, :])

    @pl.loop(0, rows_all // L)
    def _(c):
        t0 = pl.multiple_of(c * L, L)
        for half in range(2):
            lanes = slice(half * L, half * L + L)
            v = conv(bcl_ref[pl.ds(t0, L + PAD), lanes], bcp_ref[0:4, lanes], bcp_ref[4:5, lanes])
            bca_scr[pl.ds(t0, L), lanes] = (v * sigmoid(v)).astype(bf16)

    s_scr[...] = jnp.zeros_like(s_scr)
    hp = hp_ref[...]

    @pl.loop(0, rows_all // L)
    def _(c):
        t0 = pl.multiple_of(c * L, L)
        rows = pl.ds(t0, L)
        lo = lane_iota((L, L)) < HEAD
        mlo = (lane_iota((1, L)) < HEAD).astype(bf16)
        mhi = (lane_iota((1, L)) >= HEAD).astype(bf16)
        tri = row_iota((L, L)) >= lane_iota((L, L))
        _, dt, cum, cum_t = span_decay(dtl_ref[rows, :], hp)
        bm = bca_scr[rows, 0:L]
        cm = bca_scr[rows, L : 2 * L]
        both = nt(cm, bm)
        sb = s_scr[...].astype(bf16)
        sin_ref[c] = sb
        cs_scr[...] = nn(cm, sb)
        squares = jnp.zeros((L, L), f32)
        inner = jnp.zeros((L, L), f32)
        for p in range(pairs):
            lanes = slice(p * L, p * L + L)
            xc = conv(xl_ref[pl.ds(t0, L + PAD), lanes], prm_ref[0:4, lanes], prm_ref[4:5, lanes])
            x = xc * sigmoid(xc)
            h0, h1 = 2 * p, 2 * p + 1
            a0, a1 = spread(cum, h0), spread(cum, h1)
            ap = jnp.where(lo, a0, a1)
            k0 = both * jnp.exp(jnp.where(tri, a0 - cum_t[h0 : h0 + 1], -jnp.inf))
            k1 = both * jnp.exp(jnp.where(tri, a1 - cum_t[h1 : h1 + 1], -jnp.inf))
            xdt = x * jnp.where(lo, spread(dt, h0), spread(dt, h1))
            xb = xdt.astype(bf16)
            fin = ap[L - 1 : L]
            within = nn(
                jnp.concatenate([k0.astype(bf16), k1.astype(bf16)], axis=1),
                jnp.concatenate([xb * mlo, xb * mhi], axis=0),
            )
            y = within + jnp.exp(ap) * cs_scr[:, lanes] + prm_ref[5:6, lanes] * x
            xs_scr[:, lanes] = (xdt * jnp.exp(fin - ap)).astype(bf16)
            s_scr[:, lanes] = s_scr[:, lanes] * jnp.exp(fin)
            y_ref[rows, lanes] = y
            z = z_ref[rows, lanes]
            gated = y * (z * sigmoid(z))
            q = gated * prm_ref[6:7, lanes]
            q_scr[rows, lanes] = q.astype(bf16)
            squares = squares + gated * gated
            inner = inner + u_ref[rows, lanes] * q
        s_scr[...] += nn(bm.T, xs_scr[...])
        s0 = jnp.sum(squares, axis=1, keepdims=True)
        s1 = jnp.sum(inner, axis=1, keepdims=True)
        lane = lane_iota((L, L))
        stat = jnp.where(lane == 0, s0, jnp.where(lane == 1, s1, 0.0))
        st_ref[:, rows] = stat.T[0:2]

    @pl.loop(0, model // 256)
    def _(j):
        cols = pl.ds(pl.multiple_of(j * 256, 256), 256)
        po_ref[:, cols] = nn(q_scr[...], wo_ref[:, cols]).astype(bf16)


def gate_kernel(
    width,
    own,
    inner_total,
    ncore,
    ny,
    _seq,
    st_ref,
    g_ref,
    hid_ref,
    z_ref,
    y_ref,
    u_ref,
    prm_ref,
    po_ref,
    x_ref,
    dz_ref,
    dy_ref,
    gz_ref,
    go_ref,
    ggg_ref,
    bo_ref,
    stot_ref,
    q_scr,
    sc_scr,
    acc_scr,
    st_in,
    send_scr,
    recv_scr,
    po_in,
    po_own,
    x_own,
    st_send,
    st_recv,
    core_send,
    core_recv,
    po_send,
    po_recv,
    local,
):
    rows_all = z_ref.shape[0]
    here = pl.program_id(0)
    spot = lax.axis_index("tensor")
    core, yy = lax.rem(spot, ncore), spot // ncore
    ys = [lax.rem(yy + d, ny) for d in range(1, ny)]
    peers = [{"tensor": v * ncore + core} for v in ys]
    twin = {"tensor": spot + 1 - 2 * core}
    nloc, _, Ry, _ = po_ref.shape

    def po_copies():
        return [
            remote(po_ref.at[:, ys[d]], po_in.at[d], po_send.at[d], po_recv.at[d], peers[d])
            for d in range(ny - 1)
        ]

    def own_copies():
        return [
            pltpu.make_async_copy(po_ref.at[:, yy], po_own, local.at[0]),
            pltpu.make_async_copy(x_ref.at[pl.ds(core * nloc, nloc), yy], x_own, local.at[1]),
        ]

    @pl.when(here == 0)
    def _():
        greet(peers + ([twin] if ncore == 2 else []))
        copies = [
            remote(st_ref, st_in.at[d], st_send.at[d], st_recv.at[d], peers[d])
            for d in range(ny - 1)
        ]
        for copy in copies:
            copy.start()
        for copy in copies:
            copy.wait()
        total = st_ref[...]
        for d in range(ny - 1):
            total = total + st_in[d]
        stot_ref[...] = total
        for copy in po_copies() + own_copies():
            copy.start()

    model = g_ref.shape[1]
    pairs = width // L

    @pl.when(pl.program_id(0) == 0)
    def _():
        acc_scr[...] = jnp.zeros_like(acc_scr)
        ggg_ref[...] = jnp.zeros_like(ggg_ref)

    @pl.loop(0, rows_all // L)
    def _(c):
        rows = pl.ds(pl.multiple_of(c * L, L), L)
        st = stot_ref[here, :, rows]
        r_row = lax.rsqrt(st[0:1] / inner_total + epsilon)
        c_row = r_row * r_row * r_row * (st[1:2] / inner_total)
        cols8 = jnp.concatenate([r_row, c_row, jnp.zeros((6, L), f32)], axis=0).T
        r = jnp.broadcast_to(cols8[:, 0:1], (L, L))
        c2 = jnp.broadcast_to(cols8[:, 1:2], (L, L))
        for m in range(model // L):
            lanes = slice(m * L, m * L + L)
            sc_scr[rows, lanes] = (g_ref[rows, lanes].astype(f32) * r).astype(bf16)
        for p in range(pairs):
            lanes = slice(p * L, p * L + L)
            gg = prm_ref[6:7, lanes]
            z = z_ref[rows, lanes]
            y = y_ref[rows, lanes]
            sg = sigmoid(z)
            silz = z * sg
            gated = y * silz
            q_scr[rows, lanes] = (gated * gg).astype(bf16)
            dq = r * u_ref[rows, lanes]
            ggg_ref[:, lanes] += fold_rows(dq * gated)
            dgated = dq * gg - c2 * gated
            dy_ref[rows, lanes] = (dgated * silz).astype(bf16)
            dz_ref[rows, lanes] = (dgated * y * (sg + silz * (1.0 - sg))).astype(bf16)

    @pl.loop(0, model // 256)
    def _(j):
        cols = pl.ds(pl.multiple_of(j * 256, 256), 256)
        acc_scr[cols, 0:width] += tn(hid_ref[:, cols], dz_ref[...])
        acc_scr[cols, width : 2 * width] += tn(sc_scr[:, cols], q_scr[...])

    @pl.when(here == pl.num_programs(0) - 1)
    def _():
        if ncore == 2:
            send_scr[:, 0:own] = acc_scr[:, own:width].astype(bf16)
            send_scr[:, own : 2 * own] = acc_scr[:, width + own : 2 * width].astype(bf16)
            copy = remote(send_scr, recv_scr, core_send, core_recv, twin)
            copy.start()
            copy.wait()
            theirs = recv_scr[...].astype(f32)
        else:
            theirs = jnp.zeros((model, 2 * own), f32)
        gz_ref[...] = (acc_scr[:, 0:own] + theirs[:, 0:own]).astype(bf16)
        mine = acc_scr[:, width : width + own] + theirs[:, own : 2 * own]
        go_ref[...] = mine.astype(bf16)
        for copy in po_copies() + own_copies():
            copy.wait()
        for i in range(nloc):
            for h in range(Ry // L):
                lanes = pl.ds(pl.multiple_of(yy * Ry + h * L, L), L)
                r_row = lax.rsqrt(stot_ref[i, 0:1, lanes] / inner_total + epsilon)
                r = jnp.broadcast_to(r_row, (8, L)).T[:, 0:1]

                @pl.loop(0, model // L)
                def _(m, i=i, h=h, r=r):
                    cols = pl.ds(pl.multiple_of(m * L, L), L)
                    rows = slice(h * L, h * L + L)
                    total = po_own[i, rows, cols].astype(f32)
                    for d in range(ny - 1):
                        total = total + po_in[d, i, rows, cols].astype(f32)
                    bo_ref[i, rows, cols] = (x_own[i, rows, cols].astype(f32) + r * total).astype(bf16)


def scan_kernel(
    width,
    own,
    heads,
    ncore,
    ny,
    ndp,
    nloc_static,
    _seq,
    hid_ref,
    dz_ref,
    dy_ref,
    xl_ref,
    bcl_ref,
    dtl_ref,
    sin_ref,
    w_ref,
    prm_ref,
    bcp_ref,
    hp_ref,
    ggg_ref,
    gain_ref,
    gz_ref,
    go_ref,
    bo_ref,
    x_ref,
    dh_ref,
    gw_ref,
    gbcw_ref,
    small_ref,
    other_ref,
    shared_ref,
    corr_ref,
    fz_ref,
    fo_ref,
    boy_ref,
    bot_ref,
    boty_ref,
    d_scr,
    bcc_scr,
    bca_scr,
    ds_scr,
    dsb_scr,
    cs_scr,
    bds_scr,
    xs_scr,
    dye_scr,
    nx_scr,
    nbc_scr,
    gx_ref,
    gbc_ref,
    gdt_ref,
    gpre_ref,
    acc_scr,
    send_scr,
    recv_scr,
    dh_scr,
    dh_in,
    x_own,
    core_send,
    core_recv,
    y_sems,
    bo_sems,
    local,
    *machine,
):
    rows_all = dz_ref.shape[0]
    model = hid_ref.shape[1]
    pairs = width // L
    spans = rows_all // L
    Ry = rows_all // ny
    seq, back = pl.program_id(0), pl.program_id(1)
    step = seq * spans + back
    spot = lax.axis_index("tensor")
    core, yy = lax.rem(spot, ncore), spot // ncore
    twin = {"tensor": spot + 1 - 2 * core}
    ys = [lax.rem(yy + d, ny) for d in range(1, ny)]
    peers = [{"tensor": v * ncore + core} for v in ys]
    nbits = log2(ndp)
    dp_peers, dp_bits = bit_peers("dp", 1, 0, nbits)
    links = list(zip(dp_peers, dp_bits))
    swapped = [links[1], links[0]] + links[2:] if nbits > 1 else links
    half = len(machine) // 2
    mz, mo = machine[:half], machine[half:]
    jobs = [
        Halving(links, model, gz_ref, mz[0], mz[1:-1], fz_ref, mz[-1]),
        Halving(swapped, model, go_ref, mo[0], mo[1:-1], fo_ref, mo[-1]),
    ]
    last_step = nloc_static * spans - 1

    def bo_first():
        out = [
            remote(bo_ref, boy_ref.at[d], bo_sems.at[0, d], bo_sems.at[1, d], peers[d])
            for d in range(ny - 1)
        ]
        if ncore == 2:
            out.append(remote(bo_ref, bot_ref, bo_sems.at[0, ny - 1], bo_sems.at[1, ny - 1], twin))
        return out

    def bo_second():
        if ncore != 2:
            return []
        return [
            remote(boy_ref.at[d], boty_ref.at[d], bo_sems.at[0, ny + d], bo_sems.at[1, ny + d], twin)
            for d in range(ny - 1)
        ]

    def dh_copies():
        return [
            remote(
                dh_scr.at[pl.ds(pl.multiple_of(ys[d] * Ry, Ry), Ry)],
                dh_in.at[seq - 1, d],
                y_sems.at[0, seq - 1, d],
                y_sems.at[1, seq - 1, d],
                peers[d],
            )
            for d in range(ny - 1)
        ]

    def x_copy():
        return pltpu.make_async_copy(x_ref.at[core * nloc_static + seq - 1, yy], x_own, local.at[0])

    @pl.when(step == 0)
    def _():
        greet(peers + dp_peers + ([twin] if ncore == 2 else []))
        for copy in bo_first():
            copy.start()
        acc_scr[...] = jnp.zeros_like(acc_scr)
        gx_ref[...] = jnp.zeros_like(gx_ref)
        gbc_ref[...] = jnp.zeros_like(gbc_ref)
        gdt_ref[...] = jnp.zeros_like(gdt_ref)
        gpre_ref[...] = jnp.zeros_like(gpre_ref)

    events = 2 * nbits + 1
    for j in range(events):

        @pl.when(step == (j * last_step + nbits) // (events - 1))
        def _(j=j):
            for job in jobs:
                job.close(j)
            for job in jobs:
                job.begin(j)

    @pl.when(step == last_step // 2)
    def _():
        for copy in bo_first():
            copy.wait()
        for copy in bo_second():
            copy.start()

    @pl.when(jnp.logical_and(seq > 0, back == 0))
    def _():
        for copy in dh_copies():
            copy.start()
        x_copy().start()

    @pl.when(jnp.logical_and(seq > 0, back == spans - 2))
    def _():
        for copy in dh_copies():
            copy.wait()
        x_copy().wait()

        @pl.loop(0, Ry // 32)
        def _(i):
            rows = pl.ds(pl.multiple_of(i * 32, 32), 32)
            mine = pl.ds(pl.multiple_of(yy * Ry + i * 32, 32), 32)
            dh = dh_scr[mine, :].astype(f32)
            for d in range(ny - 1):
                dh = dh + dh_in[seq - 1, d, rows, :].astype(f32)
            corr_ref[seq - 1, rows, :] = correction(x_own[rows, :], dh, gain_ref[...]).astype(bf16)

    hp = hp_ref[...]

    @pl.when(back == 0)
    def _():
        ds_scr[...] = jnp.zeros_like(ds_scr)
        nx_scr[...] = jnp.zeros_like(nx_scr)
        nbc_scr[...] = jnp.zeros_like(nbc_scr)

        @pl.loop(0, spans)
        def _(c):
            t0 = pl.multiple_of(c * L, L)
            for half in range(2):
                lanes = slice(half * L, half * L + L)
                v = conv(bcl_ref[pl.ds(t0, L + PAD), lanes], bcp_ref[0:4, lanes], bcp_ref[4:5, lanes])
                bcc_scr[pl.ds(t0, L), lanes] = v
                bca_scr[pl.ds(t0, L), lanes] = (v * sigmoid(v)).astype(bf16)

    def one_chunk():
        c = spans - 1 - back
        t0 = pl.multiple_of(c * L, L)
        rows = pl.ds(t0, L)
        lane = lane_iota((L, L))
        lo = lane < HEAD
        mlo = (lane_iota((1, L)) < HEAD).astype(bf16)
        mhi = (lane_iota((1, L)) >= HEAD).astype(bf16)
        tri = row_iota((L, L)) >= lane
        pre, dt, cum, cum_t = span_decay(dtl_ref[rows, :], hp)
        bm = bca_scr[rows, 0:L]
        cm = bca_scr[rows, L : 2 * L]
        both = nt(cm, bm)
        sb = sin_ref[c]
        dsb_scr[...] = ds_scr[...].astype(bf16)
        cs_scr[...] = nn(cm, sb)
        bds_scr[...] = nn(bm, dsb_scr[...])
        d_both = jnp.zeros((L, L), f32)
        d_cum = jnp.zeros((L, L), f32)
        d_dt = jnp.zeros((L, L), f32)
        d_far = jnp.zeros((L, L), f32)
        d_end = jnp.zeros((1, L), f32)
        for p in range(pairs):
            lanes = slice(p * L, p * L + L)
            window = xl_ref[pl.ds(t0, L + PAD), lanes]
            shifted = [window[PAD - 3 + k : PAD - 3 + k + L] for k in range(4)]
            taps = prm_ref[0:4, lanes]
            xc = prm_ref[4:5, lanes]
            for k in range(4):
                xc = xc + shifted[k] * taps[k : k + 1]
            sg = sigmoid(xc)
            x = xc * sg
            h0, h1 = 2 * p, 2 * p + 1
            a0, a1 = spread(cum, h0), spread(cum, h1)
            ap = jnp.where(lo, a0, a1)
            e0 = jnp.exp(jnp.where(tri, a0 - cum_t[h0 : h0 + 1], -jnp.inf))
            e1 = jnp.exp(jnp.where(tri, a1 - cum_t[h1 : h1 + 1], -jnp.inf))
            k0 = (both * e0).astype(bf16)
            k1 = (both * e1).astype(bf16)
            dtp = jnp.where(lo, spread(dt, h0), spread(dt, h1))
            xdt = x * dtp
            xb = xdt.astype(bf16)
            bdx = jnp.concatenate([xb * mlo, xb * mhi], axis=0)
            ecum = jnp.exp(ap)
            fin = ap[L - 1 : L]
            sd = jnp.exp(fin - ap)
            y = nn(jnp.concatenate([k0, k1], axis=1), bdx) + ecum * cs_scr[:, lanes]
            dyb = dy_ref[rows, lanes]
            dy = dyb.astype(f32)
            dk = nt(dyb, bdx)
            d_both = d_both + dk[:, 0:L] * e0 + dk[:, L : 2 * L] * e1
            bdy = jnp.concatenate([dyb * mlo, dyb * mhi], axis=0)
            near = tn(jnp.concatenate([k0, k1], axis=0), bdy)
            far = sd * bds_scr[:, lanes]
            dxdt = near + far
            v = dy * y - xb.astype(f32) * near
            u = dxdt * x
            w = xdt * far
            ends = jnp.exp(fin)
            through = ends * jnp.sum(sb[:, lanes].astype(f32) * ds_scr[:, lanes], axis=0, keepdims=True)
            for h, keep in ((h0, lo), (h1, jnp.logical_not(lo))):
                here = lane == h
                d_cum = jnp.where(here, jnp.sum(jnp.where(keep, v, 0.0), axis=1, keepdims=True), d_cum)
                d_dt = jnp.where(here, jnp.sum(jnp.where(keep, u, 0.0), axis=1, keepdims=True), d_dt)
                d_far = jnp.where(here, jnp.sum(jnp.where(keep, w, 0.0), axis=1, keepdims=True), d_far)
                whole = jnp.sum(jnp.where(keep[0:1], through, 0.0), axis=1, keepdims=True)
                d_end = jnp.where(here[0:1], whole, d_end)
            dx = dxdt * dtp + dy * prm_ref[5:6, lanes]
            dxc = dx * (sg + x * (1.0 - sg))
            for k in range(4):
                gx_ref[k, :, lanes] += fold_rows(dxc * shifted[k])
            gx_ref[4, :, lanes] += fold_rows(dxc)
            gx_ref[5, :, lanes] += fold_rows(dy * x)
            ext = jnp.concatenate([dxc, nx_scr[:, lanes]], axis=0)
            dxl = ext[0:L] * taps[3:4]
            for k in range(3):
                dxl = dxl + ext[3 - k : 3 - k + L] * taps[k : k + 1]
            nx_scr[:, lanes] = dxc[0:8]
            d_scr[rows, lanes] = dxl.astype(bf16)
            xs_scr[:, lanes] = (xdt * sd).astype(bf16)
            dye_scr[:, lanes] = (dy * ecum).astype(bf16)
            ds_scr[:, lanes] = ds_scr[:, lanes] * ends
        ds_scr[...] += nn(cm.T, dye_scr[...])
        utri = (row_iota((L, L)) <= lane).astype(f32)
        before = (row_iota((L, L)) > lane).astype(f32)
        d_a = exact(utri, d_cum) + exact(before, d_far) + d_end
        d_dt = d_dt + d_a * hp[1:2]
        d_pre = d_dt * sigmoid(pre)
        gdt_ref[0] += fold_rows(d_pre)
        gdt_ref[1] += fold_rows(d_a * dt * hp[1:2])
        d_scr[rows, width + 256 : width + 384] = d_pre.astype(bf16)
        dgb = d_both.astype(bf16)
        d_c = nt(dye_scr[...], sb) + nn(dgb, bm)
        d_b = nt(xs_scr[...], dsb_scr[...]) + nn(dgb.T, cm)
        for half, dv in ((0, d_b), (1, d_c)):
            lanes = slice(half * L, half * L + L)
            pre_act = bcc_scr[rows, lanes]
            sg = sigmoid(pre_act)
            dvc = dv * (sg + pre_act * sg * (1.0 - sg))
            window = bcl_ref[pl.ds(t0, L + PAD), lanes]
            for k in range(4):
                gbc_ref[k, :, lanes] += fold_rows(dvc * window[PAD - 3 + k : PAD - 3 + k + L])
            gbc_ref[4, :, lanes] += fold_rows(dvc)
            ext = jnp.concatenate([dvc, nbc_scr[:, lanes]], axis=0)
            dvl = ext[0:L] * bcp_ref[3:4, lanes]
            for k in range(3):
                dvl = dvl + ext[3 - k : 3 - k + L] * bcp_ref[k : k + 1, lanes]
            nbc_scr[:, lanes] = dvc[0:8]
            d_scr[rows, width + half * L : width + half * L + L] = dvl.astype(bf16)

    one_chunk()

    @pl.when(back == spans - 1)
    def _():
        @pl.loop(0, model // 256)
        def _(j):
            cols = pl.ds(pl.multiple_of(j * 256, 256), 256)
            dh = nt(dz_ref[...], w_ref[cols, 0:width]) + nt(d_scr[...], w_ref[cols, width:])
            dh_scr[:, cols] = dh.astype(bf16)
            gpre_ref[:, cols] += fold_rows(dh * hid_ref[:, cols].astype(f32))
            acc_scr[cols, :] += tn(hid_ref[:, cols], d_scr[...])

    @pl.when(step == last_step)
    def _():
        tail = acc_scr[:, width + 256 : width + 384]
        if ncore == 2:
            send_scr[:, 0:own] = acc_scr[:, own:width].astype(bf16)
            send_scr[:, own : own + L] = tail.astype(bf16)
        dh_ref[...] = dh_scr[...]
        gbcw_ref[...] = acc_scr[:, width : width + 256].astype(gbcw_ref.dtype)
        if ncore == 2:
            copy = remote(send_scr, recv_scr, core_send, core_recv, twin)
            copy.start()
        rows = [jnp.sum(gx_ref[k], axis=0, keepdims=True) for k in range(6)]
        rows.append(jnp.sum(ggg_ref[...], axis=0, keepdims=True))
        dts = [jnp.sum(gdt_ref[k], axis=0, keepdims=True) for k in range(2)]
        small_ref[...] = jnp.zeros_like(small_ref)
        other_ref[...] = jnp.zeros_like(other_ref)
        for k in range(7):
            small_ref[k : k + 1, :] = rows[k][:, 0:own]
            if ncore == 2:
                other_ref[k : k + 1, :] = rows[k][:, own:width]
        for k in range(2):
            small_ref[7 + k : 8 + k, 0:L] = dts[k]
            if ncore == 2:
                moved = pltpu.roll(jnp.broadcast_to(dts[k], (8, L)), L - heads, axis=1)
                other_ref[7 + k : 8 + k, 0:L] = moved[0:1]
        shared_ref[...] = jnp.zeros_like(shared_ref)
        shared_ref[0:1, :] = jnp.sum(gpre_ref[...], axis=0, keepdims=True) / gain_ref[...]
        for k in range(5):
            shared_ref[k + 1 : k + 2, 0:256] = jnp.sum(gbc_ref[k], axis=0, keepdims=True)
        if ncore == 2:
            copy.wait()
            theirs = recv_scr[...].astype(f32)
            gw_ref[:, 0:own] = (acc_scr[:, 0:own] + theirs[:, 0:own]).astype(bf16)
            tail = tail + pltpu.roll(theirs[:, own : own + L], L - heads, axis=1)
        else:
            gw_ref[:, 0:own] = acc_scr[:, 0:own].astype(bf16)
        gw_ref[:, own : own + L] = tail.astype(bf16)
        for copy in bo_second():
            copy.wait()


def tail_kernel(
    own,
    ncore,
    ny,
    ndp,
    gw_ref,
    gbcw_ref,
    small_ref,
    other_ref,
    shared_ref,
    dh_ref,
    gain_ref,
    corr_ref,
    x_ref,
    fw_ref,
    fb_ref,
    small_out,
    shared_out,
    last_ref,
    cy_ref,
    ct_ref,
    cty_ref,
    ly_ref,
    lt_ref,
    lty_ref,
    dh_in,
    x_own,
    small_in,
    core_sems,
    y_sems,
    c_sems,
    l_sems,
    local,
    *machine,
):
    model = gw_ref.shape[0]
    Ry, nloc = x_own.shape[0], corr_ref.shape[0] + 1
    spot = lax.axis_index("tensor")
    core, yy = lax.rem(spot, ncore), spot // ncore
    twin = {"tensor": spot + 1 - 2 * core}
    ys = [lax.rem(yy + d, ny) for d in range(1, ny)]
    peers = [{"tensor": v * ncore + core} for v in ys]
    nbits = log2(ndp)
    dp_peers, dp_bits = bit_peers("dp", 1, 0, nbits)
    t_peers, t_bits = bit_peers("tensor", 1, 0, log2(ncore * ny))
    links = list(zip(dp_peers, dp_bits))
    swapped = [links[1], links[0]] + links[2:] if nbits > 1 else links
    t_links = list(zip(t_peers, t_bits))
    per = nbits + 2
    a, b = machine[:per], machine[per : 2 * per]
    per_bc = nbits + len(t_links) + 2
    c = machine[2 * per : 2 * per + per_bc]
    sm, sh = machine[2 * per + per_bc : 2 * per + per_bc + 3], machine[2 * per + per_bc + 3 :]
    mid = model // 2
    job_a = Halving(links, mid, gw_ref.at[0:mid], a[0], a[1:-1], fw_ref.at[0:mid], a[-1])
    job_b = Halving(swapped, mid, gw_ref.at[mid:model], b[0], b[1:-1], fw_ref.at[mid:model], b[-1])
    job_c = Halving(t_links + links, model, gbcw_ref, c[0], c[1:-1], fb_ref, c[-1])
    job_sm = Doubling(dp_peers, *sm)
    job_sh = Doubling(t_peers + dp_peers, *sh)

    def dh_copies():
        return [
            remote(
                dh_ref.at[pl.ds(pl.multiple_of(ys[d] * Ry, Ry), Ry)],
                dh_in.at[d],
                y_sems.at[0, d],
                y_sems.at[1, d],
                peers[d],
            )
            for d in range(ny - 1)
        ]

    def first(src, toy, tot, sems):
        out = [
            remote(src, toy.at[d], sems.at[0, d], sems.at[1, d], peers[d]) for d in range(ny - 1)
        ]
        if ncore == 2:
            out.append(remote(src, tot, sems.at[0, ny - 1], sems.at[1, ny - 1], twin))
        return out

    def second(toy, toty, sems):
        if ncore != 2:
            return []
        return [
            remote(toy.at[d], toty.at[d], sems.at[0, ny + d], sems.at[1, ny + d], twin)
            for d in range(ny - 1)
        ]

    early = (corr_ref, cy_ref, ct_ref, c_sems)
    late = (last_ref, ly_ref, lt_ref, l_sems)
    x_copy = pltpu.make_async_copy(x_ref.at[core * nloc + nloc - 1, yy], x_own, local.at[0])
    others = peers + ([twin] if ncore == 2 else [])
    greet(others + dp_peers)
    x_copy.start()

    def turn(*pairs):
        for job, j in pairs:
            job.close(j)
        for job, j in pairs:
            job.begin(j)

    job_sh.acc[0] = shared_ref[...]
    turn((job_c, 0), (job_a, 0), (job_b, 0))
    if ncore == 2:
        small_copy = remote(other_ref, small_in, core_sems.at[0], core_sems.at[1], twin)
        small_copy.start()
    turn((job_c, 1), (job_sh, 0))
    for copy in dh_copies():
        copy.start()
    for copy in first(*early):
        copy.start()
    if ncore == 2:
        small_copy.wait()
        job_sm.acc[0] = small_ref[...] + small_in[...]
    else:
        job_sm.acc[0] = small_ref[...]
    turn((job_sh, 1), (job_sm, 0))
    steps = [
        (job_c, iter(range(2, 2 * job_c.n + 1))),
        (job_sm, iter(range(1, len(job_sm.peers) + 1))),
        (job_sh, iter(range(2, len(job_sh.peers) + 1))),
    ]

    def smaller():
        found = []
        for job, left in steps:
            j = next(left, None)
            if j is not None:
                found.append((job, j))
        return found

    turn((job_a, 1), (job_b, 1), *smaller())
    for copy in dh_copies():
        copy.wait()
    x_copy.wait()

    @pl.loop(0, Ry // 32)
    def _(i):
        rows = pl.ds(pl.multiple_of(i * 32, 32), 32)
        mine = pl.ds(pl.multiple_of(yy * Ry + i * 32, 32), 32)
        dh = dh_ref[mine, :].astype(f32)
        for d in range(ny - 1):
            dh = dh + dh_in[d, rows, :].astype(f32)
        last_ref[rows, :] = correction(x_own[rows, :], dh, gain_ref[...]).astype(bf16)

    turn(*smaller())
    for copy in first(*late):
        copy.start()
    for j in range(2, 2 * nbits + 1):
        turn((job_a, j), (job_b, j), *smaller())
    for copy in first(*early):
        copy.wait()
    for copy in second(cy_ref, cty_ref, c_sems):
        copy.start()
    for _ in range(2 * job_c.n):
        turn(*smaller())
    small_out[...] = job_sm.acc[len(job_sm.peers)]
    shared_out[...] = job_sh.acc[len(job_sh.peers)]
    for copy in first(*late):
        copy.wait()
    for copy in second(ly_ref, lty_ref, l_sems):
        copy.start()
    for copy in second(cy_ref, cty_ref, c_sems) + second(ly_ref, lty_ref, l_sems):
        copy.wait()


def finish_kernel(pieces, nloc, _idx, g_ref, *refs):
    gi_ref, bo_ref = refs[-2:]
    early, late, outs = refs[:pieces], refs[pieces : 2 * pieces], refs[2 * pieces : 3 * pieces]
    last = pl.program_id(1) == nloc - 1
    for k in range(pieces):
        here = pl.program_id(0) == k

        @pl.when(here)
        def _(src=outs[k]):
            bo_ref[...] = src[...]

        @pl.when(jnp.logical_and(here, jnp.logical_not(last)))
        def _(src=early[k]):
            gi_ref[...] = g_ref[...].astype(f32) + src[...].astype(f32)

        @pl.when(jnp.logical_and(here, last))
        def _(src=late[k]):
            gi_ref[...] = g_ref[...].astype(f32) + src[...].astype(f32)


def unpack_kernel(own, gz_ref, go_ref, gw_ref, gzx_ref, gwo_ref):
    gzx_ref[:, 0, :] = gz_ref[...].astype(f32)
    gzx_ref[:, 1, :] = gw_ref[:, 0:own].astype(f32)
    v = go_ref[...].astype(f32)
    for k in range(own // L):
        gwo_ref[k * L : k * L + L, :] = v[:, k * L : k * L + L].T


def seq_spec(*shape):
    zeros = (0,) * len(shape)
    return pl.BlockSpec((None,) + shape, lambda i, s: (i,) + zeros)


def moved_spec(ncore, nloc, *shape):
    zeros = (0,) * len(shape)

    def index(i, s):
        return (i + lax.rem(lax.axis_index("tensor"), ncore) * nloc,) + zeros

    return pl.BlockSpec((None,) + shape, index)


def whole_spec(*shape):
    zeros = (0,) * len(shape)
    return pl.BlockSpec(shape, lambda *_: zeros, pipeline_mode=pl.Buffered(1))


def call(
    kernel, grid, in_specs, out_specs, out_shape, scratch, name, flops=0, moved=0, group=None
):
    return pl.pallas_call(
        kernel,
        grid_spec=pltpu.PrefetchScalarGridSpec(
            num_scalar_prefetch=1,
            grid=grid,
            in_specs=in_specs,
            out_specs=out_specs,
            scratch_shapes=scratch,
        ),
        out_shape=out_shape,
        cost_estimate=pl.CostEstimate(
            flops=int(flops), bytes_accessed=int(moved), transcendentals=0
        ),
        name=name,
        compiler_params=None
        if group is None
        else pltpu.CompilerParams(collective_id=group, has_side_effects=True),
    )


def sds(*shape, dtype=f32):
    return jax.ShapeDtypeStruct(shape, dtype)


def body(
    block_input,
    pre_gain,
    w_zx,
    w_bc,
    w_dt,
    conv_x_w,
    conv_x_b,
    conv_bc_w,
    conv_bc_b,
    dt_bias,
    a_log,
    d_skip,
    gate_gain,
    w_out,
    out_grad,
):
    tok, model = block_input.shape
    own = w_zx.shape[2]
    heads = w_dt.shape[1]
    nt = lax.axis_size("tensor")
    ndp = lax.axis_size("dp")
    inner_total = own * nt
    ncore = 2 if nt % 2 == 0 else 1
    ny = nt // ncore
    width = own * ncore
    t = lax.axis_index("tensor")
    me = lax.axis_index("dp")
    core, yy = t % ncore, t // ncore
    R = SEQ_LEN
    Ry = R // ny
    nseq = tok // R
    nloc = nseq // ncore
    spans = R // L
    wtot = 2 * width + 384

    def swap_core(v):
        return lax.ppermute(v, "tensor", [(i, i ^ 1) for i in range(nt)])

    def y_shift(v, d):
        pairs = [(i, ((i // ncore + d) % ny) * ncore + i % ncore) for i in range(nt)]
        return lax.ppermute(v, "tensor", pairs)

    def dp_shift(v, d):
        return lax.ppermute(v, "dp", [(i, (i + d) % ndp) for i in range(ndp)])

    def both_cores(v, axis):
        return jnp.concatenate([v, swap_core(v)], axis=axis) if ncore == 2 else v

    x3 = block_input.reshape(nseq, R, model)
    g3 = out_grad.reshape(nseq, R, model)
    x4 = block_input.reshape(nseq, ny, Ry, model)
    g4 = out_grad.reshape(nseq, ny, Ry, model)
    wz, wx = w_zx[:, 0], w_zx[:, 1]
    rowp = jnp.concatenate(
        [
            conv_x_w,
            conv_x_b[None],
            jnp.repeat(d_skip, HEAD)[None],
            gate_gain[None],
            jnp.pad(jnp.concatenate([dt_bias, -jnp.exp(a_log)]), (0, own - 2 * heads))[None],
        ],
        axis=0,
    )
    prm = both_cores(rowp, 1)
    hrow = prm[7].reshape(ncore, own)
    hp = jnp.stack([hrow[:, :heads].reshape(-1), hrow[:, heads : 2 * heads].reshape(-1)])
    hp = jnp.pad(hp, ((0, 6), (0, L - ncore * heads)))
    wdt = jnp.pad(both_cores(w_dt, 1), ((0, 0), (0, L - ncore * heads)))
    wcat = jnp.concatenate([both_cores(wz, 1), both_cores(wx, 1), w_bc, wdt], axis=1)
    wo = both_cores(w_out, 0)
    bcp = jnp.concatenate([conv_bc_w, conv_bc_b[None], jnp.zeros((3, 256), f32)], axis=0)
    gain = pre_gain[None]
    seq0 = jnp.array([core * nloc], jnp.int32)

    hid, z, xl, bcl, dtl, u, y, sin, st, po = call(
        partial(forward_kernel, width),
        (nloc,),
        [
            moved_spec(ncore, nloc, R, model),
            moved_spec(ncore, nloc, R, model),
            whole_spec(1, model),
            whole_spec(model, wtot),
            whole_spec(width, model),
            whole_spec(8, width),
            whole_spec(8, 256),
            whole_spec(8, L),
        ],
        [
            seq_spec(R, model),
            seq_spec(R, width),
            seq_spec(R + PAD, width),
            seq_spec(R + PAD, 256),
            seq_spec(R, L),
            seq_spec(R, width),
            seq_spec(R, width),
            seq_spec(spans, L, width),
            seq_spec(2, R),
            seq_spec(R, model),
        ],
        [
            sds(nloc, R, model, dtype=bf16),
            sds(nloc, R, width),
            sds(nloc, R + PAD, width),
            sds(nloc, R + PAD, 256),
            sds(nloc, R, L),
            sds(nloc, R, width),
            sds(nloc, R, width),
            sds(nloc, spans, L, width, dtype=bf16),
            sds(nloc, 2, R),
            sds(nloc, R, model, dtype=bf16),
        ],
        [
            pltpu.VMEM((R, width), bf16),
            pltpu.VMEM((R, 256), bf16),
            pltpu.VMEM((L, width), f32),
            pltpu.VMEM((L, width), f32),
            pltpu.VMEM((L, width), bf16),
        ],
        "forward",
        2 * nloc * R * model * (wtot + 2 * width),
        nloc * R * (6 * model + 20 * width),
    )(seq0, x3, g3, gain, wcat, wo, prm, bcp, hp)

    any_spec = pl.BlockSpec(memory_space=pl.ANY)
    nbits = log2(ndp)
    nother = max(ny - 1, 1)
    dma = pltpu.SemaphoreType.DMA
    po4 = po.reshape(nloc, ny, Ry, model)
    dz, dy, gz, go, ggg, bo, st = call(
        partial(gate_kernel, width, own, inner_total, ncore, ny),
        (nloc,),
        [
            whole_spec(nloc, 2, R),
            moved_spec(ncore, nloc, R, model),
            seq_spec(R, model),
            seq_spec(R, width),
            seq_spec(R, width),
            seq_spec(R, width),
            whole_spec(8, width),
            any_spec,
            any_spec,
        ],
        [
            seq_spec(R, width),
            seq_spec(R, width),
            whole_spec(model, own),
            whole_spec(model, own),
            whole_spec(8, width),
            whole_spec(nloc, Ry, model),
            whole_spec(nloc, 2, R),
        ],
        [
            sds(nloc, R, width, dtype=bf16),
            sds(nloc, R, width, dtype=bf16),
            sds(model, own, dtype=bf16),
            sds(model, own, dtype=bf16),
            sds(8, width),
            sds(nloc, Ry, model, dtype=bf16),
            sds(nloc, 2, R),
        ],
        [
            pltpu.VMEM((R, width), bf16),
            pltpu.VMEM((R, model), bf16),
            pltpu.VMEM((model, 2 * width), f32),
            pltpu.VMEM((nother, nloc, 2, R), f32),
            pltpu.VMEM((model, 2 * own), bf16),
            pltpu.VMEM((model, 2 * own), bf16),
            pltpu.VMEM((nother, nloc, Ry, model), bf16),
            pltpu.VMEM((nloc, Ry, model), bf16),
            pltpu.VMEM((nloc, Ry, model), bf16),
            dma((nother,)),
            dma((nother,)),
            dma,
            dma,
            dma((nother,)),
            dma((nother,)),
            dma((2,)),
        ],
        "gate",
        4 * nloc * R * model * width,
        nloc * R * (4 * model + 16 * width),
        1,
    )(seq0, st, g3, hid, z, y, u, prm, po4, x4)

    def chunk_spec(*shape):
        zeros = (0,) * len(shape)
        return pl.BlockSpec((None,) + shape, lambda i, b, s: (i,) + zeros)

    bc_type = bf16 if (model // (nt * ndp)) % 16 == 0 else f32
    dh, gw2, gbcw, small, other, shared, corr, fz, fo, boy, bot, boty = call(
        partial(scan_kernel, width, own, heads, ncore, ny, ndp, nloc),
        (nloc, spans),
        [
            chunk_spec(R, model),
            chunk_spec(R, width),
            chunk_spec(R, width),
            chunk_spec(R + PAD, width),
            chunk_spec(R + PAD, 256),
            chunk_spec(R, L),
            chunk_spec(spans, L, width),
            pl.BlockSpec((model, wtot), lambda i, b, s: (0, 0), pipeline_mode=pl.Buffered(1)),
            whole_spec(8, width),
            whole_spec(8, 256),
            whole_spec(8, L),
            whole_spec(8, width),
            whole_spec(1, model),
            whole_spec(model, own),
            whole_spec(model, own),
            any_spec,
            any_spec,
        ],
        [
            whole_spec(R, model),
            whole_spec(model, own + L),
            whole_spec(model, 256),
            whole_spec(16, own),
            whole_spec(16, own),
            whole_spec(8, model),
            whole_spec(nloc - 1, Ry, model),
        ]
        + [any_spec] * 5,
        [
            sds(R, model, dtype=bf16),
            sds(model, own + L, dtype=bf16),
            sds(model, 256, dtype=bc_type),
            sds(16, own),
            sds(16, own),
            sds(8, model),
            sds(nloc - 1, Ry, model, dtype=bf16),
            sds(model, own, dtype=bf16),
            sds(model, own, dtype=bf16),
            sds(nother, nloc, Ry, model, dtype=bf16),
            sds(nloc, Ry, model, dtype=bf16),
            sds(nother, nloc, Ry, model, dtype=bf16),
        ],
        [
            pltpu.VMEM((R, width + 384), bf16),
            pltpu.VMEM((R, 256), f32),
            pltpu.VMEM((R, 256), bf16),
            pltpu.VMEM((L, width), f32),
            pltpu.VMEM((L, width), bf16),
            pltpu.VMEM((L, width), f32),
            pltpu.VMEM((L, width), f32),
            pltpu.VMEM((L, width), bf16),
            pltpu.VMEM((L, width), bf16),
            pltpu.VMEM((8, width), f32),
            pltpu.VMEM((8, 256), f32),
            pltpu.VMEM((6, 8, width), f32),
            pltpu.VMEM((5, 8, 256), f32),
            pltpu.VMEM((2, 8, L), f32),
            pltpu.VMEM((8, model), f32),
            pltpu.VMEM((model, width + 384), f32),
            pltpu.VMEM((model, own + L), bf16),
            pltpu.VMEM((model, own + L), bf16),
            pltpu.VMEM((R, model), bf16),
            pltpu.VMEM((nloc - 1, nother, Ry, model), bf16),
            pltpu.VMEM((Ry, model), bf16),
            dma,
            dma,
            dma((2, nloc - 1, nother)),
            dma((2, 2 * ny)),
            dma((1,)),
        ]
        + Halving.scratch(model, own, nbits, bf16)
        + Halving.scratch(model, own, nbits, bf16),
        "scan_back",
        2 * nloc * R * model * (2 * wtot),
        nloc * R * (4 * model + 12 * width),
        2,
    )(seq0, hid, dz, dy, xl, bcl, dtl, sin, wcat, prm, bcp, hp, ggg, gain, gz, go, bo, x4)

    vm = pl.BlockSpec(memory_space=pltpu.VMEM)
    tbits = log2(nt)
    early_shape = sds(nother, nloc - 1, Ry, model, dtype=bf16)
    late_shape = sds(nother, Ry, model, dtype=bf16)
    fw, fb, small, shared, last, cy, ct, cty, ly, lt, lty = pl.pallas_call(
        partial(tail_kernel, own, ncore, ny, ndp),
        in_specs=[vm] * 7 + [any_spec] * 2,
        out_specs=[any_spec] * 2 + [vm] * 3 + [any_spec] * 6,
        out_shape=[
            sds(model, own + L, dtype=bf16),
            sds(model, 256, dtype=bc_type),
            sds(16, own),
            sds(8, model),
            sds(Ry, model, dtype=bf16),
            early_shape,
            sds(nloc - 1, Ry, model, dtype=bf16),
            early_shape,
            late_shape,
            sds(Ry, model, dtype=bf16),
            late_shape,
        ],
        scratch_shapes=[
            pltpu.VMEM((nother, Ry, model), bf16),
            pltpu.VMEM((Ry, model), bf16),
            pltpu.VMEM((16, own), f32),
            dma((2,)),
            dma((2, nother)),
            dma((2, 2 * ny)),
            dma((2, 2 * ny)),
            dma((1,)),
        ]
        + Halving.scratch(model // 2, own + L, nbits, bf16)
        + Halving.scratch(model // 2, own + L, nbits, bf16)
        + Halving.scratch(model, 256, nbits + tbits, bc_type)
        + Doubling.scratch(nbits, 16, own)
        + Doubling.scratch(nbits + tbits, 8, model),
        compiler_params=pltpu.CompilerParams(collective_id=3, has_side_effects=True),
        name="tail",
    )(gw2, gbcw, small, other, shared, dh, gain, corr, x4)

    pieces = ncore * ny
    where = jnp.stack([core, yy]).astype(jnp.int32)

    def out_index(k, i, s):
        return ((s[0] ^ (k // ny)) * nloc + i, (s[1] - k % ny + ny) % ny, 0, 0)

    def piece_spec(k, count):
        def index(j, i, s):
            i = jnp.minimum(i, count - 1)
            return (jnp.where(j == k, i, jnp.where(j > k, count - 1, 0)), 0, 0)

        return pl.BlockSpec((None, Ry, model), index)

    placed_spec = pl.BlockSpec((None, None, Ry, model), out_index)

    def all_pieces(mine, toy, tot, toty):
        got = [mine] + [toy[d] for d in range(ny - 1)]
        if ncore == 2:
            got = got + [tot] + [toty[d] for d in range(ny - 1)]
        return got

    early = all_pieces(corr, cy, ct, cty)
    late = all_pieces(last[None], ly[:, None], lt[None], lty[:, None])
    outs = all_pieces(bo, boy, bot, boty)
    grad_input, block_output = call(
        partial(finish_kernel, pieces, nloc),
        (pieces, nloc),
        [placed_spec]
        + [piece_spec(k, nloc - 1) for k in range(pieces)]
        + [piece_spec(k, 1) for k in range(pieces)]
        + [piece_spec(k, nloc) for k in range(pieces)],
        [placed_spec, placed_spec],
        [sds(nseq, ny, Ry, model), sds(nseq, ny, Ry, model, dtype=bf16)],
        [],
        "finish",
        0,
        12 * tok * model,
    )(where, g4, *early, *late, *outs)

    gzx, gwo = pl.pallas_call(
        partial(unpack_kernel, own),
        grid=(model // L,),
        in_specs=[
            pl.BlockSpec((L, own), lambda d: (d, 0)),
            pl.BlockSpec((L, own), lambda d: (d, 0)),
            pl.BlockSpec((L, own + L), lambda d: (d, 0)),
        ],
        out_specs=[
            pl.BlockSpec((L, 2, own), lambda d: (d, 0, 0)),
            pl.BlockSpec((own, L), lambda d: (0, d)),
        ],
        out_shape=[sds(model, 2, own), sds(own, model)],
        name="unpack",
    )(fz, fo, fw)
    tail = fw[:, own : own + heads].astype(f32)
    return (
        block_output.reshape(tok, model),
        grad_input.reshape(tok, model),
        shared[0],
        gzx,
        fb.astype(f32),
        tail,
        small[0:4],
        small[4],
        shared[1:5, 0:256],
        shared[5, 0:256],
        small[7, :heads],
        small[8, :heads],
        jnp.sum(small[5].reshape(heads, HEAD), axis=1),
        small[6],
        gwo,
    )


def solution(mesh):
    placed = (
        P("dp", None),
        P(),
        P(None, None, "tensor"),
        P(),
        P(None, "tensor"),
        P(None, "tensor"),
        P("tensor"),
        P(),
        P(),
        P("tensor"),
        P("tensor"),
        P("tensor"),
        P("tensor"),
        P("tensor", None),
        P("dp", None),
    )
    return jax.shard_map(
        body,
        mesh=mesh,
        in_specs=placed,
        out_specs=(
            P("dp", None),
            P("dp", None),
            P(),
            P(None, None, "tensor"),
            P(),
            P(None, "tensor"),
            P(None, "tensor"),
            P("tensor"),
            P(),
            P(),
            P("tensor"),
            P("tensor"),
            P("tensor"),
            P("tensor"),
            P("tensor", None),
        ),
        check_vma=False,
    )
```

```python
from functools import partial

import jax
import jax.numpy as jnp
from jax import lax
from jax.experimental import pallas as pl
from jax.experimental.pallas import tpu as pltpu
from jax.sharding import PartitionSpec as P

SEQ_LEN = 512
L = 128
HEAD = 64
PAD = 8
epsilon = 1e-05
f32 = jnp.float32
bf16 = jnp.bfloat16
HI = lax.Precision.HIGHEST
MESH = pl.DeviceIdType.MESH


def nn(a, b):
    return lax.dot_general(a, b, (((1,), (0,)), ((), ())), preferred_element_type=f32)


def nt(a, b):
    return lax.dot_general(a, b, (((1,), (1,)), ((), ())), preferred_element_type=f32)


def tn(a, b):
    return lax.dot_general(a, b, (((0,), (0,)), ((), ())), preferred_element_type=f32)


def exact(a, b):
    return lax.dot_general(
        a, b, (((1,), (0,)), ((), ())), precision=HI, preferred_element_type=f32
    )


def sigmoid(v):
    return 0.5 + 0.5 * jnp.tanh(0.5 * v)


def softplus(v):
    u = jnp.exp(-jnp.abs(v))
    return jnp.maximum(v, 0.0) + jnp.where(u < 1e-3, u - 0.5 * u * u, jnp.log(1.0 + u))


def fold_rows(v):
    return jnp.sum(v.reshape(v.shape[0] // 8, 8, v.shape[1]), axis=0)


def lane_iota(shape):
    return lax.broadcasted_iota(jnp.int32, shape, 1)


def row_iota(shape):
    return lax.broadcasted_iota(jnp.int32, shape, 0)


def conv(window, taps, bias):
    total = bias
    for k in range(4):
        total = total + window[PAD - 3 + k : PAD - 3 + k + L] * taps[k : k + 1]
    return total


def spread(cols, head):
    return jnp.broadcast_to(cols[:, head : head + 1], (L, L))


def span_decay(dtl, hp):
    pre = dtl + hp[0:1]
    dt = softplus(pre)
    ltri = (row_iota((L, L)) >= lane_iota((L, L))).astype(f32)
    cum = exact(ltri, dt * hp[1:2])
    return pre, dt, cum, cum.T


def remote(src, dst, send, recv, where):
    return pltpu.make_async_remote_copy(
        src_ref=src,
        dst_ref=dst,
        send_sem=send,
        recv_sem=recv,
        device_id=where,
        device_id_type=MESH,
    )


def greet(peers):
    barrier = pltpu.get_barrier_semaphore()
    for peer in peers:
        pl.semaphore_signal(barrier, inc=1, device_id=peer, device_id_type=MESH)
    pl.semaphore_wait(barrier, len(peers))


def bit_peers(axis, base, first, count):
    me = lax.axis_index(axis)
    peers, bits = [], []
    for k in range(count):
        step = base * 2**k
        bit = lax.rem(me // step, 2)
        peers.append({axis: me + step * (1 - 2 * bit)})
        bits.append(bit)
    return peers, bits


class Halving:
    def __init__(self, links, rows, src, work, recvs, full, sems):
        self.links, self.rows = links, rows
        self.src, self.work, self.recvs, self.full, self.sems = src, work, recvs, full, sems
        self.n = len(links)
        offs, size = [0], rows
        for _, bit in links:
            size //= 2
            offs.append(offs[-1] + bit * size)
        self.offs = offs

    def size(self, k):
        return self.rows >> k

    def at(self, off, size):
        return pl.ds(pl.multiple_of(off, size), size)

    def scatter(self, k):
        peer, bit = self.links[k]
        half = self.size(k + 1)
        off = self.offs[k] + (1 - bit) * half
        if k == 0:
            src = self.src.at[self.at(off, half)]
        else:
            src = self.work.at[self.at(off - self.offs[1], half)]
        return remote(src, self.recvs[k], self.sems.at[0, k], self.sems.at[1, k], peer)

    def fold(self, k):
        self.scatter(k).wait()
        half = self.size(k + 1)
        step = min(half, 64)
        keep = self.offs[k + 1]

        @pl.loop(0, half // step)
        def _(i):
            off = i * step
            rows = pl.ds(pl.multiple_of(off, step), step)
            near = pl.ds(pl.multiple_of(keep - self.offs[1] + off, step), step)
            if k == 0:
                mine = self.src[pl.ds(pl.multiple_of(keep + off, step), step), :]
            else:
                mine = self.work[near, :]
            total = mine.astype(f32) + self.recvs[k][rows, :].astype(f32)
            self.work[near, :] = total.astype(self.work.dtype)

    def own_copy(self):
        last = self.size(self.n)
        return pltpu.make_async_copy(
            self.work.at[self.at(self.offs[self.n] - self.offs[1], last)],
            self.full.at[self.at(self.offs[self.n], last)],
            self.sems.at[0, 2 * self.n],
        )

    def gather(self, k):
        peer, _ = self.links[k]
        rows = self.at(self.offs[k + 1], self.size(k + 1))
        sems = self.sems
        return remote(
            self.full.at[rows],
            self.full.at[rows],
            sems.at[0, self.n + k],
            sems.at[1, self.n + k],
            peer,
        )

    def close(self, j):
        n = self.n
        if 1 <= j <= n:
            self.fold(j - 1)
        elif j > n:
            self.gather(2 * n - j).wait()

    def begin(self, j):
        n = self.n
        if j < n:
            self.scatter(j).start()
            return
        if j == n:
            self.own_copy().start()
            self.own_copy().wait()
        if j < 2 * n:
            self.gather(2 * n - 1 - j).start()

    @staticmethod
    def scratch(rows, cols, n, dtype):
        recvs = [pltpu.VMEM((rows >> (k + 1), cols), dtype) for k in range(n)]
        return [pltpu.VMEM((rows // 2, cols), dtype)] + recvs + [
            pltpu.SemaphoreType.DMA((2, 2 * n + 1))
        ]


class Doubling:
    def __init__(self, peers, acc, recv, sems):
        self.peers, self.acc, self.recv, self.sems = peers, acc, recv, sems

    def copy(self, k):
        return remote(
            self.acc.at[k],
            self.recv.at[k],
            self.sems.at[0, k],
            self.sems.at[1, k],
            self.peers[k],
        )

    def close(self, j):
        if j > 0:
            self.copy(j - 1).wait()
            self.acc[j] = self.acc[j - 1] + self.recv[j - 1]

    def begin(self, j):
        if j < len(self.peers):
            self.copy(j).start()

    @staticmethod
    def scratch(n, rows, cols):
        return [
            pltpu.VMEM((n + 1, rows, cols), f32),
            pltpu.VMEM((n, rows, cols), f32),
            pltpu.SemaphoreType.DMA((2, n)),
        ]


def correction(x, dh, gain):
    v = x.astype(f32)
    r = lax.rsqrt(jnp.mean(v * v, axis=1, keepdims=True) + epsilon)
    normed = v * r
    dn = dh * gain
    return r * (dn - normed * jnp.mean(dn * normed, axis=1, keepdims=True))


def places(ncore, ny):
    spot = lax.axis_index("tensor")
    core, yy = lax.rem(spot, ncore), spot // ncore
    ys = [lax.rem(yy + d, ny) for d in range(1, ny)]
    peers = [{"tensor": v * ncore + core} for v in ys]
    return core, yy, {"tensor": spot + 1 - 2 * core}, ys, peers


def log2(n):
    return n.bit_length() - 1


def forward_kernel(
    own,
    heads,
    ncore,
    ny,
    inner_total,
    nloc,
    _seq,
    x_ref,
    g_ref,
    gain_ref,
    wz_ref,
    wx_ref,
    wbc_ref,
    wdt_ref,
    wo_ref,
    sm_ref,
    bcp_ref,
    x4_ref,
    hid_ref,
    z_ref,
    xl_ref,
    bcl_ref,
    dtl_ref,
    u_ref,
    y_ref,
    sin_ref,
    st_ref,
    stot_ref,
    po_ref,
    bo_ref,
    prm_ref,
    hp_ref,
    wdt_out,
    wz_out,
    wx_out,
    q_scr,
    bca_scr,
    s_scr,
    cs_scr,
    xs_scr,
    wz_in,
    wx_in,
    wo_in,
    wdt_in,
    sm_in,
    po_scr,
    po_in,
    st_in,
    x_own,
    w_sems,
    po_sems,
    st_sems,
    local,
):
    rows_all = x_ref.shape[0]
    model = x_ref.shape[1]
    width = own * ncore
    pairs = width // L
    Ry = rows_all // ny
    here = pl.program_id(0)
    core, yy, twin, ys, peers = places(ncore, ny)

    def weight_copies():
        both = ((sm_ref, sm_in), (wdt_ref, wdt_in), (wz_ref, wz_in), (wx_ref, wx_in), (wo_ref, wo_in))
        return [
            remote(src, dst, w_sems.at[0, k], w_sems.at[1, k], twin)
            for k, (src, dst) in enumerate(both)
        ]

    def weight_stores():
        return [
            pltpu.make_async_copy(wz_in, wz_out, local.at[1]),
            pltpu.make_async_copy(wx_in, wx_out, local.at[2]),
        ]

    def row_copies():
        last = here - 1
        return [
            remote(
                st_ref.at[last],
                st_in.at[last, d],
                st_sems.at[0, last, d],
                st_sems.at[1, last, d],
                peers[d],
            )
            for d in range(ny - 1)
        ] + [
            remote(
                po_scr.at[pl.ds(pl.multiple_of(ys[d] * Ry, Ry), Ry)],
                po_in.at[last, d],
                po_sems.at[0, last, d],
                po_sems.at[1, last, d],
                peers[d],
            )
            for d in range(ny - 1)
        ]

    def x_copy():
        return pltpu.make_async_copy(x4_ref.at[core * nloc + here - 1, yy], x_own, local.at[0])

    @pl.when(here == 0)
    def _():
        greet(peers + ([twin] if ncore == 2 else []))
        if ncore == 2:
            for copy in weight_copies():
                copy.start()

    @pl.when(here > 0)
    def _():
        for copy in row_copies():
            copy.start()
        x_copy().start()

    @pl.loop(0, rows_all // 32)
    def _(i):
        rows = pl.ds(pl.multiple_of(i * 32, 32), 32)
        v = x_ref[rows, :].astype(f32)
        r = lax.rsqrt(jnp.mean(v * v, axis=1, keepdims=True) + epsilon)
        hid_ref[rows, :] = (v * r * gain_ref[...]).astype(bf16)

    xl_ref[0:PAD, :] = jnp.zeros((PAD, width), f32)
    bcl_ref[0:PAD, :] = jnp.zeros((PAD, 256), f32)

    def project(wz, wx, wo, base):
        @pl.loop(0, own // 256)
        def _(j):
            src = pl.ds(pl.multiple_of(j * 256, 256), 256)
            cols = pl.ds(pl.multiple_of(base + j * 256, 256), 256)
            z_ref[:, cols] = nn(hid_ref[...], wz[:, src])
            xl_ref[PAD : PAD + rows_all, cols] = nn(hid_ref[...], wx[:, src])
            u_ref[:, cols] = nt(g_ref[...], wo[src, :])

    project(wz_ref, wx_ref, wo_ref, 0)
    bcl_ref[PAD : PAD + rows_all, :] = nn(hid_ref[...], wbc_ref[...])

    @pl.when(here == 0)
    def _():
        prm_ref[:, 0:own] = sm_ref[0:8, :]
        hp_ref[...] = sm_ref[8:16, 0:L]
        wdt_out[...] = wdt_ref[...]
        if ncore == 2:
            for copy in weight_copies():
                copy.wait()
            for copy in weight_stores():
                copy.start()
            prm_ref[:, own : 2 * own] = sm_in[0:8, :]
            hp_ref[...] += pltpu.roll(sm_in[8:16, 0:L], heads, axis=1)
            theirs = pltpu.roll(wdt_in[...].astype(f32), heads, axis=1)
            wdt_out[...] = (wdt_ref[...].astype(f32) + theirs).astype(bf16)

    if ncore == 2:
        project(wz_in, wx_in, wo_in, own)
    dtl_ref[...] = nn(hid_ref[...], wdt_out[...])

    @pl.loop(0, rows_all // L)
    def _(c):
        t0 = pl.multiple_of(c * L, L)
        for half in range(2):
            lanes = slice(half * L, half * L + L)
            v = conv(bcl_ref[pl.ds(t0, L + PAD), lanes], bcp_ref[0:4, lanes], bcp_ref[4:5, lanes])
            bca_scr[pl.ds(t0, L), lanes] = (v * sigmoid(v)).astype(bf16)

    s_scr[...] = jnp.zeros_like(s_scr)
    hp = hp_ref[...]

    @pl.loop(0, rows_all // L)
    def _(c):
        t0 = pl.multiple_of(c * L, L)
        rows = pl.ds(t0, L)
        lo = lane_iota((L, L)) < HEAD
        mlo = (lane_iota((1, L)) < HEAD).astype(bf16)
        mhi = (lane_iota((1, L)) >= HEAD).astype(bf16)
        tri = row_iota((L, L)) >= lane_iota((L, L))
        _, dt, cum, cum_t = span_decay(dtl_ref[rows, :], hp)
        bm = bca_scr[rows, 0:L]
        cm = bca_scr[rows, L : 2 * L]
        both = nt(cm, bm)
        sb = s_scr[...].astype(bf16)
        sin_ref[c] = sb
        cs_scr[...] = nn(cm, sb)
        squares = jnp.zeros((L, L), f32)
        inner = jnp.zeros((L, L), f32)
        for p in range(pairs):
            lanes = slice(p * L, p * L + L)
            xc = conv(xl_ref[pl.ds(t0, L + PAD), lanes], prm_ref[0:4, lanes], prm_ref[4:5, lanes])
            x = xc * sigmoid(xc)
            h0, h1 = 2 * p, 2 * p + 1
            a0, a1 = spread(cum, h0), spread(cum, h1)
            ap = jnp.where(lo, a0, a1)
            k0 = both * jnp.exp(jnp.where(tri, a0 - cum_t[h0 : h0 + 1], -jnp.inf))
            k1 = both * jnp.exp(jnp.where(tri, a1 - cum_t[h1 : h1 + 1], -jnp.inf))
            xdt = x * jnp.where(lo, spread(dt, h0), spread(dt, h1))
            xb = xdt.astype(bf16)
            fin = ap[L - 1 : L]
            within = nn(
                jnp.concatenate([k0.astype(bf16), k1.astype(bf16)], axis=1),
                jnp.concatenate([xb * mlo, xb * mhi], axis=0),
            )
            y = within + jnp.exp(ap) * cs_scr[:, lanes] + prm_ref[5:6, lanes] * x
            xs_scr[:, lanes] = (xdt * jnp.exp(fin - ap)).astype(bf16)
            s_scr[:, lanes] = s_scr[:, lanes] * jnp.exp(fin)
            y_ref[rows, lanes] = y
            z = z_ref[rows, lanes]
            gated = y * (z * sigmoid(z))
            q = gated * prm_ref[6:7, lanes]
            q_scr[rows, lanes] = q.astype(bf16)
            squares = squares + gated * gated
            inner = inner + u_ref[rows, lanes] * q
        s_scr[...] += nn(bm.T, xs_scr[...])
        s0 = jnp.sum(squares, axis=1, keepdims=True)
        s1 = jnp.sum(inner, axis=1, keepdims=True)
        lane = lane_iota((L, L))
        stat = jnp.where(lane == 0, s0, jnp.where(lane == 1, s1, 0.0))
        st_ref[here, :, rows] = stat.T[0:2]

    @pl.when(here > 0)
    def _():
        for copy in row_copies():
            copy.wait()
        x_copy().wait()
        total = st_ref[here - 1]
        for d in range(ny - 1):
            total = total + st_in[here - 1, d]
        stot_ref[here - 1] = total
        parts = [po_in.at[here - 1, d] for d in range(ny - 1)]
        mine = po_scr.at[pl.ds(pl.multiple_of(yy * Ry, Ry), Ry)]
        block_out(inner_total, stot_ref.at[here - 1], yy, mine, parts, x_own, bo_ref.at[here - 1])

    @pl.loop(0, model // 256)
    def _(j):
        cols = pl.ds(pl.multiple_of(j * 256, 256), 256)
        po = nn(q_scr[:, 0:own], wo_ref[:, cols])
        if ncore == 2:
            po = po + nn(q_scr[:, own : 2 * own], wo_in[:, cols])
        po_scr[:, cols] = po.astype(bf16)

    @pl.when(here == nloc - 1)
    def _():
        po_ref[...] = po_scr[...]
        if ncore == 2:
            for copy in weight_stores():
                copy.wait()


def block_out(inner_total, stot, yy, mine, parts, x_own, bo):
    Ry, model = x_own.shape
    for h in range(Ry // L):
        lanes = pl.ds(pl.multiple_of(yy * Ry + h * L, L), L)
        r_row = lax.rsqrt(stot[0:1, lanes] / inner_total + epsilon)
        r = jnp.broadcast_to(r_row, (8, L)).T[:, 0:1]

        @pl.loop(0, model // L)
        def _(m, h=h, r=r):
            cols = pl.ds(pl.multiple_of(m * L, L), L)
            rows = slice(h * L, h * L + L)
            total = mine[rows, cols].astype(f32)
            for part in parts:
                total = total + part[rows, cols].astype(f32)
            bo[rows, cols] = (x_own[rows, cols].astype(f32) + r * total).astype(bf16)


def gate_kernel(
    width,
    own,
    inner_total,
    ncore,
    ny,
    _seq,
    st_ref,
    stin_ref,
    g_ref,
    hid_ref,
    z_ref,
    y_ref,
    u_ref,
    prm_ref,
    po_ref,
    bo01_ref,
    x_ref,
    dz_ref,
    dy_ref,
    gz_ref,
    go_ref,
    ggg_ref,
    bo_ref,
    q_scr,
    sc_scr,
    acc_scr,
    stot_ref,
    st_in,
    send_scr,
    recv_scr,
    po_in,
    x_own,
    st_sems,
    core_send,
    core_recv,
    po_sems,
    local,
):
    rows_all = z_ref.shape[0]
    model = g_ref.shape[1]
    pairs = width // L
    here = pl.program_id(0)
    core, yy, twin, ys, peers = places(ncore, ny)
    nloc, Ry, _ = bo_ref.shape
    last = nloc - 1

    def row_copies():
        return [
            remote(st_ref.at[last], st_in.at[d], st_sems.at[0, d], st_sems.at[1, d], peers[d])
            for d in range(ny - 1)
        ]

    def po_copies():
        return [
            remote(
                po_ref.at[pl.ds(pl.multiple_of(ys[d] * Ry, Ry), Ry)],
                po_in.at[d],
                po_sems.at[0, d],
                po_sems.at[1, d],
                peers[d],
            )
            for d in range(ny - 1)
        ]

    def x_copy():
        return pltpu.make_async_copy(x_ref.at[core * nloc + last, yy], x_own, local.at[0])

    @pl.when(here == 0)
    def _():
        greet(peers + ([twin] if ncore == 2 else []))
        for copy in row_copies() + po_copies() + [x_copy()]:
            copy.start()
        stot_ref[...] = stin_ref[...]
        for i in range(last):
            bo_ref[i] = bo01_ref[i]
        acc_scr[...] = jnp.zeros_like(acc_scr)
        ggg_ref[...] = jnp.zeros_like(ggg_ref)

    @pl.when(here == last)
    def _():
        for copy in row_copies():
            copy.wait()
        total = st_ref[last]
        for d in range(ny - 1):
            total = total + st_in[d]
        stot_ref[last] = total

    @pl.loop(0, rows_all // L)
    def _(c):
        rows = pl.ds(pl.multiple_of(c * L, L), L)
        st = stot_ref[here, :, rows]
        r_row = lax.rsqrt(st[0:1] / inner_total + epsilon)
        c_row = r_row * r_row * r_row * (st[1:2] / inner_total)
        cols8 = jnp.concatenate([r_row, c_row, jnp.zeros((6, L), f32)], axis=0).T
        r = jnp.broadcast_to(cols8[:, 0:1], (L, L))
        c2 = jnp.broadcast_to(cols8[:, 1:2], (L, L))
        for m in range(model // L):
            lanes = slice(m * L, m * L + L)
            sc_scr[rows, lanes] = (g_ref[rows, lanes].astype(f32) * r).astype(bf16)
        for p in range(pairs):
            lanes = slice(p * L, p * L + L)
            gg = prm_ref[6:7, lanes]
            z = z_ref[rows, lanes]
            y = y_ref[rows, lanes]
            sg = sigmoid(z)
            silz = z * sg
            gated = y * silz
            q_scr[rows, lanes] = (gated * gg).astype(bf16)
            dq = r * u_ref[rows, lanes]
            ggg_ref[:, lanes] += fold_rows(dq * gated)
            dgated = dq * gg - c2 * gated
            dy_ref[rows, lanes] = (dgated * silz).astype(bf16)
            dz_ref[rows, lanes] = (dgated * y * (sg + silz * (1.0 - sg))).astype(bf16)

    @pl.loop(0, model // 256)
    def _(j):
        cols = pl.ds(pl.multiple_of(j * 256, 256), 256)
        acc_scr[cols, 0:width] += tn(hid_ref[:, cols], dz_ref[...])
        acc_scr[cols, width : 2 * width] += tn(sc_scr[:, cols], q_scr[...])

    @pl.when(here == pl.num_programs(0) - 1)
    def _():
        if ncore == 2:
            send_scr[:, 0:own] = acc_scr[:, own:width].astype(bf16)
            send_scr[:, own : 2 * own] = acc_scr[:, width + own : 2 * width].astype(bf16)
            copy = remote(send_scr, recv_scr, core_send, core_recv, twin)
            copy.start()
            copy.wait()
            theirs = recv_scr[...].astype(f32)
        else:
            theirs = jnp.zeros((model, 2 * own), f32)
        gz_ref[...] = (acc_scr[:, 0:own] + theirs[:, 0:own]).astype(bf16)
        mine = acc_scr[:, width : width + own] + theirs[:, own : 2 * own]
        go_ref[...] = mine.astype(bf16)
        for copy in po_copies() + [x_copy()]:
            copy.wait()
        parts = [po_in.at[d] for d in range(ny - 1)]
        mine = po_ref.at[pl.ds(pl.multiple_of(yy * Ry, Ry), Ry)]
        block_out(inner_total, stot_ref.at[last], yy, mine, parts, x_own, bo_ref.at[last])


def scan_kernel(
    width,
    own,
    heads,
    ncore,
    ny,
    ndp,
    nloc_static,
    _seq,
    hid_ref,
    dz_ref,
    dy_ref,
    xl_ref,
    bcl_ref,
    dtl_ref,
    sin_ref,
    wz_ref,
    wzo_ref,
    wx_ref,
    wxo_ref,
    wbc_ref,
    wdt_ref,
    prm_ref,
    bcp_ref,
    hp_ref,
    ggg_ref,
    gain_ref,
    gz_ref,
    go_ref,
    bo_ref,
    x_ref,
    dh_ref,
    gw_ref,
    gbcw_ref,
    small_ref,
    other_ref,
    shared_ref,
    corr_ref,
    fz_ref,
    fo_ref,
    boy_ref,
    bot_ref,
    boty_ref,
    cy_ref,
    ct_ref,
    cty_ref,
    d_scr,
    bcc_scr,
    bca_scr,
    ds_scr,
    dsb_scr,
    cs_scr,
    bds_scr,
    xs_scr,
    dye_scr,
    nx_scr,
    nbc_scr,
    gx_ref,
    gbc_ref,
    gdt_ref,
    gpre_ref,
    acc_scr,
    send_scr,
    recv_scr,
    dh_scr,
    dh_in,
    x_own,
    core_send,
    core_recv,
    y_sems,
    bo_sems,
    c_sems,
    local,
    *machine,
):
    rows_all = dz_ref.shape[0]
    model = hid_ref.shape[1]
    pairs = width // L
    spans = rows_all // L
    Ry = rows_all // ny
    seq, back = pl.program_id(0), pl.program_id(1)
    step = seq * spans + back
    core, yy, twin, ys, peers = places(ncore, ny)
    nbits = log2(ndp)
    dp_peers, dp_bits = bit_peers("dp", 1, 0, nbits)
    links = list(zip(dp_peers, dp_bits))
    swapped = [links[1], links[0]] + links[2:] if nbits > 1 else links
    half = len(machine) // 2
    mz, mo = machine[:half], machine[half:]
    jobs = [
        Halving(links, model, gz_ref, mz[0], mz[1:-1], fz_ref, mz[-1]),
        Halving(swapped, model, go_ref, mo[0], mo[1:-1], fo_ref, mo[-1]),
    ]
    last_step = nloc_static * spans - 1

    def bo_first():
        out = [
            remote(bo_ref, boy_ref.at[d], bo_sems.at[0, d], bo_sems.at[1, d], peers[d])
            for d in range(ny - 1)
        ]
        if ncore == 2:
            out.append(remote(bo_ref, bot_ref, bo_sems.at[0, ny - 1], bo_sems.at[1, ny - 1], twin))
        return out

    def bo_second():
        if ncore != 2:
            return []
        return [
            remote(boy_ref.at[d], boty_ref.at[d], bo_sems.at[0, ny + d], bo_sems.at[1, ny + d], twin)
            for d in range(ny - 1)
        ]

    def dh_copies():
        return [
            remote(
                dh_scr.at[pl.ds(pl.multiple_of(ys[d] * Ry, Ry), Ry)],
                dh_in.at[seq - 1, d],
                y_sems.at[0, seq - 1, d],
                y_sems.at[1, seq - 1, d],
                peers[d],
            )
            for d in range(ny - 1)
        ]

    def x_copy():
        return pltpu.make_async_copy(x_ref.at[core * nloc_static + seq - 1, yy], x_own, local.at[0])

    @pl.when(step == 0)
    def _():
        greet(peers + dp_peers + ([twin] if ncore == 2 else []))
        for copy in bo_first():
            copy.start()
        acc_scr[...] = jnp.zeros_like(acc_scr)
        gx_ref[...] = jnp.zeros_like(gx_ref)
        gbc_ref[...] = jnp.zeros_like(gbc_ref)
        gdt_ref[...] = jnp.zeros_like(gdt_ref)
        gpre_ref[...] = jnp.zeros_like(gpre_ref)

    spans_of = ([2] + [1] * (nbits - 2) + [2])[:nbits]
    spans_of = spans_of + spans_of[::-1]
    for j in range(2 * nbits + 1):

        @pl.when(step == sum(spans_of[:j]) * last_step // sum(spans_of))
        def _(j=j):
            for job in jobs:
                job.close(j)
            for job in jobs:
                job.begin(j)

    @pl.when(step == last_step // 2)
    def _():
        for copy in bo_first():
            copy.wait()
        for copy in bo_second():
            copy.start()

    def corr_first(i):
        out = [
            remote(corr_ref.at[i], cy_ref.at[d, i], c_sems.at[0, i, d], c_sems.at[1, i, d], peers[d])
            for d in range(ny - 1)
        ]
        if ncore == 2:
            d = ny - 1
            out.append(remote(corr_ref.at[i], ct_ref.at[i], c_sems.at[0, i, d], c_sems.at[1, i, d], twin))
        return out

    def corr_second(i):
        if ncore != 2:
            return []
        return [
            remote(
                cy_ref.at[d, i],
                cty_ref.at[d, i],
                c_sems.at[0, i, ny + d],
                c_sems.at[1, i, ny + d],
                twin,
            )
            for d in range(ny - 1)
        ]

    for i in range(nloc_static - 2):

        @pl.when(step == (i + 2) * spans - 1)
        def _(i=i):
            for copy in corr_first(i):
                copy.start()

        @pl.when(step == (i + 2) * spans + 2)
        def _(i=i):
            for copy in corr_first(i):
                copy.wait()
            for copy in corr_second(i):
                copy.start()

    @pl.when(jnp.logical_and(seq > 0, back == 0))
    def _():
        for copy in dh_copies():
            copy.start()
        x_copy().start()

    @pl.when(jnp.logical_and(seq > 0, back == spans - 2))
    def _():
        for copy in dh_copies():
            copy.wait()
        x_copy().wait()

        @pl.loop(0, Ry // 32)
        def _(i):
            rows = pl.ds(pl.multiple_of(i * 32, 32), 32)
            mine = pl.ds(pl.multiple_of(yy * Ry + i * 32, 32), 32)
            dh = dh_scr[mine, :].astype(f32)
            for d in range(ny - 1):
                dh = dh + dh_in[seq - 1, d, rows, :].astype(f32)
            corr_ref[seq - 1, rows, :] = correction(x_own[rows, :], dh, gain_ref[...]).astype(bf16)

    hp = hp_ref[...]

    @pl.when(back == 0)
    def _():
        ds_scr[...] = jnp.zeros_like(ds_scr)
        nx_scr[...] = jnp.zeros_like(nx_scr)
        nbc_scr[...] = jnp.zeros_like(nbc_scr)

        @pl.loop(0, spans)
        def _(c):
            t0 = pl.multiple_of(c * L, L)
            for half in range(2):
                lanes = slice(half * L, half * L + L)
                v = conv(bcl_ref[pl.ds(t0, L + PAD), lanes], bcp_ref[0:4, lanes], bcp_ref[4:5, lanes])
                bcc_scr[pl.ds(t0, L), lanes] = v
                bca_scr[pl.ds(t0, L), lanes] = (v * sigmoid(v)).astype(bf16)

    def one_chunk():
        c = spans - 1 - back
        t0 = pl.multiple_of(c * L, L)
        rows = pl.ds(t0, L)
        lane = lane_iota((L, L))
        lo = lane < HEAD
        mlo = (lane_iota((1, L)) < HEAD).astype(bf16)
        mhi = (lane_iota((1, L)) >= HEAD).astype(bf16)
        tri = row_iota((L, L)) >= lane
        pre, dt, cum, cum_t = span_decay(dtl_ref[rows, :], hp)
        bm = bca_scr[rows, 0:L]
        cm = bca_scr[rows, L : 2 * L]
        both = nt(cm, bm)
        sb = sin_ref[c]
        dsb_scr[...] = ds_scr[...].astype(bf16)
        cs_scr[...] = nn(cm, sb)
        bds_scr[...] = nn(bm, dsb_scr[...])
        d_both = jnp.zeros((L, L), f32)
        d_cum = jnp.zeros((L, L), f32)
        d_dt = jnp.zeros((L, L), f32)
        d_far = jnp.zeros((L, L), f32)
        d_end = jnp.zeros((1, L), f32)
        for p in range(pairs):
            lanes = slice(p * L, p * L + L)
            window = xl_ref[pl.ds(t0, L + PAD), lanes]
            shifted = [window[PAD - 3 + k : PAD - 3 + k + L] for k in range(4)]
            taps = prm_ref[0:4, lanes]
            xc = prm_ref[4:5, lanes]
            for k in range(4):
                xc = xc + shifted[k] * taps[k : k + 1]
            sg = sigmoid(xc)
            x = xc * sg
            h0, h1 = 2 * p, 2 * p + 1
            a0, a1 = spread(cum, h0), spread(cum, h1)
            ap = jnp.where(lo, a0, a1)
            e0 = jnp.exp(jnp.where(tri, a0 - cum_t[h0 : h0 + 1], -jnp.inf))
            e1 = jnp.exp(jnp.where(tri, a1 - cum_t[h1 : h1 + 1], -jnp.inf))
            k0 = (both * e0).astype(bf16)
            k1 = (both * e1).astype(bf16)
            dtp = jnp.where(lo, spread(dt, h0), spread(dt, h1))
            xdt = x * dtp
            xb = xdt.astype(bf16)
            bdx = jnp.concatenate([xb * mlo, xb * mhi], axis=0)
            ecum = jnp.exp(ap)
            fin = ap[L - 1 : L]
            sd = jnp.exp(fin - ap)
            y = nn(jnp.concatenate([k0, k1], axis=1), bdx) + ecum * cs_scr[:, lanes]
            dyb = dy_ref[rows, lanes]
            dy = dyb.astype(f32)
            dk = nt(dyb, bdx)
            d_both = d_both + dk[:, 0:L] * e0 + dk[:, L : 2 * L] * e1
            bdy = jnp.concatenate([dyb * mlo, dyb * mhi], axis=0)
            near = tn(jnp.concatenate([k0, k1], axis=0), bdy)
            far = sd * bds_scr[:, lanes]
            dxdt = near + far
            v = dy * y - xb.astype(f32) * near
            u = dxdt * x
            w = xdt * far
            ends = jnp.exp(fin)
            through = ends * jnp.sum(sb[:, lanes].astype(f32) * ds_scr[:, lanes], axis=0, keepdims=True)
            for h, keep in ((h0, lo), (h1, jnp.logical_not(lo))):
                here = lane == h
                d_cum = jnp.where(here, jnp.sum(jnp.where(keep, v, 0.0), axis=1, keepdims=True), d_cum)
                d_dt = jnp.where(here, jnp.sum(jnp.where(keep, u, 0.0), axis=1, keepdims=True), d_dt)
                d_far = jnp.where(here, jnp.sum(jnp.where(keep, w, 0.0), axis=1, keepdims=True), d_far)
                whole = jnp.sum(jnp.where(keep[0:1], through, 0.0), axis=1, keepdims=True)
                d_end = jnp.where(here[0:1], whole, d_end)
            dx = dxdt * dtp + dy * prm_ref[5:6, lanes]
            dxc = dx * (sg + x * (1.0 - sg))
            for k in range(4):
                gx_ref[k, :, lanes] += fold_rows(dxc * shifted[k])
            gx_ref[4, :, lanes] += fold_rows(dxc)
            gx_ref[5, :, lanes] += fold_rows(dy * x)
            ext = jnp.concatenate([dxc, nx_scr[:, lanes]], axis=0)
            dxl = ext[0:L] * taps[3:4]
            for k in range(3):
                dxl = dxl + ext[3 - k : 3 - k + L] * taps[k : k + 1]
            nx_scr[:, lanes] = dxc[0:8]
            d_scr[rows, lanes] = dxl.astype(bf16)
            xs_scr[:, lanes] = (xdt * sd).astype(bf16)
            dye_scr[:, lanes] = (dy * ecum).astype(bf16)
            ds_scr[:, lanes] = ds_scr[:, lanes] * ends
        ds_scr[...] += nn(cm.T, dye_scr[...])
        utri = (row_iota((L, L)) <= lane).astype(f32)
        before = (row_iota((L, L)) > lane).astype(f32)
        d_a = exact(utri, d_cum) + exact(before, d_far) + d_end
        d_dt = d_dt + d_a * hp[1:2]
        d_pre = d_dt * sigmoid(pre)
        gdt_ref[0] += fold_rows(d_pre)
        gdt_ref[1] += fold_rows(d_a * dt * hp[1:2])
        d_scr[rows, width + 256 : width + 384] = d_pre.astype(bf16)
        dgb = d_both.astype(bf16)
        d_c = nt(dye_scr[...], sb) + nn(dgb, bm)
        d_b = nt(xs_scr[...], dsb_scr[...]) + nn(dgb.T, cm)
        for half, dv in ((0, d_b), (1, d_c)):
            lanes = slice(half * L, half * L + L)
            pre_act = bcc_scr[rows, lanes]
            sg = sigmoid(pre_act)
            dvc = dv * (sg + pre_act * sg * (1.0 - sg))
            window = bcl_ref[pl.ds(t0, L + PAD), lanes]
            for k in range(4):
                gbc_ref[k, :, lanes] += fold_rows(dvc * window[PAD - 3 + k : PAD - 3 + k + L])
            gbc_ref[4, :, lanes] += fold_rows(dvc)
            ext = jnp.concatenate([dvc, nbc_scr[:, lanes]], axis=0)
            dvl = ext[0:L] * bcp_ref[3:4, lanes]
            for k in range(3):
                dvl = dvl + ext[3 - k : 3 - k + L] * bcp_ref[k : k + 1, lanes]
            nbc_scr[:, lanes] = dvc[0:8]
            d_scr[rows, width + half * L : width + half * L + L] = dvl.astype(bf16)

    one_chunk()

    @pl.when(back == spans - 1)
    def _():
        @pl.loop(0, model // 256)
        def _(j):
            cols = pl.ds(pl.multiple_of(j * 256, 256), 256)
            dh = nt(dz_ref[:, 0:own], wz_ref[cols, :]) + nt(d_scr[:, 0:own], wx_ref[cols, :])
            if ncore == 2:
                dh = dh + nt(dz_ref[:, own:width], wzo_ref[cols, :])
                dh = dh + nt(d_scr[:, own:width], wxo_ref[cols, :])
            dh = dh + nt(d_scr[:, width : width + 256], wbc_ref[cols, :])
            dh = dh + nt(d_scr[:, width + 256 :], wdt_ref[cols, :])
            dh_scr[:, cols] = dh.astype(bf16)
            gpre_ref[:, cols] += fold_rows(dh * hid_ref[:, cols].astype(f32))
            acc_scr[cols, :] += tn(hid_ref[:, cols], d_scr[...])

    @pl.when(step == last_step)
    def _():
        tail = acc_scr[:, width + 256 : width + 384]
        if ncore == 2:
            send_scr[:, 0:own] = acc_scr[:, own:width].astype(bf16)
            send_scr[:, own : own + L] = tail.astype(bf16)
        dh_ref[...] = dh_scr[...]
        gbcw_ref[...] = acc_scr[:, width : width + 256].astype(gbcw_ref.dtype)
        if ncore == 2:
            copy = remote(send_scr, recv_scr, core_send, core_recv, twin)
            copy.start()
        rows = [jnp.sum(gx_ref[k], axis=0, keepdims=True) for k in range(6)]
        rows.append(jnp.sum(ggg_ref[...], axis=0, keepdims=True))
        dts = [jnp.sum(gdt_ref[k], axis=0, keepdims=True) for k in range(2)]
        small_ref[...] = jnp.zeros_like(small_ref)
        other_ref[...] = jnp.zeros_like(other_ref)
        for k in range(7):
            small_ref[k : k + 1, :] = rows[k][:, 0:own]
            if ncore == 2:
                other_ref[k : k + 1, :] = rows[k][:, own:width]
        for k in range(2):
            small_ref[7 + k : 8 + k, 0:L] = dts[k]
            if ncore == 2:
                moved = pltpu.roll(jnp.broadcast_to(dts[k], (8, L)), L - heads, axis=1)
                other_ref[7 + k : 8 + k, 0:L] = moved[0:1]
        shared_ref[...] = jnp.zeros_like(shared_ref)
        shared_ref[0:1, :] = jnp.sum(gpre_ref[...], axis=0, keepdims=True) / gain_ref[...]
        for k in range(5):
            shared_ref[k + 1 : k + 2, 0:256] = jnp.sum(gbc_ref[k], axis=0, keepdims=True)
        if ncore == 2:
            copy.wait()
            theirs = recv_scr[...].astype(f32)
            gw_ref[:, 0:own] = (acc_scr[:, 0:own] + theirs[:, 0:own]).astype(bf16)
            tail = tail + pltpu.roll(theirs[:, own : own + L], L - heads, axis=1)
        else:
            gw_ref[:, 0:own] = acc_scr[:, 0:own].astype(bf16)
        gw_ref[:, own : own + L] = tail.astype(bf16)
        for copy in bo_second():
            copy.wait()
        for i in range(nloc_static - 2):
            for copy in corr_second(i):
                copy.wait()


def tail_kernel(
    own,
    ncore,
    ny,
    ndp,
    gw_ref,
    gbcw_ref,
    small_ref,
    other_ref,
    shared_ref,
    dh_ref,
    gain_ref,
    corr_ref,
    x_ref,
    fw_ref,
    fb_ref,
    small_out,
    shared_out,
    last_ref,
    cy_ref,
    ct_ref,
    cty_ref,
    ly_ref,
    lt_ref,
    lty_ref,
    dh_in,
    x_own,
    small_in,
    core_sems,
    y_sems,
    c_sems,
    l_sems,
    local,
    *machine,
):
    model = gw_ref.shape[0]
    Ry, nloc = x_own.shape[0], corr_ref.shape[0] + 1
    core, yy, twin, ys, peers = places(ncore, ny)
    nbits = log2(ndp)
    dp_peers, dp_bits = bit_peers("dp", 1, 0, nbits)
    t_peers, t_bits = bit_peers("tensor", 1, 0, log2(ncore * ny))
    links = list(zip(dp_peers, dp_bits))
    swapped = [links[1], links[0]] + links[2:] if nbits > 1 else links
    t_links = list(zip(t_peers, t_bits))
    per = nbits + 2
    a, b = machine[:per], machine[per : 2 * per]
    per_bc = nbits + len(t_links) + 2
    c = machine[2 * per : 2 * per + per_bc]
    sm, sh = machine[2 * per + per_bc : 2 * per + per_bc + 3], machine[2 * per + per_bc + 3 :]
    mid = model // 2
    job_a = Halving(links, mid, gw_ref.at[0:mid], a[0], a[1:-1], fw_ref.at[0:mid], a[-1])
    job_b = Halving(swapped, mid, gw_ref.at[mid:model], b[0], b[1:-1], fw_ref.at[mid:model], b[-1])
    job_c = Halving(t_links + links, model, gbcw_ref, c[0], c[1:-1], fb_ref, c[-1])
    job_sm = Doubling(dp_peers, *sm)
    job_sh = Doubling(t_peers + dp_peers, *sh)

    def dh_copies():
        return [
            remote(
                dh_ref.at[pl.ds(pl.multiple_of(ys[d] * Ry, Ry), Ry)],
                dh_in.at[d],
                y_sems.at[0, d],
                y_sems.at[1, d],
                peers[d],
            )
            for d in range(ny - 1)
        ]

    def first(src, toy, tot, sems):
        out = [
            remote(src, toy.at[d], sems.at[0, d], sems.at[1, d], peers[d]) for d in range(ny - 1)
        ]
        if ncore == 2:
            out.append(remote(src, tot, sems.at[0, ny - 1], sems.at[1, ny - 1], twin))
        return out

    def second(toy, toty, sems):
        if ncore != 2:
            return []
        return [
            remote(toy.at[d], toty.at[d], sems.at[0, ny + d], sems.at[1, ny + d], twin)
            for d in range(ny - 1)
        ]

    early = (corr_ref.at[nloc - 2], cy_ref, ct_ref, c_sems)
    late = (last_ref, ly_ref, lt_ref, l_sems)
    x_copy = pltpu.make_async_copy(x_ref.at[core * nloc + nloc - 1, yy], x_own, local.at[0])
    others = peers + ([twin] if ncore == 2 else [])
    greet(others + dp_peers)
    x_copy.start()

    def turn(*pairs):
        for job, j in pairs:
            job.close(j)
        for job, j in pairs:
            job.begin(j)

    job_sh.acc[0] = shared_ref[...]
    turn((job_c, 0), (job_a, 0), (job_b, 0), (job_sh, 0))
    if ncore == 2:
        small_copy = remote(other_ref, small_in, core_sems.at[0], core_sems.at[1], twin)
        small_copy.start()
    turn((job_c, 1), (job_sh, 1))
    for copy in dh_copies():
        copy.start()
    for copy in first(*early):
        copy.start()
    if ncore == 2:
        small_copy.wait()
        job_sm.acc[0] = small_ref[...] + small_in[...]
    else:
        job_sm.acc[0] = small_ref[...]
    turn((job_sm, 0))
    steps = [
        (job_c, iter(range(2, 2 * job_c.n + 1))),
        (job_sm, iter(range(1, len(job_sm.peers) + 1))),
        (job_sh, iter(range(2, len(job_sh.peers) + 1))),
    ]

    def smaller():
        found = []
        for job, left in steps:
            j = next(left, None)
            if j is not None:
                found.append((job, j))
        return found

    turn((job_a, 1), (job_b, 1), *smaller())
    for copy in dh_copies():
        copy.wait()
    x_copy.wait()

    @pl.loop(0, Ry // 32)
    def _(i):
        rows = pl.ds(pl.multiple_of(i * 32, 32), 32)
        mine = pl.ds(pl.multiple_of(yy * Ry + i * 32, 32), 32)
        dh = dh_ref[mine, :].astype(f32)
        for d in range(ny - 1):
            dh = dh + dh_in[d, rows, :].astype(f32)
        last_ref[rows, :] = correction(x_own[rows, :], dh, gain_ref[...]).astype(bf16)

    turn(*smaller())
    for copy in first(*late):
        copy.start()
    for j in range(2, 2 * nbits + 1):
        turn((job_a, j), (job_b, j), *smaller())
    for copy in first(*early):
        copy.wait()
    for copy in second(cy_ref, cty_ref, c_sems):
        copy.start()
    for _ in range(2 * job_c.n):
        turn(*smaller())
    small_out[...] = job_sm.acc[len(job_sm.peers)]
    shared_out[...] = job_sh.acc[len(job_sh.peers)]
    for copy in first(*late):
        copy.wait()
    for copy in second(ly_ref, lty_ref, l_sems):
        copy.start()
    for copy in second(cy_ref, cty_ref, c_sems) + second(ly_ref, lty_ref, l_sems):
        copy.wait()


def finish_kernel(pieces, nloc, _idx, g_ref, *refs):
    gi_ref, bo_ref = refs[-2:]
    groups = [refs[n * pieces : (n + 1) * pieces] for n in range(4)]
    now = pl.program_id(1)
    for k in range(pieces):
        here = pl.program_id(0) == k

        @pl.when(here)
        def _(src=groups[3][k]):
            bo_ref[...] = src[...]

        for n in range(3):
            if n == 0:
                turn = now < nloc - 2
            else:
                turn = now == nloc - 3 + n

            @pl.when(jnp.logical_and(here, turn))
            def _(src=groups[n][k]):
                gi_ref[...] = g_ref[...].astype(f32) + src[...].astype(f32)


def unpack_kernel(own, gz_ref, go_ref, gw_ref, gzx_ref, gwo_ref):
    gzx_ref[:, 0, :] = gz_ref[...].astype(f32)
    gzx_ref[:, 1, :] = gw_ref[:, 0:own].astype(f32)
    v = go_ref[...].astype(f32)
    for k in range(own // L):
        gwo_ref[k * L : k * L + L, :] = v[:, k * L : k * L + L].T


def seq_spec(*shape):
    zeros = (0,) * len(shape)
    return pl.BlockSpec((None,) + shape, lambda i, s: (i,) + zeros)


def moved_spec(ncore, nloc, *shape):
    zeros = (0,) * len(shape)

    def index(i, s):
        return (i + lax.rem(lax.axis_index("tensor"), ncore) * nloc,) + zeros

    return pl.BlockSpec((None,) + shape, index)


def whole_spec(*shape):
    zeros = (0,) * len(shape)
    return pl.BlockSpec(shape, lambda *_: zeros, pipeline_mode=pl.Buffered(1))


def call(
    kernel, grid, in_specs, out_specs, out_shape, scratch, name, flops=0, moved=0, group=None
):
    return pl.pallas_call(
        kernel,
        grid_spec=pltpu.PrefetchScalarGridSpec(
            num_scalar_prefetch=1,
            grid=grid,
            in_specs=in_specs,
            out_specs=out_specs,
            scratch_shapes=scratch,
        ),
        out_shape=out_shape,
        cost_estimate=pl.CostEstimate(
            flops=int(flops), bytes_accessed=int(moved), transcendentals=0
        ),
        name=name,
        compiler_params=None
        if group is None
        else pltpu.CompilerParams(collective_id=group, has_side_effects=True),
    )


def sds(*shape, dtype=f32):
    return jax.ShapeDtypeStruct(shape, dtype)


def body(
    block_input,
    pre_gain,
    w_zx,
    w_bc,
    w_dt,
    conv_x_w,
    conv_x_b,
    conv_bc_w,
    conv_bc_b,
    dt_bias,
    a_log,
    d_skip,
    gate_gain,
    w_out,
    out_grad,
):
    tok, model = block_input.shape
    own = w_zx.shape[2]
    heads = w_dt.shape[1]
    nt = lax.axis_size("tensor")
    ndp = lax.axis_size("dp")
    inner_total = own * nt
    ncore = 2 if nt % 2 == 0 else 1
    ny = nt // ncore
    width = own * ncore
    t = lax.axis_index("tensor")
    core, yy = t % ncore, t // ncore
    R = SEQ_LEN
    Ry = R // ny
    nseq = tok // R
    nloc = nseq // ncore
    spans = R // L
    wtot = 2 * width + 384

    x3 = block_input.reshape(nseq, R, model)
    g3 = out_grad.reshape(nseq, R, model)
    x4 = block_input.reshape(nseq, ny, Ry, model)
    g4 = out_grad.reshape(nseq, ny, Ry, model)
    wz, wx = w_zx[:, 0], w_zx[:, 1]
    sm = jnp.concatenate(
        [
            conv_x_w,
            conv_x_b[None],
            jnp.repeat(d_skip, HEAD)[None],
            gate_gain[None],
            jnp.zeros((1, own), f32),
            jnp.pad(jnp.stack([dt_bias, -jnp.exp(a_log)]), ((0, 6), (0, own - heads))),
        ],
        axis=0,
    )
    wdt = jnp.pad(w_dt, ((0, 0), (0, L - heads)))
    bcp = jnp.concatenate([conv_bc_w, conv_bc_b[None], jnp.zeros((3, 256), f32)], axis=0)
    gain = pre_gain[None]
    seq0 = jnp.zeros((1,), jnp.int32)
    any_spec = pl.BlockSpec(memory_space=pl.ANY)
    nother = max(ny - 1, 1)
    dma = pltpu.SemaphoreType.DMA

    hid, z, xl, bcl, dtl, u, y, sin, st, stot, po, bo01, prm, hp, wdt, wzo, wxo = call(
        partial(forward_kernel, own, heads, ncore, ny, inner_total, nloc),
        (nloc,),
        [
            moved_spec(ncore, nloc, R, model),
            moved_spec(ncore, nloc, R, model),
            whole_spec(1, model),
            whole_spec(model, own),
            whole_spec(model, own),
            whole_spec(model, 256),
            whole_spec(model, L),
            whole_spec(own, model),
            whole_spec(16, own),
            whole_spec(8, 256),
            any_spec,
        ],
        [
            seq_spec(R, model),
            seq_spec(R, width),
            seq_spec(R + PAD, width),
            seq_spec(R + PAD, 256),
            seq_spec(R, L),
            seq_spec(R, width),
            seq_spec(R, width),
            seq_spec(spans, L, width),
            whole_spec(nloc, 2, R),
            whole_spec(nloc, 2, R),
            whole_spec(R, model),
            whole_spec(nloc - 1, Ry, model),
            whole_spec(8, width),
            whole_spec(8, L),
            whole_spec(model, L),
            any_spec,
            any_spec,
        ],
        [
            sds(nloc, R, model, dtype=bf16),
            sds(nloc, R, width),
            sds(nloc, R + PAD, width),
            sds(nloc, R + PAD, 256),
            sds(nloc, R, L),
            sds(nloc, R, width),
            sds(nloc, R, width),
            sds(nloc, spans, L, width, dtype=bf16),
            sds(nloc, 2, R),
            sds(nloc, 2, R),
            sds(R, model, dtype=bf16),
            sds(nloc - 1, Ry, model, dtype=bf16),
            sds(8, width),
            sds(8, L),
            sds(model, L, dtype=bf16),
            sds(model, own, dtype=bf16),
            sds(model, own, dtype=bf16),
        ],
        [
            pltpu.VMEM((R, width), bf16),
            pltpu.VMEM((R, 256), bf16),
            pltpu.VMEM((L, width), f32),
            pltpu.VMEM((L, width), f32),
            pltpu.VMEM((L, width), bf16),
            pltpu.VMEM((model, own), bf16),
            pltpu.VMEM((model, own), bf16),
            pltpu.VMEM((own, model), bf16),
            pltpu.VMEM((model, L), bf16),
            pltpu.VMEM((16, own), f32),
            pltpu.VMEM((R, model), bf16),
            pltpu.VMEM((nloc - 1, nother, Ry, model), bf16),
            pltpu.VMEM((nloc - 1, nother, 2, R), f32),
            pltpu.VMEM((Ry, model), bf16),
            dma((2, 5)),
            dma((2, nloc - 1, nother)),
            dma((2, nloc - 1, nother)),
            dma((3,)),
        ],
        "forward",
        2 * nloc * R * model * (wtot + 2 * width),
        nloc * R * (6 * model + 20 * width),
        4,
    )(seq0, x3, g3, gain, wz, wx, w_bc, wdt, w_out, sm, bcp, x4)

    nbits = log2(ndp)
    dz, dy, gz, go, ggg, bo = call(
        partial(gate_kernel, width, own, inner_total, ncore, ny),
        (nloc,),
        [
            whole_spec(nloc, 2, R),
            whole_spec(nloc, 2, R),
            moved_spec(ncore, nloc, R, model),
            seq_spec(R, model),
            seq_spec(R, width),
            seq_spec(R, width),
            seq_spec(R, width),
            whole_spec(8, width),
            whole_spec(R, model),
            whole_spec(nloc - 1, Ry, model),
            any_spec,
        ],
        [
            seq_spec(R, width),
            seq_spec(R, width),
            whole_spec(model, own),
            whole_spec(model, own),
            whole_spec(8, width),
            whole_spec(nloc, Ry, model),
        ],
        [
            sds(nloc, R, width, dtype=bf16),
            sds(nloc, R, width, dtype=bf16),
            sds(model, own, dtype=bf16),
            sds(model, own, dtype=bf16),
            sds(8, width),
            sds(nloc, Ry, model, dtype=bf16),
        ],
        [
            pltpu.VMEM((R, width), bf16),
            pltpu.VMEM((R, model), bf16),
            pltpu.VMEM((model, 2 * width), f32),
            pltpu.VMEM((nloc, 2, R), f32),
            pltpu.VMEM((nother, 2, R), f32),
            pltpu.VMEM((model, 2 * own), bf16),
            pltpu.VMEM((model, 2 * own), bf16),
            pltpu.VMEM((nother, Ry, model), bf16),
            pltpu.VMEM((Ry, model), bf16),
            dma((2, nother)),
            dma,
            dma,
            dma((2, nother)),
            dma((1,)),
        ],
        "gate",
        4 * nloc * R * model * width,
        nloc * R * (4 * model + 16 * width),
        1,
    )(seq0, st, stot, g3, hid, z, y, u, prm, po, bo01, x4)

    def chunk_spec(*shape):
        zeros = (0,) * len(shape)
        return pl.BlockSpec((None,) + shape, lambda i, b, s: (i,) + zeros)

    bc_type = bf16 if (model // (nt * ndp)) % 16 == 0 else f32
    early_n = max(nloc - 2, 1)
    dh, gw2, gbcw, small, other, shared, corr, fz, fo, boy, bot, boty, cy0, ct0, cty0 = call(
        partial(scan_kernel, width, own, heads, ncore, ny, ndp, nloc),
        (nloc, spans),
        [
            chunk_spec(R, model),
            chunk_spec(R, width),
            chunk_spec(R, width),
            chunk_spec(R + PAD, width),
            chunk_spec(R + PAD, 256),
            chunk_spec(R, L),
            chunk_spec(spans, L, width),
            whole_spec(model, own),
            whole_spec(model, own),
            whole_spec(model, own),
            whole_spec(model, own),
            whole_spec(model, 256),
            whole_spec(model, L),
            whole_spec(8, width),
            whole_spec(8, 256),
            whole_spec(8, L),
            whole_spec(8, width),
            whole_spec(1, model),
            whole_spec(model, own),
            whole_spec(model, own),
            any_spec,
            any_spec,
        ],
        [
            whole_spec(R, model),
            whole_spec(model, own + L),
            whole_spec(model, 256),
            whole_spec(16, own),
            whole_spec(16, own),
            whole_spec(8, model),
            whole_spec(nloc - 1, Ry, model),
        ]
        + [any_spec] * 8,
        [
            sds(R, model, dtype=bf16),
            sds(model, own + L, dtype=bf16),
            sds(model, 256, dtype=bc_type),
            sds(16, own),
            sds(16, own),
            sds(8, model),
            sds(nloc - 1, Ry, model, dtype=bf16),
            sds(model, own, dtype=bf16),
            sds(model, own, dtype=bf16),
            sds(nother, nloc, Ry, model, dtype=bf16),
            sds(nloc, Ry, model, dtype=bf16),
            sds(nother, nloc, Ry, model, dtype=bf16),
            sds(nother, early_n, Ry, model, dtype=bf16),
            sds(early_n, Ry, model, dtype=bf16),
            sds(nother, early_n, Ry, model, dtype=bf16),
        ],
        [
            pltpu.VMEM((R, width + 384), bf16),
            pltpu.VMEM((R, 256), f32),
            pltpu.VMEM((R, 256), bf16),
            pltpu.VMEM((L, width), f32),
            pltpu.VMEM((L, width), bf16),
            pltpu.VMEM((L, width), f32),
            pltpu.VMEM((L, width), f32),
            pltpu.VMEM((L, width), bf16),
            pltpu.VMEM((L, width), bf16),
            pltpu.VMEM((8, width), f32),
            pltpu.VMEM((8, 256), f32),
            pltpu.VMEM((6, 8, width), f32),
            pltpu.VMEM((5, 8, 256), f32),
            pltpu.VMEM((2, 8, L), f32),
            pltpu.VMEM((8, model), f32),
            pltpu.VMEM((model, width + 384), f32),
            pltpu.VMEM((model, own + L), bf16),
            pltpu.VMEM((model, own + L), bf16),
            pltpu.VMEM((R, model), bf16),
            pltpu.VMEM((nloc - 1, nother, Ry, model), bf16),
            pltpu.VMEM((Ry, model), bf16),
            dma,
            dma,
            dma((2, nloc - 1, nother)),
            dma((2, 2 * ny)),
            dma((2, early_n, 2 * ny)),
            dma((1,)),
        ]
        + Halving.scratch(model, own, nbits, bf16)
        + Halving.scratch(model, own, nbits, bf16),
        "scan_back",
        2 * nloc * R * model * (2 * wtot),
        nloc * R * (4 * model + 12 * width),
        2,
    )(seq0, hid, dz, dy, xl, bcl, dtl, sin, wz, wzo, wx, wxo, w_bc, wdt, prm, bcp, hp, ggg, gain, gz, go, bo, x4)

    vm = pl.BlockSpec(memory_space=pltpu.VMEM)
    tbits = log2(nt)
    late_shape = sds(nother, Ry, model, dtype=bf16)
    fw, fb, small, shared, last, cy, ct, cty, ly, lt, lty = pl.pallas_call(
        partial(tail_kernel, own, ncore, ny, ndp),
        in_specs=[vm] * 7 + [any_spec] * 2,
        out_specs=[any_spec] * 2 + [vm] * 3 + [any_spec] * 6,
        out_shape=[
            sds(model, own + L, dtype=bf16),
            sds(model, 256, dtype=bc_type),
            sds(16, own),
            sds(8, model),
            sds(Ry, model, dtype=bf16),
            late_shape,
            sds(Ry, model, dtype=bf16),
            late_shape,
            late_shape,
            sds(Ry, model, dtype=bf16),
            late_shape,
        ],
        scratch_shapes=[
            pltpu.VMEM((nother, Ry, model), bf16),
            pltpu.VMEM((Ry, model), bf16),
            pltpu.VMEM((16, own), f32),
            dma((2,)),
            dma((2, nother)),
            dma((2, 2 * ny)),
            dma((2, 2 * ny)),
            dma((1,)),
        ]
        + Halving.scratch(model // 2, own + L, nbits, bf16)
        + Halving.scratch(model // 2, own + L, nbits, bf16)
        + Halving.scratch(model, 256, nbits + tbits, bc_type)
        + Doubling.scratch(nbits, 16, own)
        + Doubling.scratch(nbits + tbits, 8, model),
        compiler_params=pltpu.CompilerParams(collective_id=3, has_side_effects=True),
        name="tail",
    )(gw2, gbcw, small, other, shared, dh, gain, corr, x4)

    pieces = ncore * ny
    where = jnp.stack([core, yy]).astype(jnp.int32)

    def out_index(k, i, s):
        return ((s[0] ^ (k // ny)) * nloc + i, (s[1] - k % ny + ny) % ny, 0, 0)

    def spec_of(base, seq_of, d):
        if d is None:
            return pl.BlockSpec(
                (None, Ry, model), lambda j, i, s: (seq_of(j, i) - base, 0, 0)
            )
        return pl.BlockSpec(
            (None, None, Ry, model), lambda j, i, s: (d, seq_of(j, i) - base, 0, 0)
        )

    placed_spec = pl.BlockSpec((None, None, Ry, model), out_index)
    specs, arrays = [], []

    def add_group(first, count, mine, mine_base, toy, tot, toty):
        for k in range(pieces):

            def seq_of(j, i, k=k):
                i = jnp.clip(i, first, first + count - 1)
                return jnp.where(j == k, i, jnp.where(j > k, first + count - 1, first))

            d = k % ny - 1
            if k == 0:
                array, spec = mine, spec_of(mine_base, seq_of, None)
            elif k < ny:
                array, spec = toy, spec_of(first, seq_of, d)
            elif d < 0:
                array, spec = tot, spec_of(first, seq_of, None)
            else:
                array, spec = toty, spec_of(first, seq_of, d)
            arrays.append(array)
            specs.append(spec)

    def as_seq(v, axis):
        return jnp.expand_dims(v, axis)

    add_group(0, early_n, corr, 0, cy0, ct0, cty0)
    add_group(nloc - 2, 1, corr, 0, as_seq(cy, 1), as_seq(ct, 0), as_seq(cty, 1))
    add_group(nloc - 1, 1, as_seq(last, 0), nloc - 1, as_seq(ly, 1), as_seq(lt, 0), as_seq(lty, 1))
    add_group(0, nloc, bo, 0, boy, bot, boty)
    grad_input, block_output = call(
        partial(finish_kernel, pieces, nloc),
        (pieces, nloc),
        [placed_spec] + specs,
        [placed_spec, placed_spec],
        [sds(nseq, ny, Ry, model), sds(nseq, ny, Ry, model, dtype=bf16)],
        [],
        "finish",
        0,
        12 * tok * model,
    )(where, g4, *arrays)

    gzx, gwo = pl.pallas_call(
        partial(unpack_kernel, own),
        grid=(model // L,),
        in_specs=[
            pl.BlockSpec((L, own), lambda d: (d, 0)),
            pl.BlockSpec((L, own), lambda d: (d, 0)),
            pl.BlockSpec((L, own + L), lambda d: (d, 0)),
        ],
        out_specs=[
            pl.BlockSpec((L, 2, own), lambda d: (d, 0, 0)),
            pl.BlockSpec((own, L), lambda d: (0, d)),
        ],
        out_shape=[sds(model, 2, own), sds(own, model)],
        name="unpack",
    )(fz, fo, fw)
    tail = fw[:, own : own + heads].astype(f32)
    return (
        block_output.reshape(tok, model),
        grad_input.reshape(tok, model),
        shared[0],
        gzx,
        fb.astype(f32),
        tail,
        small[0:4],
        small[4],
        shared[1:5, 0:256],
        shared[5, 0:256],
        small[7, :heads],
        small[8, :heads],
        jnp.sum(small[5].reshape(heads, HEAD), axis=1),
        small[6],
        gwo,
    )


def solution(mesh):
    placed = (
        P("dp", None),
        P(),
        P(None, None, "tensor"),
        P(),
        P(None, "tensor"),
        P(None, "tensor"),
        P("tensor"),
        P(),
        P(),
        P("tensor"),
        P("tensor"),
        P("tensor"),
        P("tensor"),
        P("tensor", None),
        P("dp", None),
    )
    return jax.shard_map(
        body,
        mesh=mesh,
        in_specs=placed,
        out_specs=(
            P("dp", None),
            P("dp", None),
            P(),
            P(None, None, "tensor"),
            P(),
            P(None, "tensor"),
            P(None, "tensor"),
            P("tensor"),
            P(),
            P(),
            P("tensor"),
            P("tensor"),
            P("tensor"),
            P("tensor"),
            P("tensor", None),
        ),
        check_vma=False,
    )
```

```python
from functools import partial

import jax
import jax.numpy as jnp
from jax import lax
from jax.experimental import pallas as pl
from jax.experimental.pallas import tpu as pltpu
from jax.sharding import PartitionSpec as P

SEQ_LEN = 512
L = 128
HEAD = 64
LOG2E = 1.4426950408889634
PAD = 8
epsilon = 1e-05
f32 = jnp.float32
bf16 = jnp.bfloat16
HI = lax.Precision.HIGHEST
MESH = pl.DeviceIdType.MESH


def nn(a, b):
    return lax.dot_general(a, b, (((1,), (0,)), ((), ())), preferred_element_type=f32)


def nt(a, b):
    return lax.dot_general(a, b, (((1,), (1,)), ((), ())), preferred_element_type=f32)


def tn(a, b):
    return lax.dot_general(a, b, (((0,), (0,)), ((), ())), preferred_element_type=f32)


def exact(a, b):
    return lax.dot_general(
        a, b, (((1,), (0,)), ((), ())), precision=HI, preferred_element_type=f32
    )


def sigmoid(v):
    return 0.5 + 0.5 * jnp.tanh(0.5 * v)


def softplus(v):
    u = jnp.exp(-jnp.abs(v))
    return jnp.maximum(v, 0.0) + jnp.where(u < 1e-3, u - 0.5 * u * u, jnp.log(1.0 + u))


def fold_rows(v):
    return jnp.sum(v.reshape(v.shape[0] // 8, 8, v.shape[1]), axis=0)


def lane_iota(shape):
    return lax.broadcasted_iota(jnp.int32, shape, 1)


def row_iota(shape):
    return lax.broadcasted_iota(jnp.int32, shape, 0)


def tap(win, k):
    return win[PAD - 3 + k : PAD - 3 + k + L, :]


def conv(ref, t0, win, lanes, taps, bias):
    win[...] = ref[pl.ds(t0, L + PAD), lanes]
    total = bias
    for k in range(4):
        total = total + tap(win, k) * taps[k : k + 1]
    return total


def spread(cols, head):
    return jnp.broadcast_to(cols[:, head : head + 1], (L, L))


def span_decay(dtl, hp):
    pre = dtl + hp[0:1]
    dt = softplus(pre)
    ltri = (row_iota((L, L)) >= lane_iota((L, L))).astype(f32)
    cum = exact(ltri, dt * (hp[1:2] * LOG2E))
    return pre, dt, cum, cum.T


def remote(src, dst, send, recv, where):
    return pltpu.make_async_remote_copy(
        src_ref=src,
        dst_ref=dst,
        send_sem=send,
        recv_sem=recv,
        device_id=where,
        device_id_type=MESH,
    )


def greet(peers):
    barrier = pltpu.get_barrier_semaphore()
    for peer in peers:
        pl.semaphore_signal(barrier, inc=1, device_id=peer, device_id_type=MESH)
    pl.semaphore_wait(barrier, len(peers))


def bit_peers(axis, base, first, count):
    me = lax.axis_index(axis)
    peers, bits = [], []
    for k in range(count):
        step = base * 2**k
        bit = lax.rem(me // step, 2)
        peers.append({axis: me + step * (1 - 2 * bit)})
        bits.append(bit)
    return peers, bits


class Halving:
    def __init__(self, links, rows, src, work, recvs, full, sems):
        self.links, self.rows = links, rows
        self.src, self.work, self.recvs, self.full, self.sems = src, work, recvs, full, sems
        self.n = len(links)
        offs, size = [0], rows
        for _, bit in links:
            size //= 2
            offs.append(offs[-1] + bit * size)
        self.offs = offs

    def size(self, k):
        return self.rows >> k

    def at(self, off, size):
        return pl.ds(pl.multiple_of(off, size), size)

    def scatter(self, k):
        peer, bit = self.links[k]
        half = self.size(k + 1)
        off = self.offs[k] + (1 - bit) * half
        if k == 0:
            src = self.src.at[self.at(off, half)]
        else:
            src = self.work.at[self.at(off - self.offs[1], half)]
        return remote(src, self.recvs[k], self.sems.at[0, k], self.sems.at[1, k], peer)

    def fold(self, k):
        self.scatter(k).wait()
        half = self.size(k + 1)
        step = min(half, 64)
        keep = self.offs[k + 1]

        @pl.loop(0, half // step)
        def _(i):
            off = i * step
            rows = pl.ds(pl.multiple_of(off, step), step)
            near = pl.ds(pl.multiple_of(keep - self.offs[1] + off, step), step)
            if k == 0:
                mine = self.src[pl.ds(pl.multiple_of(keep + off, step), step), :]
            else:
                mine = self.work[near, :]
            total = mine.astype(f32) + self.recvs[k][rows, :].astype(f32)
            self.work[near, :] = total.astype(self.work.dtype)

    def own_copy(self):
        last = self.size(self.n)
        return pltpu.make_async_copy(
            self.work.at[self.at(self.offs[self.n] - self.offs[1], last)],
            self.full.at[self.at(self.offs[self.n], last)],
            self.sems.at[0, 2 * self.n],
        )

    def gather(self, k):
        peer, _ = self.links[k]
        rows = self.at(self.offs[k + 1], self.size(k + 1))
        sems = self.sems
        return remote(
            self.full.at[rows],
            self.full.at[rows],
            sems.at[0, self.n + k],
            sems.at[1, self.n + k],
            peer,
        )

    def close(self, j):
        n = self.n
        if 1 <= j <= n:
            self.fold(j - 1)
        elif j > n:
            self.gather(2 * n - j).wait()

    def begin(self, j):
        n = self.n
        if j < n:
            self.scatter(j).start()
            return
        if j == n:
            self.own_copy().start()
            self.own_copy().wait()
        if j < 2 * n:
            self.gather(2 * n - 1 - j).start()

    @staticmethod
    def scratch(rows, cols, n, dtype):
        recvs = [pltpu.VMEM((rows >> (k + 1), cols), dtype) for k in range(n)]
        return [pltpu.VMEM((rows // 2, cols), dtype)] + recvs + [
            pltpu.SemaphoreType.DMA((2, 2 * n + 1))
        ]


class Doubling:
    def __init__(self, peers, acc, recv, sems):
        self.peers, self.acc, self.recv, self.sems = peers, acc, recv, sems

    def copy(self, k):
        return remote(
            self.acc.at[k],
            self.recv.at[k],
            self.sems.at[0, k],
            self.sems.at[1, k],
            self.peers[k],
        )

    def close(self, j):
        if j > 0:
            self.copy(j - 1).wait()
            self.acc[j] = self.acc[j - 1] + self.recv[j - 1]

    def begin(self, j):
        if j < len(self.peers):
            self.copy(j).start()

    @staticmethod
    def scratch(n, rows, cols):
        return [
            pltpu.VMEM((n + 1, rows, cols), f32),
            pltpu.VMEM((n, rows, cols), f32),
            pltpu.SemaphoreType.DMA((2, n)),
        ]


class Spread:
    def __init__(self, src, toy, tot, toty, sems, place):
        self.src, self.toy, self.tot, self.toty, self.sems = src, toy, tot, toty, sems
        self.twin, self.peers, self.ncore = place

    def first(self):
        n = len(self.peers)
        sems = self.sems
        out = [
            remote(self.src, self.toy.at[d], sems.at[0, d], sems.at[1, d], self.peers[d])
            for d in range(n)
        ]
        if self.ncore == 2:
            out.append(remote(self.src, self.tot, sems.at[0, n], sems.at[1, n], self.twin))
        return out

    def second(self):
        n = len(self.peers)
        if self.ncore != 2:
            return []
        sems = self.sems
        return [
            remote(
                self.toy.at[d], self.toty.at[d], sems.at[0, n + 1 + d], sems.at[1, n + 1 + d], self.twin
            )
            for d in range(n)
        ]


def start(copies):
    for copy in copies:
        copy.start()


def wait(copies):
    for copy in copies:
        copy.wait()


def correction(x, dh, gain):
    v = x.astype(f32)
    r = lax.rsqrt(jnp.mean(v * v, axis=1, keepdims=True) + epsilon)
    normed = v * r
    dn = dh * gain
    return r * (dn - normed * jnp.mean(dn * normed, axis=1, keepdims=True))


def places(ncore, ny):
    spot = lax.axis_index("tensor")
    core, yy = lax.rem(spot, ncore), spot // ncore
    ys = [lax.rem(yy + d, ny) for d in range(1, ny)]
    peers = [{"tensor": v * ncore + core} for v in ys]
    return core, yy, {"tensor": spot + 1 - 2 * core}, ys, peers


def log2(n):
    return n.bit_length() - 1


def forward_kernel(
    own,
    heads,
    ncore,
    ny,
    inner_total,
    nloc,
    _seq,
    x_ref,
    g_ref,
    gain_ref,
    wz_ref,
    wx_ref,
    wbc_ref,
    wdt_ref,
    wo_ref,
    sm_ref,
    bcp_ref,
    x4_ref,
    hid_ref,
    z_ref,
    xl_ref,
    bcl_ref,
    dtl_ref,
    u_ref,
    y_ref,
    sin_ref,
    st_ref,
    stot_ref,
    po_ref,
    bo_ref,
    prm_ref,
    hp_ref,
    wdt_out,
    wz_out,
    wx_out,
    boy_ref,
    bot_ref,
    boty_ref,
    q_scr,
    bca_scr,
    s_scr,
    cs_scr,
    xs_scr,
    wx_scr,
    wbc_scr,
    wz_in,
    wx_in,
    wo_in,
    wdt_in,
    sm_in,
    po_scr,
    po_in,
    st_in,
    x_own,
    w_sems,
    po_sems,
    st_sems,
    bo_sems,
    local,
):
    rows_all = x_ref.shape[0]
    model = x_ref.shape[1]
    width = own * ncore
    pairs = width // L
    Ry = rows_all // ny
    here = pl.program_id(0)
    core, yy, twin, ys, peers = places(ncore, ny)

    def weight_copies():
        both = ((sm_ref, sm_in), (wdt_ref, wdt_in), (wz_ref, wz_in), (wx_ref, wx_in), (wo_ref, wo_in))
        return [
            remote(src, dst, w_sems.at[0, k], w_sems.at[1, k], twin)
            for k, (src, dst) in enumerate(both)
        ]

    def weight_stores():
        return [
            pltpu.make_async_copy(wz_in, wz_out, local.at[1]),
            pltpu.make_async_copy(wx_in, wx_out, local.at[2]),
        ]

    def row_copies():
        last = here - 1
        return [
            remote(
                st_ref.at[last],
                st_in.at[last, d],
                st_sems.at[0, last, d],
                st_sems.at[1, last, d],
                peers[d],
            )
            for d in range(ny - 1)
        ] + [
            remote(
                po_scr.at[lax.rem(last, 2), pl.ds(pl.multiple_of(ys[d] * Ry, Ry), Ry)],
                po_in.at[last, d],
                po_sems.at[0, last, d],
                po_sems.at[1, last, d],
                peers[d],
            )
            for d in range(ny - 1)
        ]

    def x_copy():
        return pltpu.make_async_copy(x4_ref.at[core * nloc + here - 1, yy], x_own, local.at[0])

    def bo_spread(i):
        return Spread(
            bo_ref.at[i],
            boy_ref.at[:, i],
            bot_ref.at[i],
            boty_ref.at[:, i],
            bo_sems.at[:, i],
            (twin, peers, ncore),
        )

    @pl.when(here == 0)
    def _():
        greet(peers + ([twin] if ncore == 2 else []))
        if ncore == 2:
            for copy in weight_copies():
                copy.start()

    @pl.when(here > 0)
    def _():
        start(row_copies())
        x_copy().start()

    @pl.loop(0, rows_all // 32)
    def _(i):
        rows = pl.ds(pl.multiple_of(i * 32, 32), 32)
        v = x_ref[rows, :].astype(f32)
        r = lax.rsqrt(jnp.mean(v * v, axis=1, keepdims=True) + epsilon)
        hid_ref[rows, :] = (v * r * gain_ref[...]).astype(bf16)

    xl_ref[0:PAD, :] = jnp.zeros((PAD, width), f32)
    bcl_ref[0:PAD, :] = jnp.zeros((PAD, 256), f32)

    def project(wz, wx, wo, base):
        @pl.loop(0, own // 256)
        def _(j):
            src = pl.ds(pl.multiple_of(j * 256, 256), 256)
            cols = pl.ds(pl.multiple_of(base + j * 256, 256), 256)
            z_ref[:, cols] = nn(hid_ref[...], wz[:, src])
            xl_ref[PAD : PAD + rows_all, cols] = nn(hid_ref[...], wx[:, src])
            u_ref[:, cols] = nt(g_ref[...], wo[src, :])

    project(wz_ref, wx_ref, wo_ref, 0)
    bcl_ref[PAD : PAD + rows_all, :] = nn(hid_ref[...], wbc_ref[...])

    @pl.when(here == 0)
    def _():
        prm_ref[:, 0:own] = sm_ref[0:8, :]
        hp_ref[...] = sm_ref[8:16, 0:L]
        wdt_out[...] = wdt_ref[...]
        if ncore == 2:
            for copy in weight_copies():
                copy.wait()
            for copy in weight_stores():
                copy.start()
            prm_ref[:, own : 2 * own] = sm_in[0:8, :]
            hp_ref[...] += pltpu.roll(sm_in[8:16, 0:L], heads, axis=1)
            theirs = pltpu.roll(wdt_in[...].astype(f32), heads, axis=1)
            wdt_out[...] = (wdt_ref[...].astype(f32) + theirs).astype(bf16)

    if ncore == 2:
        project(wz_in, wx_in, wo_in, own)
    dtl_ref[...] = nn(hid_ref[...], wdt_out[...])

    @pl.loop(0, rows_all // L)
    def _(c):
        t0 = pl.multiple_of(c * L, L)
        for half in range(2):
            lanes = slice(half * L, half * L + L)
            v = conv(bcl_ref, t0, wbc_scr.at[half], lanes, bcp_ref[0:4, lanes], bcp_ref[4:5, lanes])
            bca_scr[pl.ds(t0, L), lanes] = (v * sigmoid(v)).astype(bf16)

    s_scr[...] = jnp.zeros_like(s_scr)
    hp = hp_ref[...]

    def block_done():
        wait(row_copies())
        x_copy().wait()
        total = st_ref[here - 1]
        for d in range(ny - 1):
            total = total + st_in[here - 1, d]
        stot_ref[here - 1] = total
        parts = [po_in.at[here - 1, d] for d in range(ny - 1)]
        mine = po_scr.at[lax.rem(here - 1, 2), pl.ds(pl.multiple_of(yy * Ry, Ry), Ry)]
        block_out(inner_total, stot_ref.at[here - 1], yy, mine, parts, x_own, bo_ref.at[here - 1])

    @pl.loop(0, rows_all // L)
    def _(c):
        early = jnp.logical_and(here > 0, here < nloc - 1)

        @pl.when(jnp.logical_and(early, c == rows_all // L - 1))
        def _():
            block_done()
            start(bo_spread(here - 1).first())

        t0 = pl.multiple_of(c * L, L)
        rows = pl.ds(t0, L)
        lo = lane_iota((L, L)) < HEAD
        mlo = (lane_iota((1, L)) < HEAD).astype(bf16)
        mhi = (lane_iota((1, L)) >= HEAD).astype(bf16)
        tri = row_iota((L, L)) >= lane_iota((L, L))
        _, dt, cum, cum_t = span_decay(dtl_ref[rows, :], hp)
        bm = bca_scr[rows, 0:L]
        cm = bca_scr[rows, L : 2 * L]
        both = nt(cm, bm)
        sb = s_scr[...].astype(bf16)
        sin_ref[c] = sb
        cs_scr[...] = nn(cm, sb)
        squares = jnp.zeros((L, L), f32)
        inner = jnp.zeros((L, L), f32)
        for p in range(pairs):
            lanes = slice(p * L, p * L + L)
            xc = conv(xl_ref, t0, wx_scr.at[p], lanes, prm_ref[0:4, lanes], prm_ref[4:5, lanes])
            x = xc * sigmoid(xc)
            h0, h1 = 2 * p, 2 * p + 1
            a0, a1 = spread(cum, h0), spread(cum, h1)
            ap = jnp.where(lo, a0, a1)
            k0 = both * jnp.exp2(jnp.where(tri, a0 - cum_t[h0 : h0 + 1], -jnp.inf))
            k1 = both * jnp.exp2(jnp.where(tri, a1 - cum_t[h1 : h1 + 1], -jnp.inf))
            xdt = x * jnp.where(lo, spread(dt, h0), spread(dt, h1))
            xb = xdt.astype(bf16)
            fin = ap[L - 1 : L]
            within = nn(
                jnp.concatenate([k0.astype(bf16), k1.astype(bf16)], axis=1),
                jnp.concatenate([xb * mlo, xb * mhi], axis=0),
            )
            y = within + jnp.exp2(ap) * cs_scr[:, lanes] + prm_ref[5:6, lanes] * x
            xs_scr[:, lanes] = (xdt * jnp.exp2(fin - ap)).astype(bf16)
            s_scr[:, lanes] = s_scr[:, lanes] * jnp.exp2(fin)
            y_ref[rows, lanes] = y
            z = z_ref[rows, lanes]
            gated = y * (z * sigmoid(z))
            q = gated * prm_ref[6:7, lanes]
            q_scr[rows, lanes] = q.astype(bf16)
            squares = squares + gated * gated
            inner = inner + u_ref[rows, lanes] * q
        s_scr[...] += nn(bm.T, xs_scr[...])
        s0 = jnp.sum(squares, axis=1, keepdims=True)
        s1 = jnp.sum(inner, axis=1, keepdims=True)
        lane = lane_iota((L, L))
        stat = jnp.where(lane == 0, s0, jnp.where(lane == 1, s1, 0.0))
        st_ref[here, :, rows] = stat.T[0:2]

    @pl.loop(0, model // 256)
    def _(j):
        cols = pl.ds(pl.multiple_of(j * 256, 256), 256)
        po = nn(q_scr[:, 0:own], wo_ref[:, cols])
        if ncore == 2:
            po = po + nn(q_scr[:, own : 2 * own], wo_in[:, cols])
        po_scr[lax.rem(here, 2), :, cols] = po.astype(bf16)

    @pl.when(here > 1)
    def _():
        wait(bo_spread(here - 2).first())
        start(bo_spread(here - 2).second())

    @pl.when(here == nloc - 1)
    def _():
        po_ref[...] = po_scr[(nloc - 1) % 2]
        block_done()

    @pl.when(here > 1)
    def _():
        wait(bo_spread(here - 2).second())

    @pl.when(here == nloc - 1)
    def _():
        if ncore == 2:
            for copy in weight_stores():
                copy.wait()


def block_out(inner_total, stot, yy, mine, parts, x_own, bo):
    Ry, model = x_own.shape
    for h in range(Ry // L):
        lanes = pl.ds(pl.multiple_of(yy * Ry + h * L, L), L)
        r_row = lax.rsqrt(stot[0:1, lanes] / inner_total + epsilon)
        r = jnp.broadcast_to(r_row, (8, L)).T[:, 0:1]

        @pl.loop(0, model // L)
        def _(m, h=h, r=r):
            cols = pl.ds(pl.multiple_of(m * L, L), L)
            rows = slice(h * L, h * L + L)
            total = mine[rows, cols].astype(f32)
            for part in parts:
                total = total + part[rows, cols].astype(f32)
            bo[rows, cols] = (x_own[rows, cols].astype(f32) + r * total).astype(bf16)


def gate_kernel(
    width,
    own,
    inner_total,
    ncore,
    ny,
    _seq,
    st_ref,
    stin_ref,
    g_ref,
    hid_ref,
    z_ref,
    y_ref,
    u_ref,
    prm_ref,
    po_ref,
    bo01_ref,
    x_ref,
    dz_ref,
    dy_ref,
    gz_ref,
    go_ref,
    ggg_ref,
    bo_ref,
    boy_ref,
    bot_ref,
    boty_ref,
    q_scr,
    sc_scr,
    dz_scr,
    stot_ref,
    st_in,
    send_scr,
    recv_scr,
    po_in,
    x_own,
    st_sems,
    core_send,
    core_recv,
    po_sems,
    bo_sems,
    local,
):
    rows_all = z_ref.shape[0]
    model = g_ref.shape[1]
    pairs = width // L
    here = pl.program_id(0)
    core, yy, twin, ys, peers = places(ncore, ny)
    nloc, Ry, _ = bo_ref.shape
    last = nloc - 1

    def row_copies():
        return [
            remote(st_ref.at[last], st_in.at[d], st_sems.at[0, d], st_sems.at[1, d], peers[d])
            for d in range(ny - 1)
        ]

    def po_copies():
        return [
            remote(
                po_ref.at[pl.ds(pl.multiple_of(ys[d] * Ry, Ry), Ry)],
                po_in.at[d],
                po_sems.at[0, d],
                po_sems.at[1, d],
                peers[d],
            )
            for d in range(ny - 1)
        ]

    def x_copy():
        return pltpu.make_async_copy(x_ref.at[core * nloc + last, yy], x_own, local.at[0])

    spread = Spread(
        bo01_ref.at[last - 1], boy_ref, bot_ref, boty_ref, bo_sems, (twin, peers, ncore)
    )

    @pl.when(here == 0)
    def _():
        greet(peers + ([twin] if ncore == 2 else []))
        start(row_copies() + po_copies() + [x_copy()] + spread.first())
        stot_ref[...] = stin_ref[...]
        for i in range(last):
            bo_ref[i] = bo01_ref[i]
        ggg_ref[...] = jnp.zeros_like(ggg_ref)

    @pl.when(here == last)
    def _():
        for copy in row_copies():
            copy.wait()
        total = st_ref[last]
        for d in range(ny - 1):
            total = total + st_in[d]
        stot_ref[last] = total

    @pl.loop(0, rows_all // L)
    def _(c):
        rows = pl.ds(pl.multiple_of(c * L, L), L)
        st = stot_ref[here, :, rows]
        r_row = lax.rsqrt(st[0:1] / inner_total + epsilon)
        c_row = r_row * r_row * r_row * (st[1:2] / inner_total)
        cols8 = jnp.concatenate([r_row, c_row, jnp.zeros((6, L), f32)], axis=0).T
        r = jnp.broadcast_to(cols8[:, 0:1], (L, L))
        c2 = jnp.broadcast_to(cols8[:, 1:2], (L, L))
        for m in range(model // L):
            lanes = slice(m * L, m * L + L)
            sc_scr[here, rows, lanes] = (g_ref[rows, lanes].astype(f32) * r).astype(bf16)
        for p in range(pairs):
            lanes = slice(p * L, p * L + L)
            gg = prm_ref[6:7, lanes]
            z = z_ref[rows, lanes]
            y = y_ref[rows, lanes]
            sg = sigmoid(z)
            silz = z * sg
            gated = y * silz
            q_scr[here, rows, lanes] = (gated * gg).astype(bf16)
            dq = r * u_ref[rows, lanes]
            ggg_ref[:, lanes] += fold_rows(dq * gated)
            dgated = dq * gg - c2 * gated
            dy_ref[rows, lanes] = (dgated * silz).astype(bf16)
            dz = (dgated * y * (sg + silz * (1.0 - sg))).astype(bf16)
            dz_ref[rows, lanes] = dz
            dz_scr[here, rows, lanes] = dz

    @pl.when(here == last)
    def _():
        hid = hid_ref.reshape(nloc * rows_all, model)
        dz = dz_scr.reshape(nloc * rows_all, width)
        q = q_scr.reshape(nloc * rows_all, width)
        sc = sc_scr.reshape(nloc * rows_all, model)

        def sums(half, out_z, out_o):
            lanes = slice(half * own, half * own + own)

            @pl.loop(0, model // 256)
            def _(j):
                cols = pl.ds(pl.multiple_of(j * 256, 256), 256)
                gz = tn(hid[:, cols], dz[:, lanes])
                go = tn(sc[:, cols], q[:, lanes])
                out_z[cols, :] = gz.astype(bf16)
                out_o[cols, :] = go.astype(bf16)

        if ncore == 2:
            sums(1, send_scr.at[:, 0:own], send_scr.at[:, own : 2 * own])
        if ncore == 2:
            copy = remote(send_scr, recv_scr, core_send, core_recv, twin)
            copy.start()
        sums(0, gz_ref, go_ref)
        if ncore == 2:
            copy.wait()

            @pl.loop(0, model // 64)
            def _(j):
                rows = pl.ds(pl.multiple_of(j * 64, 64), 64)
                for ref, first in ((gz_ref, 0), (go_ref, own)):
                    theirs = recv_scr[rows, first : first + own].astype(f32)
                    ref[rows, :] = (ref[rows, :].astype(f32) + theirs).astype(bf16)

        for copy in po_copies() + [x_copy()]:
            copy.wait()
        parts = [po_in.at[d] for d in range(ny - 1)]
        mine = po_ref.at[pl.ds(pl.multiple_of(yy * Ry, Ry), Ry)]
        block_out(inner_total, stot_ref.at[last], yy, mine, parts, x_own, bo_ref.at[last])
        wait(spread.first())
        start(spread.second())
        wait(spread.second())


def scan_kernel(
    width,
    own,
    heads,
    ncore,
    ny,
    ndp,
    nloc_static,
    _seq,
    hid_ref,
    dz_ref,
    dy_ref,
    xl_ref,
    bcl_ref,
    dtl_ref,
    sin_ref,
    wz_ref,
    wzo_ref,
    wx_ref,
    wxo_ref,
    wbc_ref,
    wdt_ref,
    prm_ref,
    bcp_ref,
    hp_ref,
    ggg_ref,
    gain_ref,
    gz_ref,
    go_ref,
    bo_ref,
    x_ref,
    dh_ref,
    gw_ref,
    gbcw_ref,
    small_ref,
    other_ref,
    shared_ref,
    corr_ref,
    fz_ref,
    fo_ref,
    boy_ref,
    bot_ref,
    boty_ref,
    cy_ref,
    ct_ref,
    cty_ref,
    d_scr,
    bcc_scr,
    bca_scr,
    ds_scr,
    dsb_scr,
    cs_scr,
    bds_scr,
    xs_scr,
    dye_scr,
    nx_scr,
    nbc_scr,
    wx_scr,
    wbc_scr,
    red_scr,
    end_scr,
    pick_scr,
    gx_ref,
    gbc_ref,
    gdt_ref,
    gpre_ref,
    acc_scr,
    send_scr,
    recv_scr,
    dh_scr,
    dh_in,
    x_own,
    core_send,
    core_recv,
    y_sems,
    bo_sems,
    c_sems,
    local,
    *machine,
):
    rows_all = dz_ref.shape[0]
    model = hid_ref.shape[1]
    pairs = width // L
    spans = rows_all // L
    Ry = rows_all // ny
    seq, back = pl.program_id(0), pl.program_id(1)
    step = seq * spans + back
    core, yy, twin, ys, peers = places(ncore, ny)
    nbits = log2(ndp)
    dp_peers, dp_bits = bit_peers("dp", 1, 0, nbits)
    links = list(zip(dp_peers, dp_bits))
    swapped = [links[1], links[0]] + links[2:] if nbits > 1 else links
    half = len(machine) // 2
    mz, mo = machine[:half], machine[half:]
    jobs = [
        Halving(links, model, gz_ref, mz[0], mz[1:-1], fz_ref, mz[-1]),
        Halving(swapped, model, go_ref, mo[0], mo[1:-1], fo_ref, mo[-1]),
    ]
    last_step = nloc_static * spans - 1

    place = (twin, peers, ncore)
    bo_spread = Spread(bo_ref.at[nloc_static - 1], boy_ref, bot_ref, boty_ref, bo_sems, place)

    def corr_spread(i):
        return Spread(
            corr_ref.at[i], cy_ref.at[:, i], ct_ref.at[i], cty_ref.at[:, i], c_sems.at[:, i], place
        )

    def dh_copies():
        return [
            remote(
                dh_scr.at[pl.ds(pl.multiple_of(ys[d] * Ry, Ry), Ry)],
                dh_in.at[seq - 1, d],
                y_sems.at[0, seq - 1, d],
                y_sems.at[1, seq - 1, d],
                peers[d],
            )
            for d in range(ny - 1)
        ]

    def x_copy():
        return pltpu.make_async_copy(x_ref.at[core * nloc_static + seq - 1, yy], x_own, local.at[0])

    @pl.when(step == 0)
    def _():
        greet(peers + dp_peers + ([twin] if ncore == 2 else []))
        start(bo_spread.first())
        acc_scr[...] = jnp.zeros_like(acc_scr)
        end_scr[...] = jnp.zeros_like(end_scr)
        pick = row_iota((width, L)) // HEAD == lane_iota((width, L))
        pick_scr[...] = pick.astype(f32).astype(bf16)
        gx_ref[...] = jnp.zeros_like(gx_ref)
        gbc_ref[...] = jnp.zeros_like(gbc_ref)
        gdt_ref[...] = jnp.zeros_like(gdt_ref)
        gpre_ref[...] = jnp.zeros_like(gpre_ref)

    spans_of = ([2] + [1] * (nbits - 2) + [2])[:nbits]
    spans_of = spans_of + spans_of[::-1]
    for j in range(2 * nbits + 1):

        @pl.when(step == sum(spans_of[:j]) * last_step // sum(spans_of))
        def _(j=j):
            for job in jobs:
                job.close(j)
            for job in jobs:
                job.begin(j)

    @pl.when(step == spans)
    def _():
        wait(bo_spread.first())
        start(bo_spread.second())

    for i in range(nloc_static - 2):

        @pl.when(step == (i + 2) * spans + 2)
        def _(i=i):
            wait(corr_spread(i).first())
            start(corr_spread(i).second())

    @pl.when(jnp.logical_and(seq > 0, back == 0))
    def _():
        for copy in dh_copies():
            copy.start()
        x_copy().start()

    @pl.when(jnp.logical_and(seq > 0, back == spans - 1))
    def _():
        for copy in dh_copies():
            copy.wait()
        x_copy().wait()

        @pl.loop(0, Ry // 32)
        def _(i):
            rows = pl.ds(pl.multiple_of(i * 32, 32), 32)
            mine = pl.ds(pl.multiple_of(yy * Ry + i * 32, 32), 32)
            dh = dh_scr[mine, :].astype(f32)
            for d in range(ny - 1):
                dh = dh + dh_in[seq - 1, d, rows, :].astype(f32)
            corr_ref[seq - 1, rows, :] = correction(x_own[rows, :], dh, gain_ref[...]).astype(bf16)

        start(corr_spread(seq - 1).first())

    hp = hp_ref[...]

    @pl.when(back == 0)
    def _():
        ds_scr[...] = jnp.zeros_like(ds_scr)
        nx_scr[...] = jnp.zeros_like(nx_scr)
        nbc_scr[...] = jnp.zeros_like(nbc_scr)

        @pl.loop(0, spans)
        def _(c):
            t0 = pl.multiple_of(c * L, L)
            for half in range(2):
                lanes = slice(half * L, half * L + L)
                v = conv(bcl_ref, t0, wbc_scr.at[half], lanes, bcp_ref[0:4, lanes], bcp_ref[4:5, lanes])
                bcc_scr[pl.ds(t0, L), lanes] = v
                bca_scr[pl.ds(t0, L), lanes] = (v * sigmoid(v)).astype(bf16)

    def one_chunk():
        c = spans - 1 - back
        t0 = pl.multiple_of(c * L, L)
        rows = pl.ds(t0, L)
        lane = lane_iota((L, L))
        lo = lane < HEAD
        mlo = (lane_iota((1, L)) < HEAD).astype(bf16)
        mhi = (lane_iota((1, L)) >= HEAD).astype(bf16)
        tri = row_iota((L, L)) >= lane
        pre, dt, cum, cum_t = span_decay(dtl_ref[rows, :], hp)
        bm = bca_scr[rows, 0:L]
        cm = bca_scr[rows, L : 2 * L]
        both = nt(cm, bm)
        sb = sin_ref[c]
        dsb_scr[...] = ds_scr[...].astype(bf16)
        cs_scr[...] = nn(cm, sb)
        bds_scr[...] = nn(bm, dsb_scr[...])
        d_both = jnp.zeros((L, L), f32)
        for p in range(pairs):
            lanes = slice(p * L, p * L + L)
            taps = prm_ref[0:4, lanes]
            xc = conv(xl_ref, t0, wx_scr.at[p], lanes, taps, prm_ref[4:5, lanes])
            sg = sigmoid(xc)
            x = xc * sg
            h0, h1 = 2 * p, 2 * p + 1
            a0, a1 = spread(cum, h0), spread(cum, h1)
            ap = jnp.where(lo, a0, a1)
            e0 = jnp.exp2(jnp.where(tri, a0 - cum_t[h0 : h0 + 1], -jnp.inf))
            e1 = jnp.exp2(jnp.where(tri, a1 - cum_t[h1 : h1 + 1], -jnp.inf))
            k0 = (both * e0).astype(bf16)
            k1 = (both * e1).astype(bf16)
            dtp = jnp.where(lo, spread(dt, h0), spread(dt, h1))
            xdt = x * dtp
            xb = xdt.astype(bf16)
            bdx = jnp.concatenate([xb * mlo, xb * mhi], axis=0)
            ecum = jnp.exp2(ap)
            fin = ap[L - 1 : L]
            sd = jnp.exp2(fin - ap)
            y = nn(jnp.concatenate([k0, k1], axis=1), bdx) + ecum * cs_scr[:, lanes]
            dyb = dy_ref[rows, lanes]
            dy = dyb.astype(f32)
            dk = nt(dyb, bdx)
            d_both = d_both + dk[:, 0:L] * e0 + dk[:, L : 2 * L] * e1
            bdy = jnp.concatenate([dyb * mlo, dyb * mhi], axis=0)
            near = tn(jnp.concatenate([k0, k1], axis=0), bdy)
            far = sd * bds_scr[:, lanes]
            dxdt = near + far
            v = dy * y - xb.astype(f32) * near
            u = dxdt * x
            w = xdt * far
            ends = jnp.exp2(fin)
            through = ends * jnp.sum(sb[:, lanes].astype(f32) * ds_scr[:, lanes], axis=0, keepdims=True)
            v_hi = v.astype(bf16)
            red_scr[0:L, lanes] = v_hi
            red_scr[L : 2 * L, lanes] = (v - v_hi.astype(f32)).astype(bf16)
            red_scr[2 * L : 3 * L, lanes] = u.astype(bf16)
            red_scr[3 * L : 4 * L, lanes] = w.astype(bf16)
            end_scr[0:1, lanes] = through
            dx = dxdt * dtp + dy * prm_ref[5:6, lanes]
            dxc = dx * (sg + x * (1.0 - sg))
            for k in range(4):
                gx_ref[k, :, lanes] += fold_rows(dxc * tap(wx_scr.at[p], k))
            gx_ref[4, :, lanes] += fold_rows(dxc)
            gx_ref[5, :, lanes] += fold_rows(dy * x)
            nx_scr[p, L : L + 8] = nx_scr[p, 0:8]
            nx_scr[p, 0:L] = dxc
            dxl = dxc * taps[3:4]
            for k in range(3):
                dxl = dxl + nx_scr[p, 3 - k : 3 - k + L] * taps[k : k + 1]
            d_scr[rows, lanes] = dxl.astype(bf16)
            xs_scr[:, lanes] = (xdt * sd).astype(bf16)
            dye_scr[:, lanes] = (dy * ecum).astype(bf16)
            ds_scr[:, lanes] = ds_scr[:, lanes] * ends
        ds_scr[...] += nn(cm.T, dye_scr[...])
        sums = nn(red_scr[...], pick_scr[...])
        d_cum = sums[0:L] + sums[L : 2 * L]
        d_dt = sums[2 * L : 3 * L]
        d_far = sums[3 * L : 4 * L]
        d_end = exact(end_scr[...], pick_scr[...].astype(f32))[0:1]
        utri = (row_iota((L, L)) <= lane).astype(f32)
        before = (row_iota((L, L)) > lane).astype(f32)
        d_a = exact(utri, d_cum) + exact(before, d_far) + d_end
        d_dt = d_dt + d_a * hp[1:2]
        d_pre = d_dt * sigmoid(pre)
        gdt_ref[0] += fold_rows(d_pre)
        gdt_ref[1] += fold_rows(d_a * dt * hp[1:2])
        d_scr[rows, width + 256 : width + 384] = d_pre.astype(bf16)
        dgb = d_both.astype(bf16)
        d_c = nt(dye_scr[...], sb) + nn(dgb, bm)
        d_b = nt(xs_scr[...], dsb_scr[...]) + nn(dgb.T, cm)
        for half, dv in ((0, d_b), (1, d_c)):
            lanes = slice(half * L, half * L + L)
            pre_act = bcc_scr[rows, lanes]
            sg = sigmoid(pre_act)
            dvc = dv * (sg + pre_act * sg * (1.0 - sg))
            wbc_scr[half] = bcl_ref[pl.ds(t0, L + PAD), lanes]
            for k in range(4):
                gbc_ref[k, :, lanes] += fold_rows(dvc * tap(wbc_scr.at[half], k))
            gbc_ref[4, :, lanes] += fold_rows(dvc)
            nbc_scr[half, L : L + 8] = nbc_scr[half, 0:8]
            nbc_scr[half, 0:L] = dvc
            dvl = dvc * bcp_ref[3:4, lanes]
            for k in range(3):
                dvl = dvl + nbc_scr[half, 3 - k : 3 - k + L] * bcp_ref[k : k + 1, lanes]
            d_scr[rows, width + half * L : width + half * L + L] = dvl.astype(bf16)

    one_chunk()

    @pl.when(back == spans - 1)
    def _():
        @pl.loop(0, model // 256)
        def _(j):
            cols = pl.ds(pl.multiple_of(j * 256, 256), 256)
            dh = nt(dz_ref[:, 0:own], wz_ref[cols, :]) + nt(d_scr[:, 0:own], wx_ref[cols, :])
            if ncore == 2:
                dh = dh + nt(dz_ref[:, own:width], wzo_ref[cols, :])
                dh = dh + nt(d_scr[:, own:width], wxo_ref[cols, :])
            dh = dh + nt(d_scr[:, width : width + 256], wbc_ref[cols, :])
            dh = dh + nt(d_scr[:, width + 256 :], wdt_ref[cols, :])
            dh_scr[:, cols] = dh.astype(bf16)
            gpre_ref[:, cols] += fold_rows(dh * hid_ref[:, cols].astype(f32))
            acc_scr[cols, :] += tn(hid_ref[:, cols], d_scr[...])

    @pl.when(step == last_step)
    def _():
        tail = acc_scr[:, width + 256 : width + 384]
        if ncore == 2:
            send_scr[:, 0:own] = acc_scr[:, own:width].astype(bf16)
            send_scr[:, own : own + L] = tail.astype(bf16)
        dh_ref[...] = dh_scr[...]
        gbcw_ref[...] = acc_scr[:, width : width + 256].astype(gbcw_ref.dtype)
        if ncore == 2:
            copy = remote(send_scr, recv_scr, core_send, core_recv, twin)
            copy.start()
        rows = [jnp.sum(gx_ref[k], axis=0, keepdims=True) for k in range(6)]
        rows.append(jnp.sum(ggg_ref[...], axis=0, keepdims=True))
        dts = [jnp.sum(gdt_ref[k], axis=0, keepdims=True) for k in range(2)]
        small_ref[...] = jnp.zeros_like(small_ref)
        other_ref[...] = jnp.zeros_like(other_ref)
        for k in range(7):
            small_ref[k : k + 1, :] = rows[k][:, 0:own]
            if ncore == 2:
                other_ref[k : k + 1, :] = rows[k][:, own:width]
        for k in range(2):
            small_ref[7 + k : 8 + k, 0:L] = dts[k]
            if ncore == 2:
                moved = pltpu.roll(jnp.broadcast_to(dts[k], (8, L)), L - heads, axis=1)
                other_ref[7 + k : 8 + k, 0:L] = moved[0:1]
        shared_ref[...] = jnp.zeros_like(shared_ref)
        shared_ref[0:1, :] = jnp.sum(gpre_ref[...], axis=0, keepdims=True) / gain_ref[...]
        for k in range(5):
            shared_ref[k + 1 : k + 2, 0:256] = jnp.sum(gbc_ref[k], axis=0, keepdims=True)
        if ncore == 2:
            copy.wait()
            theirs = recv_scr[...].astype(f32)
            gw_ref[:, 0:own] = (acc_scr[:, 0:own] + theirs[:, 0:own]).astype(bf16)
            tail = tail + pltpu.roll(theirs[:, own : own + L], L - heads, axis=1)
        else:
            gw_ref[:, 0:own] = acc_scr[:, 0:own].astype(bf16)
        gw_ref[:, own : own + L] = tail.astype(bf16)
        final = corr_spread(nloc_static - 2)
        wait(final.first())
        start(final.second())
        wait(bo_spread.second())
        for i in range(nloc_static - 1):
            wait(corr_spread(i).second())


def tail_kernel(
    own,
    ncore,
    ny,
    ndp,
    nloc,
    gw_ref,
    gbcw_ref,
    small_ref,
    other_ref,
    shared_ref,
    dh_ref,
    gain_ref,
    x_ref,
    fw_ref,
    fb_ref,
    small_out,
    shared_out,
    last_ref,
    ly_ref,
    lt_ref,
    lty_ref,
    dh_in,
    x_own,
    small_in,
    core_sems,
    y_sems,
    l_sems,
    local,
    *machine,
):
    model = gw_ref.shape[0]
    Ry = x_own.shape[0]
    core, yy, twin, ys, peers = places(ncore, ny)
    nbits = log2(ndp)
    dp_peers, dp_bits = bit_peers("dp", 1, 0, nbits)
    t_peers, t_bits = bit_peers("tensor", 1, 0, log2(ncore * ny))
    links = list(zip(dp_peers, dp_bits))
    swapped = [links[1], links[0]] + links[2:] if nbits > 1 else links
    t_links = list(zip(t_peers, t_bits))
    per = nbits + 2
    a, b = machine[:per], machine[per : 2 * per]
    per_bc = nbits + len(t_links) + 2
    c = machine[2 * per : 2 * per + per_bc]
    sm, sh = machine[2 * per + per_bc : 2 * per + per_bc + 3], machine[2 * per + per_bc + 3 :]
    mid = model // 2
    job_a = Halving(links, mid, gw_ref.at[0:mid], a[0], a[1:-1], fw_ref.at[0:mid], a[-1])
    job_b = Halving(swapped, mid, gw_ref.at[mid:model], b[0], b[1:-1], fw_ref.at[mid:model], b[-1])
    job_c = Halving(t_links + links, model, gbcw_ref, c[0], c[1:-1], fb_ref, c[-1])
    job_sm = Doubling(dp_peers, *sm)
    job_sh = Doubling(t_peers + dp_peers, *sh)

    def dh_copies():
        return [
            remote(
                dh_ref.at[pl.ds(pl.multiple_of(ys[d] * Ry, Ry), Ry)],
                dh_in.at[d],
                y_sems.at[0, d],
                y_sems.at[1, d],
                peers[d],
            )
            for d in range(ny - 1)
        ]

    late = Spread(last_ref, ly_ref, lt_ref, lty_ref, l_sems, (twin, peers, ncore))
    x_copy = pltpu.make_async_copy(x_ref.at[core * nloc + nloc - 1, yy], x_own, local.at[0])
    others = peers + ([twin] if ncore == 2 else [])
    greet(others + dp_peers)
    x_copy.start()

    def turn(*pairs):
        for job, j in pairs:
            job.close(j)
        for job, j in pairs:
            job.begin(j)

    job_sh.acc[0] = shared_ref[...]
    turn((job_sh, 0), (job_c, 0), (job_a, 0), (job_b, 0))
    if ncore == 2:
        small_copy = remote(other_ref, small_in, core_sems.at[0], core_sems.at[1], twin)
        small_copy.start()
    turn((job_c, 1), (job_sh, 1))
    start(dh_copies())
    if ncore == 2:
        small_copy.wait()
        job_sm.acc[0] = small_ref[...] + small_in[...]
    else:
        job_sm.acc[0] = small_ref[...]
    turn((job_sm, 0))
    steps = [
        (job_c, iter(range(2, 2 * job_c.n + 1))),
        (job_sm, iter(range(1, len(job_sm.peers) + 1))),
        (job_sh, iter(range(2, len(job_sh.peers) + 1))),
    ]

    def smaller():
        found = []
        for job, left in steps:
            j = next(left, None)
            if j is not None:
                found.append((job, j))
        return found

    turn(*smaller(), (job_a, 1), (job_b, 1))
    for copy in dh_copies():
        copy.wait()
    x_copy.wait()

    @pl.loop(0, Ry // 32)
    def _(i):
        rows = pl.ds(pl.multiple_of(i * 32, 32), 32)
        mine = pl.ds(pl.multiple_of(yy * Ry + i * 32, 32), 32)
        dh = dh_ref[mine, :].astype(f32)
        for d in range(ny - 1):
            dh = dh + dh_in[d, rows, :].astype(f32)
        last_ref[rows, :] = correction(x_own[rows, :], dh, gain_ref[...]).astype(bf16)

    turn(*smaller())
    start(late.first())
    for j in range(2, 2 * nbits + 1):
        turn(*smaller(), (job_a, j), (job_b, j))
    for _ in range(2 * job_c.n):
        turn(*smaller())
    small_out[...] = job_sm.acc[len(job_sm.peers)]
    shared_out[...] = job_sh.acc[len(job_sh.peers)]
    wait(late.first())
    start(late.second())
    wait(late.second())


def finish_kernel(pieces, nloc, _idx, g_ref, *refs):
    gi_ref, bo_ref = refs[-2:]
    groups = [refs[n * pieces : (n + 1) * pieces] for n in range(5)]
    now = pl.program_id(1)
    for k in range(pieces):
        here = pl.program_id(0) == k

        def when(turn, here=here):
            return pl.when(jnp.logical_and(here, turn))

        for n, turn in ((0, now < nloc - 1), (1, now == nloc - 1)):

            @when(turn)
            def _(src=groups[n][k]):
                gi_ref[...] = g_ref[...].astype(f32) + src[...].astype(f32)

        for n, turn in ((2, now < nloc - 2), (3, now == nloc - 2), (4, now == nloc - 1)):

            @when(turn)
            def _(src=groups[n][k]):
                bo_ref[...] = src[...]


def unpack_kernel(own, heads, gz_ref, go_ref, gw_ref, fb_ref, small_ref, shared_ref, *outs):
    gzx_ref, gwo_ref, gwdt_ref, gwbc_ref = outs[:4]
    gcxw_ref, gcxb_ref, gd_ref, ggg_ref, gdtb_ref, galog_ref, gpre_ref, gcbw_ref, gcbb_ref = outs[4:]
    gzx_ref[:, 0, :] = gz_ref[...].astype(f32)
    gzx_ref[:, 1, :] = gw_ref[:, 0:own].astype(f32)
    gwdt_ref[...] = gw_ref[:, own : own + L].astype(f32)[:, 0:heads]
    gwbc_ref[...] = fb_ref[...].astype(f32)
    v = go_ref[...].astype(f32)
    for k in range(own // L):
        gwo_ref[k * L : k * L + L, :] = v[:, k * L : k * L + L].T

    @pl.when(pl.program_id(0) == 0)
    def _():
        gcxw_ref[...] = small_ref[0:4]
        gcxb_ref[...] = small_ref[4:5]
        ggg_ref[...] = small_ref[6:7]
        gdtb_ref[...] = small_ref[7:8, 0:heads]
        galog_ref[...] = small_ref[8:9, 0:heads]
        pick = (row_iota((own, L)) // HEAD == lane_iota((own, L))).astype(f32)
        gd_ref[...] = exact(small_ref[0:8], pick)[5:6, 0:heads]
        gpre_ref[...] = shared_ref[0:1]
        gcbw_ref[...] = shared_ref[1:5, 0:256]
        gcbb_ref[...] = shared_ref[5:6, 0:256]


def seq_spec(*shape):
    zeros = (0,) * len(shape)
    return pl.BlockSpec((None,) + shape, lambda i, s: (i,) + zeros)


def moved_spec(ncore, nloc, *shape):
    zeros = (0,) * len(shape)

    def index(i, s):
        return (i + lax.rem(lax.axis_index("tensor"), ncore) * nloc,) + zeros

    return pl.BlockSpec((None,) + shape, index)


def whole_spec(*shape):
    zeros = (0,) * len(shape)
    return pl.BlockSpec(shape, lambda *_: zeros, pipeline_mode=pl.Buffered(1))


def call(
    kernel, grid, in_specs, out_specs, out_shape, scratch, name, flops=0, moved=0, group=None
):
    return pl.pallas_call(
        kernel,
        grid_spec=pltpu.PrefetchScalarGridSpec(
            num_scalar_prefetch=1,
            grid=grid,
            in_specs=in_specs,
            out_specs=out_specs,
            scratch_shapes=scratch,
        ),
        out_shape=out_shape,
        cost_estimate=pl.CostEstimate(
            flops=int(flops), bytes_accessed=int(moved), transcendentals=0
        ),
        name=name,
        compiler_params=None
        if group is None
        else pltpu.CompilerParams(collective_id=group, has_side_effects=True),
    )


def sds(*shape, dtype=f32):
    return jax.ShapeDtypeStruct(shape, dtype)


def body(
    block_input,
    pre_gain,
    w_zx,
    w_bc,
    w_dt,
    conv_x_w,
    conv_x_b,
    conv_bc_w,
    conv_bc_b,
    dt_bias,
    a_log,
    d_skip,
    gate_gain,
    w_out,
    out_grad,
):
    tok, model = block_input.shape
    own = w_zx.shape[2]
    heads = w_dt.shape[1]
    nt = lax.axis_size("tensor")
    ndp = lax.axis_size("dp")
    inner_total = own * nt
    ncore = 2 if nt % 2 == 0 else 1
    ny = nt // ncore
    width = own * ncore
    t = lax.axis_index("tensor")
    core, yy = t % ncore, t // ncore
    R = SEQ_LEN
    Ry = R // ny
    nseq = tok // R
    nloc = nseq // ncore
    spans = R // L
    wtot = 2 * width + 384
    pairs = width // L

    x3 = block_input.reshape(nseq, R, model)
    g3 = out_grad.reshape(nseq, R, model)
    x4 = block_input.reshape(nseq, ny, Ry, model)
    g4 = out_grad.reshape(nseq, ny, Ry, model)
    wz, wx = w_zx[:, 0], w_zx[:, 1]
    sm = jnp.concatenate(
        [
            conv_x_w,
            conv_x_b[None],
            jnp.repeat(d_skip, HEAD)[None],
            gate_gain[None],
            jnp.zeros((1, own), f32),
            jnp.pad(jnp.stack([dt_bias, -jnp.exp(a_log)]), ((0, 6), (0, own - heads))),
        ],
        axis=0,
    )
    wdt = jnp.pad(w_dt, ((0, 0), (0, L - heads)))
    bcp = jnp.concatenate([conv_bc_w, conv_bc_b[None], jnp.zeros((3, 256), f32)], axis=0)
    gain = pre_gain[None]
    seq0 = jnp.zeros((1,), jnp.int32)
    any_spec = pl.BlockSpec(memory_space=pl.ANY)
    nother = max(ny - 1, 1)
    dma = pltpu.SemaphoreType.DMA

    early_n = max(nloc - 2, 1)
    f_out = call(
        partial(forward_kernel, own, heads, ncore, ny, inner_total, nloc),
        (nloc,),
        [
            moved_spec(ncore, nloc, R, model),
            moved_spec(ncore, nloc, R, model),
            whole_spec(1, model),
            whole_spec(model, own),
            whole_spec(model, own),
            whole_spec(model, 256),
            whole_spec(model, L),
            whole_spec(own, model),
            whole_spec(16, own),
            whole_spec(8, 256),
            any_spec,
        ],
        [
            seq_spec(R, model),
            seq_spec(R, width),
            seq_spec(R + PAD, width),
            seq_spec(R + PAD, 256),
            seq_spec(R, L),
            seq_spec(R, width),
            seq_spec(R, width),
            seq_spec(spans, L, width),
            whole_spec(nloc, 2, R),
            whole_spec(nloc, 2, R),
            whole_spec(R, model),
            whole_spec(nloc - 1, Ry, model),
            whole_spec(8, width),
            whole_spec(8, L),
            whole_spec(model, L),
        ]
        + [any_spec] * 5,
        [
            sds(nloc, R, model, dtype=bf16),
            sds(nloc, R, width),
            sds(nloc, R + PAD, width),
            sds(nloc, R + PAD, 256),
            sds(nloc, R, L),
            sds(nloc, R, width),
            sds(nloc, R, width),
            sds(nloc, spans, L, width, dtype=bf16),
            sds(nloc, 2, R),
            sds(nloc, 2, R),
            sds(R, model, dtype=bf16),
            sds(nloc - 1, Ry, model, dtype=bf16),
            sds(8, width),
            sds(8, L),
            sds(model, L, dtype=bf16),
            sds(model, own, dtype=bf16),
            sds(model, own, dtype=bf16),
            sds(nother, early_n, Ry, model, dtype=bf16),
            sds(early_n, Ry, model, dtype=bf16),
            sds(nother, early_n, Ry, model, dtype=bf16),
        ],
        [
            pltpu.VMEM((R, width), bf16),
            pltpu.VMEM((R, 256), bf16),
            pltpu.VMEM((L, width), f32),
            pltpu.VMEM((L, width), f32),
            pltpu.VMEM((L, width), bf16),
            pltpu.VMEM((pairs, L + PAD, L), f32),
            pltpu.VMEM((2, L + PAD, L), f32),
            pltpu.VMEM((model, own), bf16),
            pltpu.VMEM((model, own), bf16),
            pltpu.VMEM((own, model), bf16),
            pltpu.VMEM((model, L), bf16),
            pltpu.VMEM((16, own), f32),
            pltpu.VMEM((2, R, model), bf16),
            pltpu.VMEM((nloc - 1, nother, Ry, model), bf16),
            pltpu.VMEM((nloc - 1, nother, 2, R), f32),
            pltpu.VMEM((Ry, model), bf16),
            dma((2, 5)),
            dma((2, nloc - 1, nother)),
            dma((2, nloc - 1, nother)),
            dma((2, early_n, 2 * ny)),
            dma((3,)),
        ],
        "forward",
        2 * nloc * R * model * (wtot + 2 * width),
        nloc * R * (6 * model + 20 * width),
        4,
    )(seq0, x3, g3, gain, wz, wx, w_bc, wdt, w_out, sm, bcp, x4)
    hid, z, xl, bcl, dtl, u, y, sin, st, stot, po, bo01, prm, hp, wdt, wzo, wxo = f_out[:17]
    bo_early = f_out[17:]

    nbits = log2(ndp)
    one = sds(nother, Ry, model, dtype=bf16)
    dz, dy, gz, go, ggg, bo, *bo_mid = call(
        partial(gate_kernel, width, own, inner_total, ncore, ny),
        (nloc,),
        [
            whole_spec(nloc, 2, R),
            whole_spec(nloc, 2, R),
            moved_spec(ncore, nloc, R, model),
            whole_spec(nloc, R, model),
            seq_spec(R, width),
            seq_spec(R, width),
            seq_spec(R, width),
            whole_spec(8, width),
            whole_spec(R, model),
            whole_spec(nloc - 1, Ry, model),
            any_spec,
        ],
        [
            seq_spec(R, width),
            seq_spec(R, width),
            whole_spec(model, own),
            whole_spec(model, own),
            whole_spec(8, width),
            whole_spec(nloc, Ry, model),
        ]
        + [any_spec] * 3,
        [
            sds(nloc, R, width, dtype=bf16),
            sds(nloc, R, width, dtype=bf16),
            sds(model, own, dtype=bf16),
            sds(model, own, dtype=bf16),
            sds(8, width),
            sds(nloc, Ry, model, dtype=bf16),
            one,
            sds(Ry, model, dtype=bf16),
            one,
        ],
        [
            pltpu.VMEM((nloc, R, width), bf16),
            pltpu.VMEM((nloc, R, model), bf16),
            pltpu.VMEM((nloc, R, width), bf16),
            pltpu.VMEM((nloc, 2, R), f32),
            pltpu.VMEM((nother, 2, R), f32),
            pltpu.VMEM((model, 2 * own), bf16),
            pltpu.VMEM((model, 2 * own), bf16),
            pltpu.VMEM((nother, Ry, model), bf16),
            pltpu.VMEM((Ry, model), bf16),
            dma((2, nother)),
            dma,
            dma,
            dma((2, nother)),
            dma((2, 2 * ny)),
            dma((1,)),
        ],
        "gate",
        4 * nloc * R * model * width,
        nloc * R * (4 * model + 16 * width),
        1,
    )(seq0, st, stot, g3, hid, z, y, u, prm, po, bo01, x4)

    def chunk_spec(*shape):
        zeros = (0,) * len(shape)
        return pl.BlockSpec((None,) + shape, lambda i, b, s: (i,) + zeros)

    bc_type = bf16 if (model // (nt * ndp)) % 16 == 0 else f32
    dh, gw2, gbcw, small, other, shared, corr, fz, fo, boy, bot, boty, cy0, ct0, cty0 = call(
        partial(scan_kernel, width, own, heads, ncore, ny, ndp, nloc),
        (nloc, spans),
        [
            chunk_spec(R, model),
            chunk_spec(R, width),
            chunk_spec(R, width),
            chunk_spec(R + PAD, width),
            chunk_spec(R + PAD, 256),
            chunk_spec(R, L),
            chunk_spec(spans, L, width),
            whole_spec(model, own),
            whole_spec(model, own),
            whole_spec(model, own),
            whole_spec(model, own),
            whole_spec(model, 256),
            whole_spec(model, L),
            whole_spec(8, width),
            whole_spec(8, 256),
            whole_spec(8, L),
            whole_spec(8, width),
            whole_spec(1, model),
            whole_spec(model, own),
            whole_spec(model, own),
            any_spec,
            any_spec,
        ],
        [
            whole_spec(R, model),
            whole_spec(model, own + L),
            whole_spec(model, 256),
            whole_spec(16, own),
            whole_spec(16, own),
            whole_spec(8, model),
            whole_spec(nloc - 1, Ry, model),
        ]
        + [any_spec] * 8,
        [
            sds(R, model, dtype=bf16),
            sds(model, own + L, dtype=bf16),
            sds(model, 256, dtype=bc_type),
            sds(16, own),
            sds(16, own),
            sds(8, model),
            sds(nloc - 1, Ry, model, dtype=bf16),
            sds(model, own, dtype=bf16),
            sds(model, own, dtype=bf16),
            one,
            sds(Ry, model, dtype=bf16),
            one,
            sds(nother, nloc - 1, Ry, model, dtype=bf16),
            sds(nloc - 1, Ry, model, dtype=bf16),
            sds(nother, nloc - 1, Ry, model, dtype=bf16),
        ],
        [
            pltpu.VMEM((R, width + 384), bf16),
            pltpu.VMEM((R, 256), f32),
            pltpu.VMEM((R, 256), bf16),
            pltpu.VMEM((L, width), f32),
            pltpu.VMEM((L, width), bf16),
            pltpu.VMEM((L, width), f32),
            pltpu.VMEM((L, width), f32),
            pltpu.VMEM((L, width), bf16),
            pltpu.VMEM((L, width), bf16),
            pltpu.VMEM((pairs, L + 8, L), f32),
            pltpu.VMEM((2, L + 8, L), f32),
            pltpu.VMEM((pairs, L + PAD, L), f32),
            pltpu.VMEM((2, L + PAD, L), f32),
            pltpu.VMEM((4 * L, width), bf16),
            pltpu.VMEM((8, width), f32),
            pltpu.VMEM((width, L), bf16),
            pltpu.VMEM((6, 8, width), f32),
            pltpu.VMEM((5, 8, 256), f32),
            pltpu.VMEM((2, 8, L), f32),
            pltpu.VMEM((8, model), f32),
            pltpu.VMEM((model, width + 384), f32),
            pltpu.VMEM((model, own + L), bf16),
            pltpu.VMEM((model, own + L), bf16),
            pltpu.VMEM((R, model), bf16),
            pltpu.VMEM((nloc - 1, nother, Ry, model), bf16),
            pltpu.VMEM((Ry, model), bf16),
            dma,
            dma,
            dma((2, nloc - 1, nother)),
            dma((2, 2 * ny)),
            dma((2, nloc - 1, 2 * ny)),
            dma((1,)),
        ]
        + Halving.scratch(model, own, nbits, bf16)
        + Halving.scratch(model, own, nbits, bf16),
        "scan_back",
        2 * nloc * R * model * (2 * wtot),
        nloc * R * (4 * model + 12 * width),
        2,
    )(seq0, hid, dz, dy, xl, bcl, dtl, sin, wz, wzo, wx, wxo, w_bc, wdt, prm, bcp, hp, ggg, gain, gz, go, bo, x4)

    vm = pl.BlockSpec(memory_space=pltpu.VMEM)
    tbits = log2(nt)
    late_shape = sds(nother, Ry, model, dtype=bf16)
    fw, fb, small, shared, last, ly, lt, lty = pl.pallas_call(
        partial(tail_kernel, own, ncore, ny, ndp, nloc),
        in_specs=[vm] * 7 + [any_spec],
        out_specs=[any_spec] * 2 + [vm] * 3 + [any_spec] * 3,
        out_shape=[
            sds(model, own + L, dtype=bf16),
            sds(model, 256, dtype=bc_type),
            sds(16, own),
            sds(8, model),
            sds(Ry, model, dtype=bf16),
            late_shape,
            sds(Ry, model, dtype=bf16),
            late_shape,
        ],
        scratch_shapes=[
            pltpu.VMEM((nother, Ry, model), bf16),
            pltpu.VMEM((Ry, model), bf16),
            pltpu.VMEM((16, own), f32),
            dma((2,)),
            dma((2, nother)),
            dma((2, 2 * ny)),
            dma((1,)),
        ]
        + Halving.scratch(model // 2, own + L, nbits, bf16)
        + Halving.scratch(model // 2, own + L, nbits, bf16)
        + Halving.scratch(model, 256, nbits + tbits, bc_type)
        + Doubling.scratch(nbits, 16, own)
        + Doubling.scratch(nbits + tbits, 8, model),
        compiler_params=pltpu.CompilerParams(collective_id=3, has_side_effects=True),
        name="tail",
    )(gw2, gbcw, small, other, shared, dh, gain, x4)

    pieces = ncore * ny
    where = jnp.stack([core, yy]).astype(jnp.int32)

    def out_index(k, i, s):
        return ((s[0] ^ (k // ny)) * nloc + i, (s[1] - k % ny + ny) % ny, 0, 0)

    def spec_of(base, seq_of, d):
        if d is None:
            return pl.BlockSpec(
                (None, Ry, model), lambda j, i, s: (seq_of(j, i) - base, 0, 0)
            )
        return pl.BlockSpec(
            (None, None, Ry, model), lambda j, i, s: (d, seq_of(j, i) - base, 0, 0)
        )

    placed_spec = pl.BlockSpec((None, None, Ry, model), out_index)
    specs, arrays = [], []

    def add_group(first, count, mine, mine_base, toy, tot, toty):
        for k in range(pieces):

            def seq_of(j, i, k=k):
                i = jnp.clip(i, first, first + count - 1)
                return jnp.where(j == k, i, jnp.where(j > k, first + count - 1, first))

            d = k % ny - 1
            if k == 0:
                array, spec = mine, spec_of(mine_base, seq_of, None)
            elif k < ny:
                array, spec = toy, spec_of(first, seq_of, d)
            elif d < 0:
                array, spec = tot, spec_of(first, seq_of, None)
            else:
                array, spec = toty, spec_of(first, seq_of, d)
            arrays.append(array)
            specs.append(spec)

    def as_seq(v, axis):
        return jnp.expand_dims(v, axis)

    add_group(0, nloc - 1, corr, 0, cy0, ct0, cty0)
    add_group(nloc - 1, 1, as_seq(last, 0), nloc - 1, as_seq(ly, 1), as_seq(lt, 0), as_seq(lty, 1))

    def add_late(first, got):
        toy, tot, toty = got
        add_group(first, 1, bo, 0, as_seq(toy, 1), as_seq(tot, 0), as_seq(toty, 1))

    add_group(0, early_n, bo, 0, *bo_early)
    add_late(nloc - 2, bo_mid)
    add_late(nloc - 1, (boy, bot, boty))
    grad_input, block_output = call(
        partial(finish_kernel, pieces, nloc),
        (pieces, nloc),
        [placed_spec] + specs,
        [placed_spec, placed_spec],
        [sds(nseq, ny, Ry, model), sds(nseq, ny, Ry, model, dtype=bf16)],
        [],
        "finish",
        0,
        12 * tok * model,
    )(where, g4, *arrays)

    def row_block(cols):
        return pl.BlockSpec((L, cols), lambda d: (d, 0))

    outs = pl.pallas_call(
        partial(unpack_kernel, own, heads),
        grid=(model // L,),
        in_specs=[row_block(own), row_block(own), row_block(own + L), row_block(256)]
        + [whole_spec(16, own), whole_spec(8, model)],
        out_specs=[
            pl.BlockSpec((L, 2, own), lambda d: (d, 0, 0)),
            pl.BlockSpec((own, L), lambda d: (0, d)),
            row_block(heads),
            row_block(256),
            whole_spec(4, own),
            whole_spec(1, own),
            whole_spec(1, heads),
            whole_spec(1, own),
            whole_spec(1, heads),
            whole_spec(1, heads),
            whole_spec(1, model),
            whole_spec(4, 256),
            whole_spec(1, 256),
        ],
        out_shape=[
            sds(model, 2, own),
            sds(own, model),
            sds(model, heads),
            sds(model, 256),
            sds(4, own),
            sds(1, own),
            sds(1, heads),
            sds(1, own),
            sds(1, heads),
            sds(1, heads),
            sds(1, model),
            sds(4, 256),
            sds(1, 256),
        ],
        name="unpack",
    )(fz, fo, fw, fb, small, shared)
    gzx, gwo, gwdt, gwbc, gcxw, gcxb, gd, ggg, gdtb, galog, gpre, gcbw, gcbb = outs
    return (
        block_output.reshape(tok, model),
        grad_input.reshape(tok, model),
        gpre[0],
        gzx,
        gwbc,
        gwdt,
        gcxw,
        gcxb[0],
        gcbw,
        gcbb[0],
        gdtb[0],
        galog[0],
        gd[0],
        ggg[0],
        gwo,
    )


def solution(mesh):
    placed = (
        P("dp", None),
        P(),
        P(None, None, "tensor"),
        P(),
        P(None, "tensor"),
        P(None, "tensor"),
        P("tensor"),
        P(),
        P(),
        P("tensor"),
        P("tensor"),
        P("tensor"),
        P("tensor"),
        P("tensor", None),
        P("dp", None),
    )
    return jax.shard_map(
        body,
        mesh=mesh,
        in_specs=placed,
        out_specs=(
            P("dp", None),
            P("dp", None),
            P(),
            P(None, None, "tensor"),
            P(),
            P(None, "tensor"),
            P(None, "tensor"),
            P("tensor"),
            P(),
            P(),
            P("tensor"),
            P("tensor"),
            P("tensor"),
            P("tensor"),
            P("tensor", None),
        ),
        check_vma=False,
    )
```

```python
from functools import partial

import jax
import jax.numpy as jnp
from jax import lax
from jax.experimental import pallas as pl
from jax.experimental.pallas import tpu as pltpu
from jax.sharding import PartitionSpec as P

SEQ_LEN = 512
L = 128
HEAD = 64
LOG2E = 1.4426950408889634
PAD = 8
epsilon = 1e-05
f32 = jnp.float32
bf16 = jnp.bfloat16
HI = lax.Precision.HIGHEST
MESH = pl.DeviceIdType.MESH


def nn(a, b):
    return lax.dot_general(a, b, (((1,), (0,)), ((), ())), preferred_element_type=f32)


def nt(a, b):
    return lax.dot_general(a, b, (((1,), (1,)), ((), ())), preferred_element_type=f32)


def tn(a, b):
    return lax.dot_general(a, b, (((0,), (0,)), ((), ())), preferred_element_type=f32)


def exact(a, b):
    return lax.dot_general(
        a, b, (((1,), (0,)), ((), ())), precision=HI, preferred_element_type=f32
    )


def sigmoid(v):
    return 0.5 + 0.5 * jnp.tanh(0.5 * v)


def softplus(v):
    u = jnp.exp(-jnp.abs(v))
    return jnp.maximum(v, 0.0) + jnp.where(u < 1e-3, u - 0.5 * u * u, jnp.log(1.0 + u))


def fold_rows(v):
    return jnp.sum(v.reshape(v.shape[0] // 8, 8, v.shape[1]), axis=0)


def lane_iota(shape):
    return lax.broadcasted_iota(jnp.int32, shape, 1)


def row_iota(shape):
    return lax.broadcasted_iota(jnp.int32, shape, 0)


def tap(win, k):
    return win[PAD - 3 + k : PAD - 3 + k + L, :]


def conv(ref, t0, win, lanes, taps, bias):
    win[...] = ref[pl.ds(t0, L + PAD), lanes]
    total = bias
    for k in range(4):
        total = total + tap(win, k) * taps[k : k + 1]
    return total


def spread(cols, head):
    return jnp.broadcast_to(cols[:, head : head + 1], (L, L))


def span_decay(dtl, hp):
    pre = dtl + hp[0:1]
    dt = softplus(pre)
    ltri = (row_iota((L, L)) >= lane_iota((L, L))).astype(f32)
    cum = exact(ltri, dt * (hp[1:2] * LOG2E))
    return pre, dt, cum, cum.T


def remote(src, dst, send, recv, where):
    return pltpu.make_async_remote_copy(
        src_ref=src,
        dst_ref=dst,
        send_sem=send,
        recv_sem=recv,
        device_id=where,
        device_id_type=MESH,
    )


def greet(peers):
    barrier = pltpu.get_barrier_semaphore()
    for peer in peers:
        pl.semaphore_signal(barrier, inc=1, device_id=peer, device_id_type=MESH)
    pl.semaphore_wait(barrier, len(peers))


def bit_peers(axis, base, first, count):
    me = lax.axis_index(axis)
    peers, bits = [], []
    for k in range(count):
        step = base * 2**k
        bit = lax.rem(me // step, 2)
        peers.append({axis: me + step * (1 - 2 * bit)})
        bits.append(bit)
    return peers, bits


class Halving:
    def __init__(self, links, rows, src, work, recvs, full, sems):
        self.links, self.rows = links, rows
        self.src, self.work, self.recvs, self.full, self.sems = src, work, recvs, full, sems
        self.n = len(links)
        offs, size = [0], rows
        for _, bit in links:
            size //= 2
            offs.append(offs[-1] + bit * size)
        self.offs = offs

    def size(self, k):
        return self.rows >> k

    def at(self, off, size):
        return pl.ds(pl.multiple_of(off, size), size)

    def scatter(self, k):
        peer, bit = self.links[k]
        half = self.size(k + 1)
        off = self.offs[k] + (1 - bit) * half
        if k == 0:
            src = self.src.at[self.at(off, half)]
        else:
            src = self.work.at[self.at(off - self.offs[1], half)]
        return remote(src, self.recvs[k], self.sems.at[0, k], self.sems.at[1, k], peer)

    def fold(self, k):
        self.scatter(k).wait()
        half = self.size(k + 1)
        step = min(half, 64)
        keep = self.offs[k + 1]

        @pl.loop(0, half // step)
        def _(i):
            off = i * step
            rows = pl.ds(pl.multiple_of(off, step), step)
            near = pl.ds(pl.multiple_of(keep - self.offs[1] + off, step), step)
            if k == 0:
                mine = self.src[pl.ds(pl.multiple_of(keep + off, step), step), :]
            else:
                mine = self.work[near, :]
            total = mine.astype(f32) + self.recvs[k][rows, :].astype(f32)
            self.work[near, :] = total.astype(self.work.dtype)

    def own_copy(self):
        last = self.size(self.n)
        return pltpu.make_async_copy(
            self.work.at[self.at(self.offs[self.n] - self.offs[1], last)],
            self.full.at[self.at(self.offs[self.n], last)],
            self.sems.at[0, 2 * self.n],
        )

    def gather(self, k):
        peer, _ = self.links[k]
        rows = self.at(self.offs[k + 1], self.size(k + 1))
        sems = self.sems
        return remote(
            self.full.at[rows],
            self.full.at[rows],
            sems.at[0, self.n + k],
            sems.at[1, self.n + k],
            peer,
        )

    def close(self, j):
        n = self.n
        if 1 <= j <= n:
            self.fold(j - 1)
        elif j > n:
            self.gather(2 * n - j).wait()

    def begin(self, j):
        n = self.n
        if j < n:
            self.scatter(j).start()
            return
        if j == n:
            self.own_copy().start()
            self.own_copy().wait()
        if j < 2 * n:
            self.gather(2 * n - 1 - j).start()

    @staticmethod
    def scratch(rows, cols, n, dtype):
        recvs = [pltpu.VMEM((rows >> (k + 1), cols), dtype) for k in range(n)]
        return [pltpu.VMEM((rows // 2, cols), dtype)] + recvs + [
            pltpu.SemaphoreType.DMA((2, 2 * n + 1))
        ]


class Doubling:
    def __init__(self, peers, acc, recv, sems):
        self.peers, self.acc, self.recv, self.sems = peers, acc, recv, sems

    def copy(self, k):
        return remote(
            self.acc.at[k],
            self.recv.at[k],
            self.sems.at[0, k],
            self.sems.at[1, k],
            self.peers[k],
        )

    def close(self, j):
        if j > 0:
            self.copy(j - 1).wait()
            self.acc[j] = self.acc[j - 1] + self.recv[j - 1]

    def begin(self, j):
        if j < len(self.peers):
            self.copy(j).start()

    @staticmethod
    def scratch(n, rows, cols):
        return [
            pltpu.VMEM((n + 1, rows, cols), f32),
            pltpu.VMEM((n, rows, cols), f32),
            pltpu.SemaphoreType.DMA((2, n)),
        ]


class Spread:
    def __init__(self, src, toy, tot, toty, sems, place):
        self.src, self.toy, self.tot, self.toty, self.sems = src, toy, tot, toty, sems
        self.twin, self.peers, self.ncore = place

    def first(self):
        n = len(self.peers)
        sems = self.sems
        out = [
            remote(self.src, self.toy.at[d], sems.at[0, d], sems.at[1, d], self.peers[d])
            for d in range(n)
        ]
        if self.ncore == 2:
            out.append(remote(self.src, self.tot, sems.at[0, n], sems.at[1, n], self.twin))
        return out

    def second(self):
        n = len(self.peers)
        if self.ncore != 2:
            return []
        sems = self.sems
        return [
            remote(
                self.toy.at[d], self.toty.at[d], sems.at[0, n + 1 + d], sems.at[1, n + 1 + d], self.twin
            )
            for d in range(n)
        ]


def start(copies):
    for copy in copies:
        copy.start()


def wait(copies):
    for copy in copies:
        copy.wait()


def correction(x, dh, gain):
    v = x.astype(f32)
    r = lax.rsqrt(jnp.mean(v * v, axis=1, keepdims=True) + epsilon)
    normed = v * r
    dn = dh * gain
    return r * (dn - normed * jnp.mean(dn * normed, axis=1, keepdims=True))


def places(ncore, ny):
    spot = lax.axis_index("tensor")
    core, yy = lax.rem(spot, ncore), spot // ncore
    ys = [lax.rem(yy + d, ny) for d in range(1, ny)]
    peers = [{"tensor": v * ncore + core} for v in ys]
    return core, yy, {"tensor": spot + 1 - 2 * core}, ys, peers


def log2(n):
    return n.bit_length() - 1


def forward_kernel(
    own,
    heads,
    ncore,
    ny,
    inner_total,
    nloc,
    _seq,
    x_ref,
    g_ref,
    gain_ref,
    wz_ref,
    wx_ref,
    wbc_ref,
    wdt_ref,
    wo_ref,
    sm_ref,
    bcp_ref,
    x4_ref,
    hid_ref,
    z_ref,
    xl_ref,
    bcl_ref,
    dtl_ref,
    u_ref,
    y_ref,
    sin_ref,
    st_ref,
    stot_ref,
    po_ref,
    bo_ref,
    prm_ref,
    hp_ref,
    wdt_out,
    wz_out,
    wx_out,
    z_scr,
    u_scr,
    q_scr,
    bca_scr,
    s_scr,
    cs_scr,
    xs_scr,
    wx_scr,
    wbc_scr,
    wz_in,
    wx_in,
    wo_in,
    wdt_in,
    sm_in,
    po_scr,
    po_in,
    st_in,
    x_own,
    w_sems,
    po_sems,
    st_sems,
    local,
):
    rows_all = x_ref.shape[0]
    model = x_ref.shape[1]
    width = own * ncore
    pairs = width // L
    Ry = rows_all // ny
    here = pl.program_id(0)
    core, yy, twin, ys, peers = places(ncore, ny)

    def weight_copies():
        both = ((sm_ref, sm_in), (wdt_ref, wdt_in), (wz_ref, wz_in), (wx_ref, wx_in), (wo_ref, wo_in))
        return [
            remote(src, dst, w_sems.at[0, k], w_sems.at[1, k], twin)
            for k, (src, dst) in enumerate(both)
        ]

    def weight_stores():
        return [
            pltpu.make_async_copy(wz_in, wz_out, local.at[1]),
            pltpu.make_async_copy(wx_in, wx_out, local.at[2]),
        ]

    def row_copies():
        last = here - 1
        return [
            remote(
                st_ref.at[last],
                st_in.at[last, d],
                st_sems.at[0, last, d],
                st_sems.at[1, last, d],
                peers[d],
            )
            for d in range(ny - 1)
        ] + [
            remote(
                po_scr.at[lax.rem(last, 2), pl.ds(pl.multiple_of(ys[d] * Ry, Ry), Ry)],
                po_in.at[last, d],
                po_sems.at[0, last, d],
                po_sems.at[1, last, d],
                peers[d],
            )
            for d in range(ny - 1)
        ]

    def x_copy():
        return pltpu.make_async_copy(x4_ref.at[core * nloc + here - 1, yy], x_own, local.at[0])

    @pl.when(here == 0)
    def _():
        greet(peers + ([twin] if ncore == 2 else []))
        if ncore == 2:
            for copy in weight_copies():
                copy.start()

    @pl.when(here > 0)
    def _():
        start(row_copies())
        x_copy().start()

    @pl.loop(0, rows_all // 32)
    def _(i):
        rows = pl.ds(pl.multiple_of(i * 32, 32), 32)
        v = x_ref[rows, :].astype(f32)
        r = lax.rsqrt(jnp.mean(v * v, axis=1, keepdims=True) + epsilon)
        hid_ref[rows, :] = (v * r * gain_ref[...]).astype(bf16)

    xl_ref[0:PAD, :] = jnp.zeros((PAD, width), f32)
    bcl_ref[0:PAD, :] = jnp.zeros((PAD, 256), f32)

    def project(wz, wx, wo, base):
        @pl.loop(0, own // 256)
        def _(j):
            src = pl.ds(pl.multiple_of(j * 256, 256), 256)
            cols = pl.ds(pl.multiple_of(base + j * 256, 256), 256)
            z_scr[:, cols] = nn(hid_ref[...], wz[:, src])
            xl_ref[PAD : PAD + rows_all, cols] = nn(hid_ref[...], wx[:, src])
            u_scr[:, cols] = nt(g_ref[...], wo[src, :])

    project(wz_ref, wx_ref, wo_ref, 0)
    bcl_ref[PAD : PAD + rows_all, :] = nn(hid_ref[...], wbc_ref[...])

    @pl.when(here == 0)
    def _():
        prm_ref[:, 0:own] = sm_ref[0:8, :]
        hp_ref[...] = sm_ref[8:16, 0:L]
        wdt_out[...] = wdt_ref[...]
        if ncore == 2:
            for copy in weight_copies():
                copy.wait()
            for copy in weight_stores():
                copy.start()
            prm_ref[:, own : 2 * own] = sm_in[0:8, :]
            hp_ref[...] += pltpu.roll(sm_in[8:16, 0:L], heads, axis=1)
            theirs = pltpu.roll(wdt_in[...].astype(f32), heads, axis=1)
            wdt_out[...] = (wdt_ref[...].astype(f32) + theirs).astype(bf16)

    if ncore == 2:
        project(wz_in, wx_in, wo_in, own)
    dtl_ref[...] = nn(hid_ref[...], wdt_out[...])

    @pl.loop(0, rows_all // L)
    def _(c):
        t0 = pl.multiple_of(c * L, L)
        for half in range(2):
            lanes = slice(half * L, half * L + L)
            v = conv(bcl_ref, t0, wbc_scr.at[half], lanes, bcp_ref[0:4, lanes], bcp_ref[4:5, lanes])
            bca_scr[pl.ds(t0, L), lanes] = (v * sigmoid(v)).astype(bf16)

    s_scr[...] = jnp.zeros_like(s_scr)
    hp = hp_ref[...]

    def block_done():
        wait(row_copies())
        x_copy().wait()
        total = st_ref[here - 1]
        for d in range(ny - 1):
            total = total + st_in[here - 1, d]
        stot_ref[here - 1] = total
        parts = [po_in.at[here - 1, d] for d in range(ny - 1)]
        mine = po_scr.at[lax.rem(here - 1, 2), pl.ds(pl.multiple_of(yy * Ry, Ry), Ry)]
        block_out(inner_total, stot_ref.at[here - 1], yy, mine, parts, x_own, bo_ref.at[here - 1])

    @pl.loop(0, rows_all // L)
    def _(c):
        early = jnp.logical_and(here > 0, here < nloc - 1)

        @pl.when(jnp.logical_and(early, c == rows_all // L - 1))
        def _():
            block_done()

        t0 = pl.multiple_of(c * L, L)
        rows = pl.ds(t0, L)
        lo = lane_iota((L, L)) < HEAD
        mlo = (lane_iota((1, L)) < HEAD).astype(bf16)
        mhi = (lane_iota((1, L)) >= HEAD).astype(bf16)
        tri = row_iota((L, L)) >= lane_iota((L, L))
        _, dt, cum, cum_t = span_decay(dtl_ref[rows, :], hp)
        bm = bca_scr[rows, 0:L]
        cm = bca_scr[rows, L : 2 * L]
        both = nt(cm, bm)
        sb = s_scr[...].astype(bf16)
        sin_ref[c] = sb
        cs_scr[...] = nn(cm, sb)
        squares = jnp.zeros((L, L), f32)
        inner = jnp.zeros((L, L), f32)
        for p in range(pairs):
            lanes = slice(p * L, p * L + L)
            xc = conv(xl_ref, t0, wx_scr.at[p], lanes, prm_ref[0:4, lanes], prm_ref[4:5, lanes])
            x = xc * sigmoid(xc)
            h0, h1 = 2 * p, 2 * p + 1
            a0, a1 = spread(cum, h0), spread(cum, h1)
            ap = jnp.where(lo, a0, a1)
            k0 = both * jnp.exp2(jnp.where(tri, a0 - cum_t[h0 : h0 + 1], -jnp.inf))
            k1 = both * jnp.exp2(jnp.where(tri, a1 - cum_t[h1 : h1 + 1], -jnp.inf))
            xdt = x * jnp.where(lo, spread(dt, h0), spread(dt, h1))
            xb = xdt.astype(bf16)
            fin = ap[L - 1 : L]
            within = nn(
                jnp.concatenate([k0.astype(bf16), k1.astype(bf16)], axis=1),
                jnp.concatenate([xb * mlo, xb * mhi], axis=0),
            )
            y = within + jnp.exp2(ap) * cs_scr[:, lanes] + prm_ref[5:6, lanes] * x
            xs_scr[:, lanes] = (xdt * jnp.exp2(fin - ap)).astype(bf16)
            s_scr[:, lanes] = s_scr[:, lanes] * jnp.exp2(fin)
            y_ref[rows, lanes] = y.astype(bf16)
            z = z_scr[rows, lanes]
            u = u_scr[rows, lanes]
            z_ref[rows, lanes] = z.astype(bf16)
            u_ref[rows, lanes] = u.astype(bf16)
            gated = y * (z * sigmoid(z))
            q = gated * prm_ref[6:7, lanes]
            q_scr[rows, lanes] = q.astype(bf16)
            squares = squares + gated * gated
            inner = inner + u * q
        s_scr[...] += nn(bm.T, xs_scr[...])
        s0 = jnp.sum(squares, axis=1, keepdims=True)
        s1 = jnp.sum(inner, axis=1, keepdims=True)
        lane = lane_iota((L, L))
        stat = jnp.where(lane == 0, s0, jnp.where(lane == 1, s1, 0.0))
        st_ref[here, :, rows] = stat.T[0:2]

    @pl.loop(0, model // 256)
    def _(j):
        cols = pl.ds(pl.multiple_of(j * 256, 256), 256)
        po = nn(q_scr[:, 0:own], wo_ref[:, cols])
        if ncore == 2:
            po = po + nn(q_scr[:, own : 2 * own], wo_in[:, cols])
        po_scr[lax.rem(here, 2), :, cols] = po.astype(bf16)

    @pl.when(here == nloc - 1)
    def _():
        po_ref[...] = po_scr[(nloc - 1) % 2]
        block_done()
        if ncore == 2:
            for copy in weight_stores():
                copy.wait()


def block_out(inner_total, stot, yy, mine, parts, x_own, bo):
    Ry, model = x_own.shape
    for h in range(Ry // L):
        lanes = pl.ds(pl.multiple_of(yy * Ry + h * L, L), L)
        r_row = lax.rsqrt(stot[0:1, lanes] / inner_total + epsilon)
        r = jnp.broadcast_to(r_row, (8, L)).T[:, 0:1]

        @pl.loop(0, model // L)
        def _(m, h=h, r=r):
            cols = pl.ds(pl.multiple_of(m * L, L), L)
            rows = slice(h * L, h * L + L)
            total = mine[rows, cols].astype(f32)
            for part in parts:
                total = total + part[rows, cols].astype(f32)
            bo[rows, cols] = (x_own[rows, cols].astype(f32) + r * total).astype(bf16)


def gate_kernel(
    width,
    own,
    inner_total,
    ncore,
    ny,
    _seq,
    st_ref,
    stin_ref,
    g_ref,
    hid_ref,
    z_ref,
    y_ref,
    u_ref,
    prm_ref,
    po_ref,
    bo01_ref,
    x_ref,
    dz_ref,
    dy_ref,
    gz_ref,
    go_ref,
    ggg_ref,
    bo_ref,
    q_scr,
    sc_scr,
    dz_scr,
    stot_ref,
    st_in,
    send_scr,
    recv_scr,
    po_in,
    x_own,
    st_sems,
    core_send,
    core_recv,
    po_sems,
    local,
):
    rows_all = z_ref.shape[0]
    model = g_ref.shape[1]
    pairs = width // L
    here = pl.program_id(0)
    core, yy, twin, ys, peers = places(ncore, ny)
    nloc, Ry, _ = bo_ref.shape
    last = nloc - 1

    def row_copies():
        return [
            remote(st_ref.at[last], st_in.at[d], st_sems.at[0, d], st_sems.at[1, d], peers[d])
            for d in range(ny - 1)
        ]

    def po_copies():
        return [
            remote(
                po_ref.at[pl.ds(pl.multiple_of(ys[d] * Ry, Ry), Ry)],
                po_in.at[d],
                po_sems.at[0, d],
                po_sems.at[1, d],
                peers[d],
            )
            for d in range(ny - 1)
        ]

    def x_copy():
        return pltpu.make_async_copy(x_ref.at[core * nloc + last, yy], x_own, local.at[0])

    @pl.when(here == 0)
    def _():
        greet(peers + ([twin] if ncore == 2 else []))
        start(row_copies() + po_copies() + [x_copy()])
        stot_ref[...] = stin_ref[...]
        for i in range(last):
            bo_ref[i] = bo01_ref[i]
        ggg_ref[...] = jnp.zeros_like(ggg_ref)

    @pl.when(here == last)
    def _():
        for copy in row_copies():
            copy.wait()
        total = st_ref[last]
        for d in range(ny - 1):
            total = total + st_in[d]
        stot_ref[last] = total

    @pl.loop(0, rows_all // L)
    def _(c):
        rows = pl.ds(pl.multiple_of(c * L, L), L)
        st = stot_ref[here, :, rows]
        r_row = lax.rsqrt(st[0:1] / inner_total + epsilon)
        c_row = r_row * r_row * r_row * (st[1:2] / inner_total)
        cols8 = jnp.concatenate([r_row, c_row, jnp.zeros((6, L), f32)], axis=0).T
        r = jnp.broadcast_to(cols8[:, 0:1], (L, L))
        c2 = jnp.broadcast_to(cols8[:, 1:2], (L, L))
        for m in range(model // L):
            lanes = slice(m * L, m * L + L)
            sc_scr[here, rows, lanes] = (g_ref[rows, lanes].astype(f32) * r).astype(bf16)
        for p in range(pairs):
            lanes = slice(p * L, p * L + L)
            gg = prm_ref[6:7, lanes]
            z = z_ref[rows, lanes].astype(f32)
            y = y_ref[rows, lanes].astype(f32)
            sg = sigmoid(z)
            silz = z * sg
            gated = y * silz
            q_scr[here, rows, lanes] = (gated * gg).astype(bf16)
            dq = r * u_ref[rows, lanes].astype(f32)
            ggg_ref[:, lanes] += fold_rows(dq * gated)
            dgated = dq * gg - c2 * gated
            dy_ref[rows, lanes] = (dgated * silz).astype(bf16)
            dz = (dgated * y * (sg + silz * (1.0 - sg))).astype(bf16)
            dz_ref[rows, lanes] = dz
            dz_scr[here, rows, lanes] = dz

    @pl.when(here == last)
    def _():
        hid = hid_ref.reshape(nloc * rows_all, model)
        dz = dz_scr.reshape(nloc * rows_all, width)
        q = q_scr.reshape(nloc * rows_all, width)
        sc = sc_scr.reshape(nloc * rows_all, model)

        def sums(half, out_z, out_o):
            lanes = slice(half * own, half * own + own)

            @pl.loop(0, model // 256)
            def _(j):
                cols = pl.ds(pl.multiple_of(j * 256, 256), 256)
                gz = tn(hid[:, cols], dz[:, lanes])
                go = tn(sc[:, cols], q[:, lanes])
                out_z[cols, :] = gz.astype(bf16)
                out_o[cols, :] = go.astype(bf16)

        if ncore == 2:
            sums(1, send_scr.at[:, 0:own], send_scr.at[:, own : 2 * own])
        if ncore == 2:
            copy = remote(send_scr, recv_scr, core_send, core_recv, twin)
            copy.start()
        sums(0, gz_ref, go_ref)
        if ncore == 2:
            copy.wait()

            @pl.loop(0, model // 64)
            def _(j):
                rows = pl.ds(pl.multiple_of(j * 64, 64), 64)
                for ref, first in ((gz_ref, 0), (go_ref, own)):
                    theirs = recv_scr[rows, first : first + own].astype(f32)
                    ref[rows, :] = (ref[rows, :].astype(f32) + theirs).astype(bf16)

        for copy in po_copies() + [x_copy()]:
            copy.wait()
        parts = [po_in.at[d] for d in range(ny - 1)]
        mine = po_ref.at[pl.ds(pl.multiple_of(yy * Ry, Ry), Ry)]
        block_out(inner_total, stot_ref.at[last], yy, mine, parts, x_own, bo_ref.at[last])


def scan_kernel(
    width,
    own,
    heads,
    ncore,
    ny,
    ndp,
    nloc_static,
    _seq,
    hid_ref,
    dz_ref,
    dy_ref,
    xl_ref,
    bcl_ref,
    dtl_ref,
    sin_ref,
    wz_ref,
    wzo_ref,
    wx_ref,
    wxo_ref,
    wbc_ref,
    wdt_ref,
    prm_ref,
    bcp_ref,
    hp_ref,
    ggg_ref,
    gain_ref,
    gz_ref,
    go_ref,
    bo_ref,
    x_ref,
    dh_ref,
    gw_ref,
    gbcw_ref,
    small_ref,
    other_ref,
    shared_ref,
    corr_ref,
    fz_ref,
    fo_ref,
    boy_ref,
    bot_ref,
    boty_ref,
    cy_ref,
    ct_ref,
    cty_ref,
    d_scr,
    bcc_scr,
    bca_scr,
    ds_scr,
    dsb_scr,
    cs_scr,
    bds_scr,
    xs_scr,
    dye_scr,
    nx_scr,
    nbc_scr,
    wx_scr,
    wbc_scr,
    red_scr,
    end_scr,
    pick_scr,
    gx_ref,
    gbc_ref,
    gdt_ref,
    gpre_ref,
    acc_scr,
    send_scr,
    recv_scr,
    dh_scr,
    dh_in,
    x_own,
    core_send,
    core_recv,
    y_sems,
    bo_sems,
    c_sems,
    local,
    *machine,
):
    rows_all = dz_ref.shape[0]
    model = hid_ref.shape[1]
    pairs = width // L
    spans = rows_all // L
    Ry = rows_all // ny
    seq, back = pl.program_id(0), pl.program_id(1)
    step = seq * spans + back
    core, yy, twin, ys, peers = places(ncore, ny)
    nbits = log2(ndp)
    dp_peers, dp_bits = bit_peers("dp", 1, 0, nbits)
    links = list(zip(dp_peers, dp_bits))
    swapped = [links[1], links[0]] + links[2:] if nbits > 1 else links
    half = len(machine) // 2
    mz, mo = machine[:half], machine[half:]
    jobs = [
        Halving(links, model, gz_ref, mz[0], mz[1:-1], fz_ref, mz[-1]),
        Halving(swapped, model, go_ref, mo[0], mo[1:-1], fo_ref, mo[-1]),
    ]
    last_step = nloc_static * spans - 1

    place = (twin, peers, ncore)
    some = pl.ds(0, nloc_static - 1)
    bo_spread = Spread(bo_ref.at[some], boy_ref, bot_ref, boty_ref, bo_sems, place)

    def corr_spread(i):
        return Spread(
            corr_ref.at[i], cy_ref.at[:, i], ct_ref.at[i], cty_ref.at[:, i], c_sems.at[:, i], place
        )

    def dh_copies():
        return [
            remote(
                dh_scr.at[pl.ds(pl.multiple_of(ys[d] * Ry, Ry), Ry)],
                dh_in.at[seq - 1, d],
                y_sems.at[0, seq - 1, d],
                y_sems.at[1, seq - 1, d],
                peers[d],
            )
            for d in range(ny - 1)
        ]

    def x_copy():
        return pltpu.make_async_copy(x_ref.at[core * nloc_static + seq - 1, yy], x_own, local.at[0])

    @pl.when(step == 0)
    def _():
        greet(peers + dp_peers + ([twin] if ncore == 2 else []))
        start(bo_spread.first())
        acc_scr[...] = jnp.zeros_like(acc_scr)
        end_scr[...] = jnp.zeros_like(end_scr)
        pick = row_iota((width, L)) // HEAD == lane_iota((width, L))
        pick_scr[...] = pick.astype(f32).astype(bf16)
        gx_ref[...] = jnp.zeros_like(gx_ref)
        gbc_ref[...] = jnp.zeros_like(gbc_ref)
        gdt_ref[...] = jnp.zeros_like(gdt_ref)
        gpre_ref[...] = jnp.zeros_like(gpre_ref)

    when = [0.0, 0.25, 0.33, 0.58, 0.67, 0.83]
    if nbits != 3:
        when = [j / (2 * nbits) for j in range(2 * nbits)]
    for j in range(2 * nbits):

        @pl.when(step == int(when[j] * (last_step + 1) + 0.1))
        def _(j=j):
            for job in jobs:
                job.close(j)
            for job in jobs:
                job.begin(j)

    @pl.when(step == spans + 2)
    def _():
        wait(bo_spread.first())
        start(bo_spread.second())

    for i in range(nloc_static - 2):

        @pl.when(step == (i + 2) * spans + 2)
        def _(i=i):
            wait(corr_spread(i).first())
            start(corr_spread(i).second())

    @pl.when(jnp.logical_and(seq > 0, back == 0))
    def _():
        for copy in dh_copies():
            copy.start()
        x_copy().start()

    @pl.when(jnp.logical_and(seq > 0, back == spans - 1))
    def _():
        for copy in dh_copies():
            copy.wait()
        x_copy().wait()

        @pl.loop(0, Ry // 32)
        def _(i):
            rows = pl.ds(pl.multiple_of(i * 32, 32), 32)
            mine = pl.ds(pl.multiple_of(yy * Ry + i * 32, 32), 32)
            dh = dh_scr[mine, :].astype(f32)
            for d in range(ny - 1):
                dh = dh + dh_in[seq - 1, d, rows, :].astype(f32)
            corr_ref[seq - 1, rows, :] = correction(x_own[rows, :], dh, gain_ref[...]).astype(bf16)

        start(corr_spread(seq - 1).first())

    hp = hp_ref[...]

    @pl.when(back == 0)
    def _():
        ds_scr[...] = jnp.zeros_like(ds_scr)
        nx_scr[...] = jnp.zeros_like(nx_scr)
        nbc_scr[...] = jnp.zeros_like(nbc_scr)

        @pl.loop(0, spans)
        def _(c):
            t0 = pl.multiple_of(c * L, L)
            for half in range(2):
                lanes = slice(half * L, half * L + L)
                v = conv(bcl_ref, t0, wbc_scr.at[half], lanes, bcp_ref[0:4, lanes], bcp_ref[4:5, lanes])
                bcc_scr[pl.ds(t0, L), lanes] = v
                bca_scr[pl.ds(t0, L), lanes] = (v * sigmoid(v)).astype(bf16)

    def one_chunk():
        c = spans - 1 - back
        t0 = pl.multiple_of(c * L, L)
        rows = pl.ds(t0, L)
        lane = lane_iota((L, L))
        lo = lane < HEAD
        mlo = (lane_iota((1, L)) < HEAD).astype(bf16)
        mhi = (lane_iota((1, L)) >= HEAD).astype(bf16)
        tri = row_iota((L, L)) >= lane
        pre, dt, cum, cum_t = span_decay(dtl_ref[rows, :], hp)
        bm = bca_scr[rows, 0:L]
        cm = bca_scr[rows, L : 2 * L]
        both = nt(cm, bm)
        sb = sin_ref[c]
        dsb_scr[...] = ds_scr[...].astype(bf16)
        cs_scr[...] = nn(cm, sb)
        bds_scr[...] = nn(bm, dsb_scr[...])
        d_both = jnp.zeros((L, L), f32)
        for p in range(pairs):
            lanes = slice(p * L, p * L + L)
            taps = prm_ref[0:4, lanes]
            xc = conv(xl_ref, t0, wx_scr.at[p], lanes, taps, prm_ref[4:5, lanes])
            sg = sigmoid(xc)
            x = xc * sg
            h0, h1 = 2 * p, 2 * p + 1
            a0, a1 = spread(cum, h0), spread(cum, h1)
            ap = jnp.where(lo, a0, a1)
            e0 = jnp.exp2(jnp.where(tri, a0 - cum_t[h0 : h0 + 1], -jnp.inf))
            e1 = jnp.exp2(jnp.where(tri, a1 - cum_t[h1 : h1 + 1], -jnp.inf))
            k0 = (both * e0).astype(bf16)
            k1 = (both * e1).astype(bf16)
            dtp = jnp.where(lo, spread(dt, h0), spread(dt, h1))
            xdt = x * dtp
            xb = xdt.astype(bf16)
            bdx = jnp.concatenate([xb * mlo, xb * mhi], axis=0)
            ecum = jnp.exp2(ap)
            fin = ap[L - 1 : L]
            sd = jnp.exp2(fin - ap)
            y = nn(jnp.concatenate([k0, k1], axis=1), bdx) + ecum * cs_scr[:, lanes]
            dyb = dy_ref[rows, lanes]
            dy = dyb.astype(f32)
            dk = nt(dyb, bdx)
            d_both = d_both + dk[:, 0:L] * e0 + dk[:, L : 2 * L] * e1
            bdy = jnp.concatenate([dyb * mlo, dyb * mhi], axis=0)
            near = tn(jnp.concatenate([k0, k1], axis=0), bdy)
            far = sd * bds_scr[:, lanes]
            dxdt = near + far
            v = dy * y - xb.astype(f32) * near
            u = dxdt * x
            w = xdt * far
            ends = jnp.exp2(fin)
            through = ends * jnp.sum(sb[:, lanes].astype(f32) * ds_scr[:, lanes], axis=0, keepdims=True)
            v_hi = v.astype(bf16)
            red_scr[0:L, lanes] = v_hi
            red_scr[L : 2 * L, lanes] = (v - v_hi.astype(f32)).astype(bf16)
            red_scr[2 * L : 3 * L, lanes] = u.astype(bf16)
            red_scr[3 * L : 4 * L, lanes] = w.astype(bf16)
            end_scr[0:1, lanes] = through
            dx = dxdt * dtp + dy * prm_ref[5:6, lanes]
            dxc = dx * (sg + x * (1.0 - sg))
            for k in range(4):
                gx_ref[k, :, lanes] += fold_rows(dxc * tap(wx_scr.at[p], k))
            gx_ref[4, :, lanes] += fold_rows(dxc)
            gx_ref[5, :, lanes] += fold_rows(dy * x)
            nx_scr[p, L : L + 8] = nx_scr[p, 0:8]
            nx_scr[p, 0:L] = dxc
            dxl = dxc * taps[3:4]
            for k in range(3):
                dxl = dxl + nx_scr[p, 3 - k : 3 - k + L] * taps[k : k + 1]
            d_scr[rows, lanes] = dxl.astype(bf16)
            xs_scr[:, lanes] = (xdt * sd).astype(bf16)
            dye_scr[:, lanes] = (dy * ecum).astype(bf16)
            ds_scr[:, lanes] = ds_scr[:, lanes] * ends
        ds_scr[...] += nn(cm.T, dye_scr[...])
        sums = nn(red_scr[...], pick_scr[...])
        d_cum = sums[0:L] + sums[L : 2 * L]
        d_dt = sums[2 * L : 3 * L]
        d_far = sums[3 * L : 4 * L]
        d_end = exact(end_scr[...], pick_scr[...].astype(f32))[0:1]
        utri = (row_iota((L, L)) <= lane).astype(f32)
        before = (row_iota((L, L)) > lane).astype(f32)
        d_a = exact(utri, d_cum) + exact(before, d_far) + d_end
        d_dt = d_dt + d_a * hp[1:2]
        d_pre = d_dt * sigmoid(pre)
        gdt_ref[0] += fold_rows(d_pre)
        gdt_ref[1] += fold_rows(d_a * dt * hp[1:2])
        d_scr[rows, width + 256 : width + 384] = d_pre.astype(bf16)
        dgb = d_both.astype(bf16)
        d_c = nt(dye_scr[...], sb) + nn(dgb, bm)
        d_b = nt(xs_scr[...], dsb_scr[...]) + nn(dgb.T, cm)
        for half, dv in ((0, d_b), (1, d_c)):
            lanes = slice(half * L, half * L + L)
            pre_act = bcc_scr[rows, lanes]
            sg = sigmoid(pre_act)
            dvc = dv * (sg + pre_act * sg * (1.0 - sg))
            wbc_scr[half] = bcl_ref[pl.ds(t0, L + PAD), lanes]
            for k in range(4):
                gbc_ref[k, :, lanes] += fold_rows(dvc * tap(wbc_scr.at[half], k))
            gbc_ref[4, :, lanes] += fold_rows(dvc)
            nbc_scr[half, L : L + 8] = nbc_scr[half, 0:8]
            nbc_scr[half, 0:L] = dvc
            dvl = dvc * bcp_ref[3:4, lanes]
            for k in range(3):
                dvl = dvl + nbc_scr[half, 3 - k : 3 - k + L] * bcp_ref[k : k + 1, lanes]
            d_scr[rows, width + half * L : width + half * L + L] = dvl.astype(bf16)

    one_chunk()

    @pl.when(back == spans - 1)
    def _():
        @pl.loop(0, model // 256)
        def _(j):
            cols = pl.ds(pl.multiple_of(j * 256, 256), 256)
            dh = nt(dz_ref[:, 0:own], wz_ref[cols, :]) + nt(d_scr[:, 0:own], wx_ref[cols, :])
            if ncore == 2:
                dh = dh + nt(dz_ref[:, own:width], wzo_ref[cols, :])
                dh = dh + nt(d_scr[:, own:width], wxo_ref[cols, :])
            dh = dh + nt(d_scr[:, width : width + 256], wbc_ref[cols, :])
            dh = dh + nt(d_scr[:, width + 256 :], wdt_ref[cols, :])
            dh_scr[:, cols] = dh.astype(bf16)
            gpre_ref[:, cols] += fold_rows(dh * hid_ref[:, cols].astype(f32))
            acc_scr[cols, :] += tn(hid_ref[:, cols], d_scr[...])

    @pl.when(step == last_step)
    def _():
        tail = acc_scr[:, width + 256 : width + 384]
        if ncore == 2:
            send_scr[:, 0:own] = acc_scr[:, own:width].astype(bf16)
            send_scr[:, own : own + L] = tail.astype(bf16)
        dh_ref[...] = dh_scr[...]
        gbcw_ref[...] = acc_scr[:, width : width + 256].astype(gbcw_ref.dtype)
        if ncore == 2:
            copy = remote(send_scr, recv_scr, core_send, core_recv, twin)
            copy.start()
        rows = [jnp.sum(gx_ref[k], axis=0, keepdims=True) for k in range(6)]
        rows.append(jnp.sum(ggg_ref[...], axis=0, keepdims=True))
        dts = [jnp.sum(gdt_ref[k], axis=0, keepdims=True) for k in range(2)]
        small_ref[...] = jnp.zeros_like(small_ref)
        other_ref[...] = jnp.zeros_like(other_ref)
        for k in range(7):
            small_ref[k : k + 1, :] = rows[k][:, 0:own]
            if ncore == 2:
                other_ref[k : k + 1, :] = rows[k][:, own:width]
        for k in range(2):
            small_ref[7 + k : 8 + k, 0:L] = dts[k]
            if ncore == 2:
                moved = pltpu.roll(jnp.broadcast_to(dts[k], (8, L)), L - heads, axis=1)
                other_ref[7 + k : 8 + k, 0:L] = moved[0:1]
        shared_ref[...] = jnp.zeros_like(shared_ref)
        shared_ref[0:1, :] = jnp.sum(gpre_ref[...], axis=0, keepdims=True) / gain_ref[...]
        for k in range(5):
            shared_ref[k + 1 : k + 2, 0:256] = jnp.sum(gbc_ref[k], axis=0, keepdims=True)
        if ncore == 2:
            copy.wait()
            theirs = recv_scr[...].astype(f32)
            gw_ref[:, 0:own] = (acc_scr[:, 0:own] + theirs[:, 0:own]).astype(bf16)
            tail = tail + pltpu.roll(theirs[:, own : own + L], L - heads, axis=1)
        else:
            gw_ref[:, 0:own] = acc_scr[:, 0:own].astype(bf16)
        gw_ref[:, own : own + L] = tail.astype(bf16)
        final = corr_spread(nloc_static - 2)
        wait(final.first())
        start(final.second())
        wait(bo_spread.second())
        for i in range(nloc_static - 1):
            wait(corr_spread(i).second())
        for job in jobs:
            job.close(2 * nbits)


def tail_kernel(
    own,
    ncore,
    ny,
    ndp,
    nloc,
    gw_ref,
    gbcw_ref,
    small_ref,
    other_ref,
    shared_ref,
    dh_ref,
    gain_ref,
    x_ref,
    bo_ref,
    fw_ref,
    fb_ref,
    small_out,
    shared_out,
    last_ref,
    ly_ref,
    lt_ref,
    lty_ref,
    boy_ref,
    bot_ref,
    boty_ref,
    dh_in,
    x_own,
    small_in,
    core_sems,
    y_sems,
    l_sems,
    bo_sems,
    local,
    *machine,
):
    model = gw_ref.shape[0]
    Ry = x_own.shape[0]
    core, yy, twin, ys, peers = places(ncore, ny)
    nbits = log2(ndp)
    dp_peers, dp_bits = bit_peers("dp", 1, 0, nbits)
    t_peers, t_bits = bit_peers("tensor", 1, 0, log2(ncore * ny))
    links = list(zip(dp_peers, dp_bits))
    swapped = [links[1], links[0]] + links[2:] if nbits > 1 else links
    t_links = list(zip(t_peers, t_bits))
    per = nbits + 2
    a, b = machine[:per], machine[per : 2 * per]
    per_bc = nbits + len(t_links) + 2
    c = machine[2 * per : 2 * per + per_bc]
    sm, sh = machine[2 * per + per_bc : 2 * per + per_bc + 3], machine[2 * per + per_bc + 3 :]
    mid = model // 2
    job_a = Halving(links, mid, gw_ref.at[0:mid], a[0], a[1:-1], fw_ref.at[0:mid], a[-1])
    job_b = Halving(swapped, mid, gw_ref.at[mid:model], b[0], b[1:-1], fw_ref.at[mid:model], b[-1])
    job_c = Halving(t_links + links, model, gbcw_ref, c[0], c[1:-1], fb_ref, c[-1])
    job_sm = Doubling(dp_peers, *sm)
    job_sh = Doubling(t_peers + dp_peers, *sh)

    def dh_copies():
        return [
            remote(
                dh_ref.at[pl.ds(pl.multiple_of(ys[d] * Ry, Ry), Ry)],
                dh_in.at[d],
                y_sems.at[0, d],
                y_sems.at[1, d],
                peers[d],
            )
            for d in range(ny - 1)
        ]

    place = (twin, peers, ncore)
    late = Spread(last_ref, ly_ref, lt_ref, lty_ref, l_sems, place)
    ready = [Spread(bo_ref.at[nloc - 1], boy_ref, bot_ref, boty_ref, bo_sems, place)]
    x_copy = pltpu.make_async_copy(x_ref.at[core * nloc + nloc - 1, yy], x_own, local.at[0])
    others = peers + ([twin] if ncore == 2 else [])
    greet(others + dp_peers)
    x_copy.start()

    def turn(*pairs):
        for job, j in pairs:
            job.close(j)
        for job, j in pairs:
            job.begin(j)

    job_sh.acc[0] = shared_ref[...]
    turn((job_sh, 0), (job_c, 0), (job_a, 0), (job_b, 0))
    if ncore == 2:
        small_copy = remote(other_ref, small_in, core_sems.at[0], core_sems.at[1], twin)
        small_copy.start()
    turn((job_c, 1), (job_sh, 1))
    start(dh_copies())
    for spread in ready:
        start(spread.first())
    if ncore == 2:
        small_copy.wait()
        job_sm.acc[0] = small_ref[...] + small_in[...]
    else:
        job_sm.acc[0] = small_ref[...]
    turn((job_sm, 0))
    steps = [
        (job_c, iter(range(2, 2 * job_c.n + 1))),
        (job_sm, iter(range(1, len(job_sm.peers) + 1))),
        (job_sh, iter(range(2, len(job_sh.peers) + 1))),
    ]

    def smaller():
        found = []
        for job, left in steps:
            j = next(left, None)
            if j is not None:
                found.append((job, j))
        return found

    turn(*smaller(), (job_a, 1), (job_b, 1))
    for copy in dh_copies():
        copy.wait()
    x_copy.wait()

    @pl.loop(0, Ry // 32)
    def _(i):
        rows = pl.ds(pl.multiple_of(i * 32, 32), 32)
        mine = pl.ds(pl.multiple_of(yy * Ry + i * 32, 32), 32)
        dh = dh_ref[mine, :].astype(f32)
        for d in range(ny - 1):
            dh = dh + dh_in[d, rows, :].astype(f32)
        last_ref[rows, :] = correction(x_own[rows, :], dh, gain_ref[...]).astype(bf16)

    turn(*smaller())
    start(late.first())
    for j in range(2, 2 * nbits + 1):
        turn(*smaller())
        turn(*smaller(), (job_a, j), (job_b, j))
    for spread in ready:
        wait(spread.first())
        start(spread.second())
    for _ in range(2 * job_c.n):
        turn(*smaller())
    small_out[...] = job_sm.acc[len(job_sm.peers)]
    shared_out[...] = job_sh.acc[len(job_sh.peers)]
    wait(late.first())
    start(late.second())
    for spread in ready + [late]:
        wait(spread.second())


def finish_kernel(pieces, nloc, _idx, g_ref, *refs):
    gi_ref, bo_ref = refs[-2:]
    groups = [refs[n * pieces : (n + 1) * pieces] for n in range(4)]
    now = pl.program_id(1)
    for k in range(pieces):
        here = pl.program_id(0) == k

        def when(turn, here=here):
            return pl.when(jnp.logical_and(here, turn))

        for n, turn in ((0, now < nloc - 1), (1, now == nloc - 1)):

            @when(turn)
            def _(src=groups[n][k]):
                gi_ref[...] = g_ref[...].astype(f32) + src[...].astype(f32)

        for n, turn in ((2, now < nloc - 1), (3, now == nloc - 1)):

            @when(turn)
            def _(src=groups[n][k]):
                bo_ref[...] = src[...]


def unpack_kernel(own, heads, gz_ref, go_ref, gw_ref, fb_ref, small_ref, shared_ref, *outs):
    gzx_ref, gwo_ref, gwdt_ref, gwbc_ref = outs[:4]
    gcxw_ref, gcxb_ref, gd_ref, ggg_ref, gdtb_ref, galog_ref, gpre_ref, gcbw_ref, gcbb_ref = outs[4:]
    gzx_ref[:, 0, :] = gz_ref[...].astype(f32)
    gzx_ref[:, 1, :] = gw_ref[:, 0:own].astype(f32)
    gwdt_ref[...] = gw_ref[:, own : own + L].astype(f32)[:, 0:heads]
    gwbc_ref[...] = fb_ref[...].astype(f32)
    v = go_ref[...].astype(f32)
    for k in range(own // L):
        gwo_ref[k * L : k * L + L, :] = v[:, k * L : k * L + L].T

    @pl.when(pl.program_id(0) == 0)
    def _():
        gcxw_ref[...] = small_ref[0:4]
        gcxb_ref[...] = small_ref[4:5]
        ggg_ref[...] = small_ref[6:7]
        gdtb_ref[...] = small_ref[7:8, 0:heads]
        galog_ref[...] = small_ref[8:9, 0:heads]
        pick = (row_iota((own, L)) // HEAD == lane_iota((own, L))).astype(f32)
        gd_ref[...] = exact(small_ref[0:8], pick)[5:6, 0:heads]
        gpre_ref[...] = shared_ref[0:1]
        gcbw_ref[...] = shared_ref[1:5, 0:256]
        gcbb_ref[...] = shared_ref[5:6, 0:256]


def seq_spec(*shape):
    zeros = (0,) * len(shape)
    return pl.BlockSpec((None,) + shape, lambda i, s: (i,) + zeros)


def moved_spec(ncore, nloc, *shape):
    zeros = (0,) * len(shape)

    def index(i, s):
        return (i + lax.rem(lax.axis_index("tensor"), ncore) * nloc,) + zeros

    return pl.BlockSpec((None,) + shape, index)


def whole_spec(*shape):
    zeros = (0,) * len(shape)
    return pl.BlockSpec(shape, lambda *_: zeros, pipeline_mode=pl.Buffered(1))


def call(
    kernel, grid, in_specs, out_specs, out_shape, scratch, name, flops=0, moved=0, group=None
):
    return pl.pallas_call(
        kernel,
        grid_spec=pltpu.PrefetchScalarGridSpec(
            num_scalar_prefetch=1,
            grid=grid,
            in_specs=in_specs,
            out_specs=out_specs,
            scratch_shapes=scratch,
        ),
        out_shape=out_shape,
        cost_estimate=pl.CostEstimate(
            flops=int(flops), bytes_accessed=int(moved), transcendentals=0
        ),
        name=name,
        compiler_params=None
        if group is None
        else pltpu.CompilerParams(collective_id=group, has_side_effects=True),
    )


def sds(*shape, dtype=f32):
    return jax.ShapeDtypeStruct(shape, dtype)


def body(
    block_input,
    pre_gain,
    w_zx,
    w_bc,
    w_dt,
    conv_x_w,
    conv_x_b,
    conv_bc_w,
    conv_bc_b,
    dt_bias,
    a_log,
    d_skip,
    gate_gain,
    w_out,
    out_grad,
):
    tok, model = block_input.shape
    own = w_zx.shape[2]
    heads = w_dt.shape[1]
    nt = lax.axis_size("tensor")
    ndp = lax.axis_size("dp")
    inner_total = own * nt
    ncore = 2 if nt % 2 == 0 else 1
    ny = nt // ncore
    width = own * ncore
    t = lax.axis_index("tensor")
    core, yy = t % ncore, t // ncore
    R = SEQ_LEN
    Ry = R // ny
    nseq = tok // R
    nloc = nseq // ncore
    spans = R // L
    wtot = 2 * width + 384
    pairs = width // L

    x3 = block_input.reshape(nseq, R, model)
    g3 = out_grad.reshape(nseq, R, model)
    x4 = block_input.reshape(nseq, ny, Ry, model)
    g4 = out_grad.reshape(nseq, ny, Ry, model)
    wz, wx = w_zx[:, 0], w_zx[:, 1]
    sm = jnp.concatenate(
        [
            conv_x_w,
            conv_x_b[None],
            jnp.repeat(d_skip, HEAD)[None],
            gate_gain[None],
            jnp.zeros((1, own), f32),
            jnp.pad(jnp.stack([dt_bias, -jnp.exp(a_log)]), ((0, 6), (0, own - heads))),
        ],
        axis=0,
    )
    wdt = jnp.pad(w_dt, ((0, 0), (0, L - heads)))
    bcp = jnp.concatenate([conv_bc_w, conv_bc_b[None], jnp.zeros((3, 256), f32)], axis=0)
    gain = pre_gain[None]
    seq0 = jnp.zeros((1,), jnp.int32)
    any_spec = pl.BlockSpec(memory_space=pl.ANY)
    nother = max(ny - 1, 1)
    dma = pltpu.SemaphoreType.DMA

    hid, z, xl, bcl, dtl, u, y, sin, st, stot, po, bo01, prm, hp, wdt, wzo, wxo = call(
        partial(forward_kernel, own, heads, ncore, ny, inner_total, nloc),
        (nloc,),
        [
            moved_spec(ncore, nloc, R, model),
            moved_spec(ncore, nloc, R, model),
            whole_spec(1, model),
            whole_spec(model, own),
            whole_spec(model, own),
            whole_spec(model, 256),
            whole_spec(model, L),
            whole_spec(own, model),
            whole_spec(16, own),
            whole_spec(8, 256),
            any_spec,
        ],
        [
            seq_spec(R, model),
            seq_spec(R, width),
            seq_spec(R + PAD, width),
            seq_spec(R + PAD, 256),
            seq_spec(R, L),
            seq_spec(R, width),
            seq_spec(R, width),
            seq_spec(spans, L, width),
            whole_spec(nloc, 2, R),
            whole_spec(nloc, 2, R),
            whole_spec(R, model),
            whole_spec(nloc - 1, Ry, model),
            whole_spec(8, width),
            whole_spec(8, L),
            whole_spec(model, L),
        ]
        + [any_spec] * 2,
        [
            sds(nloc, R, model, dtype=bf16),
            sds(nloc, R, width, dtype=bf16),
            sds(nloc, R + PAD, width),
            sds(nloc, R + PAD, 256),
            sds(nloc, R, L),
            sds(nloc, R, width, dtype=bf16),
            sds(nloc, R, width, dtype=bf16),
            sds(nloc, spans, L, width, dtype=bf16),
            sds(nloc, 2, R),
            sds(nloc, 2, R),
            sds(R, model, dtype=bf16),
            sds(nloc - 1, Ry, model, dtype=bf16),
            sds(8, width),
            sds(8, L),
            sds(model, L, dtype=bf16),
            sds(model, own, dtype=bf16),
            sds(model, own, dtype=bf16),
        ],
        [
            pltpu.VMEM((R, width), f32),
            pltpu.VMEM((R, width), f32),
            pltpu.VMEM((R, width), bf16),
            pltpu.VMEM((R, 256), bf16),
            pltpu.VMEM((L, width), f32),
            pltpu.VMEM((L, width), f32),
            pltpu.VMEM((L, width), bf16),
            pltpu.VMEM((pairs, L + PAD, L), f32),
            pltpu.VMEM((2, L + PAD, L), f32),
            pltpu.VMEM((model, own), bf16),
            pltpu.VMEM((model, own), bf16),
            pltpu.VMEM((own, model), bf16),
            pltpu.VMEM((model, L), bf16),
            pltpu.VMEM((16, own), f32),
            pltpu.VMEM((2, R, model), bf16),
            pltpu.VMEM((nloc - 1, nother, Ry, model), bf16),
            pltpu.VMEM((nloc - 1, nother, 2, R), f32),
            pltpu.VMEM((Ry, model), bf16),
            dma((2, 5)),
            dma((2, nloc - 1, nother)),
            dma((2, nloc - 1, nother)),
            dma((3,)),
        ],
        "forward",
        2 * nloc * R * model * (wtot + 2 * width),
        nloc * R * (6 * model + 20 * width),
        4,
    )(seq0, x3, g3, gain, wz, wx, w_bc, wdt, w_out, sm, bcp, x4)

    nbits = log2(ndp)
    dz, dy, gz, go, ggg, bo = call(
        partial(gate_kernel, width, own, inner_total, ncore, ny),
        (nloc,),
        [
            whole_spec(nloc, 2, R),
            whole_spec(nloc, 2, R),
            moved_spec(ncore, nloc, R, model),
            whole_spec(nloc, R, model),
            seq_spec(R, width),
            seq_spec(R, width),
            seq_spec(R, width),
            whole_spec(8, width),
            whole_spec(R, model),
            whole_spec(nloc - 1, Ry, model),
            any_spec,
        ],
        [
            seq_spec(R, width),
            seq_spec(R, width),
            whole_spec(model, own),
            whole_spec(model, own),
            whole_spec(8, width),
            whole_spec(nloc, Ry, model),
        ],
        [
            sds(nloc, R, width, dtype=bf16),
            sds(nloc, R, width, dtype=bf16),
            sds(model, own, dtype=bf16),
            sds(model, own, dtype=bf16),
            sds(8, width),
            sds(nloc, Ry, model, dtype=bf16),
        ],
        [
            pltpu.VMEM((nloc, R, width), bf16),
            pltpu.VMEM((nloc, R, model), bf16),
            pltpu.VMEM((nloc, R, width), bf16),
            pltpu.VMEM((nloc, 2, R), f32),
            pltpu.VMEM((nother, 2, R), f32),
            pltpu.VMEM((model, 2 * own), bf16),
            pltpu.VMEM((model, 2 * own), bf16),
            pltpu.VMEM((nother, Ry, model), bf16),
            pltpu.VMEM((Ry, model), bf16),
            dma((2, nother)),
            dma,
            dma,
            dma((2, nother)),
            dma((1,)),
        ],
        "gate",
        4 * nloc * R * model * width,
        nloc * R * (4 * model + 16 * width),
        1,
    )(seq0, st, stot, g3, hid, z, y, u, prm, po, bo01, x4)

    def chunk_spec(*shape):
        zeros = (0,) * len(shape)
        return pl.BlockSpec((None,) + shape, lambda i, b, s: (i,) + zeros)

    bc_type = bf16 if (model // (nt * ndp)) % 16 == 0 else f32
    dh, gw2, gbcw, small, other, shared, corr, fz, fo, boy, bot, boty, cy0, ct0, cty0 = call(
        partial(scan_kernel, width, own, heads, ncore, ny, ndp, nloc),
        (nloc, spans),
        [
            chunk_spec(R, model),
            chunk_spec(R, width),
            chunk_spec(R, width),
            chunk_spec(R + PAD, width),
            chunk_spec(R + PAD, 256),
            chunk_spec(R, L),
            chunk_spec(spans, L, width),
            whole_spec(model, own),
            whole_spec(model, own),
            whole_spec(model, own),
            whole_spec(model, own),
            whole_spec(model, 256),
            whole_spec(model, L),
            whole_spec(8, width),
            whole_spec(8, 256),
            whole_spec(8, L),
            whole_spec(8, width),
            whole_spec(1, model),
            whole_spec(model, own),
            whole_spec(model, own),
            any_spec,
            any_spec,
        ],
        [
            whole_spec(R, model),
            whole_spec(model, own + L),
            whole_spec(model, 256),
            whole_spec(16, own),
            whole_spec(16, own),
            whole_spec(8, model),
            whole_spec(nloc - 1, Ry, model),
        ]
        + [any_spec] * 8,
        [
            sds(R, model, dtype=bf16),
            sds(model, own + L, dtype=bf16),
            sds(model, 256, dtype=bc_type),
            sds(16, own),
            sds(16, own),
            sds(8, model),
            sds(nloc - 1, Ry, model, dtype=bf16),
            sds(model, own, dtype=bf16),
            sds(model, own, dtype=bf16),
            sds(nother, nloc - 1, Ry, model, dtype=bf16),
            sds(nloc - 1, Ry, model, dtype=bf16),
            sds(nother, nloc - 1, Ry, model, dtype=bf16),
            sds(nother, nloc - 1, Ry, model, dtype=bf16),
            sds(nloc - 1, Ry, model, dtype=bf16),
            sds(nother, nloc - 1, Ry, model, dtype=bf16),
        ],
        [
            pltpu.VMEM((R, width + 384), bf16),
            pltpu.VMEM((R, 256), f32),
            pltpu.VMEM((R, 256), bf16),
            pltpu.VMEM((L, width), f32),
            pltpu.VMEM((L, width), bf16),
            pltpu.VMEM((L, width), f32),
            pltpu.VMEM((L, width), f32),
            pltpu.VMEM((L, width), bf16),
            pltpu.VMEM((L, width), bf16),
            pltpu.VMEM((pairs, L + 8, L), f32),
            pltpu.VMEM((2, L + 8, L), f32),
            pltpu.VMEM((pairs, L + PAD, L), f32),
            pltpu.VMEM((2, L + PAD, L), f32),
            pltpu.VMEM((4 * L, width), bf16),
            pltpu.VMEM((8, width), f32),
            pltpu.VMEM((width, L), bf16),
            pltpu.VMEM((6, 8, width), f32),
            pltpu.VMEM((5, 8, 256), f32),
            pltpu.VMEM((2, 8, L), f32),
            pltpu.VMEM((8, model), f32),
            pltpu.VMEM((model, width + 384), f32),
            pltpu.VMEM((model, own + L), bf16),
            pltpu.VMEM((model, own + L), bf16),
            pltpu.VMEM((R, model), bf16),
            pltpu.VMEM((nloc - 1, nother, Ry, model), bf16),
            pltpu.VMEM((Ry, model), bf16),
            dma,
            dma,
            dma((2, nloc - 1, nother)),
            dma((2, 2 * ny)),
            dma((2, nloc - 1, 2 * ny)),
            dma((1,)),
        ]
        + Halving.scratch(model, own, nbits, bf16)
        + Halving.scratch(model, own, nbits, bf16),
        "scan_back",
        2 * nloc * R * model * (2 * wtot),
        nloc * R * (4 * model + 12 * width),
        2,
    )(seq0, hid, dz, dy, xl, bcl, dtl, sin, wz, wzo, wx, wxo, w_bc, wdt, prm, bcp, hp, ggg, gain, gz, go, bo, x4)

    vm = pl.BlockSpec(memory_space=pltpu.VMEM)
    tbits = log2(nt)
    late_shape = sds(nother, Ry, model, dtype=bf16)
    fw, fb, small, shared, last, *late_got = pl.pallas_call(
        partial(tail_kernel, own, ncore, ny, ndp, nloc),
        in_specs=[vm] * 7 + [any_spec] * 2,
        out_specs=[any_spec] * 2 + [vm] * 3 + [any_spec] * 6,
        out_shape=[
            sds(model, own + L, dtype=bf16),
            sds(model, 256, dtype=bc_type),
            sds(16, own),
            sds(8, model),
            sds(Ry, model, dtype=bf16),
        ]
        + [late_shape, sds(Ry, model, dtype=bf16), late_shape] * 2,
        scratch_shapes=[
            pltpu.VMEM((nother, Ry, model), bf16),
            pltpu.VMEM((Ry, model), bf16),
            pltpu.VMEM((16, own), f32),
            dma((2,)),
            dma((2, nother)),
            dma((2, 2 * ny)),
            dma((2, 2 * ny)),
            dma((1,)),
        ]
        + Halving.scratch(model // 2, own + L, nbits, bf16)
        + Halving.scratch(model // 2, own + L, nbits, bf16)
        + Halving.scratch(model, 256, nbits + tbits, bc_type)
        + Doubling.scratch(nbits, 16, own)
        + Doubling.scratch(nbits + tbits, 8, model),
        compiler_params=pltpu.CompilerParams(collective_id=3, has_side_effects=True),
        name="tail",
    )(gw2, gbcw, small, other, shared, dh, gain, x4, bo)

    pieces = ncore * ny
    where = jnp.stack([core, yy]).astype(jnp.int32)

    def out_index(k, i, s):
        return ((s[0] ^ (k // ny)) * nloc + i, (s[1] - k % ny + ny) % ny, 0, 0)

    def spec_of(base, seq_of, d):
        if d is None:
            return pl.BlockSpec(
                (None, Ry, model), lambda j, i, s: (seq_of(j, i) - base, 0, 0)
            )
        return pl.BlockSpec(
            (None, None, Ry, model), lambda j, i, s: (d, seq_of(j, i) - base, 0, 0)
        )

    placed_spec = pl.BlockSpec((None, None, Ry, model), out_index)
    specs, arrays = [], []

    def add_group(first, count, mine, mine_base, toy, tot, toty):
        for k in range(pieces):

            def seq_of(j, i, k=k):
                i = jnp.clip(i, first, first + count - 1)
                return jnp.where(j == k, i, jnp.where(j > k, first + count - 1, first))

            d = k % ny - 1
            if k == 0:
                array, spec = mine, spec_of(mine_base, seq_of, None)
            elif k < ny:
                array, spec = toy, spec_of(first, seq_of, d)
            elif d < 0:
                array, spec = tot, spec_of(first, seq_of, None)
            else:
                array, spec = toty, spec_of(first, seq_of, d)
            arrays.append(array)
            specs.append(spec)

    def as_seq(v, axis):
        return jnp.expand_dims(v, axis)

    def add_late(first, mine, base, got):
        toy, tot, toty = got
        add_group(first, 1, mine, base, as_seq(toy, 1), as_seq(tot, 0), as_seq(toty, 1))

    add_group(0, nloc - 1, corr, 0, cy0, ct0, cty0)
    add_late(nloc - 1, as_seq(last, 0), nloc - 1, late_got[0:3])
    add_group(0, nloc - 1, bo, 0, boy, bot, boty)
    add_late(nloc - 1, bo, 0, late_got[3:6])
    grad_input, block_output = call(
        partial(finish_kernel, pieces, nloc),
        (pieces, nloc),
        [placed_spec] + specs,
        [placed_spec, placed_spec],
        [sds(nseq, ny, Ry, model), sds(nseq, ny, Ry, model, dtype=bf16)],
        [],
        "finish",
        0,
        12 * tok * model,
    )(where, g4, *arrays)

    def row_block(cols):
        return pl.BlockSpec((L, cols), lambda d: (d, 0))

    outs = pl.pallas_call(
        partial(unpack_kernel, own, heads),
        grid=(model // L,),
        in_specs=[row_block(own), row_block(own), row_block(own + L), row_block(256)]
        + [whole_spec(16, own), whole_spec(8, model)],
        out_specs=[
            pl.BlockSpec((L, 2, own), lambda d: (d, 0, 0)),
            pl.BlockSpec((own, L), lambda d: (0, d)),
            row_block(heads),
            row_block(256),
            whole_spec(4, own),
            whole_spec(1, own),
            whole_spec(1, heads),
            whole_spec(1, own),
            whole_spec(1, heads),
            whole_spec(1, heads),
            whole_spec(1, model),
            whole_spec(4, 256),
            whole_spec(1, 256),
        ],
        out_shape=[
            sds(model, 2, own),
            sds(own, model),
            sds(model, heads),
            sds(model, 256),
            sds(4, own),
            sds(1, own),
            sds(1, heads),
            sds(1, own),
            sds(1, heads),
            sds(1, heads),
            sds(1, model),
            sds(4, 256),
            sds(1, 256),
        ],
        name="unpack",
    )(fz, fo, fw, fb, small, shared)
    gzx, gwo, gwdt, gwbc, gcxw, gcxb, gd, ggg, gdtb, galog, gpre, gcbw, gcbb = outs
    return (
        block_output.reshape(tok, model),
        grad_input.reshape(tok, model),
        gpre[0],
        gzx,
        gwbc,
        gwdt,
        gcxw,
        gcxb[0],
        gcbw,
        gcbb[0],
        gdtb[0],
        galog[0],
        gd[0],
        ggg[0],
        gwo,
    )


def solution(mesh):
    placed = (
        P("dp", None),
        P(),
        P(None, None, "tensor"),
        P(),
        P(None, "tensor"),
        P(None, "tensor"),
        P("tensor"),
        P(),
        P(),
        P("tensor"),
        P("tensor"),
        P("tensor"),
        P("tensor"),
        P("tensor", None),
        P("dp", None),
    )
    return jax.shard_map(
        body,
        mesh=mesh,
        in_specs=placed,
        out_specs=(
            P("dp", None),
            P("dp", None),
            P(),
            P(None, None, "tensor"),
            P(),
            P(None, "tensor"),
            P(None, "tensor"),
            P("tensor"),
            P(),
            P(),
            P("tensor"),
            P("tensor"),
            P("tensor"),
            P("tensor"),
            P("tensor", None),
        ),
        check_vma=False,
    )
```

```python
from functools import partial

import jax
import jax.numpy as jnp
from jax import lax
from jax.experimental import pallas as pl
from jax.experimental.pallas import tpu as pltpu
from jax.sharding import PartitionSpec as P

SEQ_LEN = 512
L = 128
HEAD = 64
LOG2E = 1.4426950408889634
PAD = 8
epsilon = 1e-05
f32 = jnp.float32
bf16 = jnp.bfloat16
HI = lax.Precision.HIGHEST
MESH = pl.DeviceIdType.MESH


def nn(a, b):
    return lax.dot_general(a, b, (((1,), (0,)), ((), ())), preferred_element_type=f32)


def nt(a, b):
    return lax.dot_general(a, b, (((1,), (1,)), ((), ())), preferred_element_type=f32)


def tn(a, b):
    return lax.dot_general(a, b, (((0,), (0,)), ((), ())), preferred_element_type=f32)


def exact(a, b):
    return lax.dot_general(
        a, b, (((1,), (0,)), ((), ())), precision=HI, preferred_element_type=f32
    )


def sigmoid(v):
    return 0.5 + 0.5 * jnp.tanh(0.5 * v)


def softplus(v):
    u = jnp.exp(-jnp.abs(v))
    return jnp.maximum(v, 0.0) + jnp.where(u < 1e-3, u - 0.5 * u * u, jnp.log(1.0 + u))


def fold_rows(v):
    return jnp.sum(v.reshape(v.shape[0] // 8, 8, v.shape[1]), axis=0)


def lane_iota(shape):
    return lax.broadcasted_iota(jnp.int32, shape, 1)


def row_iota(shape):
    return lax.broadcasted_iota(jnp.int32, shape, 0)


def tap(win, k):
    return win[PAD - 3 + k : PAD - 3 + k + L, :]


def conv(ref, t0, win, lanes, taps, bias):
    win[...] = ref[pl.ds(t0, L + PAD), lanes]
    total = bias
    for k in range(4):
        total = total + tap(win, k) * taps[k : k + 1]
    return total


def spread(cols, head):
    return jnp.broadcast_to(cols[:, head : head + 1], (L, L))


def span_decay(dtl, hp):
    pre = dtl + hp[0:1]
    dt = softplus(pre)
    ltri = (row_iota((L, L)) >= lane_iota((L, L))).astype(f32)
    cum = exact(ltri, dt * (hp[1:2] * LOG2E))
    return pre, dt, cum, cum.T


def remote(src, dst, send, recv, where):
    return pltpu.make_async_remote_copy(
        src_ref=src,
        dst_ref=dst,
        send_sem=send,
        recv_sem=recv,
        device_id=where,
        device_id_type=MESH,
    )


def greet(peers):
    barrier = pltpu.get_barrier_semaphore()
    for peer in peers:
        pl.semaphore_signal(barrier, inc=1, device_id=peer, device_id_type=MESH)
    pl.semaphore_wait(barrier, len(peers))


def bit_peers(axis, base, first, count):
    me = lax.axis_index(axis)
    peers, bits = [], []
    for k in range(count):
        step = base * 2**k
        bit = lax.rem(me // step, 2)
        peers.append({axis: me + step * (1 - 2 * bit)})
        bits.append(bit)
    return peers, bits


class Halving:
    def __init__(self, links, rows, src, work, recvs, full, sems):
        self.links, self.rows = links, rows
        self.src, self.work, self.recvs, self.full, self.sems = src, work, recvs, full, sems
        self.n = len(links)
        offs, size = [0], rows
        for _, bit in links:
            size //= 2
            offs.append(offs[-1] + bit * size)
        self.offs = offs

    def size(self, k):
        return self.rows >> k

    def at(self, off, size):
        return pl.ds(pl.multiple_of(off, size), size)

    def scatter(self, k):
        peer, bit = self.links[k]
        half = self.size(k + 1)
        off = self.offs[k] + (1 - bit) * half
        if k == 0:
            src = self.src.at[self.at(off, half)]
        else:
            src = self.work.at[self.at(off - self.offs[1], half)]
        return remote(src, self.recvs[k], self.sems.at[0, k], self.sems.at[1, k], peer)

    def fold(self, k):
        self.scatter(k).wait()
        half = self.size(k + 1)
        step = min(half, 64)
        keep = self.offs[k + 1]

        @pl.loop(0, half // step)
        def _(i):
            off = i * step
            rows = pl.ds(pl.multiple_of(off, step), step)
            near = pl.ds(pl.multiple_of(keep - self.offs[1] + off, step), step)
            if k == 0:
                mine = self.src[pl.ds(pl.multiple_of(keep + off, step), step), :]
            else:
                mine = self.work[near, :]
            total = mine.astype(f32) + self.recvs[k][rows, :].astype(f32)
            self.work[near, :] = total.astype(self.work.dtype)

    def own_copy(self):
        last = self.size(self.n)
        return pltpu.make_async_copy(
            self.work.at[self.at(self.offs[self.n] - self.offs[1], last)],
            self.full.at[self.at(self.offs[self.n], last)],
            self.sems.at[0, 2 * self.n],
        )

    def gather(self, k):
        peer, _ = self.links[k]
        rows = self.at(self.offs[k + 1], self.size(k + 1))
        sems = self.sems
        return remote(
            self.full.at[rows],
            self.full.at[rows],
            sems.at[0, self.n + k],
            sems.at[1, self.n + k],
            peer,
        )

    def close(self, j):
        n = self.n
        if 1 <= j <= n:
            self.fold(j - 1)
        elif j > n:
            self.gather(2 * n - j).wait()

    def begin(self, j):
        n = self.n
        if j < n:
            self.scatter(j).start()
            return
        if j == n:
            self.own_copy().start()
            self.own_copy().wait()
        if j < 2 * n:
            self.gather(2 * n - 1 - j).start()

    @staticmethod
    def scratch(rows, cols, n, dtype):
        recvs = [pltpu.VMEM((rows >> (k + 1), cols), dtype) for k in range(n)]
        return [pltpu.VMEM((rows // 2, cols), dtype)] + recvs + [
            pltpu.SemaphoreType.DMA((2, 2 * n + 1))
        ]


class Doubling:
    def __init__(self, peers, acc, recv, sems):
        self.peers, self.acc, self.recv, self.sems = peers, acc, recv, sems

    def copy(self, k):
        return remote(
            self.acc.at[k],
            self.recv.at[k],
            self.sems.at[0, k],
            self.sems.at[1, k],
            self.peers[k],
        )

    def close(self, j):
        if j > 0:
            self.copy(j - 1).wait()
            self.acc[j] = self.acc[j - 1] + self.recv[j - 1]

    def begin(self, j):
        if j < len(self.peers):
            self.copy(j).start()

    @staticmethod
    def scratch(n, rows, cols):
        return [
            pltpu.VMEM((n + 1, rows, cols), f32),
            pltpu.VMEM((n, rows, cols), f32),
            pltpu.SemaphoreType.DMA((2, n)),
        ]


class Spread:
    def __init__(self, src, toy, tot, toty, sems, place):
        self.src, self.toy, self.tot, self.toty, self.sems = src, toy, tot, toty, sems
        self.twin, self.peers, self.ncore = place

    def first(self):
        n = len(self.peers)
        sems = self.sems
        out = [
            remote(self.src, self.toy.at[d], sems.at[0, d], sems.at[1, d], self.peers[d])
            for d in range(n)
        ]
        if self.ncore == 2:
            out.append(remote(self.src, self.tot, sems.at[0, n], sems.at[1, n], self.twin))
        return out

    def second(self):
        n = len(self.peers)
        if self.ncore != 2:
            return []
        sems = self.sems
        return [
            remote(
                self.toy.at[d], self.toty.at[d], sems.at[0, n + 1 + d], sems.at[1, n + 1 + d], self.twin
            )
            for d in range(n)
        ]


def start(copies):
    for copy in copies:
        copy.start()


def wait(copies):
    for copy in copies:
        copy.wait()


def correction(x, dh, gain):
    v = x.astype(f32)
    r = lax.rsqrt(jnp.mean(v * v, axis=1, keepdims=True) + epsilon)
    normed = v * r
    dn = dh * gain
    return r * (dn - normed * jnp.mean(dn * normed, axis=1, keepdims=True))


def places(ncore, ny):
    spot = lax.axis_index("tensor")
    core, yy = lax.rem(spot, ncore), spot // ncore
    ys = [lax.rem(yy + d, ny) for d in range(1, ny)]
    peers = [{"tensor": v * ncore + core} for v in ys]
    return core, yy, {"tensor": spot + 1 - 2 * core}, ys, peers


def log2(n):
    return n.bit_length() - 1


def forward_kernel(
    own,
    heads,
    ncore,
    ny,
    inner_total,
    nloc,
    _seq,
    x_ref,
    g_ref,
    gain_ref,
    wz_ref,
    wx_ref,
    wbc_ref,
    wdt_ref,
    wo_ref,
    sm_ref,
    bcp_ref,
    x4_ref,
    hid_ref,
    z_ref,
    xl_ref,
    bcl_ref,
    dtl_ref,
    u_ref,
    y_ref,
    sin_ref,
    st_ref,
    stot_ref,
    po_ref,
    bo_ref,
    prm_ref,
    hp_ref,
    wdt_out,
    wz_out,
    wx_out,
    z_scr,
    u_scr,
    q_scr,
    bca_scr,
    s_scr,
    cs_scr,
    xs_scr,
    wx_scr,
    wbc_scr,
    wz_in,
    wx_in,
    wo_in,
    wdt_in,
    sm_in,
    po_scr,
    po_in,
    st_in,
    x_own,
    w_sems,
    po_sems,
    st_sems,
    local,
):
    rows_all = x_ref.shape[0]
    model = x_ref.shape[1]
    width = own * ncore
    pairs = width // L
    Ry = rows_all // ny
    here = pl.program_id(0)
    core, yy, twin, ys, peers = places(ncore, ny)

    def weight_copies():
        both = ((sm_ref, sm_in), (wdt_ref, wdt_in), (wz_ref, wz_in), (wx_ref, wx_in), (wo_ref, wo_in))
        return [
            remote(src, dst, w_sems.at[0, k], w_sems.at[1, k], twin)
            for k, (src, dst) in enumerate(both)
        ]

    def weight_stores():
        return [
            pltpu.make_async_copy(wz_in, wz_out, local.at[1]),
            pltpu.make_async_copy(wx_in, wx_out, local.at[2]),
        ]

    def row_copies():
        last = here - 1
        return [
            remote(
                st_ref.at[last],
                st_in.at[last, d],
                st_sems.at[0, last, d],
                st_sems.at[1, last, d],
                peers[d],
            )
            for d in range(ny - 1)
        ] + [
            remote(
                po_scr.at[lax.rem(last, 2), pl.ds(pl.multiple_of(ys[d] * Ry, Ry), Ry)],
                po_in.at[last, d],
                po_sems.at[0, last, d],
                po_sems.at[1, last, d],
                peers[d],
            )
            for d in range(ny - 1)
        ]

    def x_copy():
        return pltpu.make_async_copy(x4_ref.at[core * nloc + here - 1, yy], x_own, local.at[0])

    @pl.when(here == 0)
    def _():
        greet(peers + ([twin] if ncore == 2 else []))
        if ncore == 2:
            for copy in weight_copies():
                copy.start()

    @pl.when(here > 0)
    def _():
        start(row_copies())
        x_copy().start()

    @pl.loop(0, rows_all // 32)
    def _(i):
        rows = pl.ds(pl.multiple_of(i * 32, 32), 32)
        v = x_ref[rows, :].astype(f32)
        r = lax.rsqrt(jnp.mean(v * v, axis=1, keepdims=True) + epsilon)
        hid_ref[rows, :] = (v * r * gain_ref[...]).astype(bf16)

    xl_ref[0:PAD, :] = jnp.zeros((PAD, width), f32)
    bcl_ref[0:PAD, :] = jnp.zeros((PAD, 256), f32)

    def project(wz, wx, wo, base):
        @pl.loop(0, own // 256)
        def _(j):
            src = pl.ds(pl.multiple_of(j * 256, 256), 256)
            cols = pl.ds(pl.multiple_of(base + j * 256, 256), 256)
            z_scr[:, cols] = nn(hid_ref[...], wz[:, src])
            xl_ref[PAD : PAD + rows_all, cols] = nn(hid_ref[...], wx[:, src])
            u_scr[:, cols] = nt(g_ref[...], wo[src, :])

    project(wz_ref, wx_ref, wo_ref, 0)
    bcl_ref[PAD : PAD + rows_all, :] = nn(hid_ref[...], wbc_ref[...])

    @pl.when(here == 0)
    def _():
        prm_ref[:, 0:own] = sm_ref[0:8, :]
        hp_ref[...] = sm_ref[8:16, 0:L]
        wdt_out[...] = wdt_ref[...]
        if ncore == 2:
            for copy in weight_copies():
                copy.wait()
            for copy in weight_stores():
                copy.start()
            prm_ref[:, own : 2 * own] = sm_in[0:8, :]
            hp_ref[...] += pltpu.roll(sm_in[8:16, 0:L], heads, axis=1)
            theirs = pltpu.roll(wdt_in[...].astype(f32), heads, axis=1)
            wdt_out[...] = (wdt_ref[...].astype(f32) + theirs).astype(bf16)

    if ncore == 2:
        project(wz_in, wx_in, wo_in, own)
    dtl_ref[...] = nn(hid_ref[...], wdt_out[...])

    @pl.loop(0, rows_all // L)
    def _(c):
        t0 = pl.multiple_of(c * L, L)
        for half in range(2):
            lanes = slice(half * L, half * L + L)
            v = conv(bcl_ref, t0, wbc_scr.at[half], lanes, bcp_ref[0:4, lanes], bcp_ref[4:5, lanes])
            bca_scr[pl.ds(t0, L), lanes] = (v * sigmoid(v)).astype(bf16)

    s_scr[...] = jnp.zeros_like(s_scr)
    hp = hp_ref[...]

    def block_done():
        wait(row_copies())
        x_copy().wait()
        total = st_ref[here - 1]
        for d in range(ny - 1):
            total = total + st_in[here - 1, d]
        stot_ref[here - 1] = total
        parts = [po_in.at[here - 1, d] for d in range(ny - 1)]
        mine = po_scr.at[lax.rem(here - 1, 2), pl.ds(pl.multiple_of(yy * Ry, Ry), Ry)]
        block_out(inner_total, stot_ref.at[here - 1], yy, mine, parts, x_own, bo_ref.at[here - 1])

    @pl.loop(0, rows_all // L)
    def _(c):
        early = jnp.logical_and(here > 0, here < nloc - 1)

        @pl.when(jnp.logical_and(early, c == rows_all // L - 1))
        def _():
            block_done()

        t0 = pl.multiple_of(c * L, L)
        rows = pl.ds(t0, L)
        lo = lane_iota((L, L)) < HEAD
        mlo = (lane_iota((1, L)) < HEAD).astype(bf16)
        mhi = (lane_iota((1, L)) >= HEAD).astype(bf16)
        tri = row_iota((L, L)) >= lane_iota((L, L))
        _, dt, cum, cum_t = span_decay(dtl_ref[rows, :], hp)
        bm = bca_scr[rows, 0:L]
        cm = bca_scr[rows, L : 2 * L]
        both = nt(cm, bm)
        sb = s_scr[...].astype(bf16)
        sin_ref[c] = sb
        cs_scr[...] = nn(cm, sb)
        squares = jnp.zeros((L, L), f32)
        inner = jnp.zeros((L, L), f32)
        for p in range(pairs):
            lanes = slice(p * L, p * L + L)
            xc = conv(xl_ref, t0, wx_scr.at[p], lanes, prm_ref[0:4, lanes], prm_ref[4:5, lanes])
            x = xc * sigmoid(xc)
            h0, h1 = 2 * p, 2 * p + 1
            a0, a1 = spread(cum, h0), spread(cum, h1)
            ap = jnp.where(lo, a0, a1)
            k0 = both * jnp.exp2(jnp.where(tri, a0 - cum_t[h0 : h0 + 1], -jnp.inf))
            k1 = both * jnp.exp2(jnp.where(tri, a1 - cum_t[h1 : h1 + 1], -jnp.inf))
            xdt = x * jnp.where(lo, spread(dt, h0), spread(dt, h1))
            xb = xdt.astype(bf16)
            fin = ap[L - 1 : L]
            within = nn(
                jnp.concatenate([k0.astype(bf16), k1.astype(bf16)], axis=1),
                jnp.concatenate([xb * mlo, xb * mhi], axis=0),
            )
            y = within + jnp.exp2(ap) * cs_scr[:, lanes] + prm_ref[5:6, lanes] * x
            xs_scr[:, lanes] = (xdt * jnp.exp2(fin - ap)).astype(bf16)
            s_scr[:, lanes] = s_scr[:, lanes] * jnp.exp2(fin)
            y_ref[rows, lanes] = y.astype(bf16)
            z = z_scr[rows, lanes]
            u = u_scr[rows, lanes]
            z_ref[rows, lanes] = z.astype(bf16)
            u_ref[rows, lanes] = u.astype(bf16)
            gated = y * (z * sigmoid(z))
            q = gated * prm_ref[6:7, lanes]
            q_scr[rows, lanes] = q.astype(bf16)
            squares = squares + gated * gated
            inner = inner + u * q
        s_scr[...] += nn(bm.T, xs_scr[...])
        s0 = jnp.sum(squares, axis=1, keepdims=True)
        s1 = jnp.sum(inner, axis=1, keepdims=True)
        lane = lane_iota((L, L))
        stat = jnp.where(lane == 0, s0, jnp.where(lane == 1, s1, 0.0))
        st_ref[here, :, rows] = stat.T[0:2]

    @pl.loop(0, model // 256)
    def _(j):
        cols = pl.ds(pl.multiple_of(j * 256, 256), 256)
        po = nn(q_scr[:, 0:own], wo_ref[:, cols])
        if ncore == 2:
            po = po + nn(q_scr[:, own : 2 * own], wo_in[:, cols])
        po_scr[lax.rem(here, 2), :, cols] = po.astype(bf16)

    @pl.when(here == nloc - 1)
    def _():
        po_ref[...] = po_scr[(nloc - 1) % 2]
        block_done()
        if ncore == 2:
            for copy in weight_stores():
                copy.wait()


def block_out(inner_total, stot, yy, mine, parts, x_own, bo):
    Ry, model = x_own.shape
    for h in range(Ry // L):
        lanes = pl.ds(pl.multiple_of(yy * Ry + h * L, L), L)
        r_row = lax.rsqrt(stot[0:1, lanes] / inner_total + epsilon)
        r = jnp.broadcast_to(r_row, (8, L)).T[:, 0:1]

        @pl.loop(0, model // L)
        def _(m, h=h, r=r):
            cols = pl.ds(pl.multiple_of(m * L, L), L)
            rows = slice(h * L, h * L + L)
            total = mine[rows, cols].astype(f32)
            for part in parts:
                total = total + part[rows, cols].astype(f32)
            bo[rows, cols] = (x_own[rows, cols].astype(f32) + r * total).astype(bf16)


def gate_kernel(
    width,
    own,
    inner_total,
    ncore,
    ny,
    _seq,
    st_ref,
    stin_ref,
    g_ref,
    hid_ref,
    z_ref,
    y_ref,
    u_ref,
    prm_ref,
    po_ref,
    bo01_ref,
    x_ref,
    dz_ref,
    dy_ref,
    gz_ref,
    go_ref,
    ggg_ref,
    bo_ref,
    q_scr,
    sc_scr,
    dz_scr,
    stot_ref,
    st_in,
    send_scr,
    recv_scr,
    po_in,
    x_own,
    st_sems,
    core_send,
    core_recv,
    po_sems,
    local,
):
    rows_all = z_ref.shape[0]
    model = g_ref.shape[1]
    pairs = width // L
    here = pl.program_id(0)
    core, yy, twin, ys, peers = places(ncore, ny)
    nloc, Ry, _ = bo_ref.shape
    last = nloc - 1

    def row_copies():
        return [
            remote(st_ref.at[last], st_in.at[d], st_sems.at[0, d], st_sems.at[1, d], peers[d])
            for d in range(ny - 1)
        ]

    def po_copies():
        return [
            remote(
                po_ref.at[pl.ds(pl.multiple_of(ys[d] * Ry, Ry), Ry)],
                po_in.at[d],
                po_sems.at[0, d],
                po_sems.at[1, d],
                peers[d],
            )
            for d in range(ny - 1)
        ]

    def x_copy():
        return pltpu.make_async_copy(x_ref.at[core * nloc + last, yy], x_own, local.at[0])

    @pl.when(here == 0)
    def _():
        greet(peers + ([twin] if ncore == 2 else []))
        start(row_copies() + po_copies() + [x_copy()])
        stot_ref[...] = stin_ref[...]
        for i in range(last):
            bo_ref[i] = bo01_ref[i]
        ggg_ref[...] = jnp.zeros_like(ggg_ref)

    @pl.when(here == last)
    def _():
        for copy in row_copies():
            copy.wait()
        total = st_ref[last]
        for d in range(ny - 1):
            total = total + st_in[d]
        stot_ref[last] = total

    @pl.loop(0, rows_all // L)
    def _(c):
        rows = pl.ds(pl.multiple_of(c * L, L), L)
        st = stot_ref[here, :, rows]
        r_row = lax.rsqrt(st[0:1] / inner_total + epsilon)
        c_row = r_row * r_row * r_row * (st[1:2] / inner_total)
        cols8 = jnp.concatenate([r_row, c_row, jnp.zeros((6, L), f32)], axis=0).T
        r = jnp.broadcast_to(cols8[:, 0:1], (L, L))
        c2 = jnp.broadcast_to(cols8[:, 1:2], (L, L))
        for m in range(model // L):
            lanes = slice(m * L, m * L + L)
            sc_scr[here, rows, lanes] = (g_ref[rows, lanes].astype(f32) * r).astype(bf16)
        for p in range(pairs):
            lanes = slice(p * L, p * L + L)
            gg = prm_ref[6:7, lanes]
            z = z_ref[rows, lanes].astype(f32)
            y = y_ref[rows, lanes].astype(f32)
            sg = sigmoid(z)
            silz = z * sg
            gated = y * silz
            q_scr[here, rows, lanes] = (gated * gg).astype(bf16)
            dq = r * u_ref[rows, lanes].astype(f32)
            ggg_ref[:, lanes] += fold_rows(dq * gated)
            dgated = dq * gg - c2 * gated
            dy_ref[rows, lanes] = (dgated * silz).astype(bf16)
            dz = (dgated * y * (sg + silz * (1.0 - sg))).astype(bf16)
            dz_ref[rows, lanes] = dz
            dz_scr[here, rows, lanes] = dz

    @pl.when(here == last)
    def _():
        hid = hid_ref.reshape(nloc * rows_all, model)
        dz = dz_scr.reshape(nloc * rows_all, width)
        q = q_scr.reshape(nloc * rows_all, width)
        sc = sc_scr.reshape(nloc * rows_all, model)

        def sums(half, out_z, out_o):
            lanes = slice(half * own, half * own + own)

            @pl.loop(0, model // 256)
            def _(j):
                cols = pl.ds(pl.multiple_of(j * 256, 256), 256)
                gz = tn(hid[:, cols], dz[:, lanes])
                go = tn(sc[:, cols], q[:, lanes])
                out_z[cols, :] = gz.astype(bf16)
                out_o[cols, :] = go.astype(bf16)

        if ncore == 2:
            sums(1, send_scr.at[:, 0:own], send_scr.at[:, own : 2 * own])
        if ncore == 2:
            copy = remote(send_scr, recv_scr, core_send, core_recv, twin)
            copy.start()
        sums(0, gz_ref, go_ref)
        if ncore == 2:
            copy.wait()

            @pl.loop(0, model // 64)
            def _(j):
                rows = pl.ds(pl.multiple_of(j * 64, 64), 64)
                for ref, first in ((gz_ref, 0), (go_ref, own)):
                    theirs = recv_scr[rows, first : first + own].astype(f32)
                    ref[rows, :] = (ref[rows, :].astype(f32) + theirs).astype(bf16)

        for copy in po_copies() + [x_copy()]:
            copy.wait()
        parts = [po_in.at[d] for d in range(ny - 1)]
        mine = po_ref.at[pl.ds(pl.multiple_of(yy * Ry, Ry), Ry)]
        block_out(inner_total, stot_ref.at[last], yy, mine, parts, x_own, bo_ref.at[last])


def tail_part(own, ncore, ny, ndp, nloc, given, outs, late_to, ready_to, room, machine):
    gw_ref, gbcw_ref, small_ref, other_ref, shared_ref, dh_ref, gain_ref, x_ref, bo_ref = given
    fw_ref, fb_ref, small_out, shared_out, last_ref = outs
    dh_in, x_own, small_in, core_sems, y_sems, local = room
    model = gw_ref.shape[0]
    Ry = x_own.shape[0]
    core, yy, twin, ys, peers = places(ncore, ny)
    nbits = log2(ndp)
    dp_peers, dp_bits = bit_peers("dp", 1, 0, nbits)
    t_peers, t_bits = bit_peers("tensor", 1, 0, log2(ncore * ny))
    links = list(zip(dp_peers, dp_bits))
    swapped = [links[1], links[0]] + links[2:] if nbits > 1 else links
    t_links = list(zip(t_peers, t_bits))
    per = nbits + 2
    a, b = machine[:per], machine[per : 2 * per]
    per_bc = nbits + len(t_links) + 2
    c = machine[2 * per : 2 * per + per_bc]
    sm, sh = machine[2 * per + per_bc : 2 * per + per_bc + 3], machine[2 * per + per_bc + 3 :]
    mid = model // 2
    job_a = Halving(links, mid, gw_ref.at[0:mid], a[0], a[1:-1], fw_ref.at[0:mid], a[-1])
    job_b = Halving(swapped, mid, gw_ref.at[mid:model], b[0], b[1:-1], fw_ref.at[mid:model], b[-1])
    job_c = Halving(t_links + links, model, gbcw_ref, c[0], c[1:-1], fb_ref, c[-1])
    job_sm = Doubling(dp_peers, *sm)
    job_sh = Doubling(t_peers + dp_peers, *sh)

    def dh_copies():
        return [
            remote(
                dh_ref.at[pl.ds(pl.multiple_of(ys[d] * Ry, Ry), Ry)],
                dh_in.at[d],
                y_sems.at[0, d],
                y_sems.at[1, d],
                peers[d],
            )
            for d in range(ny - 1)
        ]

    place = (twin, peers, ncore)
    late = Spread(last_ref, *late_to, place)
    ready = [Spread(bo_ref.at[nloc - 1], *ready_to, place)]
    x_copy = pltpu.make_async_copy(x_ref.at[core * nloc + nloc - 1, yy], x_own, local.at[1])
    start(dh_copies())
    x_copy.start()
    yield

    def turn(*pairs):
        for job, j in pairs:
            job.close(j)
        for job, j in pairs:
            job.begin(j)

    job_sh.acc[0] = shared_ref[...]
    turn((job_sh, 0), (job_c, 0), (job_a, 0), (job_b, 0))
    if ncore == 2:
        small_copy = remote(other_ref, small_in, core_sems.at[0], core_sems.at[1], twin)
        small_copy.start()
    turn((job_c, 1), (job_sh, 1))
    for spread in ready:
        start(spread.first())
    if ncore == 2:
        small_copy.wait()
        job_sm.acc[0] = small_ref[...] + small_in[...]
    else:
        job_sm.acc[0] = small_ref[...]
    turn((job_sm, 0))
    steps = [
        (job_c, iter(range(2, 2 * job_c.n + 1))),
        (job_sm, iter(range(1, len(job_sm.peers) + 1))),
        (job_sh, iter(range(2, len(job_sh.peers) + 1))),
    ]

    def smaller():
        found = []
        for job, left in steps:
            j = next(left, None)
            if j is not None:
                found.append((job, j))
        return found

    turn(*smaller(), (job_a, 1), (job_b, 1))
    for copy in dh_copies():
        copy.wait()
    x_copy.wait()

    @pl.loop(0, Ry // 32)
    def _(i):
        rows = pl.ds(pl.multiple_of(i * 32, 32), 32)
        mine = pl.ds(pl.multiple_of(yy * Ry + i * 32, 32), 32)
        dh = dh_ref[mine, :].astype(f32)
        for d in range(ny - 1):
            dh = dh + dh_in[d, rows, :].astype(f32)
        last_ref[rows, :] = correction(x_own[rows, :], dh, gain_ref[...]).astype(bf16)

    turn(*smaller())
    start(late.first())
    for j in range(2, 2 * nbits + 1):
        turn(*smaller())
        turn(*smaller(), (job_a, j), (job_b, j))
    for spread in ready:
        wait(spread.first())
        start(spread.second())
    for _ in range(2 * job_c.n):
        turn(*smaller())
    small_out[...] = job_sm.acc[len(job_sm.peers)]
    shared_out[...] = job_sh.acc[len(job_sh.peers)]
    wait(late.first())
    start(late.second())
    for spread in ready + [late]:
        wait(spread.second())
    yield


def scan_kernel(
    width,
    own,
    heads,
    ncore,
    ny,
    ndp,
    nloc_static,
    _seq,
    hid_ref,
    dz_ref,
    dy_ref,
    xl_ref,
    bcl_ref,
    dtl_ref,
    sin_ref,
    wz_ref,
    wzo_ref,
    wx_ref,
    wxo_ref,
    wbc_ref,
    wdt_ref,
    prm_ref,
    bcp_ref,
    hp_ref,
    ggg_ref,
    gain_ref,
    gz_ref,
    go_ref,
    bo_ref,
    x_ref,
    corr_ref,
    small_out,
    shared_out,
    last_ref,
    fz_ref,
    fo_ref,
    boy_ref,
    bot_ref,
    boty_ref,
    cy_ref,
    ct_ref,
    cty_ref,
    fw_ref,
    fb_ref,
    ly_ref,
    lt_ref,
    lty_ref,
    zy_ref,
    zt_ref,
    zty_ref,
    d_scr,
    bcc_scr,
    bca_scr,
    ds_scr,
    dsb_scr,
    cs_scr,
    bds_scr,
    xs_scr,
    dye_scr,
    nx_scr,
    nbc_scr,
    wx_scr,
    wbc_scr,
    red_scr,
    end_scr,
    pick_scr,
    gx_ref,
    gbc_ref,
    gdt_ref,
    gpre_ref,
    acc_scr,
    send_scr,
    recv_scr,
    dh_scr,
    dh_in,
    x_own,
    core_send,
    core_recv,
    y_sems,
    bo_sems,
    c_sems,
    local,
    gw_ref,
    gbcw_ref,
    small_ref,
    other_ref,
    shared_ref,
    small_in,
    end_in,
    x_end,
    core_sems,
    end_sems,
    l_sems,
    z_sems,
    *machine,
):
    rows_all = dz_ref.shape[0]
    model = hid_ref.shape[1]
    pairs = width // L
    spans = rows_all // L
    Ry = rows_all // ny
    seq, back = pl.program_id(0), pl.program_id(1)
    step = seq * spans + back
    core, yy, twin, ys, peers = places(ncore, ny)
    nbits = log2(ndp)
    dp_peers, dp_bits = bit_peers("dp", 1, 0, nbits)
    links = list(zip(dp_peers, dp_bits))
    swapped = [links[1], links[0]] + links[2:] if nbits > 1 else links
    per = nbits + 2
    mz, mo, rest = machine[:per], machine[per : 2 * per], machine[2 * per :]
    jobs = [
        Halving(links, model, gz_ref, mz[0], mz[1:-1], fz_ref, mz[-1]),
        Halving(swapped, model, go_ref, mo[0], mo[1:-1], fo_ref, mo[-1]),
    ]
    last_step = nloc_static * spans - 1

    place = (twin, peers, ncore)
    some = pl.ds(0, nloc_static - 1)
    bo_spread = Spread(bo_ref.at[some], boy_ref, bot_ref, boty_ref, bo_sems, place)

    def corr_spread(i):
        return Spread(
            corr_ref.at[i], cy_ref.at[:, i], ct_ref.at[i], cty_ref.at[:, i], c_sems.at[:, i], place
        )

    def dh_copies():
        return [
            remote(
                dh_scr.at[pl.ds(pl.multiple_of(ys[d] * Ry, Ry), Ry)],
                dh_in.at[seq - 1, d],
                y_sems.at[0, seq - 1, d],
                y_sems.at[1, seq - 1, d],
                peers[d],
            )
            for d in range(ny - 1)
        ]

    def x_copy():
        return pltpu.make_async_copy(x_ref.at[core * nloc_static + seq - 1, yy], x_own, local.at[0])

    @pl.when(step == 0)
    def _():
        greet(peers + dp_peers + ([twin] if ncore == 2 else []))
        start(bo_spread.first())
        acc_scr[...] = jnp.zeros_like(acc_scr)
        end_scr[...] = jnp.zeros_like(end_scr)
        pick = row_iota((width, L)) // HEAD == lane_iota((width, L))
        pick_scr[...] = pick.astype(f32).astype(bf16)
        gx_ref[...] = jnp.zeros_like(gx_ref)
        gbc_ref[...] = jnp.zeros_like(gbc_ref)
        gdt_ref[...] = jnp.zeros_like(gdt_ref)
        gpre_ref[...] = jnp.zeros_like(gpre_ref)

    when = [0.0, 0.25, 0.33, 0.58, 0.67, 0.83]
    if nbits != 3:
        when = [j / (2 * nbits) for j in range(2 * nbits)]
    for j in range(2 * nbits):

        @pl.when(step == int(when[j] * (last_step + 1) + 0.1))
        def _(j=j):
            for job in jobs:
                job.close(j)
            for job in jobs:
                job.begin(j)

    @pl.when(step == spans + 2)
    def _():
        wait(bo_spread.first())
        start(bo_spread.second())

    for i in range(nloc_static - 2):

        @pl.when(step == (i + 2) * spans + 2)
        def _(i=i):
            wait(corr_spread(i).first())
            start(corr_spread(i).second())

    @pl.when(jnp.logical_and(seq > 0, back == 0))
    def _():
        for copy in dh_copies():
            copy.start()
        x_copy().start()

    @pl.when(jnp.logical_and(seq > 0, back == spans - 1))
    def _():
        for copy in dh_copies():
            copy.wait()
        x_copy().wait()

        @pl.loop(0, Ry // 32)
        def _(i):
            rows = pl.ds(pl.multiple_of(i * 32, 32), 32)
            mine = pl.ds(pl.multiple_of(yy * Ry + i * 32, 32), 32)
            dh = dh_scr[mine, :].astype(f32)
            for d in range(ny - 1):
                dh = dh + dh_in[seq - 1, d, rows, :].astype(f32)
            corr_ref[seq - 1, rows, :] = correction(x_own[rows, :], dh, gain_ref[...]).astype(bf16)

        start(corr_spread(seq - 1).first())

    hp = hp_ref[...]

    @pl.when(back == 0)
    def _():
        ds_scr[...] = jnp.zeros_like(ds_scr)
        nx_scr[...] = jnp.zeros_like(nx_scr)
        nbc_scr[...] = jnp.zeros_like(nbc_scr)

        @pl.loop(0, spans)
        def _(c):
            t0 = pl.multiple_of(c * L, L)
            for half in range(2):
                lanes = slice(half * L, half * L + L)
                v = conv(bcl_ref, t0, wbc_scr.at[half], lanes, bcp_ref[0:4, lanes], bcp_ref[4:5, lanes])
                bcc_scr[pl.ds(t0, L), lanes] = v
                bca_scr[pl.ds(t0, L), lanes] = (v * sigmoid(v)).astype(bf16)

    def one_chunk():
        c = spans - 1 - back
        t0 = pl.multiple_of(c * L, L)
        rows = pl.ds(t0, L)
        lane = lane_iota((L, L))
        lo = lane < HEAD
        mlo = (lane_iota((1, L)) < HEAD).astype(bf16)
        mhi = (lane_iota((1, L)) >= HEAD).astype(bf16)
        tri = row_iota((L, L)) >= lane
        pre, dt, cum, cum_t = span_decay(dtl_ref[rows, :], hp)
        bm = bca_scr[rows, 0:L]
        cm = bca_scr[rows, L : 2 * L]
        both = nt(cm, bm)
        sb = sin_ref[c]
        dsb_scr[...] = ds_scr[...].astype(bf16)
        cs_scr[...] = nn(cm, sb)
        bds_scr[...] = nn(bm, dsb_scr[...])
        d_both = jnp.zeros((L, L), f32)
        for p in range(pairs):
            lanes = slice(p * L, p * L + L)
            taps = prm_ref[0:4, lanes]
            xc = conv(xl_ref, t0, wx_scr.at[p], lanes, taps, prm_ref[4:5, lanes])
            sg = sigmoid(xc)
            x = xc * sg
            h0, h1 = 2 * p, 2 * p + 1
            a0, a1 = spread(cum, h0), spread(cum, h1)
            ap = jnp.where(lo, a0, a1)
            e0 = jnp.exp2(jnp.where(tri, a0 - cum_t[h0 : h0 + 1], -jnp.inf))
            e1 = jnp.exp2(jnp.where(tri, a1 - cum_t[h1 : h1 + 1], -jnp.inf))
            k0 = (both * e0).astype(bf16)
            k1 = (both * e1).astype(bf16)
            dtp = jnp.where(lo, spread(dt, h0), spread(dt, h1))
            xdt = x * dtp
            xb = xdt.astype(bf16)
            bdx = jnp.concatenate([xb * mlo, xb * mhi], axis=0)
            ecum = jnp.exp2(ap)
            fin = ap[L - 1 : L]
            sd = jnp.exp2(fin - ap)
            y = nn(jnp.concatenate([k0, k1], axis=1), bdx) + ecum * cs_scr[:, lanes]
            dyb = dy_ref[rows, lanes]
            dy = dyb.astype(f32)
            dk = nt(dyb, bdx)
            d_both = d_both + dk[:, 0:L] * e0 + dk[:, L : 2 * L] * e1
            bdy = jnp.concatenate([dyb * mlo, dyb * mhi], axis=0)
            near = tn(jnp.concatenate([k0, k1], axis=0), bdy)
            far = sd * bds_scr[:, lanes]
            dxdt = near + far
            v = dy * y - xb.astype(f32) * near
            u = dxdt * x
            w = xdt * far
            ends = jnp.exp2(fin)
            through = ends * jnp.sum(sb[:, lanes].astype(f32) * ds_scr[:, lanes], axis=0, keepdims=True)
            v_hi = v.astype(bf16)
            red_scr[0:L, lanes] = v_hi
            red_scr[L : 2 * L, lanes] = (v - v_hi.astype(f32)).astype(bf16)
            red_scr[2 * L : 3 * L, lanes] = u.astype(bf16)
            red_scr[3 * L : 4 * L, lanes] = w.astype(bf16)
            end_scr[0:1, lanes] = through
            dx = dxdt * dtp + dy * prm_ref[5:6, lanes]
            dxc = dx * (sg + x * (1.0 - sg))
            for k in range(4):
                gx_ref[k, :, lanes] += fold_rows(dxc * tap(wx_scr.at[p], k))
            gx_ref[4, :, lanes] += fold_rows(dxc)
            gx_ref[5, :, lanes] += fold_rows(dy * x)
            nx_scr[p, L : L + 8] = nx_scr[p, 0:8]
            nx_scr[p, 0:L] = dxc
            dxl = dxc * taps[3:4]
            for k in range(3):
                dxl = dxl + nx_scr[p, 3 - k : 3 - k + L] * taps[k : k + 1]
            d_scr[rows, lanes] = dxl.astype(bf16)
            xs_scr[:, lanes] = (xdt * sd).astype(bf16)
            dye_scr[:, lanes] = (dy * ecum).astype(bf16)
            ds_scr[:, lanes] = ds_scr[:, lanes] * ends
        ds_scr[...] += nn(cm.T, dye_scr[...])
        sums = nn(red_scr[...], pick_scr[...])
        d_cum = sums[0:L] + sums[L : 2 * L]
        d_dt = sums[2 * L : 3 * L]
        d_far = sums[3 * L : 4 * L]
        d_end = exact(end_scr[...], pick_scr[...].astype(f32))[0:1]
        utri = (row_iota((L, L)) <= lane).astype(f32)
        before = (row_iota((L, L)) > lane).astype(f32)
        d_a = exact(utri, d_cum) + exact(before, d_far) + d_end
        d_dt = d_dt + d_a * hp[1:2]
        d_pre = d_dt * sigmoid(pre)
        gdt_ref[0] += fold_rows(d_pre)
        gdt_ref[1] += fold_rows(d_a * dt * hp[1:2])
        d_scr[rows, width + 256 : width + 384] = d_pre.astype(bf16)
        dgb = d_both.astype(bf16)
        d_c = nt(dye_scr[...], sb) + nn(dgb, bm)
        d_b = nt(xs_scr[...], dsb_scr[...]) + nn(dgb.T, cm)
        for half, dv in ((0, d_b), (1, d_c)):
            lanes = slice(half * L, half * L + L)
            pre_act = bcc_scr[rows, lanes]
            sg = sigmoid(pre_act)
            dvc = dv * (sg + pre_act * sg * (1.0 - sg))
            wbc_scr[half] = bcl_ref[pl.ds(t0, L + PAD), lanes]
            for k in range(4):
                gbc_ref[k, :, lanes] += fold_rows(dvc * tap(wbc_scr.at[half], k))
            gbc_ref[4, :, lanes] += fold_rows(dvc)
            nbc_scr[half, L : L + 8] = nbc_scr[half, 0:8]
            nbc_scr[half, 0:L] = dvc
            dvl = dvc * bcp_ref[3:4, lanes]
            for k in range(3):
                dvl = dvl + nbc_scr[half, 3 - k : 3 - k + L] * bcp_ref[k : k + 1, lanes]
            d_scr[rows, width + half * L : width + half * L + L] = dvl.astype(bf16)

    one_chunk()

    @pl.when(back == spans - 1)
    def _():
        @pl.loop(0, model // 256)
        def _(j):
            cols = pl.ds(pl.multiple_of(j * 256, 256), 256)
            dh = nt(dz_ref[:, 0:own], wz_ref[cols, :]) + nt(d_scr[:, 0:own], wx_ref[cols, :])
            if ncore == 2:
                dh = dh + nt(dz_ref[:, own:width], wzo_ref[cols, :])
                dh = dh + nt(d_scr[:, own:width], wxo_ref[cols, :])
            dh = dh + nt(d_scr[:, width : width + 256], wbc_ref[cols, :])
            dh = dh + nt(d_scr[:, width + 256 :], wdt_ref[cols, :])
            dh_scr[:, cols] = dh.astype(bf16)
            gpre_ref[:, cols] += fold_rows(dh * hid_ref[:, cols].astype(f32))
            acc_scr[cols, :] += tn(hid_ref[:, cols], d_scr[...])

    @pl.when(step == last_step)
    def _():
        end = tail_part(
            own,
            ncore,
            ny,
            ndp,
            nloc_static,
            (gw_ref, gbcw_ref, small_ref, other_ref, shared_ref, dh_scr, gain_ref, x_ref, bo_ref),
            (fw_ref, fb_ref, small_out, shared_out, last_ref),
            (ly_ref, lt_ref, lty_ref, l_sems),
            (zy_ref, zt_ref, zty_ref, z_sems),
            (end_in, x_end, small_in, core_sems, end_sems, local),
            rest,
        )
        next(end)
        if ncore == 2:
            send_scr[...] = acc_scr[:, own:width].astype(bf16)
            copy = remote(send_scr, recv_scr, core_send, core_recv, twin)
        gbcw_ref[...] = acc_scr[:, width : width + 256].astype(gbcw_ref.dtype)
        if ncore == 2:
            copy.start()
        rows = [jnp.sum(gx_ref[k], axis=0, keepdims=True) for k in range(6)]
        rows.append(jnp.sum(ggg_ref[...], axis=0, keepdims=True))
        dts = [jnp.sum(gdt_ref[k], axis=0, keepdims=True) for k in range(2)]
        small_ref[...] = jnp.zeros_like(small_ref)
        other_ref[...] = jnp.zeros_like(other_ref)
        for k in range(7):
            small_ref[k : k + 1, :] = rows[k][:, 0:own]
            if ncore == 2:
                other_ref[k : k + 1, :] = rows[k][:, own:width]
        for d in range(model // L):
            turned = acc_scr[d * L : d * L + L, width + 256 : width + 384].T
            line, lanes = 16 + heads * (d * L // own), slice(d * L % own, d * L % own + L)
            small_ref[line : line + heads, lanes] = turned[0:heads]
            if ncore == 2:
                other_ref[line : line + heads, lanes] = turned[heads : 2 * heads]
        for k in range(2):
            small_ref[7 + k : 8 + k, 0:L] = dts[k]
            if ncore == 2:
                moved = pltpu.roll(jnp.broadcast_to(dts[k], (8, L)), L - heads, axis=1)
                other_ref[7 + k : 8 + k, 0:L] = moved[0:1]
        shared_ref[...] = jnp.zeros_like(shared_ref)
        shared_ref[0:1, :] = jnp.sum(gpre_ref[...], axis=0, keepdims=True) / gain_ref[...]
        for k in range(5):
            shared_ref[k + 1 : k + 2, 0:256] = jnp.sum(gbc_ref[k], axis=0, keepdims=True)
        for job in jobs:
            job.close(2 * nbits)
        if ncore == 2:
            copy.wait()

        @pl.loop(0, model // 64)
        def _(i):
            rows = pl.ds(pl.multiple_of(i * 64, 64), 64)
            total = acc_scr[rows, 0:own]
            if ncore == 2:
                total = total + recv_scr[rows, :].astype(f32)
            gw_ref[rows, :] = total.astype(bf16)

        for _ in end:
            pass
        final = corr_spread(nloc_static - 2)
        wait(final.first())
        start(final.second())
        wait(bo_spread.second())
        for i in range(nloc_static - 1):
            wait(corr_spread(i).second())


def finish_kernel(pieces, nloc, _idx, g_ref, *refs):
    gi_ref, bo_ref = refs[-2:]
    groups = [refs[n * pieces : (n + 1) * pieces] for n in range(4)]
    now = pl.program_id(1)
    for k in range(pieces):
        here = pl.program_id(0) == k

        def when(turn, here=here):
            return pl.when(jnp.logical_and(here, turn))

        for n, turn in ((0, now < nloc - 1), (1, now == nloc - 1)):

            @when(turn)
            def _(src=groups[n][k]):
                gi_ref[...] = g_ref[...].astype(f32) + src[...].astype(f32)

        for n, turn in ((2, now < nloc - 1), (3, now == nloc - 1)):

            @when(turn)
            def _(src=groups[n][k]):
                bo_ref[...] = src[...]


def unpack_kernel(own, heads, gz_ref, go_ref, gw_ref, fb_ref, small_ref, shared_ref, *outs):
    gzx_ref, gwo_ref, gwdt_ref, gwbc_ref = outs[:4]
    gcxw_ref, gcxb_ref, gd_ref, ggg_ref, gdtb_ref, galog_ref, gpre_ref, gcbw_ref, gcbb_ref = outs[4:]
    gzx_ref[:, 0, :] = gz_ref[...].astype(f32)
    gzx_ref[:, 1, :] = gw_ref[:, 0:own].astype(f32)
    for d in range(gpre_ref.shape[1] // L):

        @pl.when(pl.program_id(0) == d)
        def _(d=d):
            line = 16 + heads * (d * L // own)
            rows = small_ref[line : line + heads, d * L % own : d * L % own + L]
            if heads < 8:
                rows = jnp.concatenate([rows, jnp.zeros((8 - heads, L), f32)], axis=0)
            gwdt_ref[...] = rows.T[:, 0:heads]

    gwbc_ref[...] = fb_ref[...].astype(f32)
    v = go_ref[...].astype(f32)
    for k in range(own // L):
        gwo_ref[k * L : k * L + L, :] = v[:, k * L : k * L + L].T

    @pl.when(pl.program_id(0) == 0)
    def _():
        gcxw_ref[...] = small_ref[0:4]
        gcxb_ref[...] = small_ref[4:5]
        ggg_ref[...] = small_ref[6:7]
        gdtb_ref[...] = small_ref[7:8, 0:heads]
        galog_ref[...] = small_ref[8:9, 0:heads]
        pick = (row_iota((own, L)) // HEAD == lane_iota((own, L))).astype(f32)
        gd_ref[...] = exact(small_ref[0:8], pick)[5:6, 0:heads]
        gpre_ref[...] = shared_ref[0:1]
        gcbw_ref[...] = shared_ref[1:5, 0:256]
        gcbb_ref[...] = shared_ref[5:6, 0:256]


def seq_spec(*shape):
    zeros = (0,) * len(shape)
    return pl.BlockSpec((None,) + shape, lambda i, s: (i,) + zeros)


def moved_spec(ncore, nloc, *shape):
    zeros = (0,) * len(shape)

    def index(i, s):
        return (i + lax.rem(lax.axis_index("tensor"), ncore) * nloc,) + zeros

    return pl.BlockSpec((None,) + shape, index)


def whole_spec(*shape):
    zeros = (0,) * len(shape)
    return pl.BlockSpec(shape, lambda *_: zeros, pipeline_mode=pl.Buffered(1))


def call(
    kernel, grid, in_specs, out_specs, out_shape, scratch, name, flops=0, moved=0, group=None
):
    return pl.pallas_call(
        kernel,
        grid_spec=pltpu.PrefetchScalarGridSpec(
            num_scalar_prefetch=1,
            grid=grid,
            in_specs=in_specs,
            out_specs=out_specs,
            scratch_shapes=scratch,
        ),
        out_shape=out_shape,
        cost_estimate=pl.CostEstimate(
            flops=int(flops), bytes_accessed=int(moved), transcendentals=0
        ),
        name=name,
        compiler_params=None
        if group is None
        else pltpu.CompilerParams(collective_id=group, has_side_effects=True),
    )


def sds(*shape, dtype=f32):
    return jax.ShapeDtypeStruct(shape, dtype)


def body(
    block_input,
    pre_gain,
    w_zx,
    w_bc,
    w_dt,
    conv_x_w,
    conv_x_b,
    conv_bc_w,
    conv_bc_b,
    dt_bias,
    a_log,
    d_skip,
    gate_gain,
    w_out,
    out_grad,
):
    tok, model = block_input.shape
    own = w_zx.shape[2]
    heads = w_dt.shape[1]
    nt = lax.axis_size("tensor")
    ndp = lax.axis_size("dp")
    inner_total = own * nt
    ncore = 2 if nt % 2 == 0 else 1
    ny = nt // ncore
    width = own * ncore
    t = lax.axis_index("tensor")
    core, yy = t % ncore, t // ncore
    R = SEQ_LEN
    Ry = R // ny
    nseq = tok // R
    nloc = nseq // ncore
    spans = R // L
    wtot = 2 * width + 384
    pairs = width // L

    x3 = block_input.reshape(nseq, R, model)
    g3 = out_grad.reshape(nseq, R, model)
    x4 = block_input.reshape(nseq, ny, Ry, model)
    g4 = out_grad.reshape(nseq, ny, Ry, model)
    wz, wx = w_zx[:, 0], w_zx[:, 1]
    sm = jnp.concatenate(
        [
            conv_x_w,
            conv_x_b[None],
            jnp.repeat(d_skip, HEAD)[None],
            gate_gain[None],
            jnp.zeros((1, own), f32),
            jnp.pad(jnp.stack([dt_bias, -jnp.exp(a_log)]), ((0, 6), (0, own - heads))),
        ],
        axis=0,
    )
    wdt = jnp.pad(w_dt, ((0, 0), (0, L - heads)))
    bcp = jnp.concatenate([conv_bc_w, conv_bc_b[None], jnp.zeros((3, 256), f32)], axis=0)
    gain = pre_gain[None]
    seq0 = jnp.zeros((1,), jnp.int32)
    any_spec = pl.BlockSpec(memory_space=pl.ANY)
    nother = max(ny - 1, 1)
    dma = pltpu.SemaphoreType.DMA

    hid, z, xl, bcl, dtl, u, y, sin, st, stot, po, bo01, prm, hp, wdt, wzo, wxo = call(
        partial(forward_kernel, own, heads, ncore, ny, inner_total, nloc),
        (nloc,),
        [
            moved_spec(ncore, nloc, R, model),
            moved_spec(ncore, nloc, R, model),
            whole_spec(1, model),
            whole_spec(model, own),
            whole_spec(model, own),
            whole_spec(model, 256),
            whole_spec(model, L),
            whole_spec(own, model),
            whole_spec(16, own),
            whole_spec(8, 256),
            any_spec,
        ],
        [
            seq_spec(R, model),
            seq_spec(R, width),
            seq_spec(R + PAD, width),
            seq_spec(R + PAD, 256),
            seq_spec(R, L),
            seq_spec(R, width),
            seq_spec(R, width),
            seq_spec(spans, L, width),
            whole_spec(nloc, 2, R),
            whole_spec(nloc, 2, R),
            whole_spec(R, model),
            whole_spec(nloc - 1, Ry, model),
            whole_spec(8, width),
            whole_spec(8, L),
            whole_spec(model, L),
        ]
        + [any_spec] * 2,
        [
            sds(nloc, R, model, dtype=bf16),
            sds(nloc, R, width, dtype=bf16),
            sds(nloc, R + PAD, width),
            sds(nloc, R + PAD, 256),
            sds(nloc, R, L),
            sds(nloc, R, width, dtype=bf16),
            sds(nloc, R, width, dtype=bf16),
            sds(nloc, spans, L, width, dtype=bf16),
            sds(nloc, 2, R),
            sds(nloc, 2, R),
            sds(R, model, dtype=bf16),
            sds(nloc - 1, Ry, model, dtype=bf16),
            sds(8, width),
            sds(8, L),
            sds(model, L, dtype=bf16),
            sds(model, own, dtype=bf16),
            sds(model, own, dtype=bf16),
        ],
        [
            pltpu.VMEM((R, width), f32),
            pltpu.VMEM((R, width), f32),
            pltpu.VMEM((R, width), bf16),
            pltpu.VMEM((R, 256), bf16),
            pltpu.VMEM((L, width), f32),
            pltpu.VMEM((L, width), f32),
            pltpu.VMEM((L, width), bf16),
            pltpu.VMEM((pairs, L + PAD, L), f32),
            pltpu.VMEM((2, L + PAD, L), f32),
            pltpu.VMEM((model, own), bf16),
            pltpu.VMEM((model, own), bf16),
            pltpu.VMEM((own, model), bf16),
            pltpu.VMEM((model, L), bf16),
            pltpu.VMEM((16, own), f32),
            pltpu.VMEM((2, R, model), bf16),
            pltpu.VMEM((nloc - 1, nother, Ry, model), bf16),
            pltpu.VMEM((nloc - 1, nother, 2, R), f32),
            pltpu.VMEM((Ry, model), bf16),
            dma((2, 5)),
            dma((2, nloc - 1, nother)),
            dma((2, nloc - 1, nother)),
            dma((3,)),
        ],
        "forward",
        2 * nloc * R * model * (wtot + 2 * width),
        nloc * R * (6 * model + 20 * width),
        4,
    )(seq0, x3, g3, gain, wz, wx, w_bc, wdt, w_out, sm, bcp, x4)

    nbits = log2(ndp)
    dz, dy, gz, go, ggg, bo = call(
        partial(gate_kernel, width, own, inner_total, ncore, ny),
        (nloc,),
        [
            whole_spec(nloc, 2, R),
            whole_spec(nloc, 2, R),
            moved_spec(ncore, nloc, R, model),
            whole_spec(nloc, R, model),
            seq_spec(R, width),
            seq_spec(R, width),
            seq_spec(R, width),
            whole_spec(8, width),
            whole_spec(R, model),
            whole_spec(nloc - 1, Ry, model),
            any_spec,
        ],
        [
            seq_spec(R, width),
            seq_spec(R, width),
            whole_spec(model, own),
            whole_spec(model, own),
            whole_spec(8, width),
            whole_spec(nloc, Ry, model),
        ],
        [
            sds(nloc, R, width, dtype=bf16),
            sds(nloc, R, width, dtype=bf16),
            sds(model, own, dtype=bf16),
            sds(model, own, dtype=bf16),
            sds(8, width),
            sds(nloc, Ry, model, dtype=bf16),
        ],
        [
            pltpu.VMEM((nloc, R, width), bf16),
            pltpu.VMEM((nloc, R, model), bf16),
            pltpu.VMEM((nloc, R, width), bf16),
            pltpu.VMEM((nloc, 2, R), f32),
            pltpu.VMEM((nother, 2, R), f32),
            pltpu.VMEM((model, 2 * own), bf16),
            pltpu.VMEM((model, 2 * own), bf16),
            pltpu.VMEM((nother, Ry, model), bf16),
            pltpu.VMEM((Ry, model), bf16),
            dma((2, nother)),
            dma,
            dma,
            dma((2, nother)),
            dma((1,)),
        ],
        "gate",
        4 * nloc * R * model * width,
        nloc * R * (4 * model + 16 * width),
        1,
    )(seq0, st, stot, g3, hid, z, y, u, prm, po, bo01, x4)

    def chunk_spec(*shape):
        zeros = (0,) * len(shape)
        return pl.BlockSpec((None,) + shape, lambda i, b, s: (i,) + zeros)

    tbits = log2(nt)
    lines = 16 + heads * model // own
    late_shape = sds(nother, Ry, model, dtype=bf16)
    bc_type = bf16 if (model // (nt * ndp)) % 16 == 0 else f32
    s_out = call(
        partial(scan_kernel, width, own, heads, ncore, ny, ndp, nloc),
        (nloc, spans),
        [
            chunk_spec(R, model),
            chunk_spec(R, width),
            chunk_spec(R, width),
            chunk_spec(R + PAD, width),
            chunk_spec(R + PAD, 256),
            chunk_spec(R, L),
            chunk_spec(spans, L, width),
            whole_spec(model, own),
            whole_spec(model, own),
            whole_spec(model, own),
            whole_spec(model, own),
            whole_spec(model, 256),
            whole_spec(model, L),
            whole_spec(8, width),
            whole_spec(8, 256),
            whole_spec(8, L),
            whole_spec(8, width),
            whole_spec(1, model),
            whole_spec(model, own),
            whole_spec(model, own),
            any_spec,
            any_spec,
        ],
        [
            whole_spec(nloc - 1, Ry, model),
            whole_spec(lines, own),
            whole_spec(8, model),
            whole_spec(Ry, model),
        ]
        + [any_spec] * 16,
        [
            sds(nloc - 1, Ry, model, dtype=bf16),
            sds(lines, own),
            sds(8, model),
            sds(Ry, model, dtype=bf16),
            sds(model, own, dtype=bf16),
            sds(model, own, dtype=bf16),
            sds(nother, nloc - 1, Ry, model, dtype=bf16),
            sds(nloc - 1, Ry, model, dtype=bf16),
            sds(nother, nloc - 1, Ry, model, dtype=bf16),
            sds(nother, nloc - 1, Ry, model, dtype=bf16),
            sds(nloc - 1, Ry, model, dtype=bf16),
            sds(nother, nloc - 1, Ry, model, dtype=bf16),
            sds(model, own, dtype=bf16),
            sds(model, 256, dtype=bc_type),
        ]
        + [late_shape, sds(Ry, model, dtype=bf16), late_shape] * 2,
        [
            pltpu.VMEM((R, width + 384), bf16),
            pltpu.VMEM((R, 256), f32),
            pltpu.VMEM((R, 256), bf16),
            pltpu.VMEM((L, width), f32),
            pltpu.VMEM((L, width), bf16),
            pltpu.VMEM((L, width), f32),
            pltpu.VMEM((L, width), f32),
            pltpu.VMEM((L, width), bf16),
            pltpu.VMEM((L, width), bf16),
            pltpu.VMEM((pairs, L + 8, L), f32),
            pltpu.VMEM((2, L + 8, L), f32),
            pltpu.VMEM((pairs, L + PAD, L), f32),
            pltpu.VMEM((2, L + PAD, L), f32),
            pltpu.VMEM((4 * L, width), bf16),
            pltpu.VMEM((8, width), f32),
            pltpu.VMEM((width, L), bf16),
            pltpu.VMEM((6, 8, width), f32),
            pltpu.VMEM((5, 8, 256), f32),
            pltpu.VMEM((2, 8, L), f32),
            pltpu.VMEM((8, model), f32),
            pltpu.VMEM((model, width + 384), f32),
            pltpu.VMEM((model, own), bf16),
            pltpu.VMEM((model, own), bf16),
            pltpu.VMEM((R, model), bf16),
            pltpu.VMEM((nloc - 1, nother, Ry, model), bf16),
            pltpu.VMEM((Ry, model), bf16),
            dma,
            dma,
            dma((2, nloc - 1, nother)),
            dma((2, 2 * ny)),
            dma((2, nloc - 1, 2 * ny)),
            dma((2,)),
            pltpu.VMEM((model, own), bf16),
            pltpu.VMEM((model, 256), bc_type),
            pltpu.VMEM((lines, own), f32),
            pltpu.VMEM((lines, own), f32),
            pltpu.VMEM((8, model), f32),
            pltpu.VMEM((lines, own), f32),
            pltpu.VMEM((nother, Ry, model), bf16),
            pltpu.VMEM((Ry, model), bf16),
            dma((2,)),
            dma((2, nother)),
            dma((2, 2 * ny)),
            dma((2, 2 * ny)),
        ]
        + Halving.scratch(model, own, nbits, bf16)
        + Halving.scratch(model, own, nbits, bf16)
        + Halving.scratch(model // 2, own, nbits, bf16)
        + Halving.scratch(model // 2, own, nbits, bf16)
        + Halving.scratch(model, 256, nbits + tbits, bc_type)
        + Doubling.scratch(nbits, lines, own)
        + Doubling.scratch(nbits + tbits, 8, model),
        "scan_back",
        2 * nloc * R * model * (2 * wtot),
        nloc * R * (4 * model + 12 * width),
        2,
    )(seq0, hid, dz, dy, xl, bcl, dtl, sin, wz, wzo, wx, wxo, w_bc, wdt, prm, bcp, hp, ggg, gain, gz, go, bo, x4)

    corr, small, shared, last, fz, fo, boy, bot, boty, cy0, ct0, cty0, fw, fb = s_out[:14]
    late_got = s_out[14:]
    pieces = ncore * ny
    where = jnp.stack([core, yy]).astype(jnp.int32)

    def out_index(k, i, s):
        return ((s[0] ^ (k // ny)) * nloc + i, (s[1] - k % ny + ny) % ny, 0, 0)

    def spec_of(base, seq_of, d):
        if d is None:
            return pl.BlockSpec(
                (None, Ry, model), lambda j, i, s: (seq_of(j, i) - base, 0, 0)
            )
        return pl.BlockSpec(
            (None, None, Ry, model), lambda j, i, s: (d, seq_of(j, i) - base, 0, 0)
        )

    placed_spec = pl.BlockSpec((None, None, Ry, model), out_index)
    specs, arrays = [], []

    def add_group(first, count, mine, mine_base, toy, tot, toty):
        for k in range(pieces):

            def seq_of(j, i, k=k):
                i = jnp.clip(i, first, first + count - 1)
                return jnp.where(j == k, i, jnp.where(j > k, first + count - 1, first))

            d = k % ny - 1
            if k == 0:
                array, spec = mine, spec_of(mine_base, seq_of, None)
            elif k < ny:
                array, spec = toy, spec_of(first, seq_of, d)
            elif d < 0:
                array, spec = tot, spec_of(first, seq_of, None)
            else:
                array, spec = toty, spec_of(first, seq_of, d)
            arrays.append(array)
            specs.append(spec)

    def as_seq(v, axis):
        return jnp.expand_dims(v, axis)

    def add_late(first, mine, base, got):
        toy, tot, toty = got
        add_group(first, 1, mine, base, as_seq(toy, 1), as_seq(tot, 0), as_seq(toty, 1))

    add_group(0, nloc - 1, corr, 0, cy0, ct0, cty0)
    add_late(nloc - 1, as_seq(last, 0), nloc - 1, late_got[0:3])
    add_group(0, nloc - 1, bo, 0, boy, bot, boty)
    add_late(nloc - 1, bo, 0, late_got[3:6])
    grad_input, block_output = call(
        partial(finish_kernel, pieces, nloc),
        (pieces, nloc),
        [placed_spec] + specs,
        [placed_spec, placed_spec],
        [sds(nseq, ny, Ry, model), sds(nseq, ny, Ry, model, dtype=bf16)],
        [],
        "finish",
        0,
        12 * tok * model,
    )(where, g4, *arrays)

    def row_block(cols):
        return pl.BlockSpec((L, cols), lambda d: (d, 0))

    outs = pl.pallas_call(
        partial(unpack_kernel, own, heads),
        grid=(model // L,),
        in_specs=[row_block(own), row_block(own), row_block(own), row_block(256)]
        + [whole_spec(lines, own), whole_spec(8, model)],
        out_specs=[
            pl.BlockSpec((L, 2, own), lambda d: (d, 0, 0)),
            pl.BlockSpec((own, L), lambda d: (0, d)),
            row_block(heads),
            row_block(256),
            whole_spec(4, own),
            whole_spec(1, own),
            whole_spec(1, heads),
            whole_spec(1, own),
            whole_spec(1, heads),
            whole_spec(1, heads),
            whole_spec(1, model),
            whole_spec(4, 256),
            whole_spec(1, 256),
        ],
        out_shape=[
            sds(model, 2, own),
            sds(own, model),
            sds(model, heads),
            sds(model, 256),
            sds(4, own),
            sds(1, own),
            sds(1, heads),
            sds(1, own),
            sds(1, heads),
            sds(1, heads),
            sds(1, model),
            sds(4, 256),
            sds(1, 256),
        ],
        name="unpack",
    )(fz, fo, fw, fb, small, shared)
    gzx, gwo, gwdt, gwbc, gcxw, gcxb, gd, ggg, gdtb, galog, gpre, gcbw, gcbb = outs
    return (
        block_output.reshape(tok, model),
        grad_input.reshape(tok, model),
        gpre[0],
        gzx,
        gwbc,
        gwdt,
        gcxw,
        gcxb[0],
        gcbw,
        gcbb[0],
        gdtb[0],
        galog[0],
        gd[0],
        ggg[0],
        gwo,
    )


def solution(mesh):
    placed = (
        P("dp", None),
        P(),
        P(None, None, "tensor"),
        P(),
        P(None, "tensor"),
        P(None, "tensor"),
        P("tensor"),
        P(),
        P(),
        P("tensor"),
        P("tensor"),
        P("tensor"),
        P("tensor"),
        P("tensor", None),
        P("dp", None),
    )
    return jax.shard_map(
        body,
        mesh=mesh,
        in_specs=placed,
        out_specs=(
            P("dp", None),
            P("dp", None),
            P(),
            P(None, None, "tensor"),
            P(),
            P(None, "tensor"),
            P(None, "tensor"),
            P("tensor"),
            P(),
            P(),
            P("tensor"),
            P("tensor"),
            P("tensor"),
            P("tensor"),
            P("tensor", None),
        ),
        check_vma=False,
    )
```

```python
from functools import partial

import jax
import jax.numpy as jnp
from jax import lax
from jax.experimental import pallas as pl
from jax.experimental.pallas import tpu as pltpu
from jax.sharding import PartitionSpec as P

SEQ_LEN = 512
L = 128
HEAD = 64
LOG2E = 1.4426950408889634
PAD = 8
epsilon = 1e-05
f32 = jnp.float32
bf16 = jnp.bfloat16
HI = lax.Precision.HIGHEST
MESH = pl.DeviceIdType.MESH


def nn(a, b):
    return lax.dot_general(a, b, (((1,), (0,)), ((), ())), preferred_element_type=f32)


def nt(a, b):
    return lax.dot_general(a, b, (((1,), (1,)), ((), ())), preferred_element_type=f32)


def tn(a, b):
    return lax.dot_general(a, b, (((0,), (0,)), ((), ())), preferred_element_type=f32)


def exact(a, b):
    return lax.dot_general(
        a, b, (((1,), (0,)), ((), ())), precision=HI, preferred_element_type=f32
    )


def sigmoid(v):
    return 0.5 + 0.5 * jnp.tanh(0.5 * v)


def softplus(v):
    u = jnp.exp(-jnp.abs(v))
    return jnp.maximum(v, 0.0) + jnp.where(u < 1e-3, u - 0.5 * u * u, jnp.log(1.0 + u))


def fold_rows(v):
    return jnp.sum(v.reshape(v.shape[0] // 8, 8, v.shape[1]), axis=0)


def lane_iota(shape):
    return lax.broadcasted_iota(jnp.int32, shape, 1)


def row_iota(shape):
    return lax.broadcasted_iota(jnp.int32, shape, 0)


def tap(win, k):
    return win[PAD - 3 + k : PAD - 3 + k + L, :]


def conv(ref, t0, win, lanes, taps, bias):
    win[...] = ref[pl.ds(t0, L + PAD), lanes]
    total = bias
    for k in range(4):
        total = total + tap(win, k) * taps[k : k + 1]
    return total


def spread(cols, head):
    return jnp.broadcast_to(cols[:, head : head + 1], (L, L))


def span_decay(dtl, hp):
    pre = dtl + hp[0:1]
    dt = softplus(pre)
    ltri = (row_iota((L, L)) >= lane_iota((L, L))).astype(f32)
    cum = exact(ltri, dt * (hp[1:2] * LOG2E))
    return pre, dt, cum, cum.T


def remote(src, dst, send, recv, where):
    return pltpu.make_async_remote_copy(
        src_ref=src,
        dst_ref=dst,
        send_sem=send,
        recv_sem=recv,
        device_id=where,
        device_id_type=MESH,
    )


def greet(peers):
    barrier = pltpu.get_barrier_semaphore()
    for peer in peers:
        pl.semaphore_signal(barrier, inc=1, device_id=peer, device_id_type=MESH)
    pl.semaphore_wait(barrier, len(peers))


def bit_peers(axis, base, first, count):
    me = lax.axis_index(axis)
    peers, bits = [], []
    for k in range(count):
        step = base * 2**k
        bit = lax.rem(me // step, 2)
        peers.append({axis: me + step * (1 - 2 * bit)})
        bits.append(bit)
    return peers, bits


class Halving:
    def __init__(self, links, rows, src, work, recvs, full, sems):
        self.links, self.rows = links, rows
        self.src, self.work, self.recvs, self.full, self.sems = src, work, recvs, full, sems
        self.n = len(links)
        offs, size = [0], rows
        for _, bit in links:
            size //= 2
            offs.append(offs[-1] + bit * size)
        self.offs = offs

    def size(self, k):
        return self.rows >> k

    def at(self, off, size):
        return pl.ds(pl.multiple_of(off, size), size)

    def scatter(self, k):
        peer, bit = self.links[k]
        half = self.size(k + 1)
        off = self.offs[k] + (1 - bit) * half
        if k == 0:
            src = self.src.at[self.at(off, half)]
        else:
            src = self.work.at[self.at(off - self.offs[1], half)]
        return remote(src, self.recvs[k], self.sems.at[0, k], self.sems.at[1, k], peer)

    def fold(self, k):
        self.scatter(k).wait()
        half = self.size(k + 1)
        step = min(half, 64)
        keep = self.offs[k + 1]

        @pl.loop(0, half // step)
        def _(i):
            off = i * step
            rows = pl.ds(pl.multiple_of(off, step), step)
            near = pl.ds(pl.multiple_of(keep - self.offs[1] + off, step), step)
            if k == 0:
                mine = self.src[pl.ds(pl.multiple_of(keep + off, step), step), :]
            else:
                mine = self.work[near, :]
            total = mine.astype(f32) + self.recvs[k][rows, :].astype(f32)
            self.work[near, :] = total.astype(self.work.dtype)

    def own_copy(self):
        last = self.size(self.n)
        return pltpu.make_async_copy(
            self.work.at[self.at(self.offs[self.n] - self.offs[1], last)],
            self.full.at[self.at(self.offs[self.n], last)],
            self.sems.at[0, 2 * self.n],
        )

    def gather(self, k):
        peer, _ = self.links[k]
        rows = self.at(self.offs[k + 1], self.size(k + 1))
        sems = self.sems
        return remote(
            self.full.at[rows],
            self.full.at[rows],
            sems.at[0, self.n + k],
            sems.at[1, self.n + k],
            peer,
        )

    def close(self, j):
        n = self.n
        if 1 <= j <= n:
            self.fold(j - 1)
        elif j > n:
            self.gather(2 * n - j).wait()

    def begin(self, j):
        n = self.n
        if j < n:
            self.scatter(j).start()
            return
        if j == n:
            self.own_copy().start()
            self.own_copy().wait()
        if j < 2 * n:
            self.gather(2 * n - 1 - j).start()

    @staticmethod
    def scratch(rows, cols, n, dtype):
        recvs = [pltpu.VMEM((rows >> (k + 1), cols), dtype) for k in range(n)]
        return [pltpu.VMEM((rows // 2, cols), dtype)] + recvs + [
            pltpu.SemaphoreType.DMA((2, 2 * n + 1))
        ]


class Doubling:
    def __init__(self, peers, acc, recv, sems):
        self.peers, self.acc, self.recv, self.sems = peers, acc, recv, sems

    def copy(self, k):
        return remote(
            self.acc.at[k],
            self.recv.at[k],
            self.sems.at[0, k],
            self.sems.at[1, k],
            self.peers[k],
        )

    def close(self, j):
        if j > 0:
            self.copy(j - 1).wait()
            self.acc[j] = self.acc[j - 1] + self.recv[j - 1]

    def begin(self, j):
        if j < len(self.peers):
            self.copy(j).start()

    @staticmethod
    def scratch(n, rows, cols):
        return [
            pltpu.VMEM((n + 1, rows, cols), f32),
            pltpu.VMEM((n, rows, cols), f32),
            pltpu.SemaphoreType.DMA((2, n)),
        ]


class Spread:
    def __init__(self, src, toy, tot, toty, sems, place):
        self.src, self.toy, self.tot, self.toty, self.sems = src, toy, tot, toty, sems
        self.twin, self.peers, self.ncore = place

    def first(self):
        n = len(self.peers)
        sems = self.sems
        out = [
            remote(self.src, self.toy.at[d], sems.at[0, d], sems.at[1, d], self.peers[d])
            for d in range(n)
        ]
        if self.ncore == 2:
            out.append(remote(self.src, self.tot, sems.at[0, n], sems.at[1, n], self.twin))
        return out

    def second(self):
        n = len(self.peers)
        if self.ncore != 2:
            return []
        sems = self.sems
        return [
            remote(
                self.toy.at[d], self.toty.at[d], sems.at[0, n + 1 + d], sems.at[1, n + 1 + d], self.twin
            )
            for d in range(n)
        ]


def start(copies):
    for copy in copies:
        copy.start()


def wait(copies):
    for copy in copies:
        copy.wait()


def correction(x, dh, gain):
    v = x.astype(f32)
    r = lax.rsqrt(jnp.mean(v * v, axis=1, keepdims=True) + epsilon)
    normed = v * r
    dn = dh * gain
    return r * (dn - normed * jnp.mean(dn * normed, axis=1, keepdims=True))


def places(ncore, ny):
    spot = lax.axis_index("tensor")
    core, yy = lax.rem(spot, ncore), spot // ncore
    ys = [lax.rem(yy + d, ny) for d in range(1, ny)]
    peers = [{"tensor": v * ncore + core} for v in ys]
    return core, yy, {"tensor": spot + 1 - 2 * core}, ys, peers


def log2(n):
    return n.bit_length() - 1


def forward_kernel(
    own,
    heads,
    ncore,
    ny,
    inner_total,
    nloc,
    _seq,
    x_ref,
    g_ref,
    gain_ref,
    wz_ref,
    wx_ref,
    wbc_ref,
    wdt_ref,
    wo_ref,
    sm_ref,
    bcp_ref,
    x4_ref,
    hid_ref,
    z_ref,
    xl_ref,
    bcl_ref,
    dtl_ref,
    u_ref,
    y_ref,
    sin_ref,
    st_ref,
    stot_ref,
    po_ref,
    bo_ref,
    prm_ref,
    hp_ref,
    wdt_out,
    wz_out,
    wx_out,
    z_scr,
    u_scr,
    q_scr,
    bca_scr,
    s_scr,
    cs_scr,
    xs_scr,
    wx_scr,
    wbc_scr,
    wz_in,
    wx_in,
    wo_in,
    wdt_in,
    sm_in,
    po_scr,
    po_in,
    st_in,
    x_own,
    w_sems,
    po_sems,
    st_sems,
    local,
):
    rows_all = x_ref.shape[0]
    model = x_ref.shape[1]
    width = own * ncore
    pairs = width // L
    Ry = rows_all // ny
    here = pl.program_id(0)
    core, yy, twin, ys, peers = places(ncore, ny)

    def weight_copies():
        both = ((sm_ref, sm_in), (wdt_ref, wdt_in), (wz_ref, wz_in), (wx_ref, wx_in), (wo_ref, wo_in))
        return [
            remote(src, dst, w_sems.at[0, k], w_sems.at[1, k], twin)
            for k, (src, dst) in enumerate(both)
        ]

    def weight_stores():
        return [
            pltpu.make_async_copy(wz_in, wz_out, local.at[1]),
            pltpu.make_async_copy(wx_in, wx_out, local.at[2]),
        ]

    def row_copies():
        last = here - 1
        return [
            remote(
                st_ref.at[last],
                st_in.at[last, d],
                st_sems.at[0, last, d],
                st_sems.at[1, last, d],
                peers[d],
            )
            for d in range(ny - 1)
        ] + [
            remote(
                po_scr.at[lax.rem(last, 2), pl.ds(pl.multiple_of(ys[d] * Ry, Ry), Ry)],
                po_in.at[last, d],
                po_sems.at[0, last, d],
                po_sems.at[1, last, d],
                peers[d],
            )
            for d in range(ny - 1)
        ]

    def x_copy():
        return pltpu.make_async_copy(x4_ref.at[core * nloc + here - 1, yy], x_own, local.at[0])

    @pl.when(here == 0)
    def _():
        greet(peers + ([twin] if ncore == 2 else []))
        if ncore == 2:
            for copy in weight_copies():
                copy.start()

    @pl.when(here > 0)
    def _():
        start(row_copies())
        x_copy().start()

    @pl.loop(0, rows_all // 32)
    def _(i):
        rows = pl.ds(pl.multiple_of(i * 32, 32), 32)
        v = x_ref[rows, :].astype(f32)
        r = lax.rsqrt(jnp.mean(v * v, axis=1, keepdims=True) + epsilon)
        hid_ref[rows, :] = (v * r * gain_ref[...]).astype(bf16)

    xl_ref[0:PAD, :] = jnp.zeros((PAD, width), f32)
    bcl_ref[0:PAD, :] = jnp.zeros((PAD, 256), f32)

    def project(wz, wx, wo, base):
        @pl.loop(0, own // 256)
        def _(j):
            src = pl.ds(pl.multiple_of(j * 256, 256), 256)
            cols = pl.ds(pl.multiple_of(base + j * 256, 256), 256)
            z_scr[:, cols] = nn(hid_ref[...], wz[:, src])
            xl_ref[PAD : PAD + rows_all, cols] = nn(hid_ref[...], wx[:, src])
            u_scr[:, cols] = nt(g_ref[...], wo[src, :])

    project(wz_ref, wx_ref, wo_ref, 0)
    bcl_ref[PAD : PAD + rows_all, :] = nn(hid_ref[...], wbc_ref[...])

    @pl.when(here == 0)
    def _():
        prm_ref[:, 0:own] = sm_ref[0:8, :]
        hp_ref[...] = sm_ref[8:16, 0:L]
        wdt_out[...] = wdt_ref[...]
        if ncore == 2:
            for copy in weight_copies():
                copy.wait()
            for copy in weight_stores():
                copy.start()
            prm_ref[:, own : 2 * own] = sm_in[0:8, :]
            hp_ref[...] += pltpu.roll(sm_in[8:16, 0:L], heads, axis=1)
            theirs = pltpu.roll(wdt_in[...].astype(f32), heads, axis=1)
            wdt_out[...] = (wdt_ref[...].astype(f32) + theirs).astype(bf16)

    if ncore == 2:
        project(wz_in, wx_in, wo_in, own)
    dtl_ref[...] = nn(hid_ref[...], wdt_out[...])

    @pl.loop(0, rows_all // L)
    def _(c):
        t0 = pl.multiple_of(c * L, L)
        for half in range(2):
            lanes = slice(half * L, half * L + L)
            v = conv(bcl_ref, t0, wbc_scr.at[half], lanes, bcp_ref[0:4, lanes], bcp_ref[4:5, lanes])
            bca_scr[pl.ds(t0, L), lanes] = (v * sigmoid(v)).astype(bf16)

    s_scr[...] = jnp.zeros_like(s_scr)
    hp = hp_ref[...]

    def block_done():
        wait(row_copies())
        x_copy().wait()
        total = st_ref[here - 1]
        for d in range(ny - 1):
            total = total + st_in[here - 1, d]
        stot_ref[here - 1] = total
        parts = [po_in.at[here - 1, d] for d in range(ny - 1)]
        mine = po_scr.at[lax.rem(here - 1, 2), pl.ds(pl.multiple_of(yy * Ry, Ry), Ry)]
        block_out(inner_total, stot_ref.at[here - 1], yy, mine, parts, x_own, bo_ref.at[here - 1])

    @pl.loop(0, rows_all // L)
    def _(c):
        early = jnp.logical_and(here > 0, here < nloc - 1)

        @pl.when(jnp.logical_and(early, c == rows_all // L - 1))
        def _():
            block_done()

        t0 = pl.multiple_of(c * L, L)
        rows = pl.ds(t0, L)
        lo = lane_iota((L, L)) < HEAD
        mlo = (lane_iota((1, L)) < HEAD).astype(bf16)
        mhi = (lane_iota((1, L)) >= HEAD).astype(bf16)
        tri = row_iota((L, L)) >= lane_iota((L, L))
        _, dt, cum, cum_t = span_decay(dtl_ref[rows, :], hp)
        bm = bca_scr[rows, 0:L]
        cm = bca_scr[rows, L : 2 * L]
        both = nt(cm, bm)
        sb = s_scr[...].astype(bf16)
        sin_ref[c] = sb
        cs_scr[...] = nn(cm, sb)
        squares = jnp.zeros((L, L), f32)
        inner = jnp.zeros((L, L), f32)
        for p in range(pairs):
            lanes = slice(p * L, p * L + L)
            xc = conv(xl_ref, t0, wx_scr.at[p], lanes, prm_ref[0:4, lanes], prm_ref[4:5, lanes])
            x = xc * sigmoid(xc)
            h0, h1 = 2 * p, 2 * p + 1
            a0, a1 = spread(cum, h0), spread(cum, h1)
            ap = jnp.where(lo, a0, a1)
            k0 = both * jnp.exp2(jnp.where(tri, a0 - cum_t[h0 : h0 + 1], -jnp.inf))
            k1 = both * jnp.exp2(jnp.where(tri, a1 - cum_t[h1 : h1 + 1], -jnp.inf))
            xdt = x * jnp.where(lo, spread(dt, h0), spread(dt, h1))
            xb = xdt.astype(bf16)
            fin = ap[L - 1 : L]
            within = nn(
                jnp.concatenate([k0.astype(bf16), k1.astype(bf16)], axis=1),
                jnp.concatenate([xb * mlo, xb * mhi], axis=0),
            )
            y = within + jnp.exp2(ap) * cs_scr[:, lanes] + prm_ref[5:6, lanes] * x
            xs_scr[:, lanes] = (xdt * jnp.exp2(fin - ap)).astype(bf16)
            s_scr[:, lanes] = s_scr[:, lanes] * jnp.exp2(fin)
            y_ref[rows, lanes] = y.astype(bf16)
            z = z_scr[rows, lanes]
            u = u_scr[rows, lanes]
            z_ref[rows, lanes] = z.astype(bf16)
            u_ref[rows, lanes] = u.astype(bf16)
            gated = y * (z * sigmoid(z))
            q = gated * prm_ref[6:7, lanes]
            q_scr[rows, lanes] = q.astype(bf16)
            squares = squares + gated * gated
            inner = inner + u * q
        s_scr[...] += nn(bm.T, xs_scr[...])
        s0 = jnp.sum(squares, axis=1, keepdims=True)
        s1 = jnp.sum(inner, axis=1, keepdims=True)
        lane = lane_iota((L, L))
        stat = jnp.where(lane == 0, s0, jnp.where(lane == 1, s1, 0.0))
        st_ref[here, :, rows] = stat.T[0:2]

    @pl.loop(0, model // 256)
    def _(j):
        cols = pl.ds(pl.multiple_of(j * 256, 256), 256)
        po = nn(q_scr[:, 0:own], wo_ref[:, cols])
        if ncore == 2:
            po = po + nn(q_scr[:, own : 2 * own], wo_in[:, cols])
        po_scr[lax.rem(here, 2), :, cols] = po.astype(bf16)

    @pl.when(here == nloc - 1)
    def _():
        po_ref[...] = po_scr[(nloc - 1) % 2]
        block_done()
        if ncore == 2:
            for copy in weight_stores():
                copy.wait()


def block_out(inner_total, stot, yy, mine, parts, x_own, bo):
    Ry, model = x_own.shape
    for h in range(Ry // L):
        lanes = pl.ds(pl.multiple_of(yy * Ry + h * L, L), L)
        r_row = lax.rsqrt(stot[0:1, lanes] / inner_total + epsilon)
        r = jnp.broadcast_to(r_row, (8, L)).T[:, 0:1]

        @pl.loop(0, model // L)
        def _(m, h=h, r=r):
            cols = pl.ds(pl.multiple_of(m * L, L), L)
            rows = slice(h * L, h * L + L)
            total = mine[rows, cols].astype(f32)
            for part in parts:
                total = total + part[rows, cols].astype(f32)
            bo[rows, cols] = (x_own[rows, cols].astype(f32) + r * total).astype(bf16)


def gate_kernel(
    width,
    own,
    inner_total,
    ncore,
    ny,
    _seq,
    st_ref,
    stin_ref,
    g_ref,
    hid_ref,
    z_ref,
    y_ref,
    u_ref,
    prm_ref,
    po_ref,
    bo01_ref,
    x_ref,
    dz_ref,
    dy_ref,
    gz_ref,
    go_ref,
    ggg_ref,
    bo_ref,
    q_scr,
    sc_scr,
    dz_scr,
    stot_ref,
    st_in,
    send_scr,
    recv_scr,
    po_in,
    x_own,
    st_sems,
    core_send,
    core_recv,
    po_sems,
    local,
):
    rows_all = z_ref.shape[0]
    model = g_ref.shape[1]
    pairs = width // L
    here = pl.program_id(0)
    core, yy, twin, ys, peers = places(ncore, ny)
    nloc, Ry, _ = bo_ref.shape
    last = nloc - 1

    def row_copies():
        return [
            remote(st_ref.at[last], st_in.at[d], st_sems.at[0, d], st_sems.at[1, d], peers[d])
            for d in range(ny - 1)
        ]

    def po_copies():
        return [
            remote(
                po_ref.at[pl.ds(pl.multiple_of(ys[d] * Ry, Ry), Ry)],
                po_in.at[d],
                po_sems.at[0, d],
                po_sems.at[1, d],
                peers[d],
            )
            for d in range(ny - 1)
        ]

    def x_copy():
        return pltpu.make_async_copy(x_ref.at[core * nloc + last, yy], x_own, local.at[0])

    @pl.when(here == 0)
    def _():
        greet(peers + ([twin] if ncore == 2 else []))
        start(row_copies() + po_copies() + [x_copy()])
        stot_ref[...] = stin_ref[...]
        for i in range(last):
            bo_ref[i] = bo01_ref[i]
        ggg_ref[...] = jnp.zeros_like(ggg_ref)

    @pl.when(here == last)
    def _():
        for copy in row_copies():
            copy.wait()
        total = st_ref[last]
        for d in range(ny - 1):
            total = total + st_in[d]
        stot_ref[last] = total

    @pl.loop(0, rows_all // L)
    def _(c):
        rows = pl.ds(pl.multiple_of(c * L, L), L)
        st = stot_ref[here, :, rows]
        r_row = lax.rsqrt(st[0:1] / inner_total + epsilon)
        c_row = r_row * r_row * r_row * (st[1:2] / inner_total)
        cols8 = jnp.concatenate([r_row, c_row, jnp.zeros((6, L), f32)], axis=0).T
        r = jnp.broadcast_to(cols8[:, 0:1], (L, L))
        c2 = jnp.broadcast_to(cols8[:, 1:2], (L, L))
        for m in range(model // L):
            lanes = slice(m * L, m * L + L)
            sc_scr[here, rows, lanes] = (g_ref[rows, lanes].astype(f32) * r).astype(bf16)
        for p in range(pairs):
            lanes = slice(p * L, p * L + L)
            gg = prm_ref[6:7, lanes]
            z = z_ref[rows, lanes].astype(f32)
            y = y_ref[rows, lanes].astype(f32)
            sg = sigmoid(z)
            silz = z * sg
            gated = y * silz
            q_scr[here, rows, lanes] = (gated * gg).astype(bf16)
            dq = r * u_ref[rows, lanes].astype(f32)
            ggg_ref[:, lanes] += fold_rows(dq * gated)
            dgated = dq * gg - c2 * gated
            dy_ref[rows, lanes] = (dgated * silz).astype(bf16)
            dz = (dgated * y * (sg + silz * (1.0 - sg))).astype(bf16)
            dz_ref[rows, lanes] = dz
            dz_scr[here, rows, lanes] = dz

    @pl.when(here == last)
    def _():
        hid = hid_ref.reshape(nloc * rows_all, model)
        dz = dz_scr.reshape(nloc * rows_all, width)
        q = q_scr.reshape(nloc * rows_all, width)
        sc = sc_scr.reshape(nloc * rows_all, model)

        def sums(half, out_z, out_o):
            lanes = slice(half * own, half * own + own)

            @pl.loop(0, model // 256)
            def _(j):
                cols = pl.ds(pl.multiple_of(j * 256, 256), 256)
                gz = tn(hid[:, cols], dz[:, lanes])
                go = tn(sc[:, cols], q[:, lanes])
                out_z[cols, :] = gz.astype(bf16)
                out_o[cols, :] = go.astype(bf16)

        if ncore == 2:
            sums(1, send_scr.at[:, 0:own], send_scr.at[:, own : 2 * own])
        if ncore == 2:
            copy = remote(send_scr, recv_scr, core_send, core_recv, twin)
            copy.start()
        sums(0, gz_ref, go_ref)
        if ncore == 2:
            copy.wait()

            @pl.loop(0, model // 64)
            def _(j):
                rows = pl.ds(pl.multiple_of(j * 64, 64), 64)
                for ref, first in ((gz_ref, 0), (go_ref, own)):
                    theirs = recv_scr[rows, first : first + own].astype(f32)
                    ref[rows, :] = (ref[rows, :].astype(f32) + theirs).astype(bf16)

        for copy in po_copies() + [x_copy()]:
            copy.wait()
        parts = [po_in.at[d] for d in range(ny - 1)]
        mine = po_ref.at[pl.ds(pl.multiple_of(yy * Ry, Ry), Ry)]
        block_out(inner_total, stot_ref.at[last], yy, mine, parts, x_own, bo_ref.at[last])


def tail_part(own, ncore, ny, ndp, nloc, given, outs, late_to, ready_to, room, machine):
    gw_ref, gbcw_ref, small_ref, other_ref, shared_ref, dh_ref, gain_ref, x_ref, bo_ref = given
    fw_ref, fb_ref, fb_scr, small_full, small_src, small_out, shared_out, last_ref = outs
    dh_in, x_own, small_in, core_sems, y_sems, local = room
    model = gw_ref.shape[0]
    Ry = x_own.shape[0]
    core, yy, twin, ys, peers = places(ncore, ny)
    nbits = log2(ndp)
    dp_peers, dp_bits = bit_peers("dp", 1, 0, nbits)
    t_peers, t_bits = bit_peers("tensor", 1, 0, log2(ncore * ny))
    links = list(zip(dp_peers, dp_bits))
    swapped = [links[1], links[0]] + links[2:] if nbits > 1 else links
    t_links = list(zip(t_peers, t_bits))
    per = nbits + 2
    a, b = machine[:per], machine[per : 2 * per]
    per_bc = nbits + len(t_links) + 2
    c = machine[2 * per : 2 * per + per_bc]
    d, sh = machine[2 * per + per_bc : 3 * per + per_bc], machine[3 * per + per_bc :]
    mid = model // 2
    job_a = Halving(links, mid, gw_ref.at[0:mid], a[0], a[1:-1], fw_ref.at[0:mid], a[-1])
    job_b = Halving(swapped, mid, gw_ref.at[mid:model], b[0], b[1:-1], fw_ref.at[mid:model], b[-1])
    job_c = Halving(t_links + links, model, gbcw_ref, c[0], c[1:-1], fb_scr, c[-1])
    job_sm = Halving(links, small_src.shape[0], small_src, d[0], d[1:-1], small_full, d[-1])
    job_sh = Doubling(t_peers + dp_peers, *sh)

    def dh_copies():
        return [
            remote(
                dh_ref.at[pl.ds(pl.multiple_of(ys[d] * Ry, Ry), Ry)],
                dh_in.at[d],
                y_sems.at[0, d],
                y_sems.at[1, d],
                peers[d],
            )
            for d in range(ny - 1)
        ]

    place = (twin, peers, ncore)
    late = Spread(last_ref, *late_to, place)
    ready = [Spread(bo_ref.at[nloc - 1], *ready_to, place)]
    x_copy = pltpu.make_async_copy(x_ref.at[core * nloc + nloc - 1, yy], x_own, local.at[1])

    def turn(*pairs):
        for job, j in pairs:
            job.close(j)
        for job, j in pairs:
            job.begin(j)

    job_sh.acc[0] = shared_ref[...]
    turn((job_c, 0), (job_sh, 0))
    yield
    turn((job_c, 1), (job_sh, 1))
    start(dh_copies())
    x_copy.start()
    for spread in ready:
        start(spread.first())
    if ncore == 2:
        small_copy = remote(other_ref, small_in, core_sems.at[0], core_sems.at[1], twin)
        small_copy.start()
    yield
    turn((job_a, 0), (job_b, 0))
    if ncore == 2:
        small_copy.wait()
        small_src[...] = small_ref[...] + small_in[...]
    else:
        small_src[...] = small_ref[...]
    turn((job_sm, 0))
    steps = [
        (job_c, iter(range(2, 2 * job_c.n + 1))),
        (job_sm, iter(range(1, 2 * nbits + 1))),
        (job_sh, iter(range(2, len(job_sh.peers) + 1))),
    ]

    def smaller():
        found = []
        for job, left in steps:
            j = next(left, None)
            if j is not None:
                found.append((job, j))
        return found

    for j in range(1, 2 * nbits + 1):
        turn(*smaller(), (job_a, j), (job_b, j))
        if j == 2:
            wait(dh_copies())
            x_copy.wait()

            @pl.loop(0, Ry // 32)
            def _(i):
                rows = pl.ds(pl.multiple_of(i * 32, 32), 32)
                mine = pl.ds(pl.multiple_of(yy * Ry + i * 32, 32), 32)
                dh = dh_ref[mine, :].astype(f32)
                for d in range(ny - 1):
                    dh = dh + dh_in[d, rows, :].astype(f32)
                last_ref[rows, :] = correction(x_own[rows, :], dh, gain_ref[...]).astype(bf16)

            start(late.first())
    for spread in ready:
        wait(spread.first())
        start(spread.second())
    for _ in range(2 * job_c.n):
        turn(*smaller())
    fb_copy = pltpu.make_async_copy(fb_scr, fb_ref, local.at[1])
    fb_copy.start()
    small_out[...] = small_full[...]
    shared_out[...] = job_sh.acc[len(job_sh.peers)]
    wait(late.first())
    start(late.second())
    for spread in ready + [late]:
        wait(spread.second())
    fb_copy.wait()
    yield


def scan_kernel(
    width,
    own,
    heads,
    ncore,
    ny,
    ndp,
    nloc_static,
    _seq,
    hid_ref,
    dz_ref,
    dy_ref,
    xl_ref,
    bcl_ref,
    dtl_ref,
    sin_ref,
    wz_ref,
    wzo_ref,
    wx_ref,
    wxo_ref,
    wbc_ref,
    wdt_ref,
    prm_ref,
    bcp_ref,
    hp_ref,
    ggg_ref,
    gain_ref,
    gz_ref,
    go_ref,
    bo_ref,
    x_ref,
    corr_ref,
    small_out,
    shared_out,
    last_ref,
    fz_ref,
    fo_ref,
    boy_ref,
    bot_ref,
    boty_ref,
    cy_ref,
    ct_ref,
    cty_ref,
    fw_ref,
    fb_ref,
    ly_ref,
    lt_ref,
    lty_ref,
    zy_ref,
    zt_ref,
    zty_ref,
    d_scr,
    bcc_scr,
    bca_scr,
    ds_scr,
    dsb_scr,
    cs_scr,
    bds_scr,
    xs_scr,
    dye_scr,
    nx_scr,
    nbc_scr,
    wx_scr,
    wbc_scr,
    red_scr,
    end_scr,
    pick_scr,
    gx_ref,
    gbc_ref,
    gdt_ref,
    gpre_ref,
    acc_scr,
    send_scr,
    recv_scr,
    dh_scr,
    dh_in,
    x_own,
    core_send,
    core_recv,
    y_sems,
    bo_sems,
    c_sems,
    local,
    gw_ref,
    gbcw_ref,
    small_ref,
    other_ref,
    shared_ref,
    small_in,
    fb_scr,
    small_full,
    small_src,
    end_in,
    x_end,
    core_sems,
    end_sems,
    l_sems,
    z_sems,
    *machine,
):
    rows_all = dz_ref.shape[0]
    model = hid_ref.shape[1]
    pairs = width // L
    spans = rows_all // L
    Ry = rows_all // ny
    seq, back = pl.program_id(0), pl.program_id(1)
    step = seq * spans + back
    core, yy, twin, ys, peers = places(ncore, ny)
    nbits = log2(ndp)
    dp_peers, dp_bits = bit_peers("dp", 1, 0, nbits)
    links = list(zip(dp_peers, dp_bits))
    swapped = [links[1], links[0]] + links[2:] if nbits > 1 else links
    per = nbits + 2
    mz, mo, rest = machine[:per], machine[per : 2 * per], machine[2 * per :]
    jobs = [
        Halving(links, model, gz_ref, mz[0], mz[1:-1], fz_ref, mz[-1]),
        Halving(swapped, model, go_ref, mo[0], mo[1:-1], fo_ref, mo[-1]),
    ]
    last_step = nloc_static * spans - 1

    place = (twin, peers, ncore)
    some = pl.ds(0, nloc_static - 1)
    bo_spread = Spread(bo_ref.at[some], boy_ref, bot_ref, boty_ref, bo_sems, place)

    def corr_spread(i):
        return Spread(
            corr_ref.at[i], cy_ref.at[:, i], ct_ref.at[i], cty_ref.at[:, i], c_sems.at[:, i], place
        )

    def dh_copies():
        return [
            remote(
                dh_scr.at[pl.ds(pl.multiple_of(ys[d] * Ry, Ry), Ry)],
                dh_in.at[seq - 1, d],
                y_sems.at[0, seq - 1, d],
                y_sems.at[1, seq - 1, d],
                peers[d],
            )
            for d in range(ny - 1)
        ]

    def x_copy():
        return pltpu.make_async_copy(x_ref.at[core * nloc_static + seq - 1, yy], x_own, local.at[0])

    @pl.when(step == 0)
    def _():
        greet(peers + dp_peers + ([twin] if ncore == 2 else []))
        start(bo_spread.first())
        acc_scr[...] = jnp.zeros_like(acc_scr)
        end_scr[...] = jnp.zeros_like(end_scr)
        pick = row_iota((width, L)) // HEAD == lane_iota((width, L))
        pick_scr[...] = pick.astype(f32).astype(bf16)
        gx_ref[...] = jnp.zeros_like(gx_ref)
        gbc_ref[...] = jnp.zeros_like(gbc_ref)
        gdt_ref[...] = jnp.zeros_like(gdt_ref)
        gpre_ref[...] = jnp.zeros_like(gpre_ref)

    when = [0.0, 0.25, 0.33, 0.58, 0.67, 0.83]
    if nbits != 3:
        when = [j / (2 * nbits) for j in range(2 * nbits)]
    for j in range(2 * nbits):

        @pl.when(step == int(when[j] * (last_step + 1) + 0.1))
        def _(j=j):
            for job in jobs:
                job.close(j)
            for job in jobs:
                job.begin(j)

    @pl.when(step == spans + 2)
    def _():
        wait(bo_spread.first())
        start(bo_spread.second())

    for i in range(nloc_static - 2):

        @pl.when(step == (i + 2) * spans + 2)
        def _(i=i):
            wait(corr_spread(i).first())
            start(corr_spread(i).second())

    @pl.when(jnp.logical_and(seq > 0, back == 0))
    def _():
        for copy in dh_copies():
            copy.start()
        x_copy().start()

    @pl.when(jnp.logical_and(seq > 0, back == spans - 1))
    def _():
        for copy in dh_copies():
            copy.wait()
        x_copy().wait()

        @pl.loop(0, Ry // 32)
        def _(i):
            rows = pl.ds(pl.multiple_of(i * 32, 32), 32)
            mine = pl.ds(pl.multiple_of(yy * Ry + i * 32, 32), 32)
            dh = dh_scr[mine, :].astype(f32)
            for d in range(ny - 1):
                dh = dh + dh_in[seq - 1, d, rows, :].astype(f32)
            corr_ref[seq - 1, rows, :] = correction(x_own[rows, :], dh, gain_ref[...]).astype(bf16)

        start(corr_spread(seq - 1).first())

    hp = hp_ref[...]

    @pl.when(back == 0)
    def _():
        ds_scr[...] = jnp.zeros_like(ds_scr)
        nx_scr[...] = jnp.zeros_like(nx_scr)
        nbc_scr[...] = jnp.zeros_like(nbc_scr)

        @pl.loop(0, spans)
        def _(c):
            t0 = pl.multiple_of(c * L, L)
            for half in range(2):
                lanes = slice(half * L, half * L + L)
                v = conv(bcl_ref, t0, wbc_scr.at[half], lanes, bcp_ref[0:4, lanes], bcp_ref[4:5, lanes])
                bcc_scr[pl.ds(t0, L), lanes] = v
                bca_scr[pl.ds(t0, L), lanes] = (v * sigmoid(v)).astype(bf16)

    def one_chunk():
        c = spans - 1 - back
        t0 = pl.multiple_of(c * L, L)
        rows = pl.ds(t0, L)
        lane = lane_iota((L, L))
        lo = lane < HEAD
        mlo = (lane_iota((1, L)) < HEAD).astype(bf16)
        mhi = (lane_iota((1, L)) >= HEAD).astype(bf16)
        tri = row_iota((L, L)) >= lane
        pre, dt, cum, cum_t = span_decay(dtl_ref[rows, :], hp)
        bm = bca_scr[rows, 0:L]
        cm = bca_scr[rows, L : 2 * L]
        both = nt(cm, bm)
        sb = sin_ref[c]
        dsb_scr[...] = ds_scr[...].astype(bf16)
        cs_scr[...] = nn(cm, sb)
        bds_scr[...] = nn(bm, dsb_scr[...])
        d_both = jnp.zeros((L, L), f32)
        for p in range(pairs):
            lanes = slice(p * L, p * L + L)
            taps = prm_ref[0:4, lanes]
            xc = conv(xl_ref, t0, wx_scr.at[p], lanes, taps, prm_ref[4:5, lanes])
            sg = sigmoid(xc)
            x = xc * sg
            h0, h1 = 2 * p, 2 * p + 1
            a0, a1 = spread(cum, h0), spread(cum, h1)
            ap = jnp.where(lo, a0, a1)
            e0 = jnp.exp2(jnp.where(tri, a0 - cum_t[h0 : h0 + 1], -jnp.inf))
            e1 = jnp.exp2(jnp.where(tri, a1 - cum_t[h1 : h1 + 1], -jnp.inf))
            k0 = (both * e0).astype(bf16)
            k1 = (both * e1).astype(bf16)
            dtp = jnp.where(lo, spread(dt, h0), spread(dt, h1))
            xdt = x * dtp
            xb = xdt.astype(bf16)
            bdx = jnp.concatenate([xb * mlo, xb * mhi], axis=0)
            ecum = jnp.exp2(ap)
            fin = ap[L - 1 : L]
            sd = jnp.exp2(fin - ap)
            y = nn(jnp.concatenate([k0, k1], axis=1), bdx) + ecum * cs_scr[:, lanes]
            dyb = dy_ref[rows, lanes]
            dy = dyb.astype(f32)
            dk = nt(dyb, bdx)
            d_both = d_both + dk[:, 0:L] * e0 + dk[:, L : 2 * L] * e1
            bdy = jnp.concatenate([dyb * mlo, dyb * mhi], axis=0)
            near = tn(jnp.concatenate([k0, k1], axis=0), bdy)
            far = sd * bds_scr[:, lanes]
            dxdt = near + far
            v = dy * y - xb.astype(f32) * near
            u = dxdt * x
            w = xdt * far
            ends = jnp.exp2(fin)
            through = ends * jnp.sum(sb[:, lanes].astype(f32) * ds_scr[:, lanes], axis=0, keepdims=True)
            v_hi = v.astype(bf16)
            red_scr[0:L, lanes] = v_hi
            red_scr[L : 2 * L, lanes] = (v - v_hi.astype(f32)).astype(bf16)
            red_scr[2 * L : 3 * L, lanes] = u.astype(bf16)
            red_scr[3 * L : 4 * L, lanes] = w.astype(bf16)
            end_scr[0:1, lanes] = through
            dx = dxdt * dtp + dy * prm_ref[5:6, lanes]
            dxc = dx * (sg + x * (1.0 - sg))
            for k in range(4):
                gx_ref[k, :, lanes] += fold_rows(dxc * tap(wx_scr.at[p], k))
            gx_ref[4, :, lanes] += fold_rows(dxc)
            gx_ref[5, :, lanes] += fold_rows(dy * x)
            nx_scr[p, L : L + 8] = nx_scr[p, 0:8]
            nx_scr[p, 0:L] = dxc
            dxl = dxc * taps[3:4]
            for k in range(3):
                dxl = dxl + nx_scr[p, 3 - k : 3 - k + L] * taps[k : k + 1]
            d_scr[rows, lanes] = dxl.astype(bf16)
            xs_scr[:, lanes] = (xdt * sd).astype(bf16)
            dye_scr[:, lanes] = (dy * ecum).astype(bf16)
            ds_scr[:, lanes] = ds_scr[:, lanes] * ends
        ds_scr[...] += nn(cm.T, dye_scr[...])
        sums = nn(red_scr[...], pick_scr[...])
        d_cum = sums[0:L] + sums[L : 2 * L]
        d_dt = sums[2 * L : 3 * L]
        d_far = sums[3 * L : 4 * L]
        d_end = exact(end_scr[...], pick_scr[...].astype(f32))[0:1]
        utri = (row_iota((L, L)) <= lane).astype(f32)
        before = (row_iota((L, L)) > lane).astype(f32)
        d_a = exact(utri, d_cum) + exact(before, d_far) + d_end
        d_dt = d_dt + d_a * hp[1:2]
        d_pre = d_dt * sigmoid(pre)
        gdt_ref[0] += fold_rows(d_pre)
        gdt_ref[1] += fold_rows(d_a * dt * hp[1:2])
        d_scr[rows, width + 256 : width + 384] = d_pre.astype(bf16)
        dgb = d_both.astype(bf16)
        d_c = nt(dye_scr[...], sb) + nn(dgb, bm)
        d_b = nt(xs_scr[...], dsb_scr[...]) + nn(dgb.T, cm)
        for half, dv in ((0, d_b), (1, d_c)):
            lanes = slice(half * L, half * L + L)
            pre_act = bcc_scr[rows, lanes]
            sg = sigmoid(pre_act)
            dvc = dv * (sg + pre_act * sg * (1.0 - sg))
            wbc_scr[half] = bcl_ref[pl.ds(t0, L + PAD), lanes]
            for k in range(4):
                gbc_ref[k, :, lanes] += fold_rows(dvc * tap(wbc_scr.at[half], k))
            gbc_ref[4, :, lanes] += fold_rows(dvc)
            nbc_scr[half, L : L + 8] = nbc_scr[half, 0:8]
            nbc_scr[half, 0:L] = dvc
            dvl = dvc * bcp_ref[3:4, lanes]
            for k in range(3):
                dvl = dvl + nbc_scr[half, 3 - k : 3 - k + L] * bcp_ref[k : k + 1, lanes]
            d_scr[rows, width + half * L : width + half * L + L] = dvl.astype(bf16)

    one_chunk()

    @pl.when(back == spans - 1)
    def _():
        @pl.loop(0, model // 256)
        def _(j):
            cols = pl.ds(pl.multiple_of(j * 256, 256), 256)
            dh = nt(dz_ref[:, 0:own], wz_ref[cols, :]) + nt(d_scr[:, 0:own], wx_ref[cols, :])
            if ncore == 2:
                dh = dh + nt(dz_ref[:, own:width], wzo_ref[cols, :])
                dh = dh + nt(d_scr[:, own:width], wxo_ref[cols, :])
            dh = dh + nt(d_scr[:, width : width + 256], wbc_ref[cols, :])
            dh = dh + nt(d_scr[:, width + 256 :], wdt_ref[cols, :])
            dh_scr[:, cols] = dh.astype(bf16)
            gpre_ref[:, cols] += fold_rows(dh * hid_ref[:, cols].astype(f32))
            acc_scr[cols, :] += tn(hid_ref[:, cols], d_scr[...])

    @pl.when(step == last_step)
    def _():
        end = tail_part(
            own,
            ncore,
            ny,
            ndp,
            nloc_static,
            (gw_ref, gbcw_ref, small_ref, other_ref, shared_ref, dh_scr, gain_ref, x_ref, bo_ref),
            (fw_ref, fb_ref, fb_scr, small_full, small_src, small_out, shared_out, last_ref),
            (ly_ref, lt_ref, lty_ref, l_sems),
            (zy_ref, zt_ref, zty_ref, z_sems),
            (end_in, x_end, small_in, core_sems, end_sems, local),
            rest,
        )
        gbcw_ref[...] = acc_scr[:, width : width + 256].astype(gbcw_ref.dtype)
        shared_ref[...] = jnp.zeros_like(shared_ref)
        gpre = jnp.sum(gpre_ref[...], axis=0, keepdims=True) / gain_ref[...]
        for k in range(model // L):
            shared_ref[k : k + 1, 0:L] = gpre[:, k * L : k * L + L]
        for k in range(5):
            shared_ref[k : k + 1, L : L + 256] = jnp.sum(gbc_ref[k], axis=0, keepdims=True)
        next(end)
        if ncore == 2:
            send_scr[...] = acc_scr[:, own:width].astype(bf16)
            copy = remote(send_scr, recv_scr, core_send, core_recv, twin)
        rows = [jnp.sum(gx_ref[k], axis=0, keepdims=True) for k in range(6)]
        rows.append(jnp.sum(ggg_ref[...], axis=0, keepdims=True))
        dts = [jnp.sum(gdt_ref[k], axis=0, keepdims=True) for k in range(2)]
        small_ref[...] = jnp.zeros_like(small_ref)
        other_ref[...] = jnp.zeros_like(other_ref)
        lines = 16 + heads * model // own

        def put(ref, k, row):
            for q in range(own // L):
                ref[q * lines + k : q * lines + k + 1, :] = row[:, q * L : q * L + L]

        for k in range(7):
            put(small_ref, k, rows[k][:, 0:own])
            if ncore == 2:
                put(other_ref, k, rows[k][:, own:width])
        for d in range(model // L):
            turned = acc_scr[d * L : d * L + L, width + 256 : width + 384].T
            line = (d * L % own) // L * lines + 16 + heads * (d * L // own)
            small_ref[line : line + heads, :] = turned[0:heads]
            if ncore == 2:
                other_ref[line : line + heads, :] = turned[heads : 2 * heads]
        for k in range(2):
            small_ref[7 + k : 8 + k, :] = dts[k]
            if ncore == 2:
                moved = pltpu.roll(jnp.broadcast_to(dts[k], (8, L)), L - heads, axis=1)
                other_ref[7 + k : 8 + k, :] = moved[0:1]
        if ncore == 2:
            copy.start()
        next(end)
        for job in jobs:
            job.close(2 * nbits)
        if ncore == 2:
            copy.wait()

        @pl.loop(0, model // 64)
        def _(i):
            rows = pl.ds(pl.multiple_of(i * 64, 64), 64)
            total = acc_scr[rows, 0:own]
            if ncore == 2:
                total = total + recv_scr[rows, :].astype(f32)
            gw_ref[rows, :] = total.astype(bf16)

        for _ in end:
            pass
        final = corr_spread(nloc_static - 2)
        wait(final.first())
        start(final.second())
        wait(bo_spread.second())
        for i in range(nloc_static - 1):
            wait(corr_spread(i).second())


def finish_kernel(pieces, nloc, _idx, g_ref, *refs):
    gi_ref, bo_ref = refs[-2:]
    groups = [refs[n * pieces : (n + 1) * pieces] for n in range(4)]
    now = pl.program_id(1)
    for k in range(pieces):
        here = pl.program_id(0) == k

        def when(turn, here=here):
            return pl.when(jnp.logical_and(here, turn))

        for n, turn in ((0, now < nloc - 1), (1, now == nloc - 1)):

            @when(turn)
            def _(src=groups[n][k]):
                gi_ref[...] = g_ref[...].astype(f32) + src[...].astype(f32)

        for n, turn in ((2, now < nloc - 1), (3, now == nloc - 1)):

            @when(turn)
            def _(src=groups[n][k]):
                bo_ref[...] = src[...]


def unpack_kernel(own, heads, gz_total, gz_ref, go_ref, gw_ref, fb_ref, small_ref, shared_ref, *outs):
    gzx_ref, gwo_ref, gwdt_ref, gwbc_ref = outs[:4]
    lines = 16 + heads * gz_total // own
    gcxw_ref, gcxb_ref, gd_ref, ggg_ref, gdtb_ref, galog_ref, gpre_ref, gcbw_ref, gcbb_ref = outs[4:]
    gzx_ref[:, 0, :] = gz_ref[...].astype(f32)
    gzx_ref[:, 1, :] = gw_ref[:, 0:own].astype(f32)
    for d in range(gpre_ref.shape[1] // L):

        @pl.when(pl.program_id(0) == d)
        def _(d=d):
            line = (d * L % own) // L * lines + 16 + heads * (d * L // own)
            rows = small_ref[line : line + heads, :]
            if heads < 8:
                rows = jnp.concatenate([rows, jnp.zeros((8 - heads, L), f32)], axis=0)
            gwdt_ref[...] = rows.T[:, 0:heads]

    gwbc_ref[...] = fb_ref[...].astype(f32)
    v = go_ref[...].astype(f32)
    for k in range(own // L):
        gwo_ref[k * L : k * L + L, :] = v[:, k * L : k * L + L].T

    @pl.when(pl.program_id(0) == 0)
    def _():
        pick = (row_iota((L, L)) // HEAD == lane_iota((L, L))).astype(f32)
        for q in range(own // L):
            part, cols = small_ref[q * lines : q * lines + 8, :], slice(q * L, q * L + L)
            gcxw_ref[:, cols] = part[0:4]
            gcxb_ref[:, cols] = part[4:5]
            ggg_ref[:, cols] = part[6:7]
            each = L // HEAD
            gd_ref[:, q * each : q * each + each] = exact(part, pick)[5:6, 0:each]
        gdtb_ref[...] = small_ref[7:8, 0:heads]
        galog_ref[...] = small_ref[8:9, 0:heads]
        for k in range(gpre_ref.shape[1] // L):
            gpre_ref[:, k * L : k * L + L] = shared_ref[k : k + 1, 0:L]
        gcbw_ref[...] = shared_ref[0:4, L : L + 256]
        gcbb_ref[...] = shared_ref[4:5, L : L + 256]


def seq_spec(*shape):
    zeros = (0,) * len(shape)
    return pl.BlockSpec((None,) + shape, lambda i, s: (i,) + zeros)


def moved_spec(ncore, nloc, *shape):
    zeros = (0,) * len(shape)

    def index(i, s):
        return (i + lax.rem(lax.axis_index("tensor"), ncore) * nloc,) + zeros

    return pl.BlockSpec((None,) + shape, index)


def whole_spec(*shape):
    zeros = (0,) * len(shape)
    return pl.BlockSpec(shape, lambda *_: zeros, pipeline_mode=pl.Buffered(1))


def call(
    kernel, grid, in_specs, out_specs, out_shape, scratch, name, flops=0, moved=0, group=None
):
    return pl.pallas_call(
        kernel,
        grid_spec=pltpu.PrefetchScalarGridSpec(
            num_scalar_prefetch=1,
            grid=grid,
            in_specs=in_specs,
            out_specs=out_specs,
            scratch_shapes=scratch,
        ),
        out_shape=out_shape,
        cost_estimate=pl.CostEstimate(
            flops=int(flops), bytes_accessed=int(moved), transcendentals=0
        ),
        name=name,
        compiler_params=None
        if group is None
        else pltpu.CompilerParams(collective_id=group, has_side_effects=True),
    )


def sds(*shape, dtype=f32):
    return jax.ShapeDtypeStruct(shape, dtype)


def body(
    block_input,
    pre_gain,
    w_zx,
    w_bc,
    w_dt,
    conv_x_w,
    conv_x_b,
    conv_bc_w,
    conv_bc_b,
    dt_bias,
    a_log,
    d_skip,
    gate_gain,
    w_out,
    out_grad,
):
    tok, model = block_input.shape
    own = w_zx.shape[2]
    heads = w_dt.shape[1]
    nt = lax.axis_size("tensor")
    ndp = lax.axis_size("dp")
    inner_total = own * nt
    ncore = 2 if nt % 2 == 0 else 1
    ny = nt // ncore
    width = own * ncore
    t = lax.axis_index("tensor")
    core, yy = t % ncore, t // ncore
    R = SEQ_LEN
    Ry = R // ny
    nseq = tok // R
    nloc = nseq // ncore
    spans = R // L
    wtot = 2 * width + 384
    pairs = width // L

    x3 = block_input.reshape(nseq, R, model)
    g3 = out_grad.reshape(nseq, R, model)
    x4 = block_input.reshape(nseq, ny, Ry, model)
    g4 = out_grad.reshape(nseq, ny, Ry, model)
    wz, wx = w_zx[:, 0], w_zx[:, 1]
    sm = jnp.concatenate(
        [
            conv_x_w,
            conv_x_b[None],
            jnp.repeat(d_skip, HEAD)[None],
            gate_gain[None],
            jnp.zeros((1, own), f32),
            jnp.pad(jnp.stack([dt_bias, -jnp.exp(a_log)]), ((0, 6), (0, own - heads))),
        ],
        axis=0,
    )
    wdt = jnp.pad(w_dt, ((0, 0), (0, L - heads)))
    bcp = jnp.concatenate([conv_bc_w, conv_bc_b[None], jnp.zeros((3, 256), f32)], axis=0)
    gain = pre_gain[None]
    seq0 = jnp.zeros((1,), jnp.int32)
    any_spec = pl.BlockSpec(memory_space=pl.ANY)
    nother = max(ny - 1, 1)
    dma = pltpu.SemaphoreType.DMA

    hid, z, xl, bcl, dtl, u, y, sin, st, stot, po, bo01, prm, hp, wdt, wzo, wxo = call(
        partial(forward_kernel, own, heads, ncore, ny, inner_total, nloc),
        (nloc,),
        [
            moved_spec(ncore, nloc, R, model),
            moved_spec(ncore, nloc, R, model),
            whole_spec(1, model),
            whole_spec(model, own),
            whole_spec(model, own),
            whole_spec(model, 256),
            whole_spec(model, L),
            whole_spec(own, model),
            whole_spec(16, own),
            whole_spec(8, 256),
            any_spec,
        ],
        [
            seq_spec(R, model),
            seq_spec(R, width),
            seq_spec(R + PAD, width),
            seq_spec(R + PAD, 256),
            seq_spec(R, L),
            seq_spec(R, width),
            seq_spec(R, width),
            seq_spec(spans, L, width),
            whole_spec(nloc, 2, R),
            whole_spec(nloc, 2, R),
            whole_spec(R, model),
            whole_spec(nloc - 1, Ry, model),
            whole_spec(8, width),
            whole_spec(8, L),
            whole_spec(model, L),
        ]
        + [any_spec] * 2,
        [
            sds(nloc, R, model, dtype=bf16),
            sds(nloc, R, width, dtype=bf16),
            sds(nloc, R + PAD, width),
            sds(nloc, R + PAD, 256),
            sds(nloc, R, L),
            sds(nloc, R, width, dtype=bf16),
            sds(nloc, R, width, dtype=bf16),
            sds(nloc, spans, L, width, dtype=bf16),
            sds(nloc, 2, R),
            sds(nloc, 2, R),
            sds(R, model, dtype=bf16),
            sds(nloc - 1, Ry, model, dtype=bf16),
            sds(8, width),
            sds(8, L),
            sds(model, L, dtype=bf16),
            sds(model, own, dtype=bf16),
            sds(model, own, dtype=bf16),
        ],
        [
            pltpu.VMEM((R, width), f32),
            pltpu.VMEM((R, width), f32),
            pltpu.VMEM((R, width), bf16),
            pltpu.VMEM((R, 256), bf16),
            pltpu.VMEM((L, width), f32),
            pltpu.VMEM((L, width), f32),
            pltpu.VMEM((L, width), bf16),
            pltpu.VMEM((pairs, L + PAD, L), f32),
            pltpu.VMEM((2, L + PAD, L), f32),
            pltpu.VMEM((model, own), bf16),
            pltpu.VMEM((model, own), bf16),
            pltpu.VMEM((own, model), bf16),
            pltpu.VMEM((model, L), bf16),
            pltpu.VMEM((16, own), f32),
            pltpu.VMEM((2, R, model), bf16),
            pltpu.VMEM((nloc - 1, nother, Ry, model), bf16),
            pltpu.VMEM((nloc - 1, nother, 2, R), f32),
            pltpu.VMEM((Ry, model), bf16),
            dma((2, 5)),
            dma((2, nloc - 1, nother)),
            dma((2, nloc - 1, nother)),
            dma((3,)),
        ],
        "forward",
        2 * nloc * R * model * (wtot + 2 * width),
        nloc * R * (6 * model + 20 * width),
        4,
    )(seq0, x3, g3, gain, wz, wx, w_bc, wdt, w_out, sm, bcp, x4)

    nbits = log2(ndp)
    dz, dy, gz, go, ggg, bo = call(
        partial(gate_kernel, width, own, inner_total, ncore, ny),
        (nloc,),
        [
            whole_spec(nloc, 2, R),
            whole_spec(nloc, 2, R),
            moved_spec(ncore, nloc, R, model),
            whole_spec(nloc, R, model),
            seq_spec(R, width),
            seq_spec(R, width),
            seq_spec(R, width),
            whole_spec(8, width),
            whole_spec(R, model),
            whole_spec(nloc - 1, Ry, model),
            any_spec,
        ],
        [
            seq_spec(R, width),
            seq_spec(R, width),
            whole_spec(model, own),
            whole_spec(model, own),
            whole_spec(8, width),
            whole_spec(nloc, Ry, model),
        ],
        [
            sds(nloc, R, width, dtype=bf16),
            sds(nloc, R, width, dtype=bf16),
            sds(model, own, dtype=bf16),
            sds(model, own, dtype=bf16),
            sds(8, width),
            sds(nloc, Ry, model, dtype=bf16),
        ],
        [
            pltpu.VMEM((nloc, R, width), bf16),
            pltpu.VMEM((nloc, R, model), bf16),
            pltpu.VMEM((nloc, R, width), bf16),
            pltpu.VMEM((nloc, 2, R), f32),
            pltpu.VMEM((nother, 2, R), f32),
            pltpu.VMEM((model, 2 * own), bf16),
            pltpu.VMEM((model, 2 * own), bf16),
            pltpu.VMEM((nother, Ry, model), bf16),
            pltpu.VMEM((Ry, model), bf16),
            dma((2, nother)),
            dma,
            dma,
            dma((2, nother)),
            dma((1,)),
        ],
        "gate",
        4 * nloc * R * model * width,
        nloc * R * (4 * model + 16 * width),
        1,
    )(seq0, st, stot, g3, hid, z, y, u, prm, po, bo01, x4)

    def chunk_spec(*shape):
        zeros = (0,) * len(shape)
        return pl.BlockSpec((None,) + shape, lambda i, b, s: (i,) + zeros)

    tbits = log2(nt)
    lines = 16 + heads * model // own
    srows = max(own // L * lines, 8 * ndp, 128)
    late_shape = sds(nother, Ry, model, dtype=bf16)
    bc_type = bf16 if (model // (nt * ndp)) % 16 == 0 else f32
    s_out = call(
        partial(scan_kernel, width, own, heads, ncore, ny, ndp, nloc),
        (nloc, spans),
        [
            chunk_spec(R, model),
            chunk_spec(R, width),
            chunk_spec(R, width),
            chunk_spec(R + PAD, width),
            chunk_spec(R + PAD, 256),
            chunk_spec(R, L),
            chunk_spec(spans, L, width),
            whole_spec(model, own),
            whole_spec(model, own),
            whole_spec(model, own),
            whole_spec(model, own),
            whole_spec(model, 256),
            whole_spec(model, L),
            whole_spec(8, width),
            whole_spec(8, 256),
            whole_spec(8, L),
            whole_spec(8, width),
            whole_spec(1, model),
            whole_spec(model, own),
            whole_spec(model, own),
            any_spec,
            any_spec,
        ],
        [
            whole_spec(nloc - 1, Ry, model),
            whole_spec(srows, L),
            whole_spec(model // L, L + 256),
            whole_spec(Ry, model),
        ]
        + [any_spec] * 16,
        [
            sds(nloc - 1, Ry, model, dtype=bf16),
            sds(srows, L),
            sds(model // L, L + 256),
            sds(Ry, model, dtype=bf16),
            sds(model, own, dtype=bf16),
            sds(model, own, dtype=bf16),
            sds(nother, nloc - 1, Ry, model, dtype=bf16),
            sds(nloc - 1, Ry, model, dtype=bf16),
            sds(nother, nloc - 1, Ry, model, dtype=bf16),
            sds(nother, nloc - 1, Ry, model, dtype=bf16),
            sds(nloc - 1, Ry, model, dtype=bf16),
            sds(nother, nloc - 1, Ry, model, dtype=bf16),
            sds(model, own, dtype=bf16),
            sds(model, 256, dtype=bc_type),
        ]
        + [late_shape, sds(Ry, model, dtype=bf16), late_shape] * 2,
        [
            pltpu.VMEM((R, width + 384), bf16),
            pltpu.VMEM((R, 256), f32),
            pltpu.VMEM((R, 256), bf16),
            pltpu.VMEM((L, width), f32),
            pltpu.VMEM((L, width), bf16),
            pltpu.VMEM((L, width), f32),
            pltpu.VMEM((L, width), f32),
            pltpu.VMEM((L, width), bf16),
            pltpu.VMEM((L, width), bf16),
            pltpu.VMEM((pairs, L + 8, L), f32),
            pltpu.VMEM((2, L + 8, L), f32),
            pltpu.VMEM((pairs, L + PAD, L), f32),
            pltpu.VMEM((2, L + PAD, L), f32),
            pltpu.VMEM((4 * L, width), bf16),
            pltpu.VMEM((8, width), f32),
            pltpu.VMEM((width, L), bf16),
            pltpu.VMEM((6, 8, width), f32),
            pltpu.VMEM((5, 8, 256), f32),
            pltpu.VMEM((2, 8, L), f32),
            pltpu.VMEM((8, model), f32),
            pltpu.VMEM((model, width + 384), f32),
            pltpu.VMEM((model, own), bf16),
            pltpu.VMEM((model, own), bf16),
            pltpu.VMEM((R, model), bf16),
            pltpu.VMEM((nloc - 1, nother, Ry, model), bf16),
            pltpu.VMEM((Ry, model), bf16),
            dma,
            dma,
            dma((2, nloc - 1, nother)),
            dma((2, 2 * ny)),
            dma((2, nloc - 1, 2 * ny)),
            dma((2,)),
            pltpu.VMEM((model, own), bf16),
            pltpu.VMEM((model, 256), bc_type),
            pltpu.VMEM((srows, L), f32),
            pltpu.VMEM((srows, L), f32),
            pltpu.VMEM((model // L, L + 256), f32),
            pltpu.VMEM((srows, L), f32),
            pltpu.VMEM((model, 256), bc_type),
            pltpu.VMEM((srows, L), f32),
            pltpu.VMEM((srows, L), f32),
            pltpu.VMEM((nother, Ry, model), bf16),
            pltpu.VMEM((Ry, model), bf16),
            dma((2,)),
            dma((2, nother)),
            dma((2, 2 * ny)),
            dma((2, 2 * ny)),
        ]
        + Halving.scratch(model, own, nbits, bf16)
        + Halving.scratch(model, own, nbits, bf16)
        + Halving.scratch(model // 2, own, nbits, bf16)
        + Halving.scratch(model // 2, own, nbits, bf16)
        + Halving.scratch(model, 256, nbits + tbits, bc_type)
        + Halving.scratch(srows, L, nbits, f32)
        + Doubling.scratch(nbits + tbits, model // L, L + 256),
        "scan_back",
        2 * nloc * R * model * (2 * wtot),
        nloc * R * (4 * model + 12 * width),
        2,
    )(seq0, hid, dz, dy, xl, bcl, dtl, sin, wz, wzo, wx, wxo, w_bc, wdt, prm, bcp, hp, ggg, gain, gz, go, bo, x4)

    corr, small, shared, last, fz, fo, boy, bot, boty, cy0, ct0, cty0, fw, fb = s_out[:14]
    late_got = s_out[14:]
    pieces = ncore * ny
    where = jnp.stack([core, yy]).astype(jnp.int32)

    def out_index(k, i, s):
        return ((s[0] ^ (k // ny)) * nloc + i, (s[1] - k % ny + ny) % ny, 0, 0)

    def spec_of(base, seq_of, d):
        if d is None:
            return pl.BlockSpec(
                (None, Ry, model), lambda j, i, s: (seq_of(j, i) - base, 0, 0)
            )
        return pl.BlockSpec(
            (None, None, Ry, model), lambda j, i, s: (d, seq_of(j, i) - base, 0, 0)
        )

    placed_spec = pl.BlockSpec((None, None, Ry, model), out_index)
    specs, arrays = [], []

    def add_group(first, count, mine, mine_base, toy, tot, toty):
        for k in range(pieces):

            def seq_of(j, i, k=k):
                i = jnp.clip(i, first, first + count - 1)
                return jnp.where(j == k, i, jnp.where(j > k, first + count - 1, first))

            d = k % ny - 1
            if k == 0:
                array, spec = mine, spec_of(mine_base, seq_of, None)
            elif k < ny:
                array, spec = toy, spec_of(first, seq_of, d)
            elif d < 0:
                array, spec = tot, spec_of(first, seq_of, None)
            else:
                array, spec = toty, spec_of(first, seq_of, d)
            arrays.append(array)
            specs.append(spec)

    def as_seq(v, axis):
        return jnp.expand_dims(v, axis)

    def add_late(first, mine, base, got):
        toy, tot, toty = got
        add_group(first, 1, mine, base, as_seq(toy, 1), as_seq(tot, 0), as_seq(toty, 1))

    add_group(0, nloc - 1, corr, 0, cy0, ct0, cty0)
    add_late(nloc - 1, as_seq(last, 0), nloc - 1, late_got[0:3])
    add_group(0, nloc - 1, bo, 0, boy, bot, boty)
    add_late(nloc - 1, bo, 0, late_got[3:6])
    grad_input, block_output = call(
        partial(finish_kernel, pieces, nloc),
        (pieces, nloc),
        [placed_spec] + specs,
        [placed_spec, placed_spec],
        [sds(nseq, ny, Ry, model), sds(nseq, ny, Ry, model, dtype=bf16)],
        [],
        "finish",
        0,
        12 * tok * model,
    )(where, g4, *arrays)

    def row_block(cols):
        return pl.BlockSpec((L, cols), lambda d: (d, 0))

    outs = pl.pallas_call(
        partial(unpack_kernel, own, heads, model),
        grid=(model // L,),
        in_specs=[row_block(own), row_block(own), row_block(own), row_block(256)]
        + [whole_spec(srows, L), whole_spec(model // L, L + 256)],
        out_specs=[
            pl.BlockSpec((L, 2, own), lambda d: (d, 0, 0)),
            pl.BlockSpec((own, L), lambda d: (0, d)),
            row_block(heads),
            row_block(256),
            whole_spec(4, own),
            whole_spec(1, own),
            whole_spec(1, heads),
            whole_spec(1, own),
            whole_spec(1, heads),
            whole_spec(1, heads),
            whole_spec(1, model),
            whole_spec(4, 256),
            whole_spec(1, 256),
        ],
        out_shape=[
            sds(model, 2, own),
            sds(own, model),
            sds(model, heads),
            sds(model, 256),
            sds(4, own),
            sds(1, own),
            sds(1, heads),
            sds(1, own),
            sds(1, heads),
            sds(1, heads),
            sds(1, model),
            sds(4, 256),
            sds(1, 256),
        ],
        name="unpack",
    )(fz, fo, fw, fb, small, shared)
    gzx, gwo, gwdt, gwbc, gcxw, gcxb, gd, ggg, gdtb, galog, gpre, gcbw, gcbb = outs
    return (
        block_output.reshape(tok, model),
        grad_input.reshape(tok, model),
        gpre[0],
        gzx,
        gwbc,
        gwdt,
        gcxw,
        gcxb[0],
        gcbw,
        gcbb[0],
        gdtb[0],
        galog[0],
        gd[0],
        ggg[0],
        gwo,
    )


def solution(mesh):
    placed = (
        P("dp", None),
        P(),
        P(None, None, "tensor"),
        P(),
        P(None, "tensor"),
        P(None, "tensor"),
        P("tensor"),
        P(),
        P(),
        P("tensor"),
        P("tensor"),
        P("tensor"),
        P("tensor"),
        P("tensor", None),
        P("dp", None),
    )
    return jax.shard_map(
        body,
        mesh=mesh,
        in_specs=placed,
        out_specs=(
            P("dp", None),
            P("dp", None),
            P(),
            P(None, None, "tensor"),
            P(),
            P(None, "tensor"),
            P(None, "tensor"),
            P("tensor"),
            P(),
            P(),
            P("tensor"),
            P("tensor"),
            P("tensor"),
            P("tensor"),
            P("tensor", None),
        ),
        check_vma=False,
    )
```

```python
from functools import partial

import jax
import jax.numpy as jnp
from jax import lax
from jax.experimental import pallas as pl
from jax.experimental.pallas import tpu as pltpu
from jax.sharding import PartitionSpec as P

SEQ_LEN = 512
L = 128
HEAD = 64
LOG2E = 1.4426950408889634
PAD = 8
epsilon = 1e-05
f32 = jnp.float32
bf16 = jnp.bfloat16
HI = lax.Precision.HIGHEST
MESH = pl.DeviceIdType.MESH


def nn(a, b):
    return lax.dot_general(a, b, (((1,), (0,)), ((), ())), preferred_element_type=f32)


def nt(a, b):
    return lax.dot_general(a, b, (((1,), (1,)), ((), ())), preferred_element_type=f32)


def tn(a, b):
    return lax.dot_general(a, b, (((0,), (0,)), ((), ())), preferred_element_type=f32)


def exact(a, b):
    return lax.dot_general(
        a, b, (((1,), (0,)), ((), ())), precision=HI, preferred_element_type=f32
    )


def sigmoid(v):
    return 0.5 + 0.5 * jnp.tanh(0.5 * v)


def softplus(v):
    u = jnp.exp(-jnp.abs(v))
    return jnp.maximum(v, 0.0) + jnp.where(u < 1e-3, u - 0.5 * u * u, jnp.log(1.0 + u))


def fold_rows(v):
    return jnp.sum(v.reshape(v.shape[0] // 8, 8, v.shape[1]), axis=0)


def lane_iota(shape):
    return lax.broadcasted_iota(jnp.int32, shape, 1)


def row_iota(shape):
    return lax.broadcasted_iota(jnp.int32, shape, 0)


def tap(win, k):
    return win[PAD - 3 + k : PAD - 3 + k + L, :]


def conv(ref, t0, win, lanes, taps, bias):
    win[...] = ref[pl.ds(t0, L + PAD), lanes]
    total = bias
    for k in range(4):
        total = total + tap(win, k) * taps[k : k + 1]
    return total


def spread(cols, head):
    return jnp.broadcast_to(cols[:, head : head + 1], (L, L))


def span_decay(dtl, hp):
    pre = dtl + hp[0:1]
    dt = softplus(pre)
    ltri = (row_iota((L, L)) >= lane_iota((L, L))).astype(f32)
    cum = exact(ltri, dt * (hp[1:2] * LOG2E))
    return pre, dt, cum, cum.T


def remote(src, dst, send, recv, where):
    return pltpu.make_async_remote_copy(
        src_ref=src,
        dst_ref=dst,
        send_sem=send,
        recv_sem=recv,
        device_id=where,
        device_id_type=MESH,
    )


def greet(peers):
    barrier = pltpu.get_barrier_semaphore()
    for peer in peers:
        pl.semaphore_signal(barrier, inc=1, device_id=peer, device_id_type=MESH)
    pl.semaphore_wait(barrier, len(peers))


def bit_peers(axis, base, first, count):
    me = lax.axis_index(axis)
    peers, bits = [], []
    for k in range(count):
        step = base * 2**k
        bit = lax.rem(me // step, 2)
        peers.append({axis: me + step * (1 - 2 * bit)})
        bits.append(bit)
    return peers, bits


class Halving:
    def __init__(self, links, rows, src, work, recvs, full, sems):
        self.links, self.rows = links, rows
        self.src, self.work, self.recvs, self.full, self.sems = src, work, recvs, full, sems
        self.n = len(links)
        offs, size = [0], rows
        for _, bit in links:
            size //= 2
            offs.append(offs[-1] + bit * size)
        self.offs = offs

    def size(self, k):
        return self.rows >> k

    def at(self, off, size):
        return pl.ds(pl.multiple_of(off, size), size)

    def scatter(self, k):
        peer, bit = self.links[k]
        half = self.size(k + 1)
        off = self.offs[k] + (1 - bit) * half
        if k == 0:
            src = self.src.at[self.at(off, half)]
        else:
            src = self.work.at[self.at(off - self.offs[1], half)]
        return remote(src, self.recvs[k], self.sems.at[0, k], self.sems.at[1, k], peer)

    def fold(self, k):
        self.scatter(k).wait()
        half = self.size(k + 1)
        step = min(half, 64)
        keep = self.offs[k + 1]

        @pl.loop(0, half // step)
        def _(i):
            off = i * step
            rows = pl.ds(pl.multiple_of(off, step), step)
            near = pl.ds(pl.multiple_of(keep - self.offs[1] + off, step), step)
            if k == 0:
                mine = self.src[pl.ds(pl.multiple_of(keep + off, step), step), :]
            else:
                mine = self.work[near, :]
            total = mine.astype(f32) + self.recvs[k][rows, :].astype(f32)
            self.work[near, :] = total.astype(self.work.dtype)

    def own_copy(self):
        last = self.size(self.n)
        return pltpu.make_async_copy(
            self.work.at[self.at(self.offs[self.n] - self.offs[1], last)],
            self.full.at[self.at(self.offs[self.n], last)],
            self.sems.at[0, 2 * self.n],
        )

    def gather(self, k):
        peer, _ = self.links[k]
        rows = self.at(self.offs[k + 1], self.size(k + 1))
        sems = self.sems
        return remote(
            self.full.at[rows],
            self.full.at[rows],
            sems.at[0, self.n + k],
            sems.at[1, self.n + k],
            peer,
        )

    def close(self, j):
        n = self.n
        if 1 <= j <= n:
            self.fold(j - 1)
        elif j > n:
            self.gather(2 * n - j).wait()

    def begin(self, j):
        n = self.n
        if j < n:
            self.scatter(j).start()
            return
        if j == n:
            self.own_copy().start()
            self.own_copy().wait()
        if j < 2 * n:
            self.gather(2 * n - 1 - j).start()

    @staticmethod
    def scratch(rows, cols, n, dtype):
        recvs = [pltpu.VMEM((rows >> (k + 1), cols), dtype) for k in range(n)]
        return [pltpu.VMEM((rows // 2, cols), dtype)] + recvs + [
            pltpu.SemaphoreType.DMA((2, 2 * n + 1))
        ]


class Doubling:
    def __init__(self, peers, acc, recv, sems):
        self.peers, self.acc, self.recv, self.sems = peers, acc, recv, sems

    def copy(self, k):
        return remote(
            self.acc.at[k],
            self.recv.at[k],
            self.sems.at[0, k],
            self.sems.at[1, k],
            self.peers[k],
        )

    def close(self, j):
        if j > 0:
            self.copy(j - 1).wait()
            self.acc[j] = self.acc[j - 1] + self.recv[j - 1]

    def begin(self, j):
        if j < len(self.peers):
            self.copy(j).start()

    @staticmethod
    def scratch(n, rows, cols):
        return [
            pltpu.VMEM((n + 1, rows, cols), f32),
            pltpu.VMEM((n, rows, cols), f32),
            pltpu.SemaphoreType.DMA((2, n)),
        ]


class Spread:
    def __init__(self, src, toy, tot, toty, sems, place):
        self.src, self.toy, self.tot, self.toty, self.sems = src, toy, tot, toty, sems
        self.twin, self.peers, self.ncore = place

    def first(self):
        n = len(self.peers)
        sems = self.sems
        out = [
            remote(self.src, self.toy.at[d], sems.at[0, d], sems.at[1, d], self.peers[d])
            for d in range(n)
        ]
        if self.ncore == 2:
            out.append(remote(self.src, self.tot, sems.at[0, n], sems.at[1, n], self.twin))
        return out

    def second(self):
        n = len(self.peers)
        if self.ncore != 2:
            return []
        sems = self.sems
        return [
            remote(
                self.toy.at[d], self.toty.at[d], sems.at[0, n + 1 + d], sems.at[1, n + 1 + d], self.twin
            )
            for d in range(n)
        ]


def start(copies):
    for copy in copies:
        copy.start()


def wait(copies):
    for copy in copies:
        copy.wait()


def correction(x, dh, gain):
    v = x.astype(f32)
    r = lax.rsqrt(jnp.mean(v * v, axis=1, keepdims=True) + epsilon)
    normed = v * r
    dn = dh * gain
    return r * (dn - normed * jnp.mean(dn * normed, axis=1, keepdims=True))


def places(ncore, ny):
    spot = lax.axis_index("tensor")
    core, yy = lax.rem(spot, ncore), spot // ncore
    ys = [lax.rem(yy + d, ny) for d in range(1, ny)]
    peers = [{"tensor": v * ncore + core} for v in ys]
    return core, yy, {"tensor": spot + 1 - 2 * core}, ys, peers


def log2(n):
    return n.bit_length() - 1


def forward_kernel(
    own,
    heads,
    ncore,
    ny,
    inner_total,
    nloc,
    _seq,
    x_ref,
    g_ref,
    gain_ref,
    wz_ref,
    wx_ref,
    wbc_ref,
    wdt_ref,
    wo_ref,
    sm_ref,
    bcp_ref,
    x4_ref,
    hid_ref,
    z_ref,
    xl_ref,
    bcl_ref,
    dtl_ref,
    u_ref,
    y_ref,
    sin_ref,
    st_ref,
    stot_ref,
    po_ref,
    bo_ref,
    prm_ref,
    hp_ref,
    wdt_out,
    wz_out,
    wx_out,
    z_scr,
    u_scr,
    q_scr,
    bca_scr,
    s_scr,
    cs_scr,
    xs_scr,
    wx_scr,
    wbc_scr,
    wz_in,
    wx_in,
    wo_in,
    wdt_in,
    sm_in,
    po_scr,
    po_in,
    st_in,
    x_own,
    w_sems,
    po_sems,
    st_sems,
    local,
):
    rows_all = x_ref.shape[0]
    model = x_ref.shape[1]
    width = own * ncore
    pairs = width // L
    Ry = rows_all // ny
    here = pl.program_id(0)
    core, yy, twin, ys, peers = places(ncore, ny)

    def weight_copies():
        both = ((sm_ref, sm_in), (wdt_ref, wdt_in), (wz_ref, wz_in), (wx_ref, wx_in), (wo_ref, wo_in))
        return [
            remote(src, dst, w_sems.at[0, k], w_sems.at[1, k], twin)
            for k, (src, dst) in enumerate(both)
        ]

    def weight_stores():
        return [
            pltpu.make_async_copy(wz_in, wz_out, local.at[1]),
            pltpu.make_async_copy(wx_in, wx_out, local.at[2]),
        ]

    def row_copies():
        last = here - 1
        return [
            remote(
                st_ref.at[last],
                st_in.at[last, d],
                st_sems.at[0, last, d],
                st_sems.at[1, last, d],
                peers[d],
            )
            for d in range(ny - 1)
        ] + [
            remote(
                po_scr.at[lax.rem(last, 2), pl.ds(pl.multiple_of(ys[d] * Ry, Ry), Ry)],
                po_in.at[last, d],
                po_sems.at[0, last, d],
                po_sems.at[1, last, d],
                peers[d],
            )
            for d in range(ny - 1)
        ]

    def x_copy():
        return pltpu.make_async_copy(x4_ref.at[core * nloc + here - 1, yy], x_own, local.at[0])

    @pl.when(here == 0)
    def _():
        greet(peers + ([twin] if ncore == 2 else []))
        if ncore == 2:
            for copy in weight_copies():
                copy.start()

    @pl.when(here > 0)
    def _():
        start(row_copies())
        x_copy().start()

    @pl.loop(0, rows_all // 32)
    def _(i):
        rows = pl.ds(pl.multiple_of(i * 32, 32), 32)
        v = x_ref[rows, :].astype(f32)
        r = lax.rsqrt(jnp.mean(v * v, axis=1, keepdims=True) + epsilon)
        hid_ref[rows, :] = (v * r * gain_ref[...]).astype(bf16)

    xl_ref[0:PAD, :] = jnp.zeros((PAD, width), f32)
    bcl_ref[0:PAD, :] = jnp.zeros((PAD, 256), f32)

    def project(wz, wx, wo, base):
        @pl.loop(0, own // 256)
        def _(j):
            src = pl.ds(pl.multiple_of(j * 256, 256), 256)
            cols = pl.ds(pl.multiple_of(base + j * 256, 256), 256)
            z_scr[:, cols] = nn(hid_ref[...], wz[:, src])
            xl_ref[PAD : PAD + rows_all, cols] = nn(hid_ref[...], wx[:, src])
            u_scr[:, cols] = nt(g_ref[...], wo[src, :])

    project(wz_ref, wx_ref, wo_ref, 0)
    bcl_ref[PAD : PAD + rows_all, :] = nn(hid_ref[...], wbc_ref[...])

    @pl.when(here == 0)
    def _():
        prm_ref[:, 0:own] = sm_ref[0:8, :]
        hp_ref[...] = sm_ref[8:16, 0:L]
        wdt_out[...] = wdt_ref[...]
        if ncore == 2:
            for copy in weight_copies():
                copy.wait()
            for copy in weight_stores():
                copy.start()
            prm_ref[:, own : 2 * own] = sm_in[0:8, :]
            hp_ref[...] += pltpu.roll(sm_in[8:16, 0:L], heads, axis=1)
            theirs = pltpu.roll(wdt_in[...].astype(f32), heads, axis=1)
            wdt_out[...] = (wdt_ref[...].astype(f32) + theirs).astype(bf16)

    if ncore == 2:
        project(wz_in, wx_in, wo_in, own)
    dtl_ref[...] = nn(hid_ref[...], wdt_out[...])

    @pl.loop(0, rows_all // L)
    def _(c):
        t0 = pl.multiple_of(c * L, L)
        for half in range(2):
            lanes = slice(half * L, half * L + L)
            v = conv(bcl_ref, t0, wbc_scr.at[half], lanes, bcp_ref[0:4, lanes], bcp_ref[4:5, lanes])
            bca_scr[pl.ds(t0, L), lanes] = (v * sigmoid(v)).astype(bf16)

    s_scr[...] = jnp.zeros_like(s_scr)
    hp = hp_ref[...]

    def block_done():
        wait(row_copies())
        x_copy().wait()
        total = st_ref[here - 1]
        for d in range(ny - 1):
            total = total + st_in[here - 1, d]
        stot_ref[here - 1] = total
        parts = [po_in.at[here - 1, d] for d in range(ny - 1)]
        mine = po_scr.at[lax.rem(here - 1, 2), pl.ds(pl.multiple_of(yy * Ry, Ry), Ry)]
        block_out(inner_total, stot_ref.at[here - 1], yy, mine, parts, x_own, bo_ref.at[here - 1])

    @pl.loop(0, rows_all // L)
    def _(c):
        early = jnp.logical_and(here > 0, here < nloc - 1)

        @pl.when(jnp.logical_and(early, c == rows_all // L - 1))
        def _():
            block_done()

        t0 = pl.multiple_of(c * L, L)
        rows = pl.ds(t0, L)
        lo = lane_iota((L, L)) < HEAD
        mlo = (lane_iota((1, L)) < HEAD).astype(bf16)
        mhi = (lane_iota((1, L)) >= HEAD).astype(bf16)
        tri = row_iota((L, L)) >= lane_iota((L, L))
        _, dt, cum, cum_t = span_decay(dtl_ref[rows, :], hp)
        bm = bca_scr[rows, 0:L]
        cm = bca_scr[rows, L : 2 * L]
        both = nt(cm, bm)
        sb = s_scr[...].astype(bf16)
        sin_ref[c] = sb
        cs_scr[...] = nn(cm, sb)
        squares = jnp.zeros((L, L), f32)
        inner = jnp.zeros((L, L), f32)
        for p in range(pairs):
            lanes = slice(p * L, p * L + L)
            xc = conv(xl_ref, t0, wx_scr.at[p], lanes, prm_ref[0:4, lanes], prm_ref[4:5, lanes])
            x = xc * sigmoid(xc)
            h0, h1 = 2 * p, 2 * p + 1
            a0, a1 = spread(cum, h0), spread(cum, h1)
            ap = jnp.where(lo, a0, a1)
            k0 = both * jnp.exp2(jnp.where(tri, a0 - cum_t[h0 : h0 + 1], -jnp.inf))
            k1 = both * jnp.exp2(jnp.where(tri, a1 - cum_t[h1 : h1 + 1], -jnp.inf))
            xdt = x * jnp.where(lo, spread(dt, h0), spread(dt, h1))
            xb = xdt.astype(bf16)
            fin = ap[L - 1 : L]
            within = nn(
                jnp.concatenate([k0.astype(bf16), k1.astype(bf16)], axis=1),
                jnp.concatenate([xb * mlo, xb * mhi], axis=0),
            )
            y = within + jnp.exp2(ap) * cs_scr[:, lanes] + prm_ref[5:6, lanes] * x
            xs_scr[:, lanes] = (xdt * jnp.exp2(fin - ap)).astype(bf16)
            s_scr[:, lanes] = s_scr[:, lanes] * jnp.exp2(fin)
            y_ref[rows, lanes] = y.astype(bf16)
            z = z_scr[rows, lanes]
            u = u_scr[rows, lanes]
            z_ref[rows, lanes] = z.astype(bf16)
            u_ref[rows, lanes] = u.astype(bf16)
            gated = y * (z * sigmoid(z))
            q = gated * prm_ref[6:7, lanes]
            q_scr[rows, lanes] = q.astype(bf16)
            squares = squares + gated * gated
            inner = inner + u * q
        s_scr[...] += nn(bm.T, xs_scr[...])
        s0 = jnp.sum(squares, axis=1, keepdims=True)
        s1 = jnp.sum(inner, axis=1, keepdims=True)
        lane = lane_iota((L, L))
        stat = jnp.where(lane == 0, s0, jnp.where(lane == 1, s1, 0.0))
        st_ref[here, :, rows] = stat.T[0:2]

    @pl.loop(0, model // 256)
    def _(j):
        cols = pl.ds(pl.multiple_of(j * 256, 256), 256)
        po = nn(q_scr[:, 0:own], wo_ref[:, cols])
        if ncore == 2:
            po = po + nn(q_scr[:, own : 2 * own], wo_in[:, cols])
        po_scr[lax.rem(here, 2), :, cols] = po.astype(bf16)

    @pl.when(here == nloc - 1)
    def _():
        po_ref[...] = po_scr[(nloc - 1) % 2]
        block_done()
        if ncore == 2:
            for copy in weight_stores():
                copy.wait()


def block_out(inner_total, stot, yy, mine, parts, x_own, bo):
    Ry, model = x_own.shape
    for h in range(Ry // L):
        lanes = pl.ds(pl.multiple_of(yy * Ry + h * L, L), L)
        r_row = lax.rsqrt(stot[0:1, lanes] / inner_total + epsilon)
        r = jnp.broadcast_to(r_row, (8, L)).T[:, 0:1]

        @pl.loop(0, model // L)
        def _(m, h=h, r=r):
            cols = pl.ds(pl.multiple_of(m * L, L), L)
            rows = slice(h * L, h * L + L)
            total = mine[rows, cols].astype(f32)
            for part in parts:
                total = total + part[rows, cols].astype(f32)
            bo[rows, cols] = (x_own[rows, cols].astype(f32) + r * total).astype(bf16)


def gate_kernel(
    width,
    own,
    inner_total,
    ncore,
    ny,
    _seq,
    st_ref,
    stin_ref,
    g_ref,
    hid_ref,
    z_ref,
    y_ref,
    u_ref,
    prm_ref,
    po_ref,
    bo01_ref,
    x_ref,
    dz_ref,
    dy_ref,
    gz_ref,
    go_ref,
    ggg_ref,
    bo_ref,
    q_scr,
    sc_scr,
    dz_scr,
    stot_ref,
    st_in,
    send_scr,
    recv_scr,
    po_in,
    x_own,
    hid_scr,
    st_sems,
    core_send,
    core_recv,
    po_sems,
    local,
):
    rows_all = z_ref.shape[0]
    model = g_ref.shape[1]
    pairs = width // L
    here = pl.program_id(0)
    core, yy, twin, ys, peers = places(ncore, ny)
    nloc, Ry, _ = bo_ref.shape
    last = nloc - 1

    def row_copies():
        return [
            remote(st_ref.at[last], st_in.at[d], st_sems.at[0, d], st_sems.at[1, d], peers[d])
            for d in range(ny - 1)
        ]

    def po_copies():
        return [
            remote(
                po_ref.at[pl.ds(pl.multiple_of(ys[d] * Ry, Ry), Ry)],
                po_in.at[d],
                po_sems.at[0, d],
                po_sems.at[1, d],
                peers[d],
            )
            for d in range(ny - 1)
        ]

    def x_copy():
        return pltpu.make_async_copy(x_ref.at[core * nloc + last, yy], x_own, local.at[0])

    def hid_copy():
        return pltpu.make_async_copy(hid_ref, hid_scr, local.at[1])

    @pl.when(here == 0)
    def _():
        greet(peers + ([twin] if ncore == 2 else []))
        start(row_copies() + po_copies() + [x_copy(), hid_copy()])
        stot_ref[...] = stin_ref[...]
        for i in range(last):
            bo_ref[i] = bo01_ref[i]
        ggg_ref[...] = jnp.zeros_like(ggg_ref)

    @pl.when(here == last)
    def _():
        for copy in row_copies():
            copy.wait()
        total = st_ref[last]
        for d in range(ny - 1):
            total = total + st_in[d]
        stot_ref[last] = total

    @pl.loop(0, rows_all // L)
    def _(c):
        rows = pl.ds(pl.multiple_of(c * L, L), L)
        st = stot_ref[here, :, rows]
        r_row = lax.rsqrt(st[0:1] / inner_total + epsilon)
        c_row = r_row * r_row * r_row * (st[1:2] / inner_total)
        cols8 = jnp.concatenate([r_row, c_row, jnp.zeros((6, L), f32)], axis=0).T
        r = jnp.broadcast_to(cols8[:, 0:1], (L, L))
        c2 = jnp.broadcast_to(cols8[:, 1:2], (L, L))
        for m in range(model // L):
            lanes = slice(m * L, m * L + L)
            sc_scr[here, rows, lanes] = (g_ref[rows, lanes].astype(f32) * r).astype(bf16)
        for p in range(pairs):
            lanes = slice(p * L, p * L + L)
            gg = prm_ref[6:7, lanes]
            z = z_ref[rows, lanes].astype(f32)
            y = y_ref[rows, lanes].astype(f32)
            sg = sigmoid(z)
            silz = z * sg
            gated = y * silz
            q_scr[here, rows, lanes] = (gated * gg).astype(bf16)
            dq = r * u_ref[rows, lanes].astype(f32)
            ggg_ref[:, lanes] += fold_rows(dq * gated)
            dgated = dq * gg - c2 * gated
            dy_ref[rows, lanes] = (dgated * silz).astype(bf16)
            dz = (dgated * y * (sg + silz * (1.0 - sg))).astype(bf16)
            dz_ref[rows, lanes] = dz
            dz_scr[here, rows, lanes] = dz

    @pl.when(here == last)
    def _():
        hid_copy().wait()
        hid = hid_scr.reshape(nloc * rows_all, model)
        dz = dz_scr.reshape(nloc * rows_all, width)
        q = q_scr.reshape(nloc * rows_all, width)
        sc = sc_scr.reshape(nloc * rows_all, model)

        def sums(half, out_z, out_o):
            lanes = slice(half * own, half * own + own)

            @pl.loop(0, model // 256)
            def _(j):
                cols = pl.ds(pl.multiple_of(j * 256, 256), 256)
                gz = tn(hid[:, cols], dz[:, lanes])
                go = tn(sc[:, cols], q[:, lanes])
                out_z[cols, :] = gz.astype(bf16)
                out_o[cols, :] = go.astype(bf16)

        if ncore == 2:
            sums(1, send_scr.at[:, 0:own], send_scr.at[:, own : 2 * own])
        if ncore == 2:
            copy = remote(send_scr, recv_scr, core_send, core_recv, twin)
            copy.start()
        sums(0, gz_ref, go_ref)
        if ncore == 2:
            copy.wait()

            @pl.loop(0, model // 64)
            def _(j):
                rows = pl.ds(pl.multiple_of(j * 64, 64), 64)
                for ref, first in ((gz_ref, 0), (go_ref, own)):
                    theirs = recv_scr[rows, first : first + own].astype(f32)
                    ref[rows, :] = (ref[rows, :].astype(f32) + theirs).astype(bf16)

        for copy in po_copies() + [x_copy()]:
            copy.wait()
        parts = [po_in.at[d] for d in range(ny - 1)]
        mine = po_ref.at[pl.ds(pl.multiple_of(yy * Ry, Ry), Ry)]
        block_out(inner_total, stot_ref.at[last], yy, mine, parts, x_own, bo_ref.at[last])


def tail_part(own, ncore, ny, ndp, nloc, given, outs, late_to, ready_to, room, machine):
    gw_ref, gbcw_ref, small_ref, other_ref, shared_ref, dh_ref, gain_ref, x_ref, bo_ref = given
    fw_ref, fb_ref, fb_scr, small_full, small_src, small_out, shared_out, last_ref = outs
    dh_in, x_own, small_in, core_sems, y_sems, local = room
    model = gw_ref.shape[0]
    Ry = x_own.shape[0]
    core, yy, twin, ys, peers = places(ncore, ny)
    nbits = log2(ndp)
    dp_peers, dp_bits = bit_peers("dp", 1, 0, nbits)
    t_peers, t_bits = bit_peers("tensor", 1, 0, log2(ncore * ny))
    links = list(zip(dp_peers, dp_bits))
    swapped = [links[1], links[0]] + links[2:] if nbits > 1 else links
    t_links = list(zip(t_peers, t_bits))
    per = nbits + 2
    a, b = machine[:per], machine[per : 2 * per]
    per_bc = nbits + len(t_links) + 2
    c = machine[2 * per : 2 * per + per_bc]
    d, sh = machine[2 * per + per_bc : 3 * per + per_bc], machine[3 * per + per_bc :]
    mid = model // 2
    job_a = Halving(links, mid, gw_ref.at[0:mid], a[0], a[1:-1], fw_ref.at[0:mid], a[-1])
    job_b = Halving(swapped, mid, gw_ref.at[mid:model], b[0], b[1:-1], fw_ref.at[mid:model], b[-1])
    job_c = Halving(t_links + links, model, gbcw_ref, c[0], c[1:-1], fb_scr, c[-1])
    job_sm = Halving(links, small_src.shape[0], small_src, d[0], d[1:-1], small_full, d[-1])
    job_sh = Doubling(t_peers + dp_peers, *sh)

    def dh_copies():
        return [
            remote(
                dh_ref.at[pl.ds(pl.multiple_of(ys[d] * Ry, Ry), Ry)],
                dh_in.at[d],
                y_sems.at[0, d],
                y_sems.at[1, d],
                peers[d],
            )
            for d in range(ny - 1)
        ]

    place = (twin, peers, ncore)
    late = Spread(last_ref, *late_to, place)
    ready = [Spread(bo_ref.at[nloc - 1], *ready_to, place)]
    x_copy = pltpu.make_async_copy(x_ref.at[core * nloc + nloc - 1, yy], x_own, local.at[1])

    def turn(*pairs):
        for job, j in pairs:
            job.close(j)
        for job, j in pairs:
            job.begin(j)

    job_sh.acc[0] = shared_ref[...]
    turn((job_c, 0), (job_sh, 0))
    yield
    turn((job_c, 1), (job_sh, 1))
    start(dh_copies())
    x_copy.start()
    for spread in ready:
        start(spread.first())
    if ncore == 2:
        small_copy = remote(other_ref, small_in, core_sems.at[0], core_sems.at[1], twin)
        small_copy.start()
    yield
    turn((job_a, 0), (job_b, 0))
    if ncore == 2:
        small_copy.wait()
        small_src[...] = small_ref[...] + small_in[...]
    else:
        small_src[...] = small_ref[...]
    turn((job_sm, 0))
    steps = [
        (job_c, iter(range(2, 2 * job_c.n + 1))),
        (job_sm, iter(range(1, 2 * nbits + 1))),
        (job_sh, iter(range(2, len(job_sh.peers) + 1))),
    ]

    def smaller():
        found = []
        for job, left in steps:
            j = next(left, None)
            if j is not None:
                found.append((job, j))
        return found

    for j in range(1, 2 * nbits + 1):
        turn(*smaller(), (job_a, j), (job_b, j))
        if j == 2:
            wait(dh_copies())
            x_copy.wait()

            @pl.loop(0, Ry // 32)
            def _(i):
                rows = pl.ds(pl.multiple_of(i * 32, 32), 32)
                mine = pl.ds(pl.multiple_of(yy * Ry + i * 32, 32), 32)
                dh = dh_ref[mine, :].astype(f32)
                for d in range(ny - 1):
                    dh = dh + dh_in[d, rows, :].astype(f32)
                last_ref[rows, :] = correction(x_own[rows, :], dh, gain_ref[...]).astype(bf16)

            start(late.first())
    for spread in ready:
        wait(spread.first())
        start(spread.second())
    for _ in range(2 * job_c.n):
        turn(*smaller())
    fb_copy = pltpu.make_async_copy(fb_scr, fb_ref, local.at[1])
    fb_copy.start()
    small_out[...] = small_full[...]
    shared_out[...] = job_sh.acc[len(job_sh.peers)]
    wait(late.first())
    start(late.second())
    for spread in ready + [late]:
        wait(spread.second())
    fb_copy.wait()
    yield


def scan_kernel(
    width,
    own,
    heads,
    ncore,
    ny,
    ndp,
    nloc_static,
    _seq,
    hid_ref,
    dz_ref,
    dy_ref,
    xl_ref,
    bcl_ref,
    dtl_ref,
    sin_ref,
    wz_hbm,
    wzo_hbm,
    wx_hbm,
    wxo_hbm,
    wbc_ref,
    wdt_ref,
    prm_ref,
    bcp_ref,
    hp_ref,
    ggg_ref,
    gain_ref,
    gz_ref,
    go_ref,
    bo_ref,
    x_ref,
    corr_ref,
    small_out,
    shared_out,
    last_ref,
    fz_ref,
    fo_ref,
    boy_ref,
    bot_ref,
    boty_ref,
    cy_ref,
    ct_ref,
    cty_ref,
    fw_ref,
    fb_ref,
    ly_ref,
    lt_ref,
    lty_ref,
    zy_ref,
    zt_ref,
    zty_ref,
    wz_ref,
    wzo_ref,
    wx_ref,
    wxo_ref,
    w_sems,
    d_scr,
    bcc_scr,
    bca_scr,
    ds_scr,
    dsb_scr,
    cs_scr,
    bds_scr,
    xs_scr,
    dye_scr,
    nx_scr,
    nbc_scr,
    wx_scr,
    wbc_scr,
    red_scr,
    end_scr,
    pick_scr,
    gx_ref,
    gbc_ref,
    gdt_ref,
    gpre_ref,
    acc_scr,
    send_scr,
    recv_scr,
    dh_scr,
    dh_in,
    x_own,
    core_send,
    core_recv,
    y_sems,
    bo_sems,
    c_sems,
    local,
    gw_ref,
    gbcw_ref,
    small_ref,
    other_ref,
    shared_ref,
    small_in,
    fb_scr,
    small_full,
    small_src,
    end_in,
    x_end,
    core_sems,
    end_sems,
    l_sems,
    z_sems,
    *machine,
):
    rows_all = dz_ref.shape[0]
    model = hid_ref.shape[1]
    pairs = width // L
    spans = rows_all // L
    Ry = rows_all // ny
    seq, back = pl.program_id(0), pl.program_id(1)
    step = seq * spans + back
    core, yy, twin, ys, peers = places(ncore, ny)
    nbits = log2(ndp)
    dp_peers, dp_bits = bit_peers("dp", 1, 0, nbits)
    links = list(zip(dp_peers, dp_bits))
    swapped = [links[1], links[0]] + links[2:] if nbits > 1 else links
    per = nbits + 2
    mz, mo, rest = machine[:per], machine[per : 2 * per], machine[2 * per :]
    jobs = [
        Halving(links, model, gz_ref, mz[0], mz[1:-1], fz_ref, mz[-1]),
        Halving(swapped, model, go_ref, mo[0], mo[1:-1], fo_ref, mo[-1]),
    ]
    last_step = nloc_static * spans - 1

    place = (twin, peers, ncore)
    some = pl.ds(0, nloc_static - 1)
    bo_spread = Spread(bo_ref.at[some], boy_ref, bot_ref, boty_ref, bo_sems, place)

    def corr_spread(i):
        return Spread(
            corr_ref.at[i], cy_ref.at[:, i], ct_ref.at[i], cty_ref.at[:, i], c_sems.at[:, i], place
        )

    def dh_copies():
        return [
            remote(
                dh_scr.at[pl.ds(pl.multiple_of(ys[d] * Ry, Ry), Ry)],
                dh_in.at[seq - 1, d],
                y_sems.at[0, seq - 1, d],
                y_sems.at[1, seq - 1, d],
                peers[d],
            )
            for d in range(ny - 1)
        ]

    def x_copy():
        return pltpu.make_async_copy(x_ref.at[core * nloc_static + seq - 1, yy], x_own, local.at[0])

    def weight_copies():
        both = ((wz_hbm, wz_ref), (wzo_hbm, wzo_ref), (wx_hbm, wx_ref), (wxo_hbm, wxo_ref))
        return [pltpu.make_async_copy(src, dst, w_sems.at[n]) for n, (src, dst) in enumerate(both)]

    @pl.when(step == 0)
    def _():
        start(weight_copies())
        greet(peers + dp_peers + ([twin] if ncore == 2 else []))
        start(bo_spread.first())
        acc_scr[...] = jnp.zeros_like(acc_scr)
        end_scr[...] = jnp.zeros_like(end_scr)
        pick = row_iota((width, L)) // HEAD == lane_iota((width, L))
        pick_scr[...] = pick.astype(f32).astype(bf16)
        gx_ref[...] = jnp.zeros_like(gx_ref)
        gbc_ref[...] = jnp.zeros_like(gbc_ref)
        gdt_ref[...] = jnp.zeros_like(gdt_ref)
        gpre_ref[...] = jnp.zeros_like(gpre_ref)

    when = [0.0, 0.25, 0.33, 0.58, 0.67, 0.83]
    if nbits != 3:
        when = [j / (2 * nbits) for j in range(2 * nbits)]
    for j in range(2 * nbits):

        @pl.when(step == int(when[j] * (last_step + 1) + 0.1))
        def _(j=j):
            for job in jobs:
                job.close(j)
            for job in jobs:
                job.begin(j)

    @pl.when(step == spans + 2)
    def _():
        wait(bo_spread.first())
        start(bo_spread.second())

    for i in range(nloc_static - 2):

        @pl.when(step == (i + 2) * spans + 2)
        def _(i=i):
            wait(corr_spread(i).first())
            start(corr_spread(i).second())

    @pl.when(jnp.logical_and(seq > 0, back == 0))
    def _():
        for copy in dh_copies():
            copy.start()
        x_copy().start()

    @pl.when(jnp.logical_and(seq > 0, back == spans - 1))
    def _():
        for copy in dh_copies():
            copy.wait()
        x_copy().wait()

        @pl.loop(0, Ry // 32)
        def _(i):
            rows = pl.ds(pl.multiple_of(i * 32, 32), 32)
            mine = pl.ds(pl.multiple_of(yy * Ry + i * 32, 32), 32)
            dh = dh_scr[mine, :].astype(f32)
            for d in range(ny - 1):
                dh = dh + dh_in[seq - 1, d, rows, :].astype(f32)
            corr_ref[seq - 1, rows, :] = correction(x_own[rows, :], dh, gain_ref[...]).astype(bf16)

        start(corr_spread(seq - 1).first())

    hp = hp_ref[...]

    @pl.when(back == 0)
    def _():
        ds_scr[...] = jnp.zeros_like(ds_scr)
        nx_scr[...] = jnp.zeros_like(nx_scr)
        nbc_scr[...] = jnp.zeros_like(nbc_scr)

        @pl.loop(0, spans)
        def _(c):
            t0 = pl.multiple_of(c * L, L)
            for half in range(2):
                lanes = slice(half * L, half * L + L)
                v = conv(bcl_ref, t0, wbc_scr.at[half], lanes, bcp_ref[0:4, lanes], bcp_ref[4:5, lanes])
                bcc_scr[pl.ds(t0, L), lanes] = v
                bca_scr[pl.ds(t0, L), lanes] = (v * sigmoid(v)).astype(bf16)

    def one_chunk():
        c = spans - 1 - back
        t0 = pl.multiple_of(c * L, L)
        rows = pl.ds(t0, L)
        lane = lane_iota((L, L))
        lo = lane < HEAD
        mlo = (lane_iota((1, L)) < HEAD).astype(bf16)
        mhi = (lane_iota((1, L)) >= HEAD).astype(bf16)
        tri = row_iota((L, L)) >= lane
        pre, dt, cum, cum_t = span_decay(dtl_ref[rows, :], hp)
        bm = bca_scr[rows, 0:L]
        cm = bca_scr[rows, L : 2 * L]
        both = nt(cm, bm)
        sb = sin_ref[c]
        dsb_scr[...] = ds_scr[...].astype(bf16)
        cs_scr[...] = nn(cm, sb)
        bds_scr[...] = nn(bm, dsb_scr[...])
        d_both = jnp.zeros((L, L), f32)
        for p in range(pairs):
            lanes = slice(p * L, p * L + L)
            taps = prm_ref[0:4, lanes]
            xc = conv(xl_ref, t0, wx_scr.at[p], lanes, taps, prm_ref[4:5, lanes])
            sg = sigmoid(xc)
            x = xc * sg
            h0, h1 = 2 * p, 2 * p + 1
            a0, a1 = spread(cum, h0), spread(cum, h1)
            ap = jnp.where(lo, a0, a1)
            e0 = jnp.exp2(jnp.where(tri, a0 - cum_t[h0 : h0 + 1], -jnp.inf))
            e1 = jnp.exp2(jnp.where(tri, a1 - cum_t[h1 : h1 + 1], -jnp.inf))
            k0 = (both * e0).astype(bf16)
            k1 = (both * e1).astype(bf16)
            dtp = jnp.where(lo, spread(dt, h0), spread(dt, h1))
            xdt = x * dtp
            xb = xdt.astype(bf16)
            bdx = jnp.concatenate([xb * mlo, xb * mhi], axis=0)
            ecum = jnp.exp2(ap)
            fin = ap[L - 1 : L]
            sd = jnp.exp2(fin - ap)
            y = nn(jnp.concatenate([k0, k1], axis=1), bdx) + ecum * cs_scr[:, lanes]
            dyb = dy_ref[rows, lanes]
            dy = dyb.astype(f32)
            dk = nt(dyb, bdx)
            d_both = d_both + dk[:, 0:L] * e0 + dk[:, L : 2 * L] * e1
            bdy = jnp.concatenate([dyb * mlo, dyb * mhi], axis=0)
            near = tn(jnp.concatenate([k0, k1], axis=0), bdy)
            far = sd * bds_scr[:, lanes]
            dxdt = near + far
            v = dy * y - xb.astype(f32) * near
            u = dxdt * x
            w = xdt * far
            ends = jnp.exp2(fin)
            through = ends * jnp.sum(sb[:, lanes].astype(f32) * ds_scr[:, lanes], axis=0, keepdims=True)
            v_hi = v.astype(bf16)
            red_scr[0:L, lanes] = v_hi
            red_scr[L : 2 * L, lanes] = (v - v_hi.astype(f32)).astype(bf16)
            red_scr[2 * L : 3 * L, lanes] = u.astype(bf16)
            red_scr[3 * L : 4 * L, lanes] = w.astype(bf16)
            end_scr[0:1, lanes] = through
            dx = dxdt * dtp + dy * prm_ref[5:6, lanes]
            dxc = dx * (sg + x * (1.0 - sg))
            for k in range(4):
                gx_ref[k, :, lanes] += fold_rows(dxc * tap(wx_scr.at[p], k))
            gx_ref[4, :, lanes] += fold_rows(dxc)
            gx_ref[5, :, lanes] += fold_rows(dy * x)
            nx_scr[p, L : L + 8] = nx_scr[p, 0:8]
            nx_scr[p, 0:L] = dxc
            dxl = dxc * taps[3:4]
            for k in range(3):
                dxl = dxl + nx_scr[p, 3 - k : 3 - k + L] * taps[k : k + 1]
            d_scr[rows, lanes] = dxl.astype(bf16)
            xs_scr[:, lanes] = (xdt * sd).astype(bf16)
            dye_scr[:, lanes] = (dy * ecum).astype(bf16)
            ds_scr[:, lanes] = ds_scr[:, lanes] * ends
        ds_scr[...] += nn(cm.T, dye_scr[...])
        sums = nn(red_scr[...], pick_scr[...])
        d_cum = sums[0:L] + sums[L : 2 * L]
        d_dt = sums[2 * L : 3 * L]
        d_far = sums[3 * L : 4 * L]
        d_end = exact(end_scr[...], pick_scr[...].astype(f32))[0:1]
        utri = (row_iota((L, L)) <= lane).astype(f32)
        before = (row_iota((L, L)) > lane).astype(f32)
        d_a = exact(utri, d_cum) + exact(before, d_far) + d_end
        d_dt = d_dt + d_a * hp[1:2]
        d_pre = d_dt * sigmoid(pre)
        gdt_ref[0] += fold_rows(d_pre)
        gdt_ref[1] += fold_rows(d_a * dt * hp[1:2])
        d_scr[rows, width + 256 : width + 384] = d_pre.astype(bf16)
        dgb = d_both.astype(bf16)
        d_c = nt(dye_scr[...], sb) + nn(dgb, bm)
        d_b = nt(xs_scr[...], dsb_scr[...]) + nn(dgb.T, cm)
        for half, dv in ((0, d_b), (1, d_c)):
            lanes = slice(half * L, half * L + L)
            pre_act = bcc_scr[rows, lanes]
            sg = sigmoid(pre_act)
            dvc = dv * (sg + pre_act * sg * (1.0 - sg))
            wbc_scr[half] = bcl_ref[pl.ds(t0, L + PAD), lanes]
            for k in range(4):
                gbc_ref[k, :, lanes] += fold_rows(dvc * tap(wbc_scr.at[half], k))
            gbc_ref[4, :, lanes] += fold_rows(dvc)
            nbc_scr[half, L : L + 8] = nbc_scr[half, 0:8]
            nbc_scr[half, 0:L] = dvc
            dvl = dvc * bcp_ref[3:4, lanes]
            for k in range(3):
                dvl = dvl + nbc_scr[half, 3 - k : 3 - k + L] * bcp_ref[k : k + 1, lanes]
            d_scr[rows, width + half * L : width + half * L + L] = dvl.astype(bf16)

    one_chunk()

    @pl.when(step == spans - 1)
    def _():
        wait(weight_copies())

    @pl.when(back == spans - 1)
    def _():
        @pl.loop(0, model // 256)
        def _(j):
            cols = pl.ds(pl.multiple_of(j * 256, 256), 256)
            dh = nt(dz_ref[:, 0:own], wz_ref[cols, :]) + nt(d_scr[:, 0:own], wx_ref[cols, :])
            if ncore == 2:
                dh = dh + nt(dz_ref[:, own:width], wzo_ref[cols, :])
                dh = dh + nt(d_scr[:, own:width], wxo_ref[cols, :])
            dh = dh + nt(d_scr[:, width : width + 256], wbc_ref[cols, :])
            dh = dh + nt(d_scr[:, width + 256 :], wdt_ref[cols, :])
            dh_scr[:, cols] = dh.astype(bf16)
            gpre_ref[:, cols] += fold_rows(dh * hid_ref[:, cols].astype(f32))
            acc_scr[cols, :] += tn(hid_ref[:, cols], d_scr[...])

    @pl.when(step == last_step)
    def _():
        end = tail_part(
            own,
            ncore,
            ny,
            ndp,
            nloc_static,
            (gw_ref, gbcw_ref, small_ref, other_ref, shared_ref, dh_scr, gain_ref, x_ref, bo_ref),
            (fw_ref, fb_ref, fb_scr, small_full, small_src, small_out, shared_out, last_ref),
            (ly_ref, lt_ref, lty_ref, l_sems),
            (zy_ref, zt_ref, zty_ref, z_sems),
            (end_in, x_end, small_in, core_sems, end_sems, local),
            rest,
        )
        gbcw_ref[...] = acc_scr[:, width : width + 256].astype(gbcw_ref.dtype)
        shared_ref[...] = jnp.zeros_like(shared_ref)
        gpre = jnp.sum(gpre_ref[...], axis=0, keepdims=True) / gain_ref[...]
        for k in range(model // L):
            shared_ref[k : k + 1, 0:L] = gpre[:, k * L : k * L + L]
        for k in range(5):
            shared_ref[k : k + 1, L : L + 256] = jnp.sum(gbc_ref[k], axis=0, keepdims=True)
        next(end)
        if ncore == 2:
            send_scr[...] = acc_scr[:, own:width].astype(bf16)
            copy = remote(send_scr, recv_scr, core_send, core_recv, twin)
        rows = [jnp.sum(gx_ref[k], axis=0, keepdims=True) for k in range(6)]
        rows.append(jnp.sum(ggg_ref[...], axis=0, keepdims=True))
        dts = [jnp.sum(gdt_ref[k], axis=0, keepdims=True) for k in range(2)]
        small_ref[...] = jnp.zeros_like(small_ref)
        other_ref[...] = jnp.zeros_like(other_ref)
        lines = 16 + heads * model // own

        def put(ref, k, row):
            for q in range(own // L):
                ref[q * lines + k : q * lines + k + 1, :] = row[:, q * L : q * L + L]

        for k in range(7):
            put(small_ref, k, rows[k][:, 0:own])
            if ncore == 2:
                put(other_ref, k, rows[k][:, own:width])
        for d in range(model // L):
            turned = acc_scr[d * L : d * L + L, width + 256 : width + 384].T
            line = (d * L % own) // L * lines + 16 + heads * (d * L // own)
            small_ref[line : line + heads, :] = turned[0:heads]
            if ncore == 2:
                other_ref[line : line + heads, :] = turned[heads : 2 * heads]
        for k in range(2):
            small_ref[7 + k : 8 + k, :] = dts[k]
            if ncore == 2:
                moved = pltpu.roll(jnp.broadcast_to(dts[k], (8, L)), L - heads, axis=1)
                other_ref[7 + k : 8 + k, :] = moved[0:1]
        if ncore == 2:
            copy.start()
        next(end)
        for job in jobs:
            job.close(2 * nbits)
        if ncore == 2:
            copy.wait()

        @pl.loop(0, model // 64)
        def _(i):
            rows = pl.ds(pl.multiple_of(i * 64, 64), 64)
            total = acc_scr[rows, 0:own]
            if ncore == 2:
                total = total + recv_scr[rows, :].astype(f32)
            gw_ref[rows, :] = total.astype(bf16)

        for _ in end:
            pass
        final = corr_spread(nloc_static - 2)
        wait(final.first())
        start(final.second())
        wait(bo_spread.second())
        for i in range(nloc_static - 1):
            wait(corr_spread(i).second())


def finish_kernel(pieces, nloc, _idx, g_ref, *refs):
    gi_ref, bo_ref = refs[-2:]
    groups = [refs[n * pieces : (n + 1) * pieces] for n in range(4)]
    now = pl.program_id(1)
    for k in range(pieces):
        here = pl.program_id(0) == k

        def when(turn, here=here):
            return pl.when(jnp.logical_and(here, turn))

        for n, turn in ((0, now < nloc - 1), (1, now == nloc - 1)):

            @when(turn)
            def _(src=groups[n][k]):
                gi_ref[...] = g_ref[...].astype(f32) + src[...].astype(f32)

        for n, turn in ((2, now < nloc - 1), (3, now == nloc - 1)):

            @when(turn)
            def _(src=groups[n][k]):
                bo_ref[...] = src[...]


def unpack_kernel(own, heads, gz_total, gz_ref, go_ref, gw_ref, fb_ref, small_ref, shared_ref, *outs):
    gzx_ref, gwo_ref, gwdt_ref, gwbc_ref = outs[:4]
    lines = 16 + heads * gz_total // own
    gcxw_ref, gcxb_ref, gd_ref, ggg_ref, gdtb_ref, galog_ref, gpre_ref, gcbw_ref, gcbb_ref = outs[4:]
    gzx_ref[:, 0, :] = gz_ref[...].astype(f32)
    gzx_ref[:, 1, :] = gw_ref[:, 0:own].astype(f32)
    for d in range(gpre_ref.shape[1] // L):

        @pl.when(pl.program_id(0) == d)
        def _(d=d):
            line = (d * L % own) // L * lines + 16 + heads * (d * L // own)
            rows = small_ref[line : line + heads, :]
            if heads < 8:
                rows = jnp.concatenate([rows, jnp.zeros((8 - heads, L), f32)], axis=0)
            gwdt_ref[...] = rows.T[:, 0:heads]

    gwbc_ref[...] = fb_ref[...].astype(f32)
    v = go_ref[...].astype(f32)
    for k in range(own // L):
        gwo_ref[k * L : k * L + L, :] = v[:, k * L : k * L + L].T

    @pl.when(pl.program_id(0) == 0)
    def _():
        pick = (row_iota((L, L)) // HEAD == lane_iota((L, L))).astype(f32)
        for q in range(own // L):
            part, cols = small_ref[q * lines : q * lines + 8, :], slice(q * L, q * L + L)
            gcxw_ref[:, cols] = part[0:4]
            gcxb_ref[:, cols] = part[4:5]
            ggg_ref[:, cols] = part[6:7]
            each = L // HEAD
            gd_ref[:, q * each : q * each + each] = exact(part, pick)[5:6, 0:each]
        gdtb_ref[...] = small_ref[7:8, 0:heads]
        galog_ref[...] = small_ref[8:9, 0:heads]
        for k in range(gpre_ref.shape[1] // L):
            gpre_ref[:, k * L : k * L + L] = shared_ref[k : k + 1, 0:L]
        gcbw_ref[...] = shared_ref[0:4, L : L + 256]
        gcbb_ref[...] = shared_ref[4:5, L : L + 256]


def seq_spec(*shape):
    zeros = (0,) * len(shape)
    return pl.BlockSpec((None,) + shape, lambda i, s: (i,) + zeros)


def moved_spec(ncore, nloc, *shape):
    zeros = (0,) * len(shape)

    def index(i, s):
        return (i + lax.rem(lax.axis_index("tensor"), ncore) * nloc,) + zeros

    return pl.BlockSpec((None,) + shape, index)


def whole_spec(*shape):
    zeros = (0,) * len(shape)
    return pl.BlockSpec(shape, lambda *_: zeros, pipeline_mode=pl.Buffered(1))


def call(
    kernel, grid, in_specs, out_specs, out_shape, scratch, name, flops=0, moved=0, group=None
):
    return pl.pallas_call(
        kernel,
        grid_spec=pltpu.PrefetchScalarGridSpec(
            num_scalar_prefetch=1,
            grid=grid,
            in_specs=in_specs,
            out_specs=out_specs,
            scratch_shapes=scratch,
        ),
        out_shape=out_shape,
        cost_estimate=pl.CostEstimate(
            flops=int(flops), bytes_accessed=int(moved), transcendentals=0
        ),
        name=name,
        compiler_params=None
        if group is None
        else pltpu.CompilerParams(collective_id=group, has_side_effects=True),
    )


def sds(*shape, dtype=f32):
    return jax.ShapeDtypeStruct(shape, dtype)


def body(
    block_input,
    pre_gain,
    w_zx,
    w_bc,
    w_dt,
    conv_x_w,
    conv_x_b,
    conv_bc_w,
    conv_bc_b,
    dt_bias,
    a_log,
    d_skip,
    gate_gain,
    w_out,
    out_grad,
):
    tok, model = block_input.shape
    own = w_zx.shape[2]
    heads = w_dt.shape[1]
    nt = lax.axis_size("tensor")
    ndp = lax.axis_size("dp")
    inner_total = own * nt
    ncore = 2 if nt % 2 == 0 else 1
    ny = nt // ncore
    width = own * ncore
    t = lax.axis_index("tensor")
    core, yy = t % ncore, t // ncore
    R = SEQ_LEN
    Ry = R // ny
    nseq = tok // R
    nloc = nseq // ncore
    spans = R // L
    wtot = 2 * width + 384
    pairs = width // L

    x3 = block_input.reshape(nseq, R, model)
    g3 = out_grad.reshape(nseq, R, model)
    x4 = block_input.reshape(nseq, ny, Ry, model)
    g4 = out_grad.reshape(nseq, ny, Ry, model)
    wz, wx = w_zx[:, 0], w_zx[:, 1]
    sm = jnp.concatenate(
        [
            conv_x_w,
            conv_x_b[None],
            jnp.repeat(d_skip, HEAD)[None],
            gate_gain[None],
            jnp.zeros((1, own), f32),
            jnp.pad(jnp.stack([dt_bias, -jnp.exp(a_log)]), ((0, 6), (0, own - heads))),
        ],
        axis=0,
    )
    wdt = jnp.pad(w_dt, ((0, 0), (0, L - heads)))
    bcp = jnp.concatenate([conv_bc_w, conv_bc_b[None], jnp.zeros((3, 256), f32)], axis=0)
    gain = pre_gain[None]
    seq0 = jnp.zeros((1,), jnp.int32)
    any_spec = pl.BlockSpec(memory_space=pl.ANY)
    nother = max(ny - 1, 1)
    dma = pltpu.SemaphoreType.DMA

    hid, z, xl, bcl, dtl, u, y, sin, st, stot, po, bo01, prm, hp, wdt, wzo, wxo = call(
        partial(forward_kernel, own, heads, ncore, ny, inner_total, nloc),
        (nloc,),
        [
            moved_spec(ncore, nloc, R, model),
            moved_spec(ncore, nloc, R, model),
            whole_spec(1, model),
            whole_spec(model, own),
            whole_spec(model, own),
            whole_spec(model, 256),
            whole_spec(model, L),
            whole_spec(own, model),
            whole_spec(16, own),
            whole_spec(8, 256),
            any_spec,
        ],
        [
            seq_spec(R, model),
            seq_spec(R, width),
            seq_spec(R + PAD, width),
            seq_spec(R + PAD, 256),
            seq_spec(R, L),
            seq_spec(R, width),
            seq_spec(R, width),
            seq_spec(spans, L, width),
            whole_spec(nloc, 2, R),
            whole_spec(nloc, 2, R),
            whole_spec(R, model),
            whole_spec(nloc - 1, Ry, model),
            whole_spec(8, width),
            whole_spec(8, L),
            whole_spec(model, L),
        ]
        + [any_spec] * 2,
        [
            sds(nloc, R, model, dtype=bf16),
            sds(nloc, R, width, dtype=bf16),
            sds(nloc, R + PAD, width),
            sds(nloc, R + PAD, 256),
            sds(nloc, R, L),
            sds(nloc, R, width, dtype=bf16),
            sds(nloc, R, width, dtype=bf16),
            sds(nloc, spans, L, width, dtype=bf16),
            sds(nloc, 2, R),
            sds(nloc, 2, R),
            sds(R, model, dtype=bf16),
            sds(nloc - 1, Ry, model, dtype=bf16),
            sds(8, width),
            sds(8, L),
            sds(model, L, dtype=bf16),
            sds(model, own, dtype=bf16),
            sds(model, own, dtype=bf16),
        ],
        [
            pltpu.VMEM((R, width), f32),
            pltpu.VMEM((R, width), f32),
            pltpu.VMEM((R, width), bf16),
            pltpu.VMEM((R, 256), bf16),
            pltpu.VMEM((L, width), f32),
            pltpu.VMEM((L, width), f32),
            pltpu.VMEM((L, width), bf16),
            pltpu.VMEM((pairs, L + PAD, L), f32),
            pltpu.VMEM((2, L + PAD, L), f32),
            pltpu.VMEM((model, own), bf16),
            pltpu.VMEM((model, own), bf16),
            pltpu.VMEM((own, model), bf16),
            pltpu.VMEM((model, L), bf16),
            pltpu.VMEM((16, own), f32),
            pltpu.VMEM((2, R, model), bf16),
            pltpu.VMEM((nloc - 1, nother, Ry, model), bf16),
            pltpu.VMEM((nloc - 1, nother, 2, R), f32),
            pltpu.VMEM((Ry, model), bf16),
            dma((2, 5)),
            dma((2, nloc - 1, nother)),
            dma((2, nloc - 1, nother)),
            dma((3,)),
        ],
        "forward",
        2 * nloc * R * model * (wtot + 2 * width),
        nloc * R * (6 * model + 20 * width),
        4,
    )(seq0, x3, g3, gain, wz, wx, w_bc, wdt, w_out, sm, bcp, x4)

    nbits = log2(ndp)
    dz, dy, gz, go, ggg, bo = call(
        partial(gate_kernel, width, own, inner_total, ncore, ny),
        (nloc,),
        [
            whole_spec(nloc, 2, R),
            whole_spec(nloc, 2, R),
            moved_spec(ncore, nloc, R, model),
            any_spec,
            seq_spec(R, width),
            seq_spec(R, width),
            seq_spec(R, width),
            whole_spec(8, width),
            whole_spec(R, model),
            whole_spec(nloc - 1, Ry, model),
            any_spec,
        ],
        [
            seq_spec(R, width),
            seq_spec(R, width),
            whole_spec(model, own),
            whole_spec(model, own),
            whole_spec(8, width),
            whole_spec(nloc, Ry, model),
        ],
        [
            sds(nloc, R, width, dtype=bf16),
            sds(nloc, R, width, dtype=bf16),
            sds(model, own, dtype=bf16),
            sds(model, own, dtype=bf16),
            sds(8, width),
            sds(nloc, Ry, model, dtype=bf16),
        ],
        [
            pltpu.VMEM((nloc, R, width), bf16),
            pltpu.VMEM((nloc, R, model), bf16),
            pltpu.VMEM((nloc, R, width), bf16),
            pltpu.VMEM((nloc, 2, R), f32),
            pltpu.VMEM((nother, 2, R), f32),
            pltpu.VMEM((model, 2 * own), bf16),
            pltpu.VMEM((model, 2 * own), bf16),
            pltpu.VMEM((nother, Ry, model), bf16),
            pltpu.VMEM((Ry, model), bf16),
            pltpu.VMEM((nloc, R, model), bf16),
            dma((2, nother)),
            dma,
            dma,
            dma((2, nother)),
            dma((2,)),
        ],
        "gate",
        4 * nloc * R * model * width,
        nloc * R * (4 * model + 16 * width),
        1,
    )(seq0, st, stot, g3, hid, z, y, u, prm, po, bo01, x4)

    def chunk_spec(*shape):
        zeros = (0,) * len(shape)
        return pl.BlockSpec((None,) + shape, lambda i, b, s: (i,) + zeros)

    tbits = log2(nt)
    lines = 16 + heads * model // own
    srows = max(own // L * lines, 8 * ndp, 128)
    late_shape = sds(nother, Ry, model, dtype=bf16)
    bc_type = bf16 if (model // (nt * ndp)) % 16 == 0 else f32
    s_out = call(
        partial(scan_kernel, width, own, heads, ncore, ny, ndp, nloc),
        (nloc, spans),
        [
            chunk_spec(R, model),
            chunk_spec(R, width),
            chunk_spec(R, width),
            chunk_spec(R + PAD, width),
            chunk_spec(R + PAD, 256),
            chunk_spec(R, L),
            chunk_spec(spans, L, width),
            any_spec,
            any_spec,
            any_spec,
            any_spec,
            whole_spec(model, 256),
            whole_spec(model, L),
            whole_spec(8, width),
            whole_spec(8, 256),
            whole_spec(8, L),
            whole_spec(8, width),
            whole_spec(1, model),
            whole_spec(model, own),
            whole_spec(model, own),
            any_spec,
            any_spec,
        ],
        [
            whole_spec(nloc - 1, Ry, model),
            whole_spec(srows, L),
            whole_spec(model // L, L + 256),
            whole_spec(Ry, model),
        ]
        + [any_spec] * 16,
        [
            sds(nloc - 1, Ry, model, dtype=bf16),
            sds(srows, L),
            sds(model // L, L + 256),
            sds(Ry, model, dtype=bf16),
            sds(model, own, dtype=bf16),
            sds(model, own, dtype=bf16),
            sds(nother, nloc - 1, Ry, model, dtype=bf16),
            sds(nloc - 1, Ry, model, dtype=bf16),
            sds(nother, nloc - 1, Ry, model, dtype=bf16),
            sds(nother, nloc - 1, Ry, model, dtype=bf16),
            sds(nloc - 1, Ry, model, dtype=bf16),
            sds(nother, nloc - 1, Ry, model, dtype=bf16),
            sds(model, own, dtype=bf16),
            sds(model, 256, dtype=bc_type),
        ]
        + [late_shape, sds(Ry, model, dtype=bf16), late_shape] * 2,
        [
            pltpu.VMEM((model, own), bf16),
            pltpu.VMEM((model, own), bf16),
            pltpu.VMEM((model, own), bf16),
            pltpu.VMEM((model, own), bf16),
            dma((4,)),
            pltpu.VMEM((R, width + 384), bf16),
            pltpu.VMEM((R, 256), f32),
            pltpu.VMEM((R, 256), bf16),
            pltpu.VMEM((L, width), f32),
            pltpu.VMEM((L, width), bf16),
            pltpu.VMEM((L, width), f32),
            pltpu.VMEM((L, width), f32),
            pltpu.VMEM((L, width), bf16),
            pltpu.VMEM((L, width), bf16),
            pltpu.VMEM((pairs, L + 8, L), f32),
            pltpu.VMEM((2, L + 8, L), f32),
            pltpu.VMEM((pairs, L + PAD, L), f32),
            pltpu.VMEM((2, L + PAD, L), f32),
            pltpu.VMEM((4 * L, width), bf16),
            pltpu.VMEM((8, width), f32),
            pltpu.VMEM((width, L), bf16),
            pltpu.VMEM((6, 8, width), f32),
            pltpu.VMEM((5, 8, 256), f32),
            pltpu.VMEM((2, 8, L), f32),
            pltpu.VMEM((8, model), f32),
            pltpu.VMEM((model, width + 384), f32),
            pltpu.VMEM((model, own), bf16),
            pltpu.VMEM((model, own), bf16),
            pltpu.VMEM((R, model), bf16),
            pltpu.VMEM((nloc - 1, nother, Ry, model), bf16),
            pltpu.VMEM((Ry, model), bf16),
            dma,
            dma,
            dma((2, nloc - 1, nother)),
            dma((2, 2 * ny)),
            dma((2, nloc - 1, 2 * ny)),
            dma((2,)),
            pltpu.VMEM((model, own), bf16),
            pltpu.VMEM((model, 256), bc_type),
            pltpu.VMEM((srows, L), f32),
            pltpu.VMEM((srows, L), f32),
            pltpu.VMEM((model // L, L + 256), f32),
            pltpu.VMEM((srows, L), f32),
            pltpu.VMEM((model, 256), bc_type),
            pltpu.VMEM((srows, L), f32),
            pltpu.VMEM((srows, L), f32),
            pltpu.VMEM((nother, Ry, model), bf16),
            pltpu.VMEM((Ry, model), bf16),
            dma((2,)),
            dma((2, nother)),
            dma((2, 2 * ny)),
            dma((2, 2 * ny)),
        ]
        + Halving.scratch(model, own, nbits, bf16)
        + Halving.scratch(model, own, nbits, bf16)
        + Halving.scratch(model // 2, own, nbits, bf16)
        + Halving.scratch(model // 2, own, nbits, bf16)
        + Halving.scratch(model, 256, nbits + tbits, bc_type)
        + Halving.scratch(srows, L, nbits, f32)
        + Doubling.scratch(nbits + tbits, model // L, L + 256),
        "scan_back",
        2 * nloc * R * model * (2 * wtot),
        nloc * R * (4 * model + 12 * width),
        2,
    )(seq0, hid, dz, dy, xl, bcl, dtl, sin, wz, wzo, wx, wxo, w_bc, wdt, prm, bcp, hp, ggg, gain, gz, go, bo, x4)

    corr, small, shared, last, fz, fo, boy, bot, boty, cy0, ct0, cty0, fw, fb = s_out[:14]
    late_got = s_out[14:]
    pieces = ncore * ny
    where = jnp.stack([core, yy]).astype(jnp.int32)

    def out_index(k, i, s):
        return ((s[0] ^ (k // ny)) * nloc + i, (s[1] - k % ny + ny) % ny, 0, 0)

    def spec_of(base, seq_of, d):
        if d is None:
            return pl.BlockSpec(
                (None, Ry, model), lambda j, i, s: (seq_of(j, i) - base, 0, 0)
            )
        return pl.BlockSpec(
            (None, None, Ry, model), lambda j, i, s: (d, seq_of(j, i) - base, 0, 0)
        )

    placed_spec = pl.BlockSpec((None, None, Ry, model), out_index)
    specs, arrays = [], []

    def add_group(first, count, mine, mine_base, toy, tot, toty):
        for k in range(pieces):

            def seq_of(j, i, k=k):
                i = jnp.clip(i, first, first + count - 1)
                return jnp.where(j == k, i, jnp.where(j > k, first + count - 1, first))

            d = k % ny - 1
            if k == 0:
                array, spec = mine, spec_of(mine_base, seq_of, None)
            elif k < ny:
                array, spec = toy, spec_of(first, seq_of, d)
            elif d < 0:
                array, spec = tot, spec_of(first, seq_of, None)
            else:
                array, spec = toty, spec_of(first, seq_of, d)
            arrays.append(array)
            specs.append(spec)

    def as_seq(v, axis):
        return jnp.expand_dims(v, axis)

    def add_late(first, mine, base, got):
        toy, tot, toty = got
        add_group(first, 1, mine, base, as_seq(toy, 1), as_seq(tot, 0), as_seq(toty, 1))

    add_group(0, nloc - 1, corr, 0, cy0, ct0, cty0)
    add_late(nloc - 1, as_seq(last, 0), nloc - 1, late_got[0:3])
    add_group(0, nloc - 1, bo, 0, boy, bot, boty)
    add_late(nloc - 1, bo, 0, late_got[3:6])
    grad_input, block_output = call(
        partial(finish_kernel, pieces, nloc),
        (pieces, nloc),
        [placed_spec] + specs,
        [placed_spec, placed_spec],
        [sds(nseq, ny, Ry, model), sds(nseq, ny, Ry, model, dtype=bf16)],
        [],
        "finish",
        0,
        12 * tok * model,
    )(where, g4, *arrays)

    def row_block(cols):
        return pl.BlockSpec((L, cols), lambda d: (d, 0))

    outs = pl.pallas_call(
        partial(unpack_kernel, own, heads, model),
        grid=(model // L,),
        in_specs=[row_block(own), row_block(own), row_block(own), row_block(256)]
        + [whole_spec(srows, L), whole_spec(model // L, L + 256)],
        out_specs=[
            pl.BlockSpec((L, 2, own), lambda d: (d, 0, 0)),
            pl.BlockSpec((own, L), lambda d: (0, d)),
            row_block(heads),
            row_block(256),
            whole_spec(4, own),
            whole_spec(1, own),
            whole_spec(1, heads),
            whole_spec(1, own),
            whole_spec(1, heads),
            whole_spec(1, heads),
            whole_spec(1, model),
            whole_spec(4, 256),
            whole_spec(1, 256),
        ],
        out_shape=[
            sds(model, 2, own),
            sds(own, model),
            sds(model, heads),
            sds(model, 256),
            sds(4, own),
            sds(1, own),
            sds(1, heads),
            sds(1, own),
            sds(1, heads),
            sds(1, heads),
            sds(1, model),
            sds(4, 256),
            sds(1, 256),
        ],
        name="unpack",
    )(fz, fo, fw, fb, small, shared)
    gzx, gwo, gwdt, gwbc, gcxw, gcxb, gd, ggg, gdtb, galog, gpre, gcbw, gcbb = outs
    return (
        block_output.reshape(tok, model),
        grad_input.reshape(tok, model),
        gpre[0],
        gzx,
        gwbc,
        gwdt,
        gcxw,
        gcxb[0],
        gcbw,
        gcbb[0],
        gdtb[0],
        galog[0],
        gd[0],
        ggg[0],
        gwo,
    )


def solution(mesh):
    placed = (
        P("dp", None),
        P(),
        P(None, None, "tensor"),
        P(),
        P(None, "tensor"),
        P(None, "tensor"),
        P("tensor"),
        P(),
        P(),
        P("tensor"),
        P("tensor"),
        P("tensor"),
        P("tensor"),
        P("tensor", None),
        P("dp", None),
    )
    return jax.shard_map(
        body,
        mesh=mesh,
        in_specs=placed,
        out_specs=(
            P("dp", None),
            P("dp", None),
            P(),
            P(None, None, "tensor"),
            P(),
            P(None, "tensor"),
            P(None, "tensor"),
            P("tensor"),
            P(),
            P(),
            P("tensor"),
            P("tensor"),
            P("tensor"),
            P("tensor"),
            P("tensor", None),
        ),
        check_vma=False,
    )
```
